32 devices in a mesh: grp: 4 (over y, x), inner: 8 (over z, core).
Axes of the slice: x: 2, y: 2, z: 4, core: 2. Of those that a mesh axis runs over, the one named last changes fastest.
Arguments:
- tokens: bfloat16 [32, 1024, 512], P(('grp', 'inner')), may hold values from -8 to 8
- cotangent: bfloat16 [32, 1024, 512], P(('grp', 'inner')), may hold values from -6 to 6
- mixer_gain: bfloat16 [512], P(('grp', 'inner')), may hold values from 0.5 to 1.5
- forget_weight: bfloat16 [512, 1024], P('grp', 'inner'), may hold values from -0.25 to 0.25
- input_gate_weight: bfloat16 [512, 1024], P('grp', 'inner'), may hold values from -0.25 to 0.25
- candidate_weight: bfloat16 [512, 1024], P('grp', 'inner'), may hold values from -0.25 to 0.25
- forget_bias: bfloat16 [1024], P(('grp', 'inner')), may hold values from -2 to 6
- input_bias: bfloat16 [1024], P(('grp', 'inner')), may hold values from -6 to 2
- output_weight: bfloat16 [1024, 512], P('grp', 'inner'), may hold values from -0.1875 to 0.1875
- feed_norm_gain: bfloat16 [512], P(('grp', 'inner')), may hold values from 0.5 to 1.5
- up_weight: bfloat16 [512, 2048], P('grp', 'inner'), may hold values from -0.25 to 0.25
- down_weight: bfloat16 [2048, 512], P('grp', 'inner'), may hold values from -0.125 to 0.125
- mixer_second: float32 [512], P(('grp', 'inner')), may hold values from 9830.4 to 39321.6
- forget_rows: float32 [512], P('grp'), may hold values from 3276.8 to 13107.2
- forget_columns: float32 [1024], P('inner'), may hold values from 3276.8 to 13107.2
- input_rows: float32 [512], P('grp'), may hold values from 3276.8 to 13107.2
- input_columns: float32 [1024], P('inner'), may hold values from 3276.8 to 13107.2
- candidate_rows: float32 [512], P('grp'), may hold values from 3276.8 to 13107.2
- candidate_columns: float32 [1024], P('inner'), may hold values from 3276.8 to 13107.2
- forget_second: float32 [1024], P(('grp', 'inner')), may hold values from 6553.6 to 26214.4
- input_second: float32 [1024], P(('grp', 'inner')), may hold values from 6553.6 to 26214.4
- output_rows: float32 [1024], P('grp'), may hold values from 16384 to 65536
- output_columns: float32 [512], P('inner'), may hold values from 16384 to 65536
- feed_second: float32 [512], P(('grp', 'inner')), may hold values from 11468.8 to 45875.2
- up_rows: float32 [512], P('grp'), may hold values from 3276.8 to 13107.2
- up_columns: float32 [2048], P('inner'), may hold values from 3276.8 to 13107.2
- down_rows: float32 [2048], P('grp'), may hold values from 11468.8 to 45875.2
- down_columns: float32 [512], P('inner'), may hold values from 11468.8 to 45875.2
Outputs:
- block_output: bfloat16 [32, 1024, 512], P(('grp', 'inner'))
- tokens_grad: bfloat16 [32, 1024, 512], P(('grp', 'inner'))
- mixer_gain_grad: float32 [512], P(('grp', 'inner'))
- forget_weight_grad: float32 [512, 1024], P('grp', 'inner')
- input_weight_grad: float32 [512, 1024], P('grp', 'inner')
- candidate_weight_grad: float32 [512, 1024], P('grp', 'inner')
- forget_bias_grad: float32 [1024], P(('grp', 'inner'))
- input_bias_grad: float32 [1024], P(('grp', 'inner'))
- output_weight_grad: float32 [1024, 512], P('grp', 'inner')
- feed_gain_grad: float32 [512], P(('grp', 'inner'))
- up_weight_grad: float32 [512, 2048], P('grp', 'inner')
- down_weight_grad: float32 [2048, 512], P('grp', 'inner')
- mixer_gain_new: float32 [512], P(('grp', 'inner'))
- forget_weight_new: float32 [512, 1024], P('grp', 'inner')
- input_weight_new: float32 [512, 1024], P('grp', 'inner')
- candidate_weight_new: float32 [512, 1024], P('grp', 'inner')
- forget_bias_new: float32 [1024], P(('grp', 'inner'))
- next_input_bias: float32 [1024], P(('grp', 'inner'))
- output_weight_new: float32 [1024, 512], P('grp', 'inner')
- feed_gain_new: float32 [512], P(('grp', 'inner'))
- up_weight_new: float32 [512, 2048], P('grp', 'inner')
- down_weight_new: float32 [2048, 512], P('grp', 'inner')
- mixer_second_new: float32 [512], P(('grp', 'inner'))
- forget_rows_new: float32 [512], P('grp')
- forget_columns_new: float32 [1024], P('inner')
- input_rows_new: float32 [512], P('grp')
- input_columns_new: float32 [1024], P('inner')
- candidate_rows_new: float32 [512], P('grp')
- candidate_columns_new: float32 [1024], P('inner')
- forget_second_new: float32 [1024], P(('grp', 'inner'))
- input_second_new: float32 [1024], P(('grp', 'inner'))
- output_rows_new: float32 [1024], P('grp')
- output_columns_new: float32 [512], P('inner')
- feed_second_new: float32 [512], P(('grp', 'inner'))
- up_rows_new: float32 [512], P('grp')
- up_columns_new: float32 [2048], P('inner')
- down_rows_new: float32 [2048], P('grp')
- down_columns_new: float32 [512], P('inner')
- update_norms: float32 [10], replicated
The draws below stay inside these ranges and needn't reach their ends.
All inputs are finite; a program needn't handle non-finite values.
Results may differ from the reference program's by a relative error of at most 0.0065.
The reference program's roundings to bfloat16 on the way count: a program that leaves them out, or rounds other values in their place, can miss the bound.
Values may be sent and summed in bfloat16 or wider, within the bound.
A program may use at most 256 MiB of HBM per device.

```python
import math
import jax
import jax.numpy as jnp
from jax import lax

D = 512
H = 1024
FF = 2048
SEQ_LEN = 1024
SEQS = 32


def draw_tokens(key, part):
    place = jnp.arange(D, dtype=jnp.float32) / (D - 1)
    rising = jnp.exp((place - 0.5) * math.log(4.0))
    base = jax.random.normal(key, (SEQS, SEQ_LEN, D), jnp.float32)
    return jnp.clip(base * rising, -8.0, 8.0).astype(jnp.bfloat16)


def level_of(own_key, shape, shards, least, top_value):
    level, own = 1.0, jax.random.fold_in(own_key, 6)
    for position, blocks in shards:
        draws = jnp.exp(jax.random.uniform(jax.random.fold_in(own, position), (blocks,), jnp.float32, least / len(shards), top_value / len(shards)))
        level = level * jnp.repeat(draws, shape[position] // blocks).reshape([-1 if axis == position else 1 for axis in range(len(shape))])
    return level


def normal_values(stream_key, extent, spread, reach, cuts=(), kind=jnp.bfloat16):
    array = spread * jax.random.normal(stream_key, extent, jnp.float32)
    if cuts:
        array = array * level_of(stream_key, extent, cuts, -0.22, 0.18)
    return jnp.clip(array, -reach, reach).astype(kind)


def setup_inputs(seed: int = 0) -> dict:
    arg_keys = jax.random.split(jax.random.key(seed), 29)
    return {
        "tokens": draw_tokens(jax.random.fold_in(arg_keys[28], 71), 0),
        "cotangent": normal_values(arg_keys[1], (SEQS, SEQ_LEN, D), 1.0, 6.0, ((0, 32),)),
        "mixer_gain": jnp.clip(1.0 + 0.1 * jax.random.normal(arg_keys[2], (D,), jnp.float32), 0.5, 1.5).astype(jnp.bfloat16),
        "forget_weight": normal_values(arg_keys[3], (D, H), D ** -0.5, 0.25, ((0, 4), (1, 8))),
        "input_gate_weight": normal_values(arg_keys[4], (D, H), D ** -0.5, 0.25, ((0, 4), (1, 8))),
        "candidate_weight": normal_values(arg_keys[5], (D, H), D ** -0.5, 0.25, ((0, 4), (1, 8))),
        "forget_bias": jnp.clip(-2.0 + 8.0 * jax.random.uniform(arg_keys[6], (H,), jnp.float32) ** level_of(arg_keys[6], (H,), ((0, 32),), -0.2, 0.2), -2.0, 6.0).astype(jnp.bfloat16),
        "input_bias": jnp.clip(-6.0 + 8.0 * jax.random.uniform(arg_keys[7], (H,), jnp.float32) ** level_of(arg_keys[7], (H,), ((0, 32),), -0.2, 0.2), -6.0, 2.0).astype(jnp.bfloat16),
        "output_weight": normal_values(arg_keys[8], (H, D), H ** -0.5, 0.1875, ((0, 4), (1, 8))),
        "feed_norm_gain": jnp.clip(1.0 + 0.1 * jax.random.normal(arg_keys[9], (D,), jnp.float32), 0.5, 1.5).astype(jnp.bfloat16),
        "up_weight": normal_values(arg_keys[10], (D, FF), D ** -0.5, 0.25, ((0, 4), (1, 8))),
        "down_weight": normal_values(arg_keys[11], (FF, D), FF ** -0.5, 0.125, ((0, 4), (1, 8))),
        "mixer_second": jnp.clip(jnp.exp(math.log(39321.6) - 1.3862944 * jax.random.uniform(arg_keys[12], (D,), jnp.float32) ** level_of(arg_keys[12], (D,), ((0, 32),), -0.2, 0.2)), 9830.4, 39321.6),
        "forget_rows": jnp.clip(jnp.exp(math.log(13107.2) - 1.3862944 * jax.random.uniform(arg_keys[13], (D,), jnp.float32) ** level_of(arg_keys[13], (D,), ((0, 4),), -0.2, 0.2)), 3276.8, 13107.2),
        "forget_columns": jnp.clip(jnp.exp(math.log(13107.2) - 1.3862944 * jax.random.uniform(arg_keys[14], (H,), jnp.float32) ** level_of(arg_keys[14], (H,), ((0, 8),), -0.2, 0.2)), 3276.8, 13107.2),
        "input_rows": jnp.clip(jnp.exp(math.log(13107.2) - 1.3862944 * jax.random.uniform(arg_keys[15], (D,), jnp.float32) ** level_of(arg_keys[15], (D,), ((0, 4),), -0.2, 0.2)), 3276.8, 13107.2),
        "input_columns": jnp.clip(jnp.exp(math.log(13107.2) - 1.3862944 * jax.random.uniform(arg_keys[16], (H,), jnp.float32) ** level_of(arg_keys[16], (H,), ((0, 8),), -0.2, 0.2)), 3276.8, 13107.2),
        "candidate_rows": jnp.clip(jnp.exp(math.log(13107.2) - 1.3862944 * jax.random.uniform(arg_keys[17], (D,), jnp.float32) ** level_of(arg_keys[17], (D,), ((0, 4),), -0.2, 0.2)), 3276.8, 13107.2),
        "candidate_columns": jnp.clip(jnp.exp(math.log(13107.2) - 1.3862944 * jax.random.uniform(arg_keys[18], (H,), jnp.float32) ** level_of(arg_keys[18], (H,), ((0, 8),), -0.2, 0.2)), 3276.8, 13107.2),
        "forget_second": jnp.clip(jnp.exp(math.log(26214.4) - 1.3862944 * jax.random.uniform(arg_keys[19], (H,), jnp.float32) ** level_of(arg_keys[19], (H,), ((0, 32),), -0.2, 0.2)), 6553.6, 26214.4),
        "input_second": jnp.clip(jnp.exp(math.log(26214.4) - 1.3862944 * jax.random.uniform(arg_keys[20], (H,), jnp.float32) ** level_of(arg_keys[20], (H,), ((0, 32),), -0.2, 0.2)), 6553.6, 26214.4),
        "output_rows": jnp.clip(jnp.exp(math.log(65536.0) - 1.3862944 * jax.random.uniform(arg_keys[21], (H,), jnp.float32) ** level_of(arg_keys[21], (H,), ((0, 4),), -0.2, 0.2)), 16384.0, 65536.0),
        "output_columns": jnp.clip(jnp.exp(math.log(65536.0) - 1.3862944 * jax.random.uniform(arg_keys[22], (D,), jnp.float32) ** level_of(arg_keys[22], (D,), ((0, 8),), -0.2, 0.2)), 16384.0, 65536.0),
        "feed_second": jnp.clip(jnp.exp(math.log(45875.2) - 1.3862944 * jax.random.uniform(arg_keys[23], (D,), jnp.float32) ** level_of(arg_keys[23], (D,), ((0, 32),), -0.2, 0.2)), 11468.8, 45875.2),
        "up_rows": jnp.clip(jnp.exp(math.log(13107.2) - 1.3862944 * jax.random.uniform(arg_keys[24], (D,), jnp.float32) ** level_of(arg_keys[24], (D,), ((0, 4),), -0.2, 0.2)), 3276.8, 13107.2),
        "up_columns": jnp.clip(jnp.exp(math.log(13107.2) - 1.3862944 * jax.random.uniform(arg_keys[25], (FF,), jnp.float32) ** level_of(arg_keys[25], (FF,), ((0, 8),), -0.2, 0.2)), 3276.8, 13107.2),
        "down_rows": jnp.clip(jnp.exp(math.log(45875.2) - 1.3862944 * jax.random.uniform(arg_keys[26], (FF,), jnp.float32) ** level_of(arg_keys[26], (FF,), ((0, 4),), -0.2, 0.2)), 11468.8, 45875.2),
        "down_columns": jnp.clip(jnp.exp(math.log(45875.2) - 1.3862944 * jax.random.uniform(arg_keys[27], (D,), jnp.float32) ** level_of(arg_keys[27], (D,), ((0, 8),), -0.2, 0.2)), 11468.8, 45875.2),
    }


EPS = 1e-06
TINY = 1e-30
CLIP = 0.01
HIGH_PRECISION = lax.Precision.HIGHEST

@jax.custom_vjp
def low(v):
    return lax.optimization_barrier(v.astype(jnp.bfloat16)).astype(jnp.float32)

@jax.custom_vjp
def low_back(v):
    return v

def low_keep(v):
    return (low(v), None)

def low_pass(kept, grad):
    return (grad,)

def back_keep(v):
    return (v, None)

def back_low(kept, grad):
    return (low(grad),)
low.defvjp(low_keep, low_pass)
low_back.defvjp(back_keep, back_low)

def rms_norm(values, gain):
    return values * lax.rsqrt(lax.optimization_barrier(jnp.mean(values * values, axis=-1, keepdims=True)) + EPS) * gain

def log_value(candidate_preact):
    return jnp.where(candidate_preact >= 0, jnp.log(jnp.maximum(candidate_preact, 0.0) + 0.5), -jax.nn.softplus(-candidate_preact))

def linear_combine(first, second):
    return (first[0] * second[0], second[0] * first[1] + second[1])

def mixer(pre_forget, pre_input, candidate_preact):
    gap = jax.nn.softplus(-pre_forget) - jax.nn.softplus(-pre_input)
    log_keep = -jax.nn.softplus(gap)
    log_admit = -jax.nn.softplus(-gap)
    keep = jnp.exp(log_keep)
    inflow = jnp.exp(log_admit + log_value(candidate_preact))
    _, state = lax.associative_scan(linear_combine, (keep, inflow), axis=1)
    return state

def project(left_operand, right_operand):
    return jnp.einsum('mtv,va->mta', left_operand, right_operand, precision=HIGH_PRECISION)

def forward(block, params):
    mixer_gain, forget_weight, input_gate_weight, candidate_weight, forget_bias, input_bias, output_weight, feed_norm_gain, up_weight, down_weight = params
    mixer_in = low(rms_norm(block, mixer_gain))
    pre_forget = low_back(project(mixer_in, forget_weight) + forget_bias)
    pre_input = low_back(project(mixer_in, input_gate_weight) + input_bias)
    candidate_preact = low_back(project(mixer_in, candidate_weight))
    state = low(mixer(pre_forget, pre_input, candidate_preact))
    mixed = low_back(project(state, output_weight))
    resid = block + mixed
    feed_in = low(rms_norm(resid, feed_norm_gain))
    upper = low_back(project(feed_in, up_weight))
    act = low(jax.nn.gelu(upper, approximate=False))
    lower = low_back(project(act, down_weight))
    return resid + lower

def factored(weight, grad, rows_old, columns_old):
    square = grad * grad
    rows = 0.5 * rows_old + 0.5 * (lax.optimization_barrier(jnp.mean(square, axis=1)) + TINY)
    columns = 0.5 * columns_old + 0.5 * (lax.optimization_barrier(jnp.mean(square, axis=0)) + TINY)
    scaled = grad * lax.rsqrt(rows[:, None] * columns[None, :] / jnp.mean(rows))
    norm = jnp.sqrt(jnp.mean(scaled * scaled))
    fresh = weight + -jnp.sqrt(jnp.mean(weight * weight)) * scaled / jnp.maximum(CLIP, norm)
    return (fresh, rows, columns, norm)

def unfactored(weight, grad, second_old):
    second = 0.5 * second_old + 0.5 * (grad * grad + TINY)
    scaled = grad * lax.rsqrt(second)
    norm = jnp.sqrt(jnp.mean(scaled * scaled))
    fresh = weight + -jnp.sqrt(jnp.mean(weight * weight)) * scaled / jnp.maximum(CLIP, norm)
    return (fresh, second, norm)

def reference(tokens, cotangent, mixer_gain, forget_weight, input_gate_weight, candidate_weight, forget_bias, input_bias, output_weight, feed_norm_gain, up_weight, down_weight, mixer_second, forget_rows, forget_columns, input_rows, input_columns, candidate_rows, candidate_columns, forget_second, input_second, output_rows, output_columns, feed_second, up_rows, up_columns, down_rows, down_columns):
    params = tuple((p.astype(jnp.float32) for p in (mixer_gain, forget_weight, input_gate_weight, candidate_weight, forget_bias, input_bias, output_weight, feed_norm_gain, up_weight, down_weight)))
    group = math.gcd(SEQS, max(1, 4096 // SEQ_LEN))
    count = SEQS // group
    blocks = tokens.reshape(count, group, SEQ_LEN, D).astype(jnp.float32)
    pulls = cotangent.reshape(count, group, SEQ_LEN, D).astype(jnp.float32)

    def step(acc, pair):
        block, pull_in = pair
        result, pull = jax.vjp(forward, block, params)
        d_block, d_params = pull(pull_in)
        acc = jax.tree.map(lambda a, b: a + b, acc, d_params)
        return (acc, (result.astype(jnp.bfloat16), d_block.astype(jnp.bfloat16)))
    zeros = tuple((jnp.zeros_like(p) for p in params))
    grads, (results, d_blocks) = lax.scan(step, zeros, (blocks, pulls))
    block_output = results.reshape(SEQS, SEQ_LEN, D)
    tokens_grad = d_blocks.reshape(SEQS, SEQ_LEN, D)
    gain_a, second_a, norm_a = unfactored(params[0], grads[0], mixer_second)
    forget_w, forget_r, forget_c, norm_b = factored(params[1], grads[1], forget_rows, forget_columns)
    input_w, input_r, input_c, norm_c = factored(params[2], grads[2], input_rows, input_columns)
    cand_w, cand_r, cand_c, norm_d = factored(params[3], grads[3], candidate_rows, candidate_columns)
    fbias, second_b, norm_e = unfactored(params[4], grads[4], forget_second)
    ibias, second_c, norm_f = unfactored(params[5], grads[5], input_second)
    out_w, out_r, out_c, norm_g = factored(params[6], grads[6], output_rows, output_columns)
    gain_b, second_d, norm_h = unfactored(params[7], grads[7], feed_second)
    upw, up_r, up_c, norm_i = factored(params[8], grads[8], up_rows, up_columns)
    downw, down_row_factor, down_c, norm_j = factored(params[9], grads[9], down_rows, down_columns)
    update_norms = jnp.stack([norm_a, norm_b, norm_c, norm_d, norm_e, norm_f, norm_g, norm_h, norm_i, norm_j])
    return (block_output, tokens_grad, grads[0], grads[1], grads[2], grads[3], grads[4], grads[5], grads[6], grads[7], grads[8], grads[9], gain_a, forget_w, input_w, cand_w, fbias, ibias, out_w, gain_b, upw, downw, second_a, forget_r, forget_c, input_r, input_c, cand_r, cand_c, second_b, second_c, out_r, out_c, second_d, up_r, up_c, down_row_factor, down_c, update_norms)
```

```python
import functools
import math
import jax
import jax.numpy as jnp
from jax import lax
from jax.experimental import pallas as pl
from jax.sharding import PartitionSpec as P
from jax.experimental.pallas import tpu as pltpu

EPS = 1e-06
F32 = jnp.float32
BF16 = jnp.bfloat16
C = 256
LANES = 128
SUB = 8
ERFC = (
    0.2256758669, 0.2256693636, 0.2078460312, 0.1685204197, 0.1415057621,
    -0.005753053848, 0.1692475449, -0.182997133, 0.05028532412,
)


def dot(a, b):
    return jnp.dot(a, b, preferred_element_type=F32)


def dot_t(a, b):
    return lax.dot_general(a, b, (((1,), (1,)), ((), ())), preferred_element_type=F32)


def loop(steps, body):
    def run(i, carry):
        body(i)
        return carry

    lax.fori_loop(0, steps, run, 0)


def at(i, size):
    return pl.ds(pl.multiple_of(i * size, size), size)


def gelu_parts(x):
    ax = jnp.abs(x)
    e = jnp.exp(-0.5 * (x * x))
    t = 1.0 / (1.0 + (0.4 * math.sqrt(0.5)) * ax)
    poly = jnp.full_like(t, ERFC[-1])
    for c in ERFC[-2::-1]:
        poly = poly * t + c
    half = 0.5 * (poly * t * e)
    cdf = jnp.where(x >= 0, 1.0 - half, half)
    return x * cdf, cdf + (x * e) * (1.0 / math.sqrt(2.0 * math.pi))


def strided(ref, j, n):
    return ref[pl.ds(j, SUB, stride=n), :]

def gather_rows(tmp, j0, n, D):
    columns = [
        jnp.concatenate([tmp[q, pl.ds(j0 + jj, SUB, stride=n), :] for jj in range(16)], axis=0)
        for q in range(D // LANES)
    ]
    return jnp.concatenate(columns, axis=1)


def scatter_rows(tmp, j0, n, out):
    for q in range(out.shape[1] // LANES):
        for jj in range(16):
            tmp[q, pl.ds(j0 + jj, SUB, stride=n), :] = out[
                jj * SUB : (jj + 1) * SUB, q * LANES : (q + 1) * LANES
            ]


def norm_in(refs, T):
    n = T // SUB
    tmp, xf, g1 = refs.pre, refs.xf, refs.g1
    D = xf.shape[1]

    def widen(i):
        rows = at(i, LANES)
        wide = refs.tok[rows, :].astype(F32)
        for q in range(D // LANES):
            tmp[q, rows, :] = wide[:, q * LANES : (q + 1) * LANES]

    loop(T // LANES, widen)

    def place(i):
        x = gather_rows(tmp, i * 16, n, D)
        y = x * lax.rsqrt(jnp.mean(x * x, axis=-1, keepdims=True) + EPS) * g1[...]
        rows = at(i, LANES)
        xf[rows, :] = x
        refs.min[rows, :] = y.astype(BF16)
        refs.min_t[:, rows] = y.T.astype(BF16)

    loop(T // LANES, place)


def cot_in(refs, T):
    n = T // SUB
    tmp = refs.pre
    D = refs.xf.shape[1]

    def widen(i):
        rows = at(i, LANES)
        wide = refs.cot[rows, :].astype(F32)
        for q in range(D // LANES):
            tmp[q, rows, :] = wide[:, q * LANES : (q + 1) * LANES]

    loop(T // LANES, widen)

    def place(i):
        x = gather_rows(tmp, i * 16, n, D)
        rows = at(i, LANES)
        refs.cot_p[rows, :] = x.astype(BF16)
        refs.cot_t[:, rows] = x.T.astype(BF16)

    loop(T // LANES, place)


def mixer_forward(refs, z, T):
    pre, ac, st = refs.pre, refs.buf_a, refs.st
    halves = C // LANES
    width = 3 * LANES

    def project(i):
        rows = at(i, 256)
        out = dot(refs.min[rows, :], refs.wmix[z])
        for q in range(3 * halves):
            pre[q, rows, :] = out[:, q * LANES : (q + 1) * LANES]

    loop(T // 256, project)
    fb = refs.fb[z]
    ib = refs.ib[z]

    def gates(i, carry):
        r0 = pl.multiple_of(i * 64, 64)
        out = []
        for h in range(halves):
            a, b = carry[h]
            lanes = slice(h * LANES, (h + 1) * LANES)
            pf = pre[3 * h, pl.ds(r0, 64), :] + fb[:, lanes]
            pi = pre[3 * h + 1, pl.ds(r0, 64), :] + ib[:, lanes]
            pc = pre[3 * h + 2, pl.ds(r0, 64), :]
            m = jnp.minimum(jnp.minimum(pf, pi), 0.0)
            e0 = jnp.exp(m)
            ef = jnp.exp(m - pf)
            ei = jnp.exp(m - pi)
            nk = e0 + ei
            na = e0 + ef
            inv = 1.0 / (nk + na)
            keep = nk * inv
            admit = na * inv
            not_f = 1.0 / (1.0 + jnp.exp(pf))
            not_i = 1.0 / (1.0 + jnp.exp(pi))
            ec = jnp.exp(jnp.minimum(pc, 0.0))
            sg = ec / (1.0 + ec)
            positive = pc >= 0
            value = jnp.where(positive, pc + 0.5, sg)
            slope = jnp.where(positive, 1.0, sg * (1.0 - sg))
            refs.keep[z, pl.ds(r0, 64), lanes] = keep
            refs.k_f[z, pl.ds(r0, 64), lanes] = keep * not_f
            refs.k_i[z, pl.ds(r0, 64), lanes] = keep * not_i
            refs.k_c[z, pl.ds(r0, 64), lanes] = admit * slope
            inflow = admit * value
            alist, blist = [], []
            for j in range(8):
                kj = keep[j * SUB : (j + 1) * SUB]
                b = kj * b + inflow[j * SUB : (j + 1) * SUB]
                a = kj * a
                alist.append(a)
                blist.append(b)
            ac[pl.ds(r0, 64), lanes] = jnp.concatenate(alist, axis=0)
            st[z, pl.ds(r0 + SUB, 64), lanes] = jnp.concatenate(blist, axis=0)
            out.append((a, b))
        return tuple(out)

    one = jnp.ones((SUB, LANES), F32)
    zero = jnp.zeros((SUB, LANES), F32)
    ends = lax.fori_loop(0, T // 64, gates, tuple((one, zero) for _ in range(halves)))
    for h in range(halves):
        a, b = ends[h]
        rows = [jnp.zeros((1, LANES), F32)]
        for s in range(SUB - 1):
            rows.append(a[s : s + 1] * rows[-1] + b[s : s + 1])
        st[z, 0:SUB, h * LANES : (h + 1) * LANES] = jnp.concatenate(rows, axis=0)
    first = st[z, 0:SUB, :]

    def finish(i):
        r0 = pl.multiple_of(i * 64, 64)
        a = ac[pl.ds(r0, 64), :].reshape(8, SUB, C)
        b = st[z, pl.ds(r0 + SUB, 64), :].reshape(8, SUB, C)
        s = (b + a * first[None]).reshape(64, C)
        st[z, pl.ds(r0 + SUB, 64), :] = s
        refs.slow[z, pl.ds(r0, 64), :] = s.astype(BF16)

    loop(T // 64, finish)


def mix_out(refs, T):
    Z = refs.wot.shape[0]

    def body(i):
        rows = at(i, 256)
        acc = refs.xf[rows, :]
        for z in range(Z):
            acc = acc + dot_t(refs.slow[z, rows, :], refs.wot[z])
        refs.resid[rows, :] = acc
        for k in range(2):
            x = acc[k * LANES : (k + 1) * LANES]
            y = x * lax.rsqrt(jnp.mean(x * x, axis=-1, keepdims=True) + EPS) * refs.g2[...]
            sub = pl.ds(pl.multiple_of(i * 256 + k * LANES, LANES), LANES)
            refs.fin[sub, :] = y.astype(BF16)
            refs.fin_t[:, sub] = y.T.astype(BF16)

    loop(T // 256, body)


def feed(refs, f, T):
    wup, wdt = refs.wup, refs.wdt

    def body(i):
        rows = at(i, 256)
        refs.buf_a[rows, :] = dot(refs.fin[rows, :], wup[f])
        refs.buf_b[rows, :] = dot(refs.cot_p[rows, :], wdt[f])
        for k in range(4):
            sub = pl.ds(pl.multiple_of(i * 256 + k * 64, 64), 64)
            act, slope = gelu_parts(refs.buf_a[sub, :])
            refs.act[sub, :] = act.astype(BF16)
            refs.dup[sub, :] = (refs.buf_b[sub, :] * slope).astype(BF16)
        refs.oacc[rows, :] += dot_t(refs.act[rows, :], wdt[f])
        refs.dfe[rows, :] += dot_t(refs.dup[rows, :], wup[f])

    loop(T // 256, body)


def feed_back(refs, T):
    n = T // SUB
    tmp = refs.pre
    D = refs.xf.shape[1]

    def body(i, total):
        rows = at(i, LANES)
        x = refs.resid[rows, :]
        df = refs.dfe[rows, :]
        out = x + refs.oacc[rows, :]
        scatter_rows(tmp, i * 16, n, out)
        r = lax.rsqrt(jnp.mean(x * x, axis=-1, keepdims=True) + EPS)
        nrm = x * r
        dn = df * refs.g2[...]
        mean = jnp.mean(dn * nrm, axis=-1, keepdims=True)
        dres = refs.cot_p[rows, :].astype(F32) + r * (dn - nrm * mean)
        refs.dfe[rows, :] = dres
        refs.fin[rows, :] = dres.astype(BF16)
        refs.fin_t[:, rows] = dres.T.astype(BF16)
        return total + (df * nrm).reshape(16, SUB, D).sum(axis=0)

    total = lax.fori_loop(0, T // LANES, body, jnp.zeros((SUB, D), F32))
    refs.fgg[...] = jnp.sum(total, axis=0, keepdims=True)

    def emit(i):
        rows = at(i, LANES)
        for q in range(D // LANES):
            refs.block[rows, q * LANES : (q + 1) * LANES] = tmp[q, rows, :].astype(BF16)

    loop(T // LANES, emit)


def mixer_back(refs, z, T):
    ds, dc, st = refs.buf_a, refs.buf_b, refs.st
    halves = C // LANES
    width = 3 * LANES

    def project(i):
        rows = at(i, 256)
        ds[rows, :] = dot(refs.fin[rows, :], refs.wot[z])

    loop(T // 256, project)
    steps = T // 64

    def local(i, carry):
        r0 = pl.multiple_of((steps - 1 - i) * 64, 64)
        d = ds[pl.ds(r0, 64), :]
        k = refs.keep[z, pl.ds(r0, 64), :]
        e, dk = carry
        plist, dlist = [None] * 8, [None] * 8
        for j in range(7, -1, -1):
            kj = k[j * SUB : (j + 1) * SUB]
            p = d[j * SUB : (j + 1) * SUB] + e
            plist[j] = p
            dlist[j] = dk
            e = kj * p
            dk = kj * dk
        ds[pl.ds(r0, 64), :] = jnp.concatenate(plist, axis=0)
        dc[pl.ds(r0, 64), :] = jnp.concatenate(dlist, axis=0)
        return e, dk

    e, dk = lax.fori_loop(0, steps, local, (jnp.zeros((SUB, C), F32), jnp.ones((SUB, C), F32)))
    rows = [jnp.zeros((1, C), F32)]
    for s in range(SUB - 1, 0, -1):
        rows.insert(0, e[s : s + 1] + dk[s : s + 1] * rows[0])
    tail = jnp.concatenate(rows, axis=0)

    def grads(i, sums):
        r0 = pl.multiple_of(i * 64, 64)
        out = []
        for h in range(halves):
            lanes = slice(h * LANES, (h + 1) * LANES)
            sub = pl.ds(r0, 64)
            p0 = ds[sub, lanes].reshape(8, SUB, LANES)
            d0 = dc[sub, lanes].reshape(8, SUB, LANES)
            p = (p0 + d0 * tail[None, :, lanes]).reshape(64, LANES)
            x = p * (st[z, pl.ds(r0 + SUB, 64), lanes] - st[z, sub, lanes])
            df = -(refs.k_f[z, sub, lanes] * x)
            di = refs.k_i[z, sub, lanes] * x
            dcand = refs.k_c[z, sub, lanes] * p
            df16 = df.astype(BF16)
            di16 = di.astype(BF16)
            refs.dpre[sub, h * width : h * width + LANES] = df16
            refs.dpre[sub, h * width + LANES : h * width + 2 * LANES] = di16
            refs.dpre[sub, h * width + 2 * LANES : h * width + 3 * LANES] = dcand.astype(BF16)
            sf, si = sums[h]
            out.append(
                (
                    sf + df16.astype(F32).reshape(8, SUB, LANES).sum(axis=0),
                    si + di16.astype(F32).reshape(8, SUB, LANES).sum(axis=0),
                )
            )
        return tuple(out)

    zero = jnp.zeros((SUB, LANES), F32)
    sums = lax.fori_loop(0, T // 64, grads, tuple((zero, zero) for _ in range(halves)))
    for h in range(halves):
        lanes = slice(h * LANES, (h + 1) * LANES)
        refs.fbg[z, :, lanes] = jnp.sum(sums[h][0], axis=0, keepdims=True)
        refs.ibg[z, :, lanes] = jnp.sum(sums[h][1], axis=0, keepdims=True)

    def back(i):
        rows = at(i, 256)
        refs.oacc[rows, :] += dot_t(refs.dpre[rows, :], refs.wmix[z])

    loop(T // 256, back)


def norm_back(refs, T):
    n = T // SUB
    tmp = refs.pre
    D = refs.xf.shape[1]

    def body(i, total):
        rows = at(i, LANES)
        x = refs.xf[rows, :]
        d_in = refs.oacc[rows, :]
        r = lax.rsqrt(jnp.mean(x * x, axis=-1, keepdims=True) + EPS)
        nrm = x * r
        dn = d_in * refs.g1[...]
        mean = jnp.mean(dn * nrm, axis=-1, keepdims=True)
        out = refs.dfe[rows, :] + r * (dn - nrm * mean)
        scatter_rows(tmp, i * 16, n, out)
        return total + (d_in * nrm).reshape(16, SUB, D).sum(axis=0)

    total = lax.fori_loop(0, T // LANES, body, jnp.zeros((SUB, D), F32))
    refs.mgg[...] = jnp.sum(total, axis=0, keepdims=True)

    def emit(i):
        rows = at(i, LANES)
        for q in range(D // LANES):
            refs.tgrad[rows, q * LANES : (q + 1) * LANES] = tmp[q, rows, :].astype(BF16)

    loop(T // LANES, emit)


class Refs:
    def __init__(self, args):
        (
            self.tok, self.cot, self.wmix, self.wot, self.wup, self.wdt, self.g1, self.g2, self.fb, self.ib,
            self.block, self.tgrad, self.gmix, self.got, self.gup, self.gdt, self.fgg, self.mgg, self.fbg, self.ibg,
            self.xf, self.min, self.min_t, self.fin, self.fin_t, self.cot_p, self.cot_t, self.resid, self.oacc, self.dfe,
            self.pre, self.buf_a, self.buf_b, self.act, self.dup, self.dpre, self.slow, self.st, self.keep, self.k_f,
            self.k_i, self.k_c, self.gst, self.gsem,
        ) = args


def layer_kernel(*args):
    refs = Refs(args)
    T, D = refs.tok.shape
    Z = refs.wmix.shape[0]
    F = refs.wup.shape[0]
    gst, sem = refs.gst, refs.gsem
    norm_in(refs, T)
    loop(Z, lambda z: mixer_forward(refs, z, T))
    mix_out(refs, T)
    cot_in(refs, T)
    refs.oacc[...] = jnp.zeros_like(refs.oacc)
    refs.dfe[...] = jnp.zeros_like(refs.dfe)

    def feed_step(f):
        feed(refs, f, T)
        gst[0, :, 0:C] = dot(refs.cot_t[...], refs.act[...])
        gst[1, :, 0:C] = dot(refs.fin_t[...], refs.dup[...])
        one = pltpu.make_async_copy(gst.at[0, :, 0:C], refs.gdt.at[f], sem.at[0])
        two = pltpu.make_async_copy(gst.at[1, :, 0:C], refs.gup.at[f], sem.at[1])
        one.start()
        two.start()
        one.wait()
        two.wait()

    loop(F, feed_step)
    feed_back(refs, T)
    refs.oacc[...] = jnp.zeros_like(refs.oacc)

    def mixer_step(z):
        gst[0, :, 0:C] = dot(refs.fin_t[...], refs.slow[z])
        mixer_back(refs, z, T)
        gst[1, :, :] = dot(refs.min_t[...], refs.dpre[...])
        one = pltpu.make_async_copy(gst.at[0, :, 0:C], refs.got.at[z], sem.at[0])
        two = pltpu.make_async_copy(gst.at[1], refs.gmix.at[z], sem.at[1])
        one.start()
        two.start()
        one.wait()
        two.wait()

    loop(Z, mixer_step)
    norm_back(refs, T)


def layer(tok, cot, wmix, wot, wup, wdt, g1, g2, fb, ib):
    T, D = tok.shape
    Z, F = wmix.shape[0], wup.shape[0]
    sds = jax.ShapeDtypeStruct
    vm = pl.BlockSpec(memory_space=pltpu.VMEM)
    anyspec = pl.BlockSpec(memory_space=pl.ANY)
    out_shape = (
        sds((T, D), BF16), sds((T, D), BF16),
        sds((Z, D, 3 * C), F32), sds((Z, D, C), F32), sds((F, D, C), F32), sds((F, D, C), F32),
        sds((1, D), F32), sds((1, D), F32), sds((Z, 1, C), F32), sds((Z, 1, C), F32),
    )
    V = pltpu.VMEM
    scratch = [
        V((T, D), F32), V((T, D), BF16), V((D, T), BF16), V((T, D), BF16), V((D, T), BF16),
        V((T, D), BF16), V((D, T), BF16), V((T, D), F32), V((T, D), F32), V((T, D), F32),
        V((3 * C // LANES, T, LANES), F32), V((T, C), F32), V((T, C), F32), V((T, C), BF16), V((T, C), BF16),
        V((T, 3 * C), BF16), V((Z, T, C), BF16), V((Z, T + SUB, C), F32),
        V((Z, T, C), F32), V((Z, T, C), F32), V((Z, T, C), F32), V((Z, T, C), F32),
        V((2, D, 3 * C), F32), pltpu.SemaphoreType.DMA((2,)),
    ]
    return pl.pallas_call(
        layer_kernel,
        out_shape=out_shape,
        in_specs=[vm] * 10,
        out_specs=(vm, vm, anyspec, anyspec, anyspec, anyspec, vm, vm, vm, vm),
        scratch_shapes=scratch,
        compiler_params=pltpu.CompilerParams(vmem_limit_bytes=67043328),
        name="layer",
    )(tok, cot, wmix, wot, wup, wdt, g1, g2, fb, ib)


TINY = 1e-30
CLIP = 0.01


def body(
    tokens,
    cotangent,
    mixer_gain,
    forget_weight,
    input_gate_weight,
    candidate_weight,
    forget_bias,
    input_bias,
    output_weight,
    feed_norm_gain,
    up_weight,
    down_weight,
    mixer_second,
    forget_rows,
    forget_columns,
    input_rows,
    input_columns,
    candidate_rows,
    candidate_columns,
    forget_second,
    input_second,
    output_rows,
    output_columns,
    feed_second,
    up_rows,
    up_columns,
    down_rows,
    down_columns,
):
    groups = lax.axis_size("grp")
    inners = lax.axis_size("inner")
    seqs, length, width = tokens.shape
    def whole(w):
        w = lax.all_gather(w, "inner", axis=1, tiled=True)
        return lax.all_gather(w, "grp", axis=0, tiled=True)

    hidden = forget_weight.shape[1] * inners
    ff = up_weight.shape[1] * inners
    Z, F = hidden // C, ff // C
    gates = [
        whole(w).reshape(width, Z, C // LANES, 1, LANES)
        for w in (forget_weight, input_gate_weight, candidate_weight)
    ]
    wmix = jnp.concatenate(gates, axis=3).reshape(width, Z, 3 * C).transpose(1, 0, 2)
    wot = whole(output_weight).reshape(Z, C, width).transpose(0, 2, 1)
    wup = whole(up_weight).reshape(width, F, C).transpose(1, 0, 2)
    wdt = whole(down_weight).reshape(F, C, width).transpose(0, 2, 1)
    vec = lambda v: lax.all_gather(v, ("grp", "inner"), axis=0, tiled=True).astype(F32)
    (
        block_output, tokens_grad, gmix, got, gup, gdt, fgg, mgg, fbg, ibg
    ) = layer(
        tokens.reshape(length, width), cotangent.reshape(length, width),
        wmix, wot, wup, wdt,
        vec(mixer_gain).reshape(1, width), vec(feed_norm_gain).reshape(1, width),
        vec(forget_bias).reshape(Z, 1, C), vec(input_bias).reshape(Z, 1, C),
    )
    block_output = block_output.reshape(tokens.shape)
    tokens_grad = tokens_grad.reshape(tokens.shape)
    split = gmix.transpose(1, 0, 2).reshape(width, Z, C // LANES, 3, LANES)
    forget_term, input_term, cand_term = [
        split[:, :, :, k].reshape(width, hidden) for k in range(3)
    ]
    output_term = got.transpose(0, 2, 1).reshape(hidden, width)
    up_term = gup.transpose(1, 0, 2).reshape(width, ff)
    down_term = gdt.transpose(0, 2, 1).reshape(ff, width)
    gain_first_term, gain_second_term = mgg.reshape(-1), fgg.reshape(-1)
    fbias_term, ibias_term = fbg.reshape(-1), ibg.reshape(-1)
    part = (
        lax.psum_scatter(
            gain_first_term.reshape(groups, -1), "inner", scatter_dimension=1, tiled=True
        ),
        lax.psum_scatter(forget_term, "inner", scatter_dimension=1, tiled=True),
        lax.psum_scatter(input_term, "inner", scatter_dimension=1, tiled=True),
        lax.psum_scatter(cand_term, "inner", scatter_dimension=1, tiled=True),
        lax.psum_scatter(fbias_term.reshape(groups, -1), "inner", scatter_dimension=1, tiled=True),
        lax.psum_scatter(ibias_term.reshape(groups, -1), "inner", scatter_dimension=1, tiled=True),
        lax.psum_scatter(output_term, "inner", scatter_dimension=1, tiled=True),
        lax.psum_scatter(
            gain_second_term.reshape(groups, -1), "inner", scatter_dimension=1, tiled=True
        ),
        lax.psum_scatter(up_term, "inner", scatter_dimension=1, tiled=True),
        lax.psum_scatter(down_term, "inner", scatter_dimension=1, tiled=True),
    )
    mine = (
        lax.psum_scatter(part[0], "grp", scatter_dimension=0, tiled=True),
        lax.psum_scatter(part[1], "grp", scatter_dimension=0, tiled=True),
        lax.psum_scatter(part[2], "grp", scatter_dimension=0, tiled=True),
        lax.psum_scatter(part[3], "grp", scatter_dimension=0, tiled=True),
        lax.psum_scatter(part[4], "grp", scatter_dimension=0, tiled=True),
        lax.psum_scatter(part[5], "grp", scatter_dimension=0, tiled=True),
        lax.psum_scatter(part[6], "grp", scatter_dimension=0, tiled=True),
        lax.psum_scatter(part[7], "grp", scatter_dimension=0, tiled=True),
        lax.psum_scatter(part[8], "grp", scatter_dimension=0, tiled=True),
        lax.psum_scatter(part[9], "grp", scatter_dimension=0, tiled=True),
    )
    params = [
        mixer_gain,
        forget_weight,
        input_gate_weight,
        candidate_weight,
        forget_bias,
        input_bias,
        output_weight,
        feed_norm_gain,
        up_weight,
        down_weight,
    ]
    locals_f = [p.astype(jnp.float32) for p in params]
    grads = [
        mine[0].reshape(-1),
        mine[1],
        mine[2],
        mine[3],
        mine[4].reshape(-1),
        mine[5].reshape(-1),
        mine[6],
        mine[7].reshape(-1),
        mine[8],
        mine[9],
    ]
    matrix_slots = [1, 2, 3, 6, 8, 9]
    vector_slots = [0, 4, 5, 7]
    rows_old = [forget_rows, input_rows, candidate_rows, output_rows, up_rows, down_rows]
    columns_old = [
        forget_columns,
        input_columns,
        candidate_columns,
        output_columns,
        up_columns,
        down_columns,
    ]
    seconds_old = [mixer_second, forget_second, input_second, feed_second]
    counts = [params[k].size * groups * inners for k in range(10)]
    first_inner = (lax.axis_index("inner") == 0).astype(jnp.float32)
    scales = lax.psum(
        jnp.stack(
            [jnp.sum(w * w) for w in locals_f] + [jnp.sum(r) * first_inner for r in rows_old]
        ),
        ("grp", "inner"),
    )
    mats = [grads[k] for k in matrix_slots]
    row_parts = [jnp.sum(g * g, axis=1) for g in mats]
    column_parts = [jnp.sum(g * g, axis=0) for g in mats]
    row_totals = lax.psum(
        (row_parts[0], row_parts[1], row_parts[2], row_parts[3], row_parts[4], row_parts[5]),
        "inner",
    )
    column_totals = lax.psum(
        (
            column_parts[0],
            column_parts[1],
            column_parts[2],
            column_parts[3],
            column_parts[4],
            column_parts[5],
        ),
        "grp",
    )
    grand = lax.psum(jnp.stack([jnp.sum(v) for v in row_totals]), "grp")
    scaled_all = [None] * 10
    new_states = [None] * 16
    state_places = {1: (1, 2), 2: (3, 4), 3: (5, 6), 6: (9, 10), 8: (12, 13), 9: (14, 15)}
    second_places = {0: 0, 4: 7, 5: 8, 7: 11}
    for k in range(6):
        slot = matrix_slots[k]
        grad = mats[k]
        full_rows = grad.shape[0] * groups
        full_columns = grad.shape[1] * inners
        rows = 0.5 * rows_old[k] + 0.5 * (row_totals[k] / full_columns + TINY)
        columns = 0.5 * columns_old[k] + 0.5 * (column_totals[k] / full_rows + TINY)
        row_mean = 0.5 * scales[10 + k] / full_rows + 0.5 * (
            grand[k] / (full_rows * full_columns) + TINY
        )
        scaled_all[slot] = grad * lax.rsqrt(rows[:, None] * columns[None, :] / row_mean)
        new_states[state_places[slot][0]] = rows
        new_states[state_places[slot][1]] = columns
    for k in range(4):
        slot = vector_slots[k]
        grad = grads[slot]
        second = 0.5 * seconds_old[k] + 0.5 * (grad * grad + TINY)
        scaled_all[slot] = grad * lax.rsqrt(second)
        new_states[second_places[slot]] = second
    clip = lax.psum(jnp.stack([jnp.sum(s * s) for s in scaled_all]), ("grp", "inner"))
    count_array = jnp.array(counts, jnp.float32)
    update_norms = jnp.sqrt(clip / count_array)
    fresh = [
        locals_f[k]
        + -jnp.sqrt(scales[k] / counts[k]) * scaled_all[k] / jnp.maximum(CLIP, update_norms[k])
        for k in range(10)
    ]
    return (
        block_output,
        tokens_grad,
        grads[0],
        grads[1],
        grads[2],
        grads[3],
        grads[4],
        grads[5],
        grads[6],
        grads[7],
        grads[8],
        grads[9],
        fresh[0],
        fresh[1],
        fresh[2],
        fresh[3],
        fresh[4],
        fresh[5],
        fresh[6],
        fresh[7],
        fresh[8],
        fresh[9],
        new_states[0],
        new_states[1],
        new_states[2],
        new_states[3],
        new_states[4],
        new_states[5],
        new_states[6],
        new_states[7],
        new_states[8],
        new_states[9],
        new_states[10],
        new_states[11],
        new_states[12],
        new_states[13],
        new_states[14],
        new_states[15],
        update_norms,
    )


def solution(mesh):
    return jax.shard_map(
        body,
        mesh=mesh,
        in_specs=(
            P(("grp", "inner"), None, None),
            P(("grp", "inner"), None, None),
            P(("grp", "inner")),
            P("grp", "inner"),
            P("grp", "inner"),
            P("grp", "inner"),
            P(("grp", "inner")),
            P(("grp", "inner")),
            P("grp", "inner"),
            P(("grp", "inner")),
            P("grp", "inner"),
            P("grp", "inner"),
            P(("grp", "inner")),
            P("grp"),
            P("inner"),
            P("grp"),
            P("inner"),
            P("grp"),
            P("inner"),
            P(("grp", "inner")),
            P(("grp", "inner")),
            P("grp"),
            P("inner"),
            P(("grp", "inner")),
            P("grp"),
            P("inner"),
            P("grp"),
            P("inner"),
        ),
        out_specs=(
            P(("grp", "inner"), None, None),
            P(("grp", "inner"), None, None),
            P(("grp", "inner")),
            P("grp", "inner"),
            P("grp", "inner"),
            P("grp", "inner"),
            P(("grp", "inner")),
            P(("grp", "inner")),
            P("grp", "inner"),
            P(("grp", "inner")),
            P("grp", "inner"),
            P("grp", "inner"),
            P(("grp", "inner")),
            P("grp", "inner"),
            P("grp", "inner"),
            P("grp", "inner"),
            P(("grp", "inner")),
            P(("grp", "inner")),
            P("grp", "inner"),
            P(("grp", "inner")),
            P("grp", "inner"),
            P("grp", "inner"),
            P(("grp", "inner")),
            P("grp"),
            P("inner"),
            P("grp"),
            P("inner"),
            P("grp"),
            P("inner"),
            P(("grp", "inner")),
            P(("grp", "inner")),
            P("grp"),
            P("inner"),
            P(("grp", "inner")),
            P("grp"),
            P("inner"),
            P("grp"),
            P("inner"),
            P(),
        ),
        check_vma=False,
    )
```

```python
import functools
import math
import jax
import jax.numpy as jnp
from jax import lax
from jax.experimental import pallas as pl
from jax.sharding import PartitionSpec as P
from jax.experimental.pallas import tpu as pltpu

EPS = 1e-06
F32 = jnp.float32
BF16 = jnp.bfloat16
C = 256
LANES = 128
SUB = 8
ERFC = (
    0.2256758669, 0.2256693636, 0.2078460312, 0.1685204197, 0.1415057621,
    -0.005753053848, 0.1692475449, -0.182997133, 0.05028532412,
)


def dot(a, b):
    return jnp.dot(a, b, preferred_element_type=F32)


def dot_t(a, b):
    return lax.dot_general(a, b, (((1,), (1,)), ((), ())), preferred_element_type=F32)


def loop(steps, body):
    def run(i, carry):
        body(i)
        return carry

    lax.fori_loop(0, steps, run, 0)


def at(i, size):
    return pl.ds(pl.multiple_of(i * size, size), size)


def gelu_parts(x):
    ax = jnp.abs(x)
    e = jnp.exp(-0.5 * (x * x))
    t = 1.0 / (1.0 + (0.4 * math.sqrt(0.5)) * ax)
    poly = jnp.full_like(t, ERFC[-1])
    for c in ERFC[-2::-1]:
        poly = poly * t + c
    half = 0.5 * (poly * t * e)
    cdf = jnp.where(x >= 0, 1.0 - half, half)
    return x * cdf, cdf + (x * e) * (1.0 / math.sqrt(2.0 * math.pi))


def strided(ref, j, n):
    return ref[pl.ds(j, SUB, stride=n), :]

def gather_rows(tmp, j0, n, D):
    columns = [
        jnp.concatenate([tmp[q, pl.ds(j0 + jj, SUB, stride=n), :] for jj in range(16)], axis=0)
        for q in range(D // LANES)
    ]
    return jnp.concatenate(columns, axis=1)


def scatter_rows(tmp, j0, n, out):
    for q in range(out.shape[1] // LANES):
        for jj in range(16):
            tmp[q, pl.ds(j0 + jj, SUB, stride=n), :] = out[
                jj * SUB : (jj + 1) * SUB, q * LANES : (q + 1) * LANES
            ]


def norm_in(refs, T):
    n = T // SUB
    tmp, xf, g1 = refs.pre, refs.xf, refs.g1
    D = xf.shape[1]

    def widen(i):
        rows = at(i, LANES)
        wide = refs.tok[rows, :].astype(F32)
        for q in range(D // LANES):
            tmp[q, rows, :] = wide[:, q * LANES : (q + 1) * LANES]

    loop(T // LANES, widen)

    def place(i):
        x = gather_rows(tmp, i * 16, n, D)
        y = x * lax.rsqrt(jnp.mean(x * x, axis=-1, keepdims=True) + EPS) * g1[...]
        rows = at(i, LANES)
        xf[rows, :] = x
        refs.min[rows, :] = y.astype(BF16)
        refs.min_t[:, rows] = y.T.astype(BF16)

    loop(T // LANES, place)


def cot_in(refs, T):
    n = T // SUB
    tmp = refs.pre
    D = refs.xf.shape[1]

    def widen(i):
        rows = at(i, LANES)
        wide = refs.cot[rows, :].astype(F32)
        for q in range(D // LANES):
            tmp[q, rows, :] = wide[:, q * LANES : (q + 1) * LANES]

    loop(T // LANES, widen)

    def place(i):
        x = gather_rows(tmp, i * 16, n, D)
        rows = at(i, LANES)
        refs.cot_p[rows, :] = x.astype(BF16)
        refs.cot_t[:, rows] = x.T.astype(BF16)

    loop(T // LANES, place)


def mixer_forward(refs, z, T):
    pre, ac, st = refs.pre, refs.buf_a, refs.st
    halves = C // LANES
    width = 3 * LANES

    def project(i):
        rows = at(i, 256)
        out = dot(refs.min[rows, :], refs.wmix[z])
        for q in range(3 * halves):
            pre[q, rows, :] = out[:, q * LANES : (q + 1) * LANES]

    loop(T // 256, project)
    fb = refs.fb[z]
    ib = refs.ib[z]

    def gates(i, carry):
        r0 = pl.multiple_of(i * 64, 64)
        out = []
        for h in range(halves):
            a, b = carry[h]
            lanes = slice(h * LANES, (h + 1) * LANES)
            pf = pre[3 * h, pl.ds(r0, 64), :] + fb[:, lanes]
            pi = pre[3 * h + 1, pl.ds(r0, 64), :] + ib[:, lanes]
            pc = pre[3 * h + 2, pl.ds(r0, 64), :]
            m = jnp.minimum(jnp.minimum(pf, pi), 0.0)
            e0 = jnp.exp(m)
            ef = jnp.exp(m - pf)
            ei = jnp.exp(m - pi)
            nk = e0 + ei
            na = e0 + ef
            inv = 1.0 / (nk + na)
            keep = nk * inv
            admit = na * inv
            not_f = 1.0 / (1.0 + jnp.exp(pf))
            not_i = 1.0 / (1.0 + jnp.exp(pi))
            ec = jnp.exp(jnp.minimum(pc, 0.0))
            sg = ec / (1.0 + ec)
            positive = pc >= 0
            value = jnp.where(positive, pc + 0.5, sg)
            slope = jnp.where(positive, 1.0, sg * (1.0 - sg))
            refs.keep[z, pl.ds(r0, 64), lanes] = keep
            refs.k_f[z, pl.ds(r0, 64), lanes] = keep * not_f
            refs.k_i[z, pl.ds(r0, 64), lanes] = keep * not_i
            refs.k_c[z, pl.ds(r0, 64), lanes] = admit * slope
            inflow = admit * value
            alist, blist = [], []
            for j in range(8):
                kj = keep[j * SUB : (j + 1) * SUB]
                b = kj * b + inflow[j * SUB : (j + 1) * SUB]
                a = kj * a
                alist.append(a)
                blist.append(b)
            ac[pl.ds(r0, 64), lanes] = jnp.concatenate(alist, axis=0)
            st[z, pl.ds(r0 + SUB, 64), lanes] = jnp.concatenate(blist, axis=0)
            out.append((a, b))
        return tuple(out)

    one = jnp.ones((SUB, LANES), F32)
    zero = jnp.zeros((SUB, LANES), F32)
    ends = lax.fori_loop(0, T // 64, gates, tuple((one, zero) for _ in range(halves)))
    for h in range(halves):
        a, b = ends[h]
        rows = [jnp.zeros((1, LANES), F32)]
        for s in range(SUB - 1):
            rows.append(a[s : s + 1] * rows[-1] + b[s : s + 1])
        st[z, 0:SUB, h * LANES : (h + 1) * LANES] = jnp.concatenate(rows, axis=0)
    first = st[z, 0:SUB, :]

    def finish(i):
        r0 = pl.multiple_of(i * 64, 64)
        a = ac[pl.ds(r0, 64), :].reshape(8, SUB, C)
        b = st[z, pl.ds(r0 + SUB, 64), :].reshape(8, SUB, C)
        s = (b + a * first[None]).reshape(64, C)
        st[z, pl.ds(r0 + SUB, 64), :] = s
        refs.slow[z, pl.ds(r0, 64), :] = s.astype(BF16)

    loop(T // 64, finish)


def mix_out(refs, T):
    Z = refs.wot.shape[0]

    def body(i):
        rows = at(i, 256)
        acc = refs.xf[rows, :]
        for z in range(Z):
            acc = acc + dot_t(refs.slow[z, rows, :], refs.wot[z])
        refs.resid[rows, :] = acc
        for k in range(2):
            x = acc[k * LANES : (k + 1) * LANES]
            y = x * lax.rsqrt(jnp.mean(x * x, axis=-1, keepdims=True) + EPS) * refs.g2[...]
            sub = pl.ds(pl.multiple_of(i * 256 + k * LANES, LANES), LANES)
            refs.fin[sub, :] = y.astype(BF16)
            refs.fin_t[:, sub] = y.T.astype(BF16)

    loop(T // 256, body)


def feed(refs, f, T):
    wup, wdt = refs.wup, refs.wdt

    def body(i):
        rows = at(i, 256)
        refs.buf_a[rows, :] = dot(refs.fin[rows, :], wup[f])
        refs.buf_b[rows, :] = dot(refs.cot_p[rows, :], wdt[f])
        for k in range(4):
            sub = pl.ds(pl.multiple_of(i * 256 + k * 64, 64), 64)
            act, slope = gelu_parts(refs.buf_a[sub, :])
            refs.act[sub, :] = act.astype(BF16)
            refs.dup[sub, :] = (refs.buf_b[sub, :] * slope).astype(BF16)
        refs.oacc[rows, :] += dot_t(refs.act[rows, :], wdt[f])
        refs.dfe[rows, :] += dot_t(refs.dup[rows, :], wup[f])

    loop(T // 256, body)


def feed_back(refs, T):
    n = T // SUB
    tmp = refs.pre
    D = refs.xf.shape[1]

    def body(i, total):
        rows = at(i, LANES)
        x = refs.resid[rows, :]
        df = refs.dfe[rows, :]
        out = x + refs.oacc[rows, :]
        scatter_rows(tmp, i * 16, n, out)
        r = lax.rsqrt(jnp.mean(x * x, axis=-1, keepdims=True) + EPS)
        nrm = x * r
        dn = df * refs.g2[...]
        mean = jnp.mean(dn * nrm, axis=-1, keepdims=True)
        dres = refs.cot_p[rows, :].astype(F32) + r * (dn - nrm * mean)
        refs.dfe[rows, :] = dres
        refs.fin[rows, :] = dres.astype(BF16)
        refs.fin_t[:, rows] = dres.T.astype(BF16)
        return total + (df * nrm).reshape(16, SUB, D).sum(axis=0)

    total = lax.fori_loop(0, T // LANES, body, jnp.zeros((SUB, D), F32))
    refs.fgg[...] = jnp.sum(total, axis=0, keepdims=True)

    def emit(i):
        rows = at(i, LANES)
        for q in range(D // LANES):
            refs.block[rows, q * LANES : (q + 1) * LANES] = tmp[q, rows, :].astype(BF16)

    loop(T // LANES, emit)


def mixer_back(refs, z, T):
    ds, dc, st = refs.buf_a, refs.buf_b, refs.st
    halves = C // LANES
    width = 3 * LANES

    def project(i):
        rows = at(i, 256)
        ds[rows, :] = dot(refs.fin[rows, :], refs.wot[z])

    loop(T // 256, project)
    steps = T // 64

    def local(i, carry):
        r0 = pl.multiple_of((steps - 1 - i) * 64, 64)
        d = ds[pl.ds(r0, 64), :]
        k = refs.keep[z, pl.ds(r0, 64), :]
        e, dk = carry
        plist, dlist = [None] * 8, [None] * 8
        for j in range(7, -1, -1):
            kj = k[j * SUB : (j + 1) * SUB]
            p = d[j * SUB : (j + 1) * SUB] + e
            plist[j] = p
            dlist[j] = dk
            e = kj * p
            dk = kj * dk
        ds[pl.ds(r0, 64), :] = jnp.concatenate(plist, axis=0)
        dc[pl.ds(r0, 64), :] = jnp.concatenate(dlist, axis=0)
        return e, dk

    e, dk = lax.fori_loop(0, steps, local, (jnp.zeros((SUB, C), F32), jnp.ones((SUB, C), F32)))
    rows = [jnp.zeros((1, C), F32)]
    for s in range(SUB - 1, 0, -1):
        rows.insert(0, e[s : s + 1] + dk[s : s + 1] * rows[0])
    tail = jnp.concatenate(rows, axis=0)

    def grads(i, sums):
        r0 = pl.multiple_of(i * 64, 64)
        out = []
        for h in range(halves):
            lanes = slice(h * LANES, (h + 1) * LANES)
            sub = pl.ds(r0, 64)
            p0 = ds[sub, lanes].reshape(8, SUB, LANES)
            d0 = dc[sub, lanes].reshape(8, SUB, LANES)
            p = (p0 + d0 * tail[None, :, lanes]).reshape(64, LANES)
            x = p * (st[z, pl.ds(r0 + SUB, 64), lanes] - st[z, sub, lanes])
            df = -(refs.k_f[z, sub, lanes] * x)
            di = refs.k_i[z, sub, lanes] * x
            dcand = refs.k_c[z, sub, lanes] * p
            df16 = df.astype(BF16)
            di16 = di.astype(BF16)
            refs.dpre[sub, h * width : h * width + LANES] = df16
            refs.dpre[sub, h * width + LANES : h * width + 2 * LANES] = di16
            refs.dpre[sub, h * width + 2 * LANES : h * width + 3 * LANES] = dcand.astype(BF16)
            sf, si = sums[h]
            out.append(
                (
                    sf + df16.astype(F32).reshape(8, SUB, LANES).sum(axis=0),
                    si + di16.astype(F32).reshape(8, SUB, LANES).sum(axis=0),
                )
            )
        return tuple(out)

    zero = jnp.zeros((SUB, LANES), F32)
    sums = lax.fori_loop(0, T // 64, grads, tuple((zero, zero) for _ in range(halves)))
    for h in range(halves):
        lanes = slice(h * LANES, (h + 1) * LANES)
        refs.fbg[z, :, lanes] = jnp.sum(sums[h][0], axis=0, keepdims=True)
        refs.ibg[z, :, lanes] = jnp.sum(sums[h][1], axis=0, keepdims=True)

    def back(i):
        rows = at(i, 256)
        refs.oacc[rows, :] += dot_t(refs.dpre[rows, :], refs.wmix[z])

    loop(T // 256, back)


def norm_back(refs, T):
    n = T // SUB
    tmp = refs.pre
    D = refs.xf.shape[1]

    def body(i, total):
        rows = at(i, LANES)
        x = refs.xf[rows, :]
        d_in = refs.oacc[rows, :]
        r = lax.rsqrt(jnp.mean(x * x, axis=-1, keepdims=True) + EPS)
        nrm = x * r
        dn = d_in * refs.g1[...]
        mean = jnp.mean(dn * nrm, axis=-1, keepdims=True)
        out = refs.dfe[rows, :] + r * (dn - nrm * mean)
        scatter_rows(tmp, i * 16, n, out)
        return total + (d_in * nrm).reshape(16, SUB, D).sum(axis=0)

    total = lax.fori_loop(0, T // LANES, body, jnp.zeros((SUB, D), F32))
    refs.mgg[...] = jnp.sum(total, axis=0, keepdims=True)

    def emit(i):
        rows = at(i, LANES)
        for q in range(D // LANES):
            refs.tgrad[rows, q * LANES : (q + 1) * LANES] = tmp[q, rows, :].astype(BF16)

    loop(T // LANES, emit)

class Refs:
    def __init__(self, args):
        (
            self.tok, self.cot, self.wmix, self.wot, self.wup, self.wdt, self.g1, self.g2, self.fb, self.ib,
            self.block, self.tgrad, self.gmix, self.got, self.gup, self.gdt, self.fgg, self.mgg, self.fbg, self.ibg,
            self.xf, self.min, self.min_t, self.fin, self.fin_t, self.cot_p, self.cot_t, self.resid, self.oacc, self.dfe,
            self.pre, self.buf_a, self.buf_b, self.act, self.dup, self.dpre, self.slow, self.st, self.keep, self.k_f,
            self.k_i, self.k_c, self.gst, self.gsem,
        ) = args


def layer_kernel(*args):
    refs = Refs(args)
    T, D = refs.tok.shape
    Z = refs.wmix.shape[0]
    F = refs.wup.shape[0]
    gst, sem = refs.gst, refs.gsem
    norm_in(refs, T)
    loop(Z, lambda z: mixer_forward(refs, z, T))
    mix_out(refs, T)
    cot_in(refs, T)
    refs.oacc[...] = jnp.zeros_like(refs.oacc)
    refs.dfe[...] = jnp.zeros_like(refs.dfe)

    def feed_step(f):
        feed(refs, f, T)
        gst[0, :, 0:C] = dot(refs.cot_t[...], refs.act[...])
        gst[1, :, 0:C] = dot(refs.fin_t[...], refs.dup[...])
        one = pltpu.make_async_copy(gst.at[0, :, 0:C], refs.gdt.at[f], sem.at[0])
        two = pltpu.make_async_copy(gst.at[1, :, 0:C], refs.gup.at[f], sem.at[1])
        one.start()
        two.start()
        one.wait()
        two.wait()

    loop(F, feed_step)
    feed_back(refs, T)
    refs.oacc[...] = jnp.zeros_like(refs.oacc)

    def mixer_step(z):
        gst[0, :, 0:C] = dot(refs.fin_t[...], refs.slow[z])
        mixer_back(refs, z, T)
        gst[1, :, :] = dot(refs.min_t[...], refs.dpre[...])
        one = pltpu.make_async_copy(gst.at[0, :, 0:C], refs.got.at[z], sem.at[0])
        two = pltpu.make_async_copy(gst.at[1], refs.gmix.at[z], sem.at[1])
        one.start()
        two.start()
        one.wait()
        two.wait()

    loop(Z, mixer_step)
    norm_back(refs, T)


def layer(tok, cot, wmix, wot, wup, wdt, g1, g2, fb, ib):
    T, D = tok.shape
    Z, F = wmix.shape[0], wup.shape[0]
    sds = jax.ShapeDtypeStruct
    vm = pl.BlockSpec(memory_space=pltpu.VMEM)
    anyspec = pl.BlockSpec(memory_space=pl.ANY)
    out_shape = (
        sds((T, D), BF16), sds((T, D), BF16),
        sds((Z, D, 3 * C), F32), sds((Z, D, C), F32), sds((F, D, C), F32), sds((F, D, C), F32),
        sds((1, D), F32), sds((1, D), F32), sds((Z, 1, C), F32), sds((Z, 1, C), F32),
    )
    V = pltpu.VMEM
    scratch = [
        V((T, D), F32), V((T, D), BF16), V((D, T), BF16), V((T, D), BF16), V((D, T), BF16),
        V((T, D), BF16), V((D, T), BF16), V((T, D), F32), V((T, D), F32), V((T, D), F32),
        V((3 * C // LANES, T, LANES), F32), V((T, C), F32), V((T, C), F32), V((T, C), BF16), V((T, C), BF16),
        V((T, 3 * C), BF16), V((Z, T, C), BF16), V((Z, T + SUB, C), F32),
        V((Z, T, C), F32), V((Z, T, C), F32), V((Z, T, C), F32), V((Z, T, C), F32),
        V((2, D, 3 * C), F32), pltpu.SemaphoreType.DMA((2,)),
    ]
    return pl.pallas_call(
        layer_kernel,
        out_shape=out_shape,
        in_specs=[vm] * 10,
        out_specs=(vm, vm, anyspec, anyspec, anyspec, anyspec, vm, vm, vm, vm),
        scratch_shapes=scratch,
        compiler_params=pltpu.CompilerParams(vmem_limit_bytes=67043328),
        name="layer",
    )(tok, cot, wmix, wot, wup, wdt, g1, g2, fb, ib)

MESH = pl.DeviceIdType.MESH


def rcopy(src, dst, send, recv, device):
    return pltpu.make_async_remote_copy(
        src_ref=src, dst_ref=dst, send_sem=send, recv_sem=recv, device_id=device, device_id_type=MESH
    )


class Place:
    def __init__(self):
        self.g = lax.axis_index("grp")
        self.i = lax.axis_index("inner")
        self.y, self.x = self.g // 2, self.g % 2
        self.z, self.c = self.i // 2, self.i % 2
        self.me = self.g * 8 + self.i
        self.partner = (self.g, self.z * 2 + 1 - self.c)

    def flip(self, fx, fy):
        x = (self.x + fx) % 2
        y = (self.y + fy) % 2
        return y * 2 + x

    def near(self, z):
        e = z % 2
        return self.flip(1 - e, e)

    def far(self, z):
        e = z % 2
        return self.flip(e, 1 - e)

    def other(self, k):
        t = (self.me + k) % 32
        return (t // 8, t % 8)


def entry_barrier(place):
    barrier = pltpu.get_barrier_semaphore()

    def greet(k):
        pl.semaphore_signal(barrier, inc=1, device_id=place.other(k + 1), device_id_type=MESH)

    loop(31, greet)
    pl.semaphore_wait(barrier, 31)


def spread(values, start, count, total):
    lane = lax.broadcasted_iota(jnp.int32, (LANES, total), 1)
    row = lax.broadcasted_iota(jnp.int32, (LANES, total), 0)
    sel = jnp.where(row == start + lane % count, 1.0, 0.0).astype(BF16)
    picked = dot(values, sel)
    owner = lax.broadcasted_iota(jnp.int32, picked.shape, 0)
    spot = lax.broadcasted_iota(jnp.int32, picked.shape, 1)
    return jnp.sum(jnp.where(spot // count == owner, picked, 0.0), axis=0, keepdims=True)


def pack_vectors(mg, fb, ib, fg):
    parts = [mg, fb, ib, fg]
    used = sum(p.shape[0] for p in parts)
    rows = [p[...].astype(F32).reshape(1, p.shape[0]) for p in parts]
    return jnp.concatenate(rows + [jnp.zeros((1, LANES - used), F32)], axis=1)


def block_of(refs, a, g, i):
    if a == 0:
        return refs.wot.at[g, at(i, 64), :]
    if a == 1:
        return refs.wup.at[i, at(g, 128), :]
    return refs.wdt.at[pl.ds(2 * g, 2), at(i, 64), :]


def blocks_of(refs, a, i):
    if a == 0:
        return refs.wot.at[:, at(i, 64), :]
    if a == 1:
        return refs.wup.at[i]
    return refs.wdt.at[:, at(i, 64), :]


def mix_column(refs, z, c):
    return refs.wmix.at[z, :, at(c, 384)]


def gather_start(refs, p):
    refs.o16[...] = refs.ow[...].astype(F32).T.astype(BF16)
    refs.d16[...] = refs.dw[...].astype(F32).T.astype(BF16)
    local = []
    for k, w in enumerate((refs.fw, refs.iw, refs.cw)):
        spot = pl.ds(pl.multiple_of(p.c * 384 + k * 128, 128), 128)
        local.append(
            pltpu.make_async_copy(w, refs.wmix.at[p.z, at(p.g, 128), spot], refs.loc_s.at[k])
        )
    local.append(pltpu.make_async_copy(refs.o16, block_of(refs, 0, p.g, p.i), refs.loc_s.at[3]))
    local.append(pltpu.make_async_copy(refs.uw, block_of(refs, 1, p.g, p.i), refs.loc_s.at[4]))
    for k in range(2):
        local.append(
            pltpu.make_async_copy(
                refs.d16.at[:, k * 256 : (k + 1) * 256],
                refs.wdt.at[2 * p.g + k, at(p.i, 64), :],
                refs.loc_s.at[5 + k],
            )
        )
    for c in local:
        c.start()
    row = pack_vectors(refs.mg, refs.fbv, refs.ibv, refs.fg)
    refs.vstage[...] = row
    refs.vecs[p.me] = row
    entry_barrier(p)
    for c in local[:3]:
        c.wait()
    own = refs.wmix.at[p.z, at(p.g, 128), at(p.c, 384)]
    for k in range(1, 4):
        peer = p.flip(k % 2, k // 2)
        rcopy(own, own, refs.mxg_s.at[k - 1], refs.mxg_r.at[k - 1], (peer, p.i)).start()

    def vector(k):
        rcopy(refs.vstage, refs.vecs.at[p.me], refs.vec_s, refs.vec_r, p.other(k + 1)).start()

    loop(31, vector)
    for c in local[3:]:
        c.wait()
    for a in range(3):
        blk = block_of(refs, a, p.g, p.i)
        for k in range(1, 4):
            peer = (p.g, ((p.z + k) % 4) * 2 + p.c)
            rcopy(blk, blk, refs.ffz_s.at[a, k - 1], refs.ffz_r.at[a, p.z], peer).start()


def gather_vectors(refs, p):
    rows = refs.vecs.at[pl.ds(0, 31)]
    rcopy(rows, rows, refs.vec_s, refs.vec_r, p.partner).wait()
    v = refs.vecs[...].reshape(32, LANES).astype(BF16)
    refs.g1[...] = spread(v, 0, 16, 512)
    refs.g2[...] = spread(v, 80, 16, 512)
    fb = spread(v, 16, 32, 1024)
    ib = spread(v, 48, 32, 1024)
    for z in range(4):
        refs.fb[z] = fb[:, z * C : (z + 1) * C]
        refs.ib[z] = ib[:, z * C : (z + 1) * C]


def mix_exchange(refs, p, s):
    def send_partner(z):
        col = mix_column(refs, z, p.c)
        rcopy(col, col, refs.mxp_s.at[z], refs.mxp_r.at[z], p.partner).start()

    def wait_partner(z):
        col = mix_column(refs, z, 1 - p.c)
        rcopy(col, col, refs.mxp_s.at[z], refs.mxp_r.at[z], p.partner).wait_recv()

    def send_up(z):
        col = mix_column(refs, z, p.c)
        rcopy(col, col, refs.mxu_s.at[z], refs.mxz_r.at[z], (p.g, p.i + 2)).start()

    def send_down(z):
        col = mix_column(refs, z, p.c)
        rcopy(col, col, refs.mxd_s.at[z], refs.mxz_r.at[z], (p.g, p.i - 2)).start()

    def wait_line(z):
        col = mix_column(refs, z, p.c)
        rcopy(col, col, refs.mxp_s.at[z], refs.mxz_r.at[z], p.partner).wait_recv()

    @pl.when(s == 0)
    def _():
        for k in range(1, 4):
            peer = p.flip(k % 2, k // 2)
            blk = refs.wmix.at[p.z, at(peer, 128), at(p.c, 384)]
            rcopy(blk, blk, refs.mxg_s.at[k - 1], refs.mxg_r.at[k - 1], (peer, p.i)).wait()

        @pl.when(p.z < 3)
        def _():
            send_up(p.z)

        @pl.when(p.z > 0)
        def _():
            send_down(p.z)

        send_partner(p.z)
        wait_partner(p.z)

    below, above = p.z - s, p.z + s

    @pl.when((s > 0) & (below >= 0))
    def _():
        wait_line(below)

        @pl.when(p.z < 3)
        def _():
            send_up(below)

        send_partner(below)

    @pl.when((s > 0) & (above < 4))
    def _():
        wait_line(above)

        @pl.when(p.z > 0)
        def _():
            send_down(above)

        send_partner(above)

    @pl.when((s > 0) & (below >= 0))
    def _():
        wait_partner(below)

    @pl.when((s > 0) & (above < 4))
    def _():
        wait_partner(above)


def mix_drain(refs, p):
    for z in range(4):
        col = mix_column(refs, z, p.c)
        rcopy(col, col, refs.mxp_s.at[z], refs.mxp_r.at[z], p.partner).wait_send()

        @pl.when((z <= p.z) & (p.z < 3))
        def _():
            rcopy(col, col, refs.mxu_s.at[z], refs.mxz_r.at[z], p.partner).wait_send()

        @pl.when((z >= p.z) & (p.z > 0))
        def _():
            rcopy(col, col, refs.mxd_s.at[z], refs.mxz_r.at[z], p.partner).wait_send()


def feed_second(refs, p):
    for a in range(3):
        for z in range(4):
            blk = block_of(refs, a, p.g, z * 2 + p.c)

            @pl.when(p.z != z)
            def _():
                rcopy(blk, blk, refs.ffp_s.at[a, z], refs.ffz_r.at[a, z], p.partner).wait_recv()

            rcopy(blk, blk, refs.ff2_s.at[a, z], refs.ff2_r.at[a, z], (p.near(z), p.i)).start()


def feed_third(refs, p):
    for a in range(3):
        for z in range(4):
            mine = block_of(refs, a, p.g, z * 2 + p.c)
            near = block_of(refs, a, p.near(z), z * 2 + p.c)
            far = (p.far(z), p.i)
            rcopy(near, near, refs.ff2_s.at[a, z], refs.ff2_r.at[a, z], (p.near(z), p.i)).wait_recv()
            rcopy(mine, mine, refs.ff3_s.at[a, z, 0], refs.ff3_r.at[a, z, 0], far).start()
            rcopy(near, near, refs.ff3_s.at[a, z, 1], refs.ff3_r.at[a, z, 1], far).start()


def feed_fourth(refs, p):
    for a in range(3):
        for z in range(4):
            blk = block_of(refs, a, p.g, z * 2 + p.c)
            far = (p.far(z), p.i)
            for k in range(2):
                rcopy(blk, blk, refs.ff3_s.at[a, z, k], refs.ff3_r.at[a, z, k], far).wait_recv()
            full = blocks_of(refs, a, z * 2 + p.c)
            rcopy(full, full, refs.ffp_s.at[a, z], refs.ffp_r.at[a, z], p.partner).start()


def feed_last(refs, p):
    for a in range(3):
        for z in range(4):
            full = blocks_of(refs, a, z * 2 + 1 - p.c)
            rcopy(full, full, refs.ffp_s.at[a, z], refs.ffp_r.at[a, z], p.partner).wait_recv()


def feed_drain(refs, p):
    for a in range(3):
        for k in range(1, 4):
            blk = block_of(refs, a, p.g, p.i)
            rcopy(blk, blk, refs.ffz_s.at[a, k - 1], refs.ffz_r.at[a, p.z], p.partner).wait_send()
        for z in range(4):
            blk = block_of(refs, a, p.g, z * 2 + p.c)
            rcopy(blk, blk, refs.ff2_s.at[a, z], refs.ff2_r.at[a, z], p.partner).wait_send()
            for k in range(2):
                rcopy(blk, blk, refs.ff3_s.at[a, z, k], refs.ff3_r.at[a, z, k], p.partner).wait_send()
            full = blocks_of(refs, a, z * 2 + p.c)
            rcopy(full, full, refs.ffp_s.at[a, z], refs.ffp_r.at[a, z], p.partner).wait_send()


def slot_chunk(p, s):
    low = jnp.minimum(p.z, 3 - p.z)
    shift = jnp.where(s == 0, 1, jnp.where(s == 1, -1, 0))
    m = s + low * shift
    return jnp.where(p.z < 2, m, 3 - m)


def mixer_slots(refs, p, T):
    def slot(s):
        mix_exchange(refs, p, s)
        mixer_forward(refs, slot_chunk(p, s), T)

        @pl.when(s == 0)
        def _():
            feed_second(refs, p)

        @pl.when(s == 1)
        def _():
            feed_third(refs, p)

        @pl.when(s == 2)
        def _():
            feed_fourth(refs, p)

    loop(4, slot)
    mix_drain(refs, p)
    feed_last(refs, p)
    feed_drain(refs, p)

class GatherRefs:
    def __init__(self, args):
        (
            self.tok, self.cot, self.fw, self.iw, self.cw, self.ow, self.uw, self.dw,
            self.mg, self.fbv, self.ibv, self.fg,
            self.block, self.tgrad, self.gmix, self.got, self.gup, self.gdt,
            self.fgg, self.mgg, self.fbg, self.ibg,
            self.wmix, self.wot, self.wup, self.wdt, self.g1, self.g2, self.fb, self.ib,
            self.vecs, self.vstage, self.o16, self.d16,
            self.xf, self.min, self.min_t, self.fin, self.fin_t, self.cot_p, self.cot_t,
            self.resid, self.oacc, self.dfe,
            self.pre, self.buf_a, self.buf_b, self.act, self.dup, self.dpre,
            self.slow, self.st, self.keep, self.k_f, self.k_i, self.k_c, self.gsem,
            self.loc_s, self.mxg_s, self.mxg_r, self.mxu_s, self.mxd_s, self.mxz_r,
            self.mxp_s, self.mxp_r, self.vec_s, self.vec_r, self.ffz_s, self.ffz_r,
            self.ff2_s, self.ff2_r, self.ff3_s, self.ff3_r, self.ffp_s, self.ffp_r,
        ) = args


def grad_slot(refs, k, D):
    return refs.pre.at[:, k * D : (k + 1) * D, :]


def put_grad(refs, k, value):
    D = value.shape[0]
    for q in range(value.shape[1] // LANES):
        refs.pre[q, k * D : (k + 1) * D, :] = value[:, q * LANES : (q + 1) * LANES]


def send_grad(refs, k, D, width, out, sem):
    return [
        pltpu.make_async_copy(
            refs.pre.at[q, k * D : (k + 1) * D, :],
            out.at[:, q * LANES : (q + 1) * LANES],
            sem.at[q],
        )
        for q in range(width // LANES)
    ]


def layer_ag_kernel(*args):
    refs = GatherRefs(args)
    T, D = refs.tok.shape
    Z = refs.wmix.shape[0]
    F = refs.wup.shape[0]
    p = Place()
    gather_start(refs, p)
    cot_in(refs, T)
    gather_vectors(refs, p)
    norm_in(refs, T)
    mixer_slots(refs, p, T)
    mix_out(refs, T)
    refs.oacc[...] = jnp.zeros_like(refs.oacc)
    refs.dfe[...] = jnp.zeros_like(refs.dfe)

    def feed_step(f):
        feed(refs, f, T)
        put_grad(refs, 0, dot(refs.cot_t[...], refs.act[...]))
        put_grad(refs, 1, dot(refs.fin_t[...], refs.dup[...]))
        copies = send_grad(refs, 0, D, C, refs.gdt.at[f], refs.gsem.at[0])
        copies += send_grad(refs, 1, D, C, refs.gup.at[f], refs.gsem.at[1])
        for c in copies:
            c.start()
        for c in copies:
            c.wait()

    loop(F, feed_step)
    feed_back(refs, T)
    refs.oacc[...] = jnp.zeros_like(refs.oacc)

    def mixer_step(z):
        put_grad(refs, 0, dot(refs.fin_t[...], refs.slow[z]))
        mixer_back(refs, z, T)
        put_grad(refs, 1, dot(refs.min_t[...], refs.dpre[...]))
        copies = send_grad(refs, 0, D, C, refs.got.at[z], refs.gsem.at[0])
        copies += send_grad(refs, 1, D, 3 * C, refs.gmix.at[z], refs.gsem.at[1])
        for c in copies:
            c.start()
        for c in copies:
            c.wait()

    loop(Z, mixer_step)
    norm_back(refs, T)


def layer_ag(tok, cot, fw, iw, cw, ow, uw, dw, mg, fb, ib, fg):
    T, D = tok.shape
    Z, F = 4, 8
    sds = jax.ShapeDtypeStruct
    vm = pl.BlockSpec(memory_space=pltpu.VMEM)
    anyspec = pl.BlockSpec(memory_space=pl.ANY)
    out_shape = (
        sds((T, D), BF16), sds((T, D), BF16),
        sds((Z, D, 3 * C), F32), sds((Z, D, C), F32), sds((F, D, C), F32), sds((F, D, C), F32),
        sds((1, D), F32), sds((1, D), F32), sds((Z, 1, C), F32), sds((Z, 1, C), F32),
    )
    V = pltpu.VMEM
    S = pltpu.SemaphoreType.DMA
    scratch = [
        V((Z, D, 3 * C), BF16), V((Z, D, C), BF16), V((F, D, C), BF16), V((F, D, C), BF16),
        V((1, D), F32), V((1, D), F32), V((Z, 1, C), F32), V((Z, 1, C), F32),
        V((32, 1, LANES), F32), V((1, LANES), F32), V((64, C), BF16), V((64, 2 * C), BF16),
        V((T, D), F32), V((T, D), BF16), V((D, T), BF16), V((T, D), BF16), V((D, T), BF16),
        V((T, D), BF16), V((D, T), BF16), V((T, D), F32), V((T, D), F32), V((T, D), F32),
        V((3 * C // LANES, T, LANES), F32), V((T, C), F32), V((T, C), F32),
        V((T, C), BF16), V((T, C), BF16),
        V((T, 3 * C), BF16), V((Z, T, C), BF16), V((Z, T + SUB, C), F32),
        V((Z, T, C), F32), V((Z, T, C), F32), V((Z, T, C), F32), V((Z, T, C), F32),
        S((2, 6)),
        S((7,)), S((3,)), S((3,)), S((4,)), S((4,)), S((4,)),
        S((4,)), S((4,)), S(()), S(()), S((3, 3)), S((3, 4)),
        S((3, 4)), S((3, 4)), S((3, 4, 2)), S((3, 4, 2)), S((3, 4)), S((3, 4)),
    ]
    return pl.pallas_call(
        layer_ag_kernel,
        out_shape=out_shape,
        in_specs=[vm] * 12,
        out_specs=(vm, vm, anyspec, anyspec, anyspec, anyspec, vm, vm, vm, vm),
        scratch_shapes=scratch,
        compiler_params=pltpu.CompilerParams(
            vmem_limit_bytes=67043328, collective_id=0, has_side_effects=True
        ),
        name="layer_ag",
    )(tok, cot, fw, iw, cw, ow, uw, dw, mg, fb, ib, fg)


TINY = 1e-30
CLIP = 0.01


def gathered_layer(tok, cot, mix, ow, uw, dw, mg, fb, ib, fg):
    def whole(w):
        w = lax.all_gather(w, "inner", axis=1, tiled=True)
        return lax.all_gather(w, "grp", axis=0, tiled=True)

    def vec(v):
        return lax.all_gather(v, ("grp", "inner"), axis=0, tiled=True).astype(F32)

    width = tok.shape[1]
    inners = lax.axis_size("inner")
    Z, F = mix[0].shape[1] * inners // C, uw.shape[1] * inners // C
    gates = [whole(w).reshape(width, Z, C // LANES, 1, LANES) for w in mix]
    wmix = jnp.concatenate(gates, axis=3).reshape(width, Z, 3 * C).transpose(1, 0, 2)
    wot = whole(ow).reshape(Z, C, width).transpose(0, 2, 1)
    wup = whole(uw).reshape(width, F, C).transpose(1, 0, 2)
    wdt = whole(dw).reshape(F, C, width).transpose(0, 2, 1)
    return layer(
        tok, cot, wmix, wot, wup, wdt,
        vec(mg).reshape(1, width), vec(fg).reshape(1, width),
        vec(fb).reshape(Z, 1, C), vec(ib).reshape(Z, 1, C),
    )


def body(
    tokens,
    cotangent,
    mixer_gain,
    forget_weight,
    input_gate_weight,
    candidate_weight,
    forget_bias,
    input_bias,
    output_weight,
    feed_norm_gain,
    up_weight,
    down_weight,
    mixer_second,
    forget_rows,
    forget_columns,
    input_rows,
    input_columns,
    candidate_rows,
    candidate_columns,
    forget_second,
    input_second,
    output_rows,
    output_columns,
    feed_second,
    up_rows,
    up_columns,
    down_rows,
    down_columns,
):
    groups = lax.axis_size("grp")
    inners = lax.axis_size("inner")
    seqs, length, width = tokens.shape
    paired = (groups, inners) == (4, 8) and (length, width) == (1024, 512)
    hidden = forget_weight.shape[1] * inners
    ff = up_weight.shape[1] * inners
    Z, F = hidden // C, ff // C
    if paired:
        results = layer_ag(
            tokens.reshape(length, width), cotangent.reshape(length, width),
            forget_weight, input_gate_weight, candidate_weight,
            output_weight, up_weight, down_weight,
            mixer_gain, forget_bias, input_bias, feed_norm_gain,
        )
    else:
        results = gathered_layer(
            tokens.reshape(length, width), cotangent.reshape(length, width),
            (forget_weight, input_gate_weight, candidate_weight),
            output_weight, up_weight, down_weight,
            mixer_gain, forget_bias, input_bias, feed_norm_gain,
        )
    block_output, tokens_grad, gmix, got, gup, gdt, fgg, mgg, fbg, ibg = results
    block_output = block_output.reshape(tokens.shape)
    tokens_grad = tokens_grad.reshape(tokens.shape)
    split = gmix.transpose(1, 0, 2).reshape(width, Z, C // LANES, 3, LANES)
    forget_term, input_term, cand_term = [
        split[:, :, :, k].reshape(width, hidden) for k in range(3)
    ]
    output_term = got.transpose(0, 2, 1).reshape(hidden, width)
    up_term = gup.transpose(1, 0, 2).reshape(width, ff)
    down_term = gdt.transpose(0, 2, 1).reshape(ff, width)
    gain_first_term, gain_second_term = mgg.reshape(-1), fgg.reshape(-1)
    fbias_term, ibias_term = fbg.reshape(-1), ibg.reshape(-1)
    part = (
        lax.psum_scatter(
            gain_first_term.reshape(groups, -1), "inner", scatter_dimension=1, tiled=True
        ),
        lax.psum_scatter(forget_term, "inner", scatter_dimension=1, tiled=True),
        lax.psum_scatter(input_term, "inner", scatter_dimension=1, tiled=True),
        lax.psum_scatter(cand_term, "inner", scatter_dimension=1, tiled=True),
        lax.psum_scatter(fbias_term.reshape(groups, -1), "inner", scatter_dimension=1, tiled=True),
        lax.psum_scatter(ibias_term.reshape(groups, -1), "inner", scatter_dimension=1, tiled=True),
        lax.psum_scatter(output_term, "inner", scatter_dimension=1, tiled=True),
        lax.psum_scatter(
            gain_second_term.reshape(groups, -1), "inner", scatter_dimension=1, tiled=True
        ),
        lax.psum_scatter(up_term, "inner", scatter_dimension=1, tiled=True),
        lax.psum_scatter(down_term, "inner", scatter_dimension=1, tiled=True),
    )
    mine = (
        lax.psum_scatter(part[0], "grp", scatter_dimension=0, tiled=True),
        lax.psum_scatter(part[1], "grp", scatter_dimension=0, tiled=True),
        lax.psum_scatter(part[2], "grp", scatter_dimension=0, tiled=True),
        lax.psum_scatter(part[3], "grp", scatter_dimension=0, tiled=True),
        lax.psum_scatter(part[4], "grp", scatter_dimension=0, tiled=True),
        lax.psum_scatter(part[5], "grp", scatter_dimension=0, tiled=True),
        lax.psum_scatter(part[6], "grp", scatter_dimension=0, tiled=True),
        lax.psum_scatter(part[7], "grp", scatter_dimension=0, tiled=True),
        lax.psum_scatter(part[8], "grp", scatter_dimension=0, tiled=True),
        lax.psum_scatter(part[9], "grp", scatter_dimension=0, tiled=True),
    )
    params = [
        mixer_gain,
        forget_weight,
        input_gate_weight,
        candidate_weight,
        forget_bias,
        input_bias,
        output_weight,
        feed_norm_gain,
        up_weight,
        down_weight,
    ]
    locals_f = [p.astype(jnp.float32) for p in params]
    grads = [
        mine[0].reshape(-1),
        mine[1],
        mine[2],
        mine[3],
        mine[4].reshape(-1),
        mine[5].reshape(-1),
        mine[6],
        mine[7].reshape(-1),
        mine[8],
        mine[9],
    ]
    matrix_slots = [1, 2, 3, 6, 8, 9]
    vector_slots = [0, 4, 5, 7]
    rows_old = [forget_rows, input_rows, candidate_rows, output_rows, up_rows, down_rows]
    columns_old = [
        forget_columns,
        input_columns,
        candidate_columns,
        output_columns,
        up_columns,
        down_columns,
    ]
    seconds_old = [mixer_second, forget_second, input_second, feed_second]
    counts = [params[k].size * groups * inners for k in range(10)]
    first_inner = (lax.axis_index("inner") == 0).astype(jnp.float32)
    scales = lax.psum(
        jnp.stack(
            [jnp.sum(w * w) for w in locals_f] + [jnp.sum(r) * first_inner for r in rows_old]
        ),
        ("grp", "inner"),
    )
    mats = [grads[k] for k in matrix_slots]
    row_parts = [jnp.sum(g * g, axis=1) for g in mats]
    column_parts = [jnp.sum(g * g, axis=0) for g in mats]
    row_totals = lax.psum(
        (row_parts[0], row_parts[1], row_parts[2], row_parts[3], row_parts[4], row_parts[5]),
        "inner",
    )
    column_totals = lax.psum(
        (
            column_parts[0],
            column_parts[1],
            column_parts[2],
            column_parts[3],
            column_parts[4],
            column_parts[5],
        ),
        "grp",
    )
    grand = lax.psum(jnp.stack([jnp.sum(v) for v in row_totals]), "grp")
    scaled_all = [None] * 10
    new_states = [None] * 16
    state_places = {1: (1, 2), 2: (3, 4), 3: (5, 6), 6: (9, 10), 8: (12, 13), 9: (14, 15)}
    second_places = {0: 0, 4: 7, 5: 8, 7: 11}
    for k in range(6):
        slot = matrix_slots[k]
        grad = mats[k]
        full_rows = grad.shape[0] * groups
        full_columns = grad.shape[1] * inners
        rows = 0.5 * rows_old[k] + 0.5 * (row_totals[k] / full_columns + TINY)
        columns = 0.5 * columns_old[k] + 0.5 * (column_totals[k] / full_rows + TINY)
        row_mean = 0.5 * scales[10 + k] / full_rows + 0.5 * (
            grand[k] / (full_rows * full_columns) + TINY
        )
        scaled_all[slot] = grad * lax.rsqrt(rows[:, None] * columns[None, :] / row_mean)
        new_states[state_places[slot][0]] = rows
        new_states[state_places[slot][1]] = columns
    for k in range(4):
        slot = vector_slots[k]
        grad = grads[slot]
        second = 0.5 * seconds_old[k] + 0.5 * (grad * grad + TINY)
        scaled_all[slot] = grad * lax.rsqrt(second)
        new_states[second_places[slot]] = second
    clip = lax.psum(jnp.stack([jnp.sum(s * s) for s in scaled_all]), ("grp", "inner"))
    count_array = jnp.array(counts, jnp.float32)
    update_norms = jnp.sqrt(clip / count_array)
    fresh = [
        locals_f[k]
        + -jnp.sqrt(scales[k] / counts[k]) * scaled_all[k] / jnp.maximum(CLIP, update_norms[k])
        for k in range(10)
    ]
    return (
        block_output,
        tokens_grad,
        grads[0],
        grads[1],
        grads[2],
        grads[3],
        grads[4],
        grads[5],
        grads[6],
        grads[7],
        grads[8],
        grads[9],
        fresh[0],
        fresh[1],
        fresh[2],
        fresh[3],
        fresh[4],
        fresh[5],
        fresh[6],
        fresh[7],
        fresh[8],
        fresh[9],
        new_states[0],
        new_states[1],
        new_states[2],
        new_states[3],
        new_states[4],
        new_states[5],
        new_states[6],
        new_states[7],
        new_states[8],
        new_states[9],
        new_states[10],
        new_states[11],
        new_states[12],
        new_states[13],
        new_states[14],
        new_states[15],
        update_norms,
    )


def solution(mesh):
    return jax.shard_map(
        body,
        mesh=mesh,
        in_specs=(
            P(("grp", "inner"), None, None),
            P(("grp", "inner"), None, None),
            P(("grp", "inner")),
            P("grp", "inner"),
            P("grp", "inner"),
            P("grp", "inner"),
            P(("grp", "inner")),
            P(("grp", "inner")),
            P("grp", "inner"),
            P(("grp", "inner")),
            P("grp", "inner"),
            P("grp", "inner"),
            P(("grp", "inner")),
            P("grp"),
            P("inner"),
            P("grp"),
            P("inner"),
            P("grp"),
            P("inner"),
            P(("grp", "inner")),
            P(("grp", "inner")),
            P("grp"),
            P("inner"),
            P(("grp", "inner")),
            P("grp"),
            P("inner"),
            P("grp"),
            P("inner"),
        ),
        out_specs=(
            P(("grp", "inner"), None, None),
            P(("grp", "inner"), None, None),
            P(("grp", "inner")),
            P("grp", "inner"),
            P("grp", "inner"),
            P("grp", "inner"),
            P(("grp", "inner")),
            P(("grp", "inner")),
            P("grp", "inner"),
            P(("grp", "inner")),
            P("grp", "inner"),
            P("grp", "inner"),
            P(("grp", "inner")),
            P("grp", "inner"),
            P("grp", "inner"),
            P("grp", "inner"),
            P(("grp", "inner")),
            P(("grp", "inner")),
            P("grp", "inner"),
            P(("grp", "inner")),
            P("grp", "inner"),
            P("grp", "inner"),
            P(("grp", "inner")),
            P("grp"),
            P("inner"),
            P("grp"),
            P("inner"),
            P("grp"),
            P("inner"),
            P(("grp", "inner")),
            P(("grp", "inner")),
            P("grp"),
            P("inner"),
            P(("grp", "inner")),
            P("grp"),
            P("inner"),
            P("grp"),
            P("inner"),
            P(),
        ),
        check_vma=False,
    )
```

```python
import functools
import math
import jax
import jax.numpy as jnp
from jax import lax
from jax.experimental import pallas as pl
from jax.sharding import PartitionSpec as P
from jax.experimental.pallas import tpu as pltpu

EPS = 1e-06
F32 = jnp.float32
BF16 = jnp.bfloat16
C = 256
LANES = 128
SUB = 8
ERFC = (
    0.2256758669, 0.2256693636, 0.2078460312, 0.1685204197, 0.1415057621,
    -0.005753053848, 0.1692475449, -0.182997133, 0.05028532412,
)


def dot(a, b):
    return jnp.dot(a, b, preferred_element_type=F32)


def dot_t(a, b):
    return lax.dot_general(a, b, (((1,), (1,)), ((), ())), preferred_element_type=F32)


def loop(steps, body):
    def run(i, carry):
        body(i)
        return carry

    lax.fori_loop(0, steps, run, 0)


def at(i, size):
    return pl.ds(pl.multiple_of(i * size, size), size)


def gelu_parts(x):
    ax = jnp.abs(x)
    e = jnp.exp(-0.5 * (x * x))
    t = 1.0 / (1.0 + (0.4 * math.sqrt(0.5)) * ax)
    poly = jnp.full_like(t, ERFC[-1])
    for c in ERFC[-2::-1]:
        poly = poly * t + c
    half = 0.5 * (poly * t * e)
    cdf = jnp.where(x >= 0, 1.0 - half, half)
    return x * cdf, cdf + (x * e) * (1.0 / math.sqrt(2.0 * math.pi))


def strided(ref, j, n):
    return ref[pl.ds(j, SUB, stride=n), :]

def gather_rows(tmp, j0, n, D):
    columns = [
        jnp.concatenate([tmp[q, pl.ds(j0 + jj, SUB, stride=n), :] for jj in range(16)], axis=0)
        for q in range(D // LANES)
    ]
    return jnp.concatenate(columns, axis=1)


def scatter_rows(tmp, j0, n, out):
    for q in range(out.shape[1] // LANES):
        for jj in range(16):
            tmp[q, pl.ds(j0 + jj, SUB, stride=n), :] = out[
                jj * SUB : (jj + 1) * SUB, q * LANES : (q + 1) * LANES
            ]


def norm_in(refs, T):
    n = T // SUB
    tmp, xf, g1 = refs.pre, refs.xf, refs.g1
    D = xf.shape[1]

    def widen(i):
        rows = at(i, LANES)
        wide = refs.tok[rows, :].astype(F32)
        for q in range(D // LANES):
            tmp[q, rows, :] = wide[:, q * LANES : (q + 1) * LANES]

    loop(T // LANES, widen)

    def place(i):
        x = gather_rows(tmp, i * 16, n, D)
        y = x * lax.rsqrt(jnp.mean(x * x, axis=-1, keepdims=True) + EPS) * g1[...]
        rows = at(i, LANES)
        xf[rows, :] = x
        refs.min[rows, :] = y.astype(BF16)
        refs.min_t[:, rows] = y.T.astype(BF16)

    loop(T // LANES, place)


def cot_in(refs, T):
    n = T // SUB
    tmp = refs.pre
    D = refs.xf.shape[1]

    def widen(i):
        rows = at(i, LANES)
        wide = refs.cot[rows, :].astype(F32)
        for q in range(D // LANES):
            tmp[q, rows, :] = wide[:, q * LANES : (q + 1) * LANES]

    loop(T // LANES, widen)

    def place(i):
        x = gather_rows(tmp, i * 16, n, D)
        rows = at(i, LANES)
        refs.cot_p[rows, :] = x.astype(BF16)
        refs.cot_t[:, rows] = x.T.astype(BF16)

    loop(T // LANES, place)


def mixer_forward(refs, z, T):
    pre, ac, st = refs.pre, refs.buf_a, refs.st
    halves = C // LANES
    width = 3 * LANES

    def project(i):
        rows = at(i, 256)
        out = dot(refs.min[rows, :], refs.wmix[z])
        for q in range(3 * halves):
            pre[q, rows, :] = out[:, q * LANES : (q + 1) * LANES]

    loop(T // 256, project)
    fb = refs.fb[z]
    ib = refs.ib[z]

    def gates(i, carry):
        r0 = pl.multiple_of(i * 64, 64)
        out = []
        for h in range(halves):
            a, b = carry[h]
            lanes = slice(h * LANES, (h + 1) * LANES)
            pf = pre[3 * h, pl.ds(r0, 64), :] + fb[:, lanes]
            pi = pre[3 * h + 1, pl.ds(r0, 64), :] + ib[:, lanes]
            pc = pre[3 * h + 2, pl.ds(r0, 64), :]
            m = jnp.minimum(jnp.minimum(pf, pi), 0.0)
            e0 = jnp.exp(m)
            ef = jnp.exp(m - pf)
            ei = jnp.exp(m - pi)
            nk = e0 + ei
            na = e0 + ef
            inv = 1.0 / (nk + na)
            keep = nk * inv
            admit = na * inv
            not_f = 1.0 / (1.0 + jnp.exp(pf))
            not_i = 1.0 / (1.0 + jnp.exp(pi))
            ec = jnp.exp(jnp.minimum(pc, 0.0))
            sg = ec / (1.0 + ec)
            positive = pc >= 0
            value = jnp.where(positive, pc + 0.5, sg)
            slope = jnp.where(positive, 1.0, sg * (1.0 - sg))
            refs.keep[z, pl.ds(r0, 64), lanes] = keep
            refs.k_f[z, pl.ds(r0, 64), lanes] = keep * not_f
            refs.k_i[z, pl.ds(r0, 64), lanes] = keep * not_i
            refs.k_c[z, pl.ds(r0, 64), lanes] = admit * slope
            inflow = admit * value
            alist, blist = [], []
            for j in range(8):
                kj = keep[j * SUB : (j + 1) * SUB]
                b = kj * b + inflow[j * SUB : (j + 1) * SUB]
                a = kj * a
                alist.append(a)
                blist.append(b)
            ac[pl.ds(r0, 64), lanes] = jnp.concatenate(alist, axis=0)
            st[z, pl.ds(r0 + SUB, 64), lanes] = jnp.concatenate(blist, axis=0)
            out.append((a, b))
        return tuple(out)

    one = jnp.ones((SUB, LANES), F32)
    zero = jnp.zeros((SUB, LANES), F32)
    ends = lax.fori_loop(0, T // 64, gates, tuple((one, zero) for _ in range(halves)))
    for h in range(halves):
        a, b = ends[h]
        rows = [jnp.zeros((1, LANES), F32)]
        for s in range(SUB - 1):
            rows.append(a[s : s + 1] * rows[-1] + b[s : s + 1])
        st[z, 0:SUB, h * LANES : (h + 1) * LANES] = jnp.concatenate(rows, axis=0)
    first = st[z, 0:SUB, :]

    def finish(i):
        r0 = pl.multiple_of(i * 64, 64)
        a = ac[pl.ds(r0, 64), :].reshape(8, SUB, C)
        b = st[z, pl.ds(r0 + SUB, 64), :].reshape(8, SUB, C)
        s = (b + a * first[None]).reshape(64, C)
        st[z, pl.ds(r0 + SUB, 64), :] = s
        refs.slow[z, pl.ds(r0, 64), :] = s.astype(BF16)

    loop(T // 64, finish)


def mix_out(refs, T):
    Z = refs.wot.shape[0]

    def body(i):
        rows = at(i, 256)
        acc = refs.xf[rows, :]
        for z in range(Z):
            acc = acc + dot_t(refs.slow[z, rows, :], refs.wot[z])
        refs.resid[rows, :] = acc
        for k in range(2):
            x = acc[k * LANES : (k + 1) * LANES]
            y = x * lax.rsqrt(jnp.mean(x * x, axis=-1, keepdims=True) + EPS) * refs.g2[...]
            sub = pl.ds(pl.multiple_of(i * 256 + k * LANES, LANES), LANES)
            refs.fin[sub, :] = y.astype(BF16)
            refs.fin_t[:, sub] = y.T.astype(BF16)

    loop(T // 256, body)


def feed(refs, f, T):
    wup, wdt = refs.wup, refs.wdt

    def body(i):
        rows = at(i, 256)
        refs.buf_a[rows, :] = dot(refs.fin[rows, :], wup[f])
        refs.buf_b[rows, :] = dot(refs.cot_p[rows, :], wdt[f])
        for k in range(4):
            sub = pl.ds(pl.multiple_of(i * 256 + k * 64, 64), 64)
            act, slope = gelu_parts(refs.buf_a[sub, :])
            refs.act[sub, :] = act.astype(BF16)
            refs.dup[sub, :] = (refs.buf_b[sub, :] * slope).astype(BF16)
        refs.oacc[rows, :] += dot_t(refs.act[rows, :], wdt[f])
        refs.dfe[rows, :] += dot_t(refs.dup[rows, :], wup[f])

    loop(T // 256, body)


def feed_back(refs, T):
    n = T // SUB
    tmp = refs.pre
    D = refs.xf.shape[1]

    def body(i, total):
        rows = at(i, LANES)
        x = refs.resid[rows, :]
        df = refs.dfe[rows, :]
        out = x + refs.oacc[rows, :]
        scatter_rows(tmp, i * 16, n, out)
        r = lax.rsqrt(jnp.mean(x * x, axis=-1, keepdims=True) + EPS)
        nrm = x * r
        dn = df * refs.g2[...]
        mean = jnp.mean(dn * nrm, axis=-1, keepdims=True)
        dres = refs.cot_p[rows, :].astype(F32) + r * (dn - nrm * mean)
        refs.dfe[rows, :] = dres
        refs.fin[rows, :] = dres.astype(BF16)
        refs.fin_t[:, rows] = dres.T.astype(BF16)
        return total + (df * nrm).reshape(16, SUB, D).sum(axis=0)

    total = lax.fori_loop(0, T // LANES, body, jnp.zeros((SUB, D), F32))
    refs.fgg[...] = jnp.sum(total, axis=0, keepdims=True)

    def emit(i):
        rows = at(i, LANES)
        for q in range(D // LANES):
            refs.block[rows, q * LANES : (q + 1) * LANES] = tmp[q, rows, :].astype(BF16)

    loop(T // LANES, emit)


def mixer_back(refs, z, T):
    ds, dc, st = refs.buf_a, refs.buf_b, refs.st
    halves = C // LANES
    width = 3 * LANES

    def project(i):
        rows = at(i, 256)
        ds[rows, :] = dot(refs.fin[rows, :], refs.wot[z])

    loop(T // 256, project)
    steps = T // 64

    def local(i, carry):
        r0 = pl.multiple_of((steps - 1 - i) * 64, 64)
        d = ds[pl.ds(r0, 64), :]
        k = refs.keep[z, pl.ds(r0, 64), :]
        e, dk = carry
        plist, dlist = [None] * 8, [None] * 8
        for j in range(7, -1, -1):
            kj = k[j * SUB : (j + 1) * SUB]
            p = d[j * SUB : (j + 1) * SUB] + e
            plist[j] = p
            dlist[j] = dk
            e = kj * p
            dk = kj * dk
        ds[pl.ds(r0, 64), :] = jnp.concatenate(plist, axis=0)
        dc[pl.ds(r0, 64), :] = jnp.concatenate(dlist, axis=0)
        return e, dk

    e, dk = lax.fori_loop(0, steps, local, (jnp.zeros((SUB, C), F32), jnp.ones((SUB, C), F32)))
    rows = [jnp.zeros((1, C), F32)]
    for s in range(SUB - 1, 0, -1):
        rows.insert(0, e[s : s + 1] + dk[s : s + 1] * rows[0])
    tail = jnp.concatenate(rows, axis=0)

    def grads(i, sums):
        r0 = pl.multiple_of(i * 64, 64)
        out = []
        for h in range(halves):
            lanes = slice(h * LANES, (h + 1) * LANES)
            sub = pl.ds(r0, 64)
            p0 = ds[sub, lanes].reshape(8, SUB, LANES)
            d0 = dc[sub, lanes].reshape(8, SUB, LANES)
            p = (p0 + d0 * tail[None, :, lanes]).reshape(64, LANES)
            x = p * (st[z, pl.ds(r0 + SUB, 64), lanes] - st[z, sub, lanes])
            df = -(refs.k_f[z, sub, lanes] * x)
            di = refs.k_i[z, sub, lanes] * x
            dcand = refs.k_c[z, sub, lanes] * p
            df16 = df.astype(BF16)
            di16 = di.astype(BF16)
            refs.dpre[sub, h * width : h * width + LANES] = df16
            refs.dpre[sub, h * width + LANES : h * width + 2 * LANES] = di16
            refs.dpre[sub, h * width + 2 * LANES : h * width + 3 * LANES] = dcand.astype(BF16)
            sf, si = sums[h]
            out.append(
                (
                    sf + df16.astype(F32).reshape(8, SUB, LANES).sum(axis=0),
                    si + di16.astype(F32).reshape(8, SUB, LANES).sum(axis=0),
                )
            )
        return tuple(out)

    zero = jnp.zeros((SUB, LANES), F32)
    sums = lax.fori_loop(0, T // 64, grads, tuple((zero, zero) for _ in range(halves)))
    for h in range(halves):
        lanes = slice(h * LANES, (h + 1) * LANES)
        refs.fbg[z, :, lanes] = jnp.sum(sums[h][0], axis=0, keepdims=True)
        refs.ibg[z, :, lanes] = jnp.sum(sums[h][1], axis=0, keepdims=True)

    def back(i):
        rows = at(i, 256)
        refs.oacc[rows, :] += dot_t(refs.dpre[rows, :], refs.wmix[z])

    loop(T // 256, back)


def norm_back(refs, T):
    n = T // SUB
    tmp = refs.pre
    D = refs.xf.shape[1]

    def body(i, total):
        rows = at(i, LANES)
        x = refs.xf[rows, :]
        d_in = refs.oacc[rows, :]
        r = lax.rsqrt(jnp.mean(x * x, axis=-1, keepdims=True) + EPS)
        nrm = x * r
        dn = d_in * refs.g1[...]
        mean = jnp.mean(dn * nrm, axis=-1, keepdims=True)
        out = refs.dfe[rows, :] + r * (dn - nrm * mean)
        scatter_rows(tmp, i * 16, n, out)
        return total + (d_in * nrm).reshape(16, SUB, D).sum(axis=0)

    total = lax.fori_loop(0, T // LANES, body, jnp.zeros((SUB, D), F32))
    refs.mgg[...] = jnp.sum(total, axis=0, keepdims=True)

    def emit(i):
        rows = at(i, LANES)
        for q in range(D // LANES):
            refs.tgrad[rows, q * LANES : (q + 1) * LANES] = tmp[q, rows, :].astype(BF16)

    loop(T // LANES, emit)

class Refs:
    def __init__(self, args):
        (
            self.tok, self.cot, self.wmix, self.wot, self.wup, self.wdt, self.g1, self.g2, self.fb, self.ib,
            self.block, self.tgrad, self.gmix, self.got, self.gup, self.gdt, self.fgg, self.mgg, self.fbg, self.ibg,
            self.xf, self.min, self.min_t, self.fin, self.fin_t, self.cot_p, self.cot_t, self.resid, self.oacc, self.dfe,
            self.pre, self.buf_a, self.buf_b, self.act, self.dup, self.dpre, self.slow, self.st, self.keep, self.k_f,
            self.k_i, self.k_c, self.gst, self.gsem,
        ) = args


def layer_kernel(*args):
    refs = Refs(args)
    T, D = refs.tok.shape
    Z = refs.wmix.shape[0]
    F = refs.wup.shape[0]
    gst, sem = refs.gst, refs.gsem
    norm_in(refs, T)
    loop(Z, lambda z: mixer_forward(refs, z, T))
    mix_out(refs, T)
    cot_in(refs, T)
    refs.oacc[...] = jnp.zeros_like(refs.oacc)
    refs.dfe[...] = jnp.zeros_like(refs.dfe)

    def feed_step(f):
        feed(refs, f, T)
        gst[0, :, 0:C] = dot(refs.cot_t[...], refs.act[...])
        gst[1, :, 0:C] = dot(refs.fin_t[...], refs.dup[...])
        one = pltpu.make_async_copy(gst.at[0, :, 0:C], refs.gdt.at[f], sem.at[0])
        two = pltpu.make_async_copy(gst.at[1, :, 0:C], refs.gup.at[f], sem.at[1])
        one.start()
        two.start()
        one.wait()
        two.wait()

    loop(F, feed_step)
    feed_back(refs, T)
    refs.oacc[...] = jnp.zeros_like(refs.oacc)

    def mixer_step(z):
        gst[0, :, 0:C] = dot(refs.fin_t[...], refs.slow[z])
        mixer_back(refs, z, T)
        gst[1, :, :] = dot(refs.min_t[...], refs.dpre[...])
        one = pltpu.make_async_copy(gst.at[0, :, 0:C], refs.got.at[z], sem.at[0])
        two = pltpu.make_async_copy(gst.at[1], refs.gmix.at[z], sem.at[1])
        one.start()
        two.start()
        one.wait()
        two.wait()

    loop(Z, mixer_step)
    norm_back(refs, T)


def layer(tok, cot, wmix, wot, wup, wdt, g1, g2, fb, ib):
    T, D = tok.shape
    Z, F = wmix.shape[0], wup.shape[0]
    sds = jax.ShapeDtypeStruct
    vm = pl.BlockSpec(memory_space=pltpu.VMEM)
    anyspec = pl.BlockSpec(memory_space=pl.ANY)
    out_shape = (
        sds((T, D), BF16), sds((T, D), BF16),
        sds((Z, D, 3 * C), F32), sds((Z, D, C), F32), sds((F, D, C), F32), sds((F, D, C), F32),
        sds((1, D), F32), sds((1, D), F32), sds((Z, 1, C), F32), sds((Z, 1, C), F32),
    )
    V = pltpu.VMEM
    scratch = [
        V((T, D), F32), V((T, D), BF16), V((D, T), BF16), V((T, D), BF16), V((D, T), BF16),
        V((T, D), BF16), V((D, T), BF16), V((T, D), F32), V((T, D), F32), V((T, D), F32),
        V((3 * C // LANES, T, LANES), F32), V((T, C), F32), V((T, C), F32), V((T, C), BF16), V((T, C), BF16),
        V((T, 3 * C), BF16), V((Z, T, C), BF16), V((Z, T + SUB, C), F32),
        V((Z, T, C), F32), V((Z, T, C), F32), V((Z, T, C), F32), V((Z, T, C), F32),
        V((2, D, 3 * C), F32), pltpu.SemaphoreType.DMA((2,)),
    ]
    return pl.pallas_call(
        layer_kernel,
        out_shape=out_shape,
        in_specs=[vm] * 10,
        out_specs=(vm, vm, anyspec, anyspec, anyspec, anyspec, vm, vm, vm, vm),
        scratch_shapes=scratch,
        compiler_params=pltpu.CompilerParams(vmem_limit_bytes=67043328),
        name="layer",
    )(tok, cot, wmix, wot, wup, wdt, g1, g2, fb, ib)

MESH = pl.DeviceIdType.MESH


def rcopy(src, dst, send, recv, device):
    return pltpu.make_async_remote_copy(
        src_ref=src, dst_ref=dst, send_sem=send, recv_sem=recv, device_id=device, device_id_type=MESH
    )


class Place:
    def __init__(self):
        self.g = lax.axis_index("grp")
        self.i = lax.axis_index("inner")
        self.y, self.x = self.g // 2, self.g % 2
        self.z, self.c = self.i // 2, self.i % 2
        self.me = self.g * 8 + self.i
        self.partner = (self.g, self.z * 2 + 1 - self.c)

    def flip(self, fx, fy):
        x = (self.x + fx) % 2
        y = (self.y + fy) % 2
        return y * 2 + x

    def near(self, z):
        e = z % 2
        return self.flip(1 - e, e)

    def far(self, z):
        e = z % 2
        return self.flip(e, 1 - e)

    def other(self, k):
        t = (self.me + k) % 32
        return (t // 8, t % 8)


def entry_barrier(place):
    barrier = pltpu.get_barrier_semaphore()

    def greet(k):
        pl.semaphore_signal(barrier, inc=1, device_id=place.other(k + 1), device_id_type=MESH)

    loop(31, greet)
    pl.semaphore_wait(barrier, 31)


def spread(values, start, count, total):
    lane = lax.broadcasted_iota(jnp.int32, (LANES, total), 1)
    row = lax.broadcasted_iota(jnp.int32, (LANES, total), 0)
    sel = jnp.where(row == start + lane % count, 1.0, 0.0).astype(BF16)
    picked = dot(values, sel)
    owner = lax.broadcasted_iota(jnp.int32, picked.shape, 0)
    spot = lax.broadcasted_iota(jnp.int32, picked.shape, 1)
    return jnp.sum(jnp.where(spot // count == owner, picked, 0.0), axis=0, keepdims=True)


def pack_vectors(mg, fb, ib, fg):
    parts = [mg, fb, ib, fg]
    used = sum(p.shape[0] for p in parts)
    rows = [p[...].astype(F32).reshape(1, p.shape[0]) for p in parts]
    return jnp.concatenate(rows + [jnp.zeros((1, LANES - used), F32)], axis=1)


def block_of(refs, a, g, i):
    if a == 0:
        return refs.wot.at[g, at(i, 64), :]
    if a == 1:
        return refs.wup.at[i, at(g, 128), :]
    return refs.wdt.at[pl.ds(2 * g, 2), at(i, 64), :]


def blocks_of(refs, a, i):
    if a == 0:
        return refs.wot.at[:, at(i, 64), :]
    if a == 1:
        return refs.wup.at[i]
    return refs.wdt.at[:, at(i, 64), :]


def mix_column(refs, z, c):
    return refs.wmix.at[z, :, at(c, 384)]


def gather_start(refs, p):
    refs.o16[...] = refs.ow[...].astype(F32).T.astype(BF16)
    refs.d16[...] = refs.dw[...].astype(F32).T.astype(BF16)
    local = []
    for k, w in enumerate((refs.fw, refs.iw, refs.cw)):
        spot = pl.ds(pl.multiple_of(p.c * 384 + k * 128, 128), 128)
        local.append(
            pltpu.make_async_copy(w, refs.wmix.at[p.z, at(p.g, 128), spot], refs.loc_s.at[k])
        )
    local.append(pltpu.make_async_copy(refs.o16, block_of(refs, 0, p.g, p.i), refs.loc_s.at[3]))
    local.append(pltpu.make_async_copy(refs.uw, block_of(refs, 1, p.g, p.i), refs.loc_s.at[4]))
    for k in range(2):
        local.append(
            pltpu.make_async_copy(
                refs.d16.at[:, k * 256 : (k + 1) * 256],
                refs.wdt.at[2 * p.g + k, at(p.i, 64), :],
                refs.loc_s.at[5 + k],
            )
        )
    for c in local:
        c.start()
    row = pack_vectors(refs.mg, refs.fbv, refs.ibv, refs.fg)
    refs.vstage[...] = row
    refs.vecs[p.me] = row
    entry_barrier(p)
    for c in local[:3]:
        c.wait()
    own = refs.wmix.at[p.z, at(p.g, 128), at(p.c, 384)]
    for k in range(1, 4):
        peer = p.flip(k % 2, k // 2)
        rcopy(own, own, refs.mxg_s.at[k - 1], refs.mxg_r.at[k - 1], (peer, p.i)).start()

    def vector(k):
        rcopy(refs.vstage, refs.vecs.at[p.me], refs.vec_s, refs.vec_r, p.other(k + 1)).start()

    loop(31, vector)
    for c in local[3:]:
        c.wait()
    for a in range(3):
        blk = block_of(refs, a, p.g, p.i)
        for k in range(1, 4):
            peer = (p.g, ((p.z + k) % 4) * 2 + p.c)
            rcopy(blk, blk, refs.ffz_s.at[a, k - 1], refs.ffz_r.at[a, p.z], peer).start()


def gather_vectors(refs, p):
    rows = refs.vecs.at[pl.ds(0, 31)]
    rcopy(rows, rows, refs.vec_s, refs.vec_r, p.partner).wait()
    v = refs.vecs[...].reshape(32, LANES).astype(BF16)
    refs.g1[...] = spread(v, 0, 16, 512)
    refs.g2[...] = spread(v, 80, 16, 512)
    fb = spread(v, 16, 32, 1024)
    ib = spread(v, 48, 32, 1024)
    for z in range(4):
        refs.fb[z] = fb[:, z * C : (z + 1) * C]
        refs.ib[z] = ib[:, z * C : (z + 1) * C]


def mix_exchange(refs, p, s):
    def send_partner(z):
        col = mix_column(refs, z, p.c)
        rcopy(col, col, refs.mxp_s.at[z], refs.mxp_r.at[z], p.partner).start()

    def wait_partner(z):
        col = mix_column(refs, z, 1 - p.c)
        rcopy(col, col, refs.mxp_s.at[z], refs.mxp_r.at[z], p.partner).wait_recv()

    def send_up(z):
        col = mix_column(refs, z, p.c)
        rcopy(col, col, refs.mxu_s.at[z], refs.mxz_r.at[z], (p.g, p.i + 2)).start()

    def send_down(z):
        col = mix_column(refs, z, p.c)
        rcopy(col, col, refs.mxd_s.at[z], refs.mxz_r.at[z], (p.g, p.i - 2)).start()

    def wait_line(z):
        col = mix_column(refs, z, p.c)
        rcopy(col, col, refs.mxp_s.at[z], refs.mxz_r.at[z], p.partner).wait_recv()

    @pl.when(s == 0)
    def _():
        for k in range(1, 4):
            peer = p.flip(k % 2, k // 2)
            blk = refs.wmix.at[p.z, at(peer, 128), at(p.c, 384)]
            rcopy(blk, blk, refs.mxg_s.at[k - 1], refs.mxg_r.at[k - 1], (peer, p.i)).wait()

        @pl.when(p.z < 3)
        def _():
            send_up(p.z)

        @pl.when(p.z > 0)
        def _():
            send_down(p.z)

        send_partner(p.z)
        wait_partner(p.z)

    below, above = p.z - s, p.z + s

    @pl.when((s > 0) & (below >= 0))
    def _():
        wait_line(below)

        @pl.when(p.z < 3)
        def _():
            send_up(below)

        send_partner(below)

    @pl.when((s > 0) & (above < 4))
    def _():
        wait_line(above)

        @pl.when(p.z > 0)
        def _():
            send_down(above)

        send_partner(above)

    @pl.when((s > 0) & (below >= 0))
    def _():
        wait_partner(below)

    @pl.when((s > 0) & (above < 4))
    def _():
        wait_partner(above)


def mix_drain(refs, p):
    for z in range(4):
        col = mix_column(refs, z, p.c)
        rcopy(col, col, refs.mxp_s.at[z], refs.mxp_r.at[z], p.partner).wait_send()

        @pl.when((z <= p.z) & (p.z < 3))
        def _():
            rcopy(col, col, refs.mxu_s.at[z], refs.mxz_r.at[z], p.partner).wait_send()

        @pl.when((z >= p.z) & (p.z > 0))
        def _():
            rcopy(col, col, refs.mxd_s.at[z], refs.mxz_r.at[z], p.partner).wait_send()


def feed_second(refs, p):
    for a in range(3):
        for z in range(4):
            blk = block_of(refs, a, p.g, z * 2 + p.c)

            @pl.when(p.z != z)
            def _():
                rcopy(blk, blk, refs.ffp_s.at[a, z], refs.ffz_r.at[a, z], p.partner).wait_recv()

            rcopy(blk, blk, refs.ff2_s.at[a, z], refs.ff2_r.at[a, z], (p.near(z), p.i)).start()


def feed_third(refs, p):
    for a in range(3):
        for z in range(4):
            mine = block_of(refs, a, p.g, z * 2 + p.c)
            near = block_of(refs, a, p.near(z), z * 2 + p.c)
            far = (p.far(z), p.i)
            rcopy(near, near, refs.ff2_s.at[a, z], refs.ff2_r.at[a, z], (p.near(z), p.i)).wait_recv()
            rcopy(mine, mine, refs.ff3_s.at[a, z, 0], refs.ff3_r.at[a, z, 0], far).start()
            rcopy(near, near, refs.ff3_s.at[a, z, 1], refs.ff3_r.at[a, z, 1], far).start()


def feed_fourth(refs, p):
    for a in range(3):
        for z in range(4):
            blk = block_of(refs, a, p.g, z * 2 + p.c)
            far = (p.far(z), p.i)
            for k in range(2):
                rcopy(blk, blk, refs.ff3_s.at[a, z, k], refs.ff3_r.at[a, z, k], far).wait_recv()
            full = blocks_of(refs, a, z * 2 + p.c)
            rcopy(full, full, refs.ffp_s.at[a, z], refs.ffp_r.at[a, z], p.partner).start()


def feed_last(refs, p):
    for a in range(3):
        for z in range(4):
            full = blocks_of(refs, a, z * 2 + 1 - p.c)
            rcopy(full, full, refs.ffp_s.at[a, z], refs.ffp_r.at[a, z], p.partner).wait_recv()


def feed_drain(refs, p):
    for a in range(3):
        for k in range(1, 4):
            blk = block_of(refs, a, p.g, p.i)
            rcopy(blk, blk, refs.ffz_s.at[a, k - 1], refs.ffz_r.at[a, p.z], p.partner).wait_send()
        for z in range(4):
            blk = block_of(refs, a, p.g, z * 2 + p.c)
            rcopy(blk, blk, refs.ff2_s.at[a, z], refs.ff2_r.at[a, z], p.partner).wait_send()
            for k in range(2):
                rcopy(blk, blk, refs.ff3_s.at[a, z, k], refs.ff3_r.at[a, z, k], p.partner).wait_send()
            full = blocks_of(refs, a, z * 2 + p.c)
            rcopy(full, full, refs.ffp_s.at[a, z], refs.ffp_r.at[a, z], p.partner).wait_send()


def slot_chunk(p, s):
    low = jnp.minimum(p.z, 3 - p.z)
    shift = jnp.where(s == 0, 1, jnp.where(s == 1, -1, 0))
    m = s + low * shift
    return jnp.where(p.z < 2, m, 3 - m)


def mixer_slots(refs, p, T):
    def slot(s):
        mix_exchange(refs, p, s)
        mixer_forward(refs, slot_chunk(p, s), T)

        @pl.when(s == 0)
        def _():
            feed_second(refs, p)

        @pl.when(s == 1)
        def _():
            feed_third(refs, p)

        @pl.when(s == 2)
        def _():
            feed_fourth(refs, p)

    loop(4, slot)
    mix_drain(refs, p)
    feed_last(refs, p)
    feed_drain(refs, p)

class GatherRefs:
    def __init__(self, args):
        (
            self.tok, self.cot, self.fw, self.iw, self.cw, self.ow, self.uw, self.dw,
            self.mg, self.fbv, self.ibv, self.fg,
            self.block, self.tgrad, self.gmix, self.got, self.gup, self.gdt,
            self.fgg, self.mgg, self.fbg, self.ibg,
            self.wmix, self.wot, self.wup, self.wdt, self.g1, self.g2, self.fb, self.ib,
            self.vecs, self.vstage, self.o16, self.d16,
            self.xf, self.min, self.min_t, self.fin, self.fin_t, self.cot_p, self.cot_t,
            self.resid, self.oacc, self.dfe,
            self.pre, self.buf_a, self.buf_b, self.act, self.dup, self.dpre,
            self.slow, self.st, self.keep, self.k_f, self.k_i, self.k_c, self.gsem,
            self.loc_s, self.mxg_s, self.mxg_r, self.mxu_s, self.mxd_s, self.mxz_r,
            self.mxp_s, self.mxp_r, self.vec_s, self.vec_r, self.ffz_s, self.ffz_r,
            self.ff2_s, self.ff2_r, self.ff3_s, self.ff3_r, self.ffp_s, self.ffp_r,
        ) = args


def grad_slot(refs, k, D):
    return refs.pre.at[:, k * D : (k + 1) * D, :]


def put_grad(refs, k, value):
    D = value.shape[0]
    for q in range(value.shape[1] // LANES):
        refs.pre[q, k * D : (k + 1) * D, :] = value[:, q * LANES : (q + 1) * LANES]


def send_grad(refs, k, D, width, out, sem):
    return [
        pltpu.make_async_copy(
            refs.pre.at[q, k * D : (k + 1) * D, :],
            out.at[:, q * LANES : (q + 1) * LANES],
            sem.at[q],
        )
        for q in range(width // LANES)
    ]


def layer_ag_kernel(*args):
    refs = GatherRefs(args)
    T, D = refs.tok.shape
    Z = refs.wmix.shape[0]
    F = refs.wup.shape[0]
    p = Place()
    gather_start(refs, p)
    cot_in(refs, T)
    gather_vectors(refs, p)
    norm_in(refs, T)
    mixer_slots(refs, p, T)
    mix_out(refs, T)
    refs.oacc[...] = jnp.zeros_like(refs.oacc)
    refs.dfe[...] = jnp.zeros_like(refs.dfe)

    def feed_step(f):
        feed(refs, f, T)
        put_grad(refs, 0, dot(refs.cot_t[...], refs.act[...]))
        put_grad(refs, 1, dot(refs.fin_t[...], refs.dup[...]))
        copies = send_grad(refs, 0, D, C, refs.gdt.at[f], refs.gsem.at[0])
        copies += send_grad(refs, 1, D, C, refs.gup.at[f], refs.gsem.at[1])
        for c in copies:
            c.start()
        for c in copies:
            c.wait()

    loop(F, feed_step)
    feed_back(refs, T)
    refs.oacc[...] = jnp.zeros_like(refs.oacc)

    def mixer_step(z):
        put_grad(refs, 0, dot(refs.fin_t[...], refs.slow[z]))
        mixer_back(refs, z, T)
        put_grad(refs, 1, dot(refs.min_t[...], refs.dpre[...]))
        copies = send_grad(refs, 0, D, C, refs.got.at[z], refs.gsem.at[0])
        copies += send_grad(refs, 1, D, 3 * C, refs.gmix.at[z], refs.gsem.at[1])
        for c in copies:
            c.start()
        for c in copies:
            c.wait()

    loop(Z, mixer_step)
    norm_back(refs, T)


def layer_ag(tok, cot, fw, iw, cw, ow, uw, dw, mg, fb, ib, fg):
    T, D = tok.shape
    Z, F = 4, 8
    sds = jax.ShapeDtypeStruct
    vm = pl.BlockSpec(memory_space=pltpu.VMEM)
    anyspec = pl.BlockSpec(memory_space=pl.ANY)
    out_shape = (
        sds((T, D), BF16), sds((T, D), BF16),
        sds((Z, D, 3 * C), F32), sds((Z, D, C), F32), sds((F, D, C), F32), sds((F, D, C), F32),
        sds((1, D), F32), sds((1, D), F32), sds((Z, 1, C), F32), sds((Z, 1, C), F32),
    )
    V = pltpu.VMEM
    S = pltpu.SemaphoreType.DMA
    scratch = [
        V((Z, D, 3 * C), BF16), V((Z, D, C), BF16), V((F, D, C), BF16), V((F, D, C), BF16),
        V((1, D), F32), V((1, D), F32), V((Z, 1, C), F32), V((Z, 1, C), F32),
        V((32, 1, LANES), F32), V((1, LANES), F32), V((64, C), BF16), V((64, 2 * C), BF16),
        V((T, D), F32), V((T, D), BF16), V((D, T), BF16), V((T, D), BF16), V((D, T), BF16),
        V((T, D), BF16), V((D, T), BF16), V((T, D), F32), V((T, D), F32), V((T, D), F32),
        V((3 * C // LANES, T, LANES), F32), V((T, C), F32), V((T, C), F32),
        V((T, C), BF16), V((T, C), BF16),
        V((T, 3 * C), BF16), V((Z, T, C), BF16), V((Z, T + SUB, C), F32),
        V((Z, T, C), F32), V((Z, T, C), F32), V((Z, T, C), F32), V((Z, T, C), F32),
        S((2, 6)),
        S((7,)), S((3,)), S((3,)), S((4,)), S((4,)), S((4,)),
        S((4,)), S((4,)), S(()), S(()), S((3, 3)), S((3, 4)),
        S((3, 4)), S((3, 4)), S((3, 4, 2)), S((3, 4, 2)), S((3, 4)), S((3, 4)),
    ]
    return pl.pallas_call(
        layer_ag_kernel,
        out_shape=out_shape,
        in_specs=[vm] * 12,
        out_specs=(vm, vm, anyspec, anyspec, anyspec, anyspec, vm, vm, vm, vm),
        scratch_shapes=scratch,
        compiler_params=pltpu.CompilerParams(
            vmem_limit_bytes=67043328, collective_id=0, has_side_effects=True
        ),
        name="layer_ag",
    )(tok, cot, fw, iw, cw, ow, uw, dw, mg, fb, ib, fg)

SHAPES = ((128, 256), (128, 256), (128, 384), (64, 256))
UP, DOWN, MIX, OUT = 0, 1, 2, 3
TINY = 1e-30
CLIP = 0.01
MATRICES = (
    (512, 1024), (512, 1024), (512, 1024), (1024, 512), (512, 2048), (2048, 512)
)
MATRIX_SLOTS = (1, 2, 3, 6, 8, 9)
VECTORS = ((0, 0, 16), (4, 16, 32), (5, 48, 32), (7, 80, 16))
COUNTS = (512, 524288, 524288, 524288, 1024, 1024, 524288, 512, 1048576, 1048576)


def piece(refs, a, g, z, c):
    i = z * 2 + c
    if a == UP:
        return refs.gup[i, g * 128 : (g + 1) * 128, :]
    if a == DOWN:
        return jnp.concatenate([refs.gdt[2 * g + h, at(i, 64), :] for h in range(2)], axis=0)
    if a == MIX:
        return refs.gmix[z, g * 128 : (g + 1) * 128, at(c, 384)]
    return refs.got[g, at(i, 64), :]


def rs_fill(refs, p, a, z):
    for g in range(4):
        refs.psend[a][z, g] = piece(refs, a, g, z, 1 - p.c).astype(BF16)


def rs_copy(refs, p, stage, a, z):
    if stage == 0:
        src, dst, dev = refs.psend[a].at[z], refs.precv[a].at[z], p.partner
    elif stage == 1:
        src, dst, dev = refs.buf1[a].at[z, 1], refs.r1[a].at[z], (p.near(z), p.i)
    else:
        src, dst, dev = refs.buf2[a].at[z, 1], refs.r2[a].at[z], (p.far(z), p.i)
    return rcopy(src, dst, refs.rs_s.at[stage, a, z], refs.rs_r.at[stage, a, z], dev)


def rs_first(refs, p, a, z):
    rs_copy(refs, p, 0, a, z).wait_recv()
    e = z % 2
    for g in range(4):
        y, x = g // 2, g % 2
        v = piece(refs, a, g, z, p.c) + refs.precv[a][z, g].astype(F32)
        role = (1 - e) * ((x + p.x) % 2) + e * ((y + p.y) % 2)
        refs.buf1[a][z, role, (1 - e) * y + e * x] = v.astype(BF16)


def rs_second(refs, p, a, z):
    rs_copy(refs, p, 1, a, z).wait_recv()
    e = z % 2
    for k in range(2):
        v = refs.buf1[a][z, 0, k].astype(F32) + refs.r1[a][z, k].astype(F32)
        refs.buf2[a][z, (k + (1 - e) * p.y + e * p.x) % 2] = v.astype(BF16)


def rs_line(refs, p, a, z, owner):
    return rcopy(
        refs.buf3[a].at[z], refs.r3[a].at[owner], refs.r3_s.at[a, z], refs.r3_r.at[a, owner],
        (p.g, z * 2 + p.c),
    )


def rs_third(refs, p, a, z):
    rs_copy(refs, p, 2, a, z).wait_recv()
    v = refs.buf2[a][z, 0].astype(F32) + refs.r2[a][z].astype(F32)
    refs.buf3[a][z] = v.astype(BF16)

    @pl.when(z == p.z)
    def _():
        refs.fin[a][...] = v


def rs_third_send(refs, p, a, z):
    @pl.when(z != p.z)
    def _():
        rs_line(refs, p, a, z, p.z).start()


def rs_last(refs, p, a):
    for k in range(1, 4):
        z = (p.z + k) % 4
        rs_line(refs, p, a, z, z).wait_recv()
        refs.fin[a][...] += refs.r3[a][z].astype(F32)


def rs_drain(refs, p):
    def one(z):
        for a in range(4):
            for stage in range(3):
                rs_copy(refs, p, stage, a, z).wait_send()

            @pl.when(z != p.z)
            def _():
                rs_line(refs, p, a, z, p.z).wait_send()

    loop(4, one)


def own_row(x):
    return jnp.sum(x, axis=0, keepdims=True)


def lane_sum(x):
    folded = sum(x[:, k : k + LANES] for k in range(0, x.shape[1], LANES))
    return own_row(folded.T)


def wide(row):
    return jnp.concatenate([row, jnp.zeros((1, LANES - row.shape[1]), F32)], axis=1)


def cut(row):
    return [row[:, k : k + LANES] for k in range(0, row.shape[1], LANES)]


def stand(row):
    return jnp.broadcast_to(row, (LANES, LANES)).T


def scalars(values):
    lane = lax.broadcasted_iota(jnp.int32, (1, LANES), 1)
    out = jnp.zeros((1, LANES), F32)
    for k, v in enumerate(values):
        out = out + jnp.where(lane == k, v, 0.0)
    return out


def total(x):
    return jnp.sum(jnp.sum(x, axis=0, keepdims=True), axis=1, keepdims=True)


def segment(row, start, count):
    lane = lax.broadcasted_iota(jnp.int32, row.shape, 1)
    keep = (lane >= start) & (lane < start + count)
    return jnp.sum(jnp.where(keep, row, 0.0), axis=1, keepdims=True)


def gather_row(term, start, count):
    size = term.shape[1]
    owner = lax.broadcasted_iota(jnp.int32, (32, size), 0)
    spot = lax.broadcasted_iota(jnp.int32, (32, size), 1)
    masked = jnp.where(spot // count == owner, term, 0.0)
    lane = lax.broadcasted_iota(jnp.int32, (LANES, size), 0)
    from_spot = lax.broadcasted_iota(jnp.int32, (LANES, size), 1)
    sel = jnp.where(lane == start + from_spot % count, 1.0, 0.0).astype(BF16)
    out = jnp.zeros((32, LANES), F32)
    for _ in range(3):
        part = masked.astype(BF16)
        out = out + dot_t(part, sel)
        masked = masked - part.astype(F32)
    return out


def parameter_blocks(refs):
    return [
        refs.fw[...].astype(F32), refs.iw[...].astype(F32), refs.cw[...].astype(F32),
        refs.ow[...].astype(F32).T, refs.uw[...].astype(F32), refs.dw[...].astype(F32).T,
    ]


def old_rows(refs):
    rows = []
    for r in (refs.row_f, refs.row_i, refs.row_c, refs.row_o, refs.row_u, refs.row_d):
        rows += cut(r[...].reshape(1, r.shape[0]))
    return rows


def old_columns(refs):
    rows = []
    for r in (refs.col_f, refs.col_i, refs.col_c, refs.col_o, refs.col_u, refs.col_d):
        row = r[...].reshape(1, r.shape[0])
        rows += [wide(row)] if r.shape[0] < LANES else cut(row)
    return rows


ROW_PLACES = ((0, 1), (1, 2), (2, 3), (3, 5), (5, 6), (6, 10))
COLUMN_PLACES = ((0, 1), (1, 2), (2, 3), (3, 4), (4, 6), (6, 7))


def broadcast_row(src, box, send, recv, p):
    def one(k):
        rcopy(src, box.at[p.me], send, recv, p.other(k + 1)).start()

    loop(31, one)


def settle_row(box, send, recv, p):
    rows = box.at[pl.ds(0, 31)]
    rcopy(rows, rows, send, recv, p.partner).wait()


def vector_exchange(refs, p):
    rows = (
        gather_row(refs.mgg[...], 0, 16)
        + gather_row(jnp.concatenate([refs.fbg[z] for z in range(4)], axis=1), 16, 32)
        + gather_row(jnp.concatenate([refs.ibg[z] for z in range(4)], axis=1), 48, 32)
        + gather_row(refs.fgg[...], 80, 16)
    )
    refs.vout[...] = rows.reshape(32, 1, LANES)
    refs.vin[p.me] = refs.vout[p.me]

    def one(k):
        t = (p.me + k + 1) % 32
        rcopy(refs.vout.at[t], refs.vin.at[p.me], refs.vex_s, refs.vex_r, p.other(k + 1)).start()

    loop(31, one)


def gradient_blocks(refs):
    mix = refs.fin[MIX][...]
    down = refs.fin[DOWN][...]
    return [
        mix[:, 0:128], mix[:, 128:256], mix[:, 256:384], refs.fin[OUT][...], refs.fin[UP][...],
        jnp.concatenate([down[0:64], down[64:128]], axis=1),
    ]


def adafactor(refs, p):
    grads = gradient_blocks(refs)
    flipped = (False, False, False, True, False, True)
    row_parts, column_parts, totals = [], [], []
    for grad, flip in zip(grads, flipped):
        sq = grad * grad
        down, across = own_row(sq), lane_sum(sq)
        row_parts += cut(down) if flip else [across]
        column_parts += [wide(across)] if flip else cut(down)
        totals.append(jnp.sum(down, axis=1, keepdims=True))
    refs.rowst[...] = jnp.concatenate(row_parts + [jnp.zeros((6, LANES), F32)], axis=0)
    refs.colst[...] = jnp.concatenate(column_parts + [jnp.zeros((1, LANES), F32)], axis=0)
    weights = parameter_blocks(refs)
    params = pack_vectors(refs.mg, refs.fbv, refs.ibv, refs.fg)
    squares = [None] * 10
    for slot, w in zip(MATRIX_SLOTS, weights):
        squares[slot] = total(w * w)
    for slot, start, count in VECTORS:
        squares[slot] = segment(params * params, start, count)
    rows_old, columns_old = old_rows(refs), old_columns(refs)
    first = jnp.where(p.i == 0, 1.0, 0.0)
    row_sums = [first * total(jnp.concatenate(rows_old[a:b], axis=0)) for a, b in ROW_PLACES]
    refs.scal[...] = scalars(totals + squares + row_sums)
    refs.rowin[p.i] = refs.rowst[...]
    refs.colin[p.g] = refs.colst[...]
    refs.scin[p.me] = refs.scal[...]
    for k in range(1, 8):
        peer = (p.g, (p.i + k) % 8)
        rcopy(
            refs.rowst, refs.rowin.at[p.i], refs.row_s.at[k - 1], refs.row_r.at[k - 1], peer
        ).start()
    for k in range(1, 4):
        peer = ((p.g + k) % 4, p.i)
        rcopy(
            refs.colst, refs.colin.at[p.g], refs.col_s.at[k - 1], refs.col_r.at[k - 1], peer
        ).start()
    broadcast_row(refs.scal, refs.scin, refs.sc_s, refs.sc_r, p)
    vec_rows = refs.vin.at[pl.ds(0, 31)]
    rcopy(vec_rows, vec_rows, refs.vex_s, refs.vex_r, p.partner).wait()
    vector_grad = jnp.sum(refs.vin[...].reshape(32, LANES), axis=0, keepdims=True)
    seconds = pack_vectors(refs.sec_m, refs.sec_f, refs.sec_i, refs.sec_g)
    second = 0.5 * seconds + 0.5 * (vector_grad * vector_grad + TINY)
    vector_scaled = vector_grad * lax.rsqrt(second)
    for k in range(1, 8):
        rcopy(
            refs.rowst, refs.rowin.at[p.i], refs.row_s.at[k - 1], refs.row_r.at[k - 1], p.partner
        ).wait()
    for k in range(1, 4):
        rcopy(
            refs.colst, refs.colin.at[p.g], refs.col_s.at[k - 1], refs.col_r.at[k - 1], p.partner
        ).wait()
    settle_row(refs.scin, refs.sc_s, refs.sc_r, p)
    row_total = sum(refs.rowin[k] for k in range(8))
    column_total = sum(refs.colin[k] for k in range(4))
    sc = jnp.sum(refs.scin[...].reshape(32, LANES), axis=0, keepdims=True)
    rows_new, columns_new, scaled = [], [], []
    for k, (r, c) in enumerate(MATRICES):
        ra, rb = ROW_PLACES[k]
        ca, cb = COLUMN_PLACES[k]
        rows = [
            0.5 * rows_old[j] + 0.5 * (row_total[j : j + 1] / c + TINY) for j in range(ra, rb)
        ]
        columns = [
            0.5 * columns_old[j] + 0.5 * (column_total[j : j + 1] / r + TINY)
            for j in range(ca, cb)
        ]
        mean = 0.5 * sc[:, 16 + k : 17 + k] / r + 0.5 * (sc[:, k : k + 1] / (r * c) + TINY)
        lying, standing = (rows, columns) if flipped[k] else (columns, rows)
        tall = stand(standing[0])[0 : grads[k].shape[0]]
        lying = jnp.concatenate(lying, axis=1)
        tall = jnp.concatenate([tall] * (lying.shape[1] // LANES), axis=1)
        scaled.append(grads[k] * lax.rsqrt(tall * lying / mean))
        rows_new += rows
        columns_new += columns
    refs.rows_out[...] = jnp.concatenate(rows_new + [jnp.zeros((6, LANES), F32)], axis=0)
    refs.columns_out[...] = jnp.concatenate(columns_new + [jnp.zeros((1, LANES), F32)], axis=0)
    clips = [None] * 10
    for slot, s in zip(MATRIX_SLOTS, scaled):
        clips[slot] = total(s * s)
    for slot, start, count in VECTORS:
        clips[slot] = segment(vector_scaled * vector_scaled, start, count)
    refs.clip[...] = scalars(clips)
    refs.clin[p.me] = refs.clip[...]
    broadcast_row(refs.clip, refs.clin, refs.cl_s, refs.cl_r, p)
    settle_row(refs.clin, refs.cl_s, refs.cl_r, p)
    clip = jnp.sum(refs.clin[...].reshape(32, LANES), axis=0, keepdims=True)
    norms = [jnp.sqrt(clip[:, k : k + 1] / COUNTS[k]) for k in range(10)]
    steps = [
        -jnp.sqrt(sc[:, 6 + k : 7 + k] / COUNTS[k]) / jnp.maximum(CLIP, norms[k])
        for k in range(10)
    ]
    fresh = [w + steps[slot] * s for slot, w, s in zip(MATRIX_SLOTS, weights, scaled)]
    refs.grad_mix[...] = refs.fin[MIX][...]
    refs.grad_out[...] = grads[3]
    refs.grad_up[...] = grads[4]
    refs.grad_down[...] = grads[5]
    refs.new_mix[...] = jnp.concatenate(fresh[0:3], axis=1)
    refs.new_out[...] = fresh[3]
    refs.new_up[...] = fresh[4]
    refs.new_down[...] = fresh[5]
    lane = lax.broadcasted_iota(jnp.int32, (1, LANES), 1)
    step_row = jnp.zeros((1, LANES), F32)
    for slot, start, count in VECTORS:
        step_row = step_row + jnp.where((lane >= start) & (lane < start + count), steps[slot], 0.0)
    refs.vectors[...] = jnp.concatenate(
        [vector_grad, params + step_row * vector_scaled, second, scalars(norms)]
        + [jnp.zeros((4, LANES), F32)],
        axis=0,
    )


class ExchangeRefs:
    def __init__(self, args):
        (
            self.gmix, self.got, self.gup, self.gdt, self.fgg, self.mgg, self.fbg, self.ibg,
            self.fw, self.iw, self.cw, self.ow, self.uw, self.dw,
            self.mg, self.fbv, self.ibv, self.fg,
            self.sec_m, self.row_f, self.col_f, self.row_i, self.col_i, self.row_c, self.col_c,
            self.sec_f, self.sec_i, self.row_o, self.col_o, self.sec_g,
            self.row_u, self.col_u, self.row_d, self.col_d,
            self.grad_mix, self.grad_out, self.grad_up, self.grad_down,
            self.new_mix, self.new_out, self.new_up, self.new_down,
            self.vectors, self.rows_out, self.columns_out,
        ) = args[:45]
        rest = list(args[45:])
        take = lambda n: [rest.pop(0) for _ in range(n)]
        self.psend, self.precv, self.buf1, self.r1 = take(4), take(4), take(4), take(4)
        self.buf2, self.r2, self.buf3, self.r3, self.fin = (
            take(4), take(4), take(4), take(4), take(4)
        )
        (
            self.vout, self.vin, self.rowst, self.rowin, self.colst, self.colin,
            self.scal, self.scin, self.clip, self.clin,
            self.rs_s, self.rs_r, self.r3_s, self.r3_r, self.vex_s, self.vex_r,
            self.row_s, self.row_r, self.col_s, self.col_r, self.sc_s, self.sc_r,
            self.cl_s, self.cl_r,
        ) = rest


def exchange_kernel(*args):
    refs = ExchangeRefs(args)
    p = Place()
    entry_barrier(p)
    arrays = (UP, DOWN, OUT, MIX)
    for a in arrays:
        loop(4, lambda z: rs_fill(refs, p, a, z))
        loop(4, lambda z: rs_copy(refs, p, 0, a, z).start())
    vector_exchange(refs, p)
    for a in arrays:
        loop(4, lambda z: rs_first(refs, p, a, z))
        loop(4, lambda z: rs_copy(refs, p, 1, a, z).start())
    for a in arrays:
        loop(4, lambda z: rs_second(refs, p, a, z))
        loop(4, lambda z: rs_copy(refs, p, 2, a, z).start())
    for a in arrays:
        loop(4, lambda z: rs_third(refs, p, a, z))
        loop(4, lambda z: rs_third_send(refs, p, a, z))
    for a in arrays:
        rs_last(refs, p, a)
    rs_drain(refs, p)
    adafactor(refs, p)


def finish_kernel(
    grad_mix, grad_out, grad_up, grad_down, new_mix, new_out, new_up, new_down,
    vectors, rows, columns,
    g_mg, g_f, g_i, g_c, g_fb, g_ib, g_o, g_fg, g_u, g_d,
    n_mg, n_f, n_i, n_c, n_fb, n_ib, n_o, n_fg, n_u, n_d,
    s_m, r_f, c_f, r_i, c_i, r_c, c_c, s_f, s_i, r_o, c_o, s_g, r_u, c_u, r_d, c_d, norms,
):
    for src, outs in ((grad_mix, (g_f, g_i, g_c)), (new_mix, (n_f, n_i, n_c))):
        for k, o in enumerate(outs):
            o[...] = src[:, k * 128 : (k + 1) * 128]
    for src, o in ((grad_out, g_o), (new_out, n_o), (grad_down, g_d), (new_down, n_d)):
        o[...] = src[...].T
    g_u[...] = grad_up[...]
    n_u[...] = new_up[...]
    for row, outs in (
        (0, (g_mg, g_fb, g_ib, g_fg)), (1, (n_mg, n_fb, n_ib, n_fg)), (2, (s_m, s_f, s_i, s_g))
    ):
        for (_, start, count), o in zip(VECTORS, outs):
            o[...] = vectors[row, start : start + count]
    norms[...] = vectors[3, 0:10]
    for src, places, outs in (
        (rows, ROW_PLACES, (r_f, r_i, r_c, r_o, r_u, r_d)),
        (columns, COLUMN_PLACES, (c_f, c_i, c_c, c_o, c_u, c_d)),
    ):
        for (a, b), o in zip(places, outs):
            if b - a == 1:
                o[...] = src[a, 0 : o.shape[0]]
            else:
                for k in range(a, b):
                    o[(k - a) * LANES : (k - a + 1) * LANES] = src[k, :]


def exchange(grads, shards, states):
    sds = jax.ShapeDtypeStruct
    vm = pl.BlockSpec(memory_space=pltpu.VMEM)
    V = pltpu.VMEM
    S = pltpu.SemaphoreType.DMA
    packed = (
        sds((128, 384), F32), sds((64, 256), F32), sds((128, 256), F32), sds((64, 512), F32),
        sds((128, 384), F32), sds((64, 256), F32), sds((128, 256), F32), sds((64, 512), F32),
        sds((8, LANES), F32), sds((16, LANES), F32), sds((8, LANES), F32),
    )
    scratch = (
        [V((4, 4) + s, BF16) for s in SHAPES] * 2
        + [V((4, 2, 2) + s, BF16) for s in SHAPES]
        + [V((4, 2) + s, BF16) for s in SHAPES]
        + [V((4, 2) + s, BF16) for s in SHAPES]
        + [V((4,) + s, BF16) for s in SHAPES] * 3
        + [V(s, F32) for s in SHAPES]
    )
    row = V((1, LANES), F32)
    box = V((32, 1, LANES), F32)
    scratch += [
        box, box, V((16, LANES), F32), V((8, 16, LANES), F32),
        V((8, LANES), F32), V((4, 8, LANES), F32), row, box, row, box,
        S((3, 4, 4)), S((3, 4, 4)), S((4, 4)), S((4, 4)), S(()), S(()),
        S((7,)), S((7,)), S((3,)), S((3,)), S(()), S(()), S(()), S(()),
    ]
    args = (*grads, *shards, *states)
    return pl.pallas_call(
        exchange_kernel,
        out_shape=packed,
        in_specs=[vm] * len(args),
        out_specs=(vm,) * len(packed),
        scratch_shapes=scratch,
        compiler_params=pltpu.CompilerParams(
            vmem_limit_bytes=67043328, collective_id=1, has_side_effects=True
        ),
        name="exchange",
    )(*args)


def finish(packed):
    sds = jax.ShapeDtypeStruct
    f = lambda *s: sds(s, F32)
    block = [f(16), f(128, 128), f(128, 128), f(128, 128), f(32), f(32), f(256, 64), f(16),
             f(128, 256), f(512, 64)]
    states = [f(16), f(128), f(128), f(128), f(128), f(128), f(128), f(32), f(32), f(256), f(64),
              f(16), f(128), f(256), f(512), f(64)]
    outs = tuple(block + block + states + [f(10)])
    vm = pl.BlockSpec(memory_space=pltpu.VMEM)
    return pl.pallas_call(
        finish_kernel,
        out_shape=outs,
        in_specs=[vm] * len(packed),
        out_specs=(vm,) * len(outs),
        name="finish",
    )(*packed)


def gathered_layer(tok, cot, mix, ow, uw, dw, mg, fb, ib, fg):
    def whole(w):
        w = lax.all_gather(w, "inner", axis=1, tiled=True)
        return lax.all_gather(w, "grp", axis=0, tiled=True)

    def vec(v):
        return lax.all_gather(v, ("grp", "inner"), axis=0, tiled=True).astype(F32)

    width = tok.shape[1]
    inners = lax.axis_size("inner")
    Z, F = mix[0].shape[1] * inners // C, uw.shape[1] * inners // C
    gates = [whole(w).reshape(width, Z, C // LANES, 1, LANES) for w in mix]
    wmix = jnp.concatenate(gates, axis=3).reshape(width, Z, 3 * C).transpose(1, 0, 2)
    wot = whole(ow).reshape(Z, C, width).transpose(0, 2, 1)
    wup = whole(uw).reshape(width, F, C).transpose(1, 0, 2)
    wdt = whole(dw).reshape(F, C, width).transpose(0, 2, 1)
    return layer(
        tok, cot, wmix, wot, wup, wdt,
        vec(mg).reshape(1, width), vec(fg).reshape(1, width),
        vec(fb).reshape(Z, 1, C), vec(ib).reshape(Z, 1, C),
    )


def body(
    tokens,
    cotangent,
    mixer_gain,
    forget_weight,
    input_gate_weight,
    candidate_weight,
    forget_bias,
    input_bias,
    output_weight,
    feed_norm_gain,
    up_weight,
    down_weight,
    mixer_second,
    forget_rows,
    forget_columns,
    input_rows,
    input_columns,
    candidate_rows,
    candidate_columns,
    forget_second,
    input_second,
    output_rows,
    output_columns,
    feed_second,
    up_rows,
    up_columns,
    down_rows,
    down_columns,
):
    groups = lax.axis_size("grp")
    inners = lax.axis_size("inner")
    seqs, length, width = tokens.shape
    paired = (groups, inners) == (4, 8) and (length, width) == (1024, 512)
    hidden = forget_weight.shape[1] * inners
    ff = up_weight.shape[1] * inners
    Z, F = hidden // C, ff // C
    if paired:
        results = layer_ag(
            tokens.reshape(length, width), cotangent.reshape(length, width),
            forget_weight, input_gate_weight, candidate_weight,
            output_weight, up_weight, down_weight,
            mixer_gain, forget_bias, input_bias, feed_norm_gain,
        )
    else:
        results = gathered_layer(
            tokens.reshape(length, width), cotangent.reshape(length, width),
            (forget_weight, input_gate_weight, candidate_weight),
            output_weight, up_weight, down_weight,
            mixer_gain, forget_bias, input_bias, feed_norm_gain,
        )
    if paired:
        packed = exchange(
            results[2:],
            (
                forget_weight, input_gate_weight, candidate_weight,
                output_weight, up_weight, down_weight,
                mixer_gain, forget_bias, input_bias, feed_norm_gain,
            ),
            (
                mixer_second, forget_rows, forget_columns, input_rows, input_columns,
                candidate_rows, candidate_columns, forget_second, input_second,
                output_rows, output_columns, feed_second,
                up_rows, up_columns, down_rows, down_columns,
            ),
        )
        return (
            results[0].reshape(tokens.shape), results[1].reshape(tokens.shape), *finish(packed)
        )
    block_output, tokens_grad, gmix, got, gup, gdt, fgg, mgg, fbg, ibg = results
    block_output = block_output.reshape(tokens.shape)
    tokens_grad = tokens_grad.reshape(tokens.shape)
    split = gmix.transpose(1, 0, 2).reshape(width, Z, C // LANES, 3, LANES)
    forget_term, input_term, cand_term = [
        split[:, :, :, k].reshape(width, hidden) for k in range(3)
    ]
    output_term = got.transpose(0, 2, 1).reshape(hidden, width)
    up_term = gup.transpose(1, 0, 2).reshape(width, ff)
    down_term = gdt.transpose(0, 2, 1).reshape(ff, width)
    gain_first_term, gain_second_term = mgg.reshape(-1), fgg.reshape(-1)
    fbias_term, ibias_term = fbg.reshape(-1), ibg.reshape(-1)
    part = (
        lax.psum_scatter(
            gain_first_term.reshape(groups, -1), "inner", scatter_dimension=1, tiled=True
        ),
        lax.psum_scatter(forget_term, "inner", scatter_dimension=1, tiled=True),
        lax.psum_scatter(input_term, "inner", scatter_dimension=1, tiled=True),
        lax.psum_scatter(cand_term, "inner", scatter_dimension=1, tiled=True),
        lax.psum_scatter(fbias_term.reshape(groups, -1), "inner", scatter_dimension=1, tiled=True),
        lax.psum_scatter(ibias_term.reshape(groups, -1), "inner", scatter_dimension=1, tiled=True),
        lax.psum_scatter(output_term, "inner", scatter_dimension=1, tiled=True),
        lax.psum_scatter(
            gain_second_term.reshape(groups, -1), "inner", scatter_dimension=1, tiled=True
        ),
        lax.psum_scatter(up_term, "inner", scatter_dimension=1, tiled=True),
        lax.psum_scatter(down_term, "inner", scatter_dimension=1, tiled=True),
    )
    mine = (
        lax.psum_scatter(part[0], "grp", scatter_dimension=0, tiled=True),
        lax.psum_scatter(part[1], "grp", scatter_dimension=0, tiled=True),
        lax.psum_scatter(part[2], "grp", scatter_dimension=0, tiled=True),
        lax.psum_scatter(part[3], "grp", scatter_dimension=0, tiled=True),
        lax.psum_scatter(part[4], "grp", scatter_dimension=0, tiled=True),
        lax.psum_scatter(part[5], "grp", scatter_dimension=0, tiled=True),
        lax.psum_scatter(part[6], "grp", scatter_dimension=0, tiled=True),
        lax.psum_scatter(part[7], "grp", scatter_dimension=0, tiled=True),
        lax.psum_scatter(part[8], "grp", scatter_dimension=0, tiled=True),
        lax.psum_scatter(part[9], "grp", scatter_dimension=0, tiled=True),
    )
    params = [
        mixer_gain,
        forget_weight,
        input_gate_weight,
        candidate_weight,
        forget_bias,
        input_bias,
        output_weight,
        feed_norm_gain,
        up_weight,
        down_weight,
    ]
    locals_f = [p.astype(jnp.float32) for p in params]
    grads = [
        mine[0].reshape(-1),
        mine[1],
        mine[2],
        mine[3],
        mine[4].reshape(-1),
        mine[5].reshape(-1),
        mine[6],
        mine[7].reshape(-1),
        mine[8],
        mine[9],
    ]
    matrix_slots = [1, 2, 3, 6, 8, 9]
    vector_slots = [0, 4, 5, 7]
    rows_old = [forget_rows, input_rows, candidate_rows, output_rows, up_rows, down_rows]
    columns_old = [
        forget_columns,
        input_columns,
        candidate_columns,
        output_columns,
        up_columns,
        down_columns,
    ]
    seconds_old = [mixer_second, forget_second, input_second, feed_second]
    counts = [params[k].size * groups * inners for k in range(10)]
    first_inner = (lax.axis_index("inner") == 0).astype(jnp.float32)
    scales = lax.psum(
        jnp.stack(
            [jnp.sum(w * w) for w in locals_f] + [jnp.sum(r) * first_inner for r in rows_old]
        ),
        ("grp", "inner"),
    )
    mats = [grads[k] for k in matrix_slots]
    row_parts = [jnp.sum(g * g, axis=1) for g in mats]
    column_parts = [jnp.sum(g * g, axis=0) for g in mats]
    row_totals = lax.psum(
        (row_parts[0], row_parts[1], row_parts[2], row_parts[3], row_parts[4], row_parts[5]),
        "inner",
    )
    column_totals = lax.psum(
        (
            column_parts[0],
            column_parts[1],
            column_parts[2],
            column_parts[3],
            column_parts[4],
            column_parts[5],
        ),
        "grp",
    )
    grand = lax.psum(jnp.stack([jnp.sum(v) for v in row_totals]), "grp")
    scaled_all = [None] * 10
    new_states = [None] * 16
    state_places = {1: (1, 2), 2: (3, 4), 3: (5, 6), 6: (9, 10), 8: (12, 13), 9: (14, 15)}
    second_places = {0: 0, 4: 7, 5: 8, 7: 11}
    for k in range(6):
        slot = matrix_slots[k]
        grad = mats[k]
        full_rows = grad.shape[0] * groups
        full_columns = grad.shape[1] * inners
        rows = 0.5 * rows_old[k] + 0.5 * (row_totals[k] / full_columns + TINY)
        columns = 0.5 * columns_old[k] + 0.5 * (column_totals[k] / full_rows + TINY)
        row_mean = 0.5 * scales[10 + k] / full_rows + 0.5 * (
            grand[k] / (full_rows * full_columns) + TINY
        )
        scaled_all[slot] = grad * lax.rsqrt(rows[:, None] * columns[None, :] / row_mean)
        new_states[state_places[slot][0]] = rows
        new_states[state_places[slot][1]] = columns
    for k in range(4):
        slot = vector_slots[k]
        grad = grads[slot]
        second = 0.5 * seconds_old[k] + 0.5 * (grad * grad + TINY)
        scaled_all[slot] = grad * lax.rsqrt(second)
        new_states[second_places[slot]] = second
    clip = lax.psum(jnp.stack([jnp.sum(s * s) for s in scaled_all]), ("grp", "inner"))
    count_array = jnp.array(counts, jnp.float32)
    update_norms = jnp.sqrt(clip / count_array)
    fresh = [
        locals_f[k]
        + -jnp.sqrt(scales[k] / counts[k]) * scaled_all[k] / jnp.maximum(CLIP, update_norms[k])
        for k in range(10)
    ]
    return (
        block_output,
        tokens_grad,
        grads[0],
        grads[1],
        grads[2],
        grads[3],
        grads[4],
        grads[5],
        grads[6],
        grads[7],
        grads[8],
        grads[9],
        fresh[0],
        fresh[1],
        fresh[2],
        fresh[3],
        fresh[4],
        fresh[5],
        fresh[6],
        fresh[7],
        fresh[8],
        fresh[9],
        new_states[0],
        new_states[1],
        new_states[2],
        new_states[3],
        new_states[4],
        new_states[5],
        new_states[6],
        new_states[7],
        new_states[8],
        new_states[9],
        new_states[10],
        new_states[11],
        new_states[12],
        new_states[13],
        new_states[14],
        new_states[15],
        update_norms,
    )


def solution(mesh):
    return jax.shard_map(
        body,
        mesh=mesh,
        in_specs=(
            P(("grp", "inner"), None, None),
            P(("grp", "inner"), None, None),
            P(("grp", "inner")),
            P("grp", "inner"),
            P("grp", "inner"),
            P("grp", "inner"),
            P(("grp", "inner")),
            P(("grp", "inner")),
            P("grp", "inner"),
            P(("grp", "inner")),
            P("grp", "inner"),
            P("grp", "inner"),
            P(("grp", "inner")),
            P("grp"),
            P("inner"),
            P("grp"),
            P("inner"),
            P("grp"),
            P("inner"),
            P(("grp", "inner")),
            P(("grp", "inner")),
            P("grp"),
            P("inner"),
            P(("grp", "inner")),
            P("grp"),
            P("inner"),
            P("grp"),
            P("inner"),
        ),
        out_specs=(
            P(("grp", "inner"), None, None),
            P(("grp", "inner"), None, None),
            P(("grp", "inner")),
            P("grp", "inner"),
            P("grp", "inner"),
            P("grp", "inner"),
            P(("grp", "inner")),
            P(("grp", "inner")),
            P("grp", "inner"),
            P(("grp", "inner")),
            P("grp", "inner"),
            P("grp", "inner"),
            P(("grp", "inner")),
            P("grp", "inner"),
            P("grp", "inner"),
            P("grp", "inner"),
            P(("grp", "inner")),
            P(("grp", "inner")),
            P("grp", "inner"),
            P(("grp", "inner")),
            P("grp", "inner"),
            P("grp", "inner"),
            P(("grp", "inner")),
            P("grp"),
            P("inner"),
            P("grp"),
            P("inner"),
            P("grp"),
            P("inner"),
            P(("grp", "inner")),
            P(("grp", "inner")),
            P("grp"),
            P("inner"),
            P(("grp", "inner")),
            P("grp"),
            P("inner"),
            P("grp"),
            P("inner"),
            P(),
        ),
        check_vma=False,
    )
```

```python
import functools
import math
import jax
import jax.numpy as jnp
from jax import lax
from jax.experimental import pallas as pl
from jax.sharding import PartitionSpec as P
from jax.experimental.pallas import tpu as pltpu

EPS = 1e-06
F32 = jnp.float32
BF16 = jnp.bfloat16
C = 256
LANES = 128
SUB = 8
ERFC = (
    0.2256758669, 0.2256693636, 0.2078460312, 0.1685204197, 0.1415057621,
    -0.005753053848, 0.1692475449, -0.182997133, 0.05028532412,
)


def dot(a, b):
    return jnp.dot(a, b, preferred_element_type=F32)


def dot_t(a, b):
    return lax.dot_general(a, b, (((1,), (1,)), ((), ())), preferred_element_type=F32)


def loop(steps, body):
    def run(i, carry):
        body(i)
        return carry

    lax.fori_loop(0, steps, run, 0)


def at(i, size):
    return pl.ds(pl.multiple_of(i * size, size), size)


def gelu_parts(x):
    ax = jnp.abs(x)
    e = jnp.exp(-0.5 * (x * x))
    t = 1.0 / (1.0 + (0.4 * math.sqrt(0.5)) * ax)
    poly = jnp.full_like(t, ERFC[-1])
    for c in ERFC[-2::-1]:
        poly = poly * t + c
    half = 0.5 * (poly * t * e)
    cdf = jnp.where(x >= 0, 1.0 - half, half)
    return x * cdf, cdf + (x * e) * (1.0 / math.sqrt(2.0 * math.pi))


def strided(ref, j, n):
    return ref[pl.ds(j, SUB, stride=n), :]


def gather_rows(tmp, j0, n, D):
    columns = [
        jnp.concatenate([tmp[q, pl.ds(j0 + jj, SUB, stride=n), :] for jj in range(16)], axis=0)
        for q in range(D // LANES)
    ]
    return jnp.concatenate(columns, axis=1)


def scatter_rows(tmp, j0, n, out):
    for q in range(out.shape[1] // LANES):
        for jj in range(16):
            tmp[q, pl.ds(j0 + jj, SUB, stride=n), :] = out[
                jj * SUB : (jj + 1) * SUB, q * LANES : (q + 1) * LANES
            ]


def load_planes(ref, rows, start=0, count=None):
    count = ref.shape[0] if count is None else count
    return jnp.concatenate([ref[q, rows, :] for q in range(start, start + count)], axis=1)


def store_planes(ref, rows, value, start=0):
    for q in range(value.shape[1] // LANES):
        ref[start + q, rows, :] = value[:, q * LANES : (q + 1) * LANES]


def add_planes(ref, rows, value):
    for q in range(value.shape[1] // LANES):
        ref[q, rows, :] += value[:, q * LANES : (q + 1) * LANES]


def clear(ref, T):
    for q in range(4):
        ref[q, 0:T, :] = jnp.zeros((T, LANES), F32)


def norm_in(refs, T):
    n = T // SUB
    tmp, g1 = refs.buf, refs.g1
    D = g1.shape[1]

    def widen(i):
        rows = at(i, LANES)
        wide = refs.tok[rows, :].astype(F32)
        for q in range(D // LANES):
            tmp[q, rows, :] = wide[:, q * LANES : (q + 1) * LANES]

    loop(T // LANES, widen)

    def place(i):
        x = gather_rows(tmp, i * 16, n, D)
        y = x * lax.rsqrt(jnp.mean(x * x, axis=-1, keepdims=True) + EPS) * g1[...]
        rows = at(i, LANES)
        refs.tok_p[rows, :] = x.astype(BF16)
        refs.min[rows, :] = y.astype(BF16)
        refs.min_t[:, rows] = y.T.astype(BF16)

    loop(T // LANES, place)


def cot_in(refs, T):
    n = T // SUB
    tmp = refs.buf
    D = refs.g1.shape[1]

    def widen(i):
        rows = at(i, LANES)
        wide = refs.cot[rows, :].astype(F32)
        for q in range(D // LANES):
            tmp[q, rows, :] = wide[:, q * LANES : (q + 1) * LANES]

    loop(T // LANES, widen)

    def place(i):
        x = gather_rows(tmp, i * 16, n, D)
        rows = at(i, LANES)
        refs.cot_p[rows, :] = x.astype(BF16)
        refs.cot_t[:, rows] = x.T.astype(BF16)

    loop(T // LANES, place)


def mixer_forward(refs, z, T):
    pre, ac, st = refs.pre, refs.buf, refs.st
    halves = C // LANES
    width = 3 * LANES

    def project(i):
        rows = at(i, 256)
        out = dot(refs.min[rows, :], refs.wmix[z])
        for q in range(3 * halves):
            pre[q, rows, :] = out[:, q * LANES : (q + 1) * LANES]

    loop(T // 256, project)
    fb = refs.fb[z]
    ib = refs.ib[z]

    def gates(i, carry):
        r0 = pl.multiple_of(i * 64, 64)
        out = []
        for h in range(halves):
            a, b = carry[h]
            lanes = slice(h * LANES, (h + 1) * LANES)
            pf = pre[3 * h, pl.ds(r0, 64), :] + fb[:, lanes]
            pi = pre[3 * h + 1, pl.ds(r0, 64), :] + ib[:, lanes]
            pc = pre[3 * h + 2, pl.ds(r0, 64), :]
            m = jnp.minimum(jnp.minimum(pf, pi), 0.0)
            e0 = jnp.exp(m)
            ef = jnp.exp(m - pf)
            ei = jnp.exp(m - pi)
            nk = e0 + ei
            na = e0 + ef
            inv = 1.0 / (nk + na)
            keep = nk * inv
            admit = na * inv
            not_f = 1.0 / (1.0 + jnp.exp(pf))
            not_i = 1.0 / (1.0 + jnp.exp(pi))
            ec = jnp.exp(jnp.minimum(pc, 0.0))
            sg = ec / (1.0 + ec)
            positive = pc >= 0
            value = jnp.where(positive, pc + 0.5, sg)
            slope = jnp.where(positive, 1.0, sg * (1.0 - sg))
            refs.keep[z, pl.ds(r0, 64), lanes] = keep
            refs.k_f[z, pl.ds(r0, 64), lanes] = keep * not_f
            refs.k_i[z, pl.ds(r0, 64), lanes] = keep * not_i
            refs.k_c[z, pl.ds(r0, 64), lanes] = admit * slope
            inflow = admit * value
            alist, blist = [], []
            for j in range(8):
                kj = keep[j * SUB : (j + 1) * SUB]
                b = kj * b + inflow[j * SUB : (j + 1) * SUB]
                a = kj * a
                alist.append(a)
                blist.append(b)
            ac[h, pl.ds(r0, 64), :] = jnp.concatenate(alist, axis=0)
            st[z, pl.ds(r0 + SUB, 64), lanes] = jnp.concatenate(blist, axis=0)
            out.append((a, b))
        return tuple(out)

    one = jnp.ones((SUB, LANES), F32)
    zero = jnp.zeros((SUB, LANES), F32)
    ends = lax.fori_loop(0, T // 64, gates, tuple((one, zero) for _ in range(halves)))
    for h in range(halves):
        a, b = ends[h]
        rows = [jnp.zeros((1, LANES), F32)]
        for s in range(SUB - 1):
            rows.append(a[s : s + 1] * rows[-1] + b[s : s + 1])
        st[z, 0:SUB, h * LANES : (h + 1) * LANES] = jnp.concatenate(rows, axis=0)
    first = st[z, 0:SUB, :]

    def finish(i):
        r0 = pl.multiple_of(i * 64, 64)
        a = load_planes(ac, pl.ds(r0, 64), 0, 2).reshape(8, SUB, C)
        b = st[z, pl.ds(r0 + SUB, 64), :].reshape(8, SUB, C)
        s = (b + a * first[None]).reshape(64, C)
        st[z, pl.ds(r0 + SUB, 64), :] = s
        refs.slow[z, pl.ds(r0, 64), :] = s.astype(BF16)

    loop(T // 64, finish)


def mix_out(refs, T):
    Z = refs.wot.shape[0]

    def body(i):
        rows = at(i, 256)
        acc = refs.tok_p[rows, :].astype(F32)
        for z in range(Z):
            acc = acc + dot_t(refs.slow[z, rows, :], refs.wot[z])
        store_planes(refs.resid, rows, acc)
        for k in range(2):
            x = acc[k * LANES : (k + 1) * LANES]
            y = x * lax.rsqrt(jnp.mean(x * x, axis=-1, keepdims=True) + EPS) * refs.g2[...]
            sub = pl.ds(pl.multiple_of(i * 256 + k * LANES, LANES), LANES)
            refs.fin[sub, :] = y.astype(BF16)
            refs.fin_t[:, sub] = y.T.astype(BF16)

    loop(T // 256, body)


def feed(refs, f, T):
    wup, wdt = refs.wup, refs.wdt

    def body(i):
        rows = at(i, 256)
        store_planes(refs.buf, rows, dot(refs.fin[rows, :], wup[f]))
        store_planes(refs.buf, rows, dot(refs.cot_p[rows, :], wdt[f]), 2)
        for k in range(4):
            sub = pl.ds(pl.multiple_of(i * 256 + k * 64, 64), 64)
            act, slope = gelu_parts(load_planes(refs.buf, sub, 0, 2))
            refs.dpre[sub, 0:C] = act.astype(BF16)
            refs.dpre[sub, C : 2 * C] = (load_planes(refs.buf, sub, 2, 2) * slope).astype(BF16)
        add_planes(refs.oacc, rows, dot_t(refs.dpre[rows, 0:C], wdt[f]))
        refs.dfe[rows, :] += dot_t(refs.dpre[rows, C : 2 * C], wup[f])

    loop(T // 256, body)


def feed_back(refs, T):
    n = T // SUB
    tmp = refs.buf
    D = refs.g1.shape[1]

    def body(i, total):
        rows = at(i, LANES)
        x = load_planes(refs.resid, rows)
        df = refs.dfe[rows, :]
        out = x + load_planes(refs.oacc, rows, 0, D // LANES)
        scatter_rows(tmp, i * 16, n, out)
        r = lax.rsqrt(jnp.mean(x * x, axis=-1, keepdims=True) + EPS)
        nrm = x * r
        dn = df * refs.g2[...]
        mean = jnp.mean(dn * nrm, axis=-1, keepdims=True)
        dres = refs.cot_p[rows, :].astype(F32) + r * (dn - nrm * mean)
        refs.dfe[rows, :] = dres
        refs.fin[rows, :] = dres.astype(BF16)
        refs.fin_t[:, rows] = dres.T.astype(BF16)
        return total + (df * nrm).reshape(16, SUB, D).sum(axis=0)

    total = lax.fori_loop(0, T // LANES, body, jnp.zeros((SUB, D), F32))
    refs.fgg[...] = jnp.sum(total, axis=0, keepdims=True)

    def emit(i):
        rows = at(i, LANES)
        for q in range(D // LANES):
            refs.block[rows, q * LANES : (q + 1) * LANES] = tmp[q, rows, :].astype(BF16)

    loop(T // LANES, emit)


def mixer_back(refs, z, T):
    buf, st = refs.buf, refs.st
    halves = C // LANES
    width = 3 * LANES

    def project(i):
        rows = at(i, 256)
        store_planes(buf, rows, dot(refs.fin[rows, :], refs.wot[z]))

    loop(T // 256, project)
    steps = T // 64

    def local(i, carry):
        r0 = pl.multiple_of((steps - 1 - i) * 64, 64)
        d = load_planes(buf, pl.ds(r0, 64), 0, 2)
        k = refs.keep[z, pl.ds(r0, 64), :]
        e, dk = carry
        plist, dlist = [None] * 8, [None] * 8
        for j in range(7, -1, -1):
            kj = k[j * SUB : (j + 1) * SUB]
            p = d[j * SUB : (j + 1) * SUB] + e
            plist[j] = p
            dlist[j] = dk
            e = kj * p
            dk = kj * dk
        store_planes(buf, pl.ds(r0, 64), jnp.concatenate(plist, axis=0))
        store_planes(buf, pl.ds(r0, 64), jnp.concatenate(dlist, axis=0), 2)
        return e, dk

    e, dk = lax.fori_loop(0, steps, local, (jnp.zeros((SUB, C), F32), jnp.ones((SUB, C), F32)))
    rows = [jnp.zeros((1, C), F32)]
    for s in range(SUB - 1, 0, -1):
        rows.insert(0, e[s : s + 1] + dk[s : s + 1] * rows[0])
    tail = jnp.concatenate(rows, axis=0)

    def grads(i, sums):
        r0 = pl.multiple_of(i * 64, 64)
        out = []
        for h in range(halves):
            lanes = slice(h * LANES, (h + 1) * LANES)
            sub = pl.ds(r0, 64)
            p0 = buf[h, sub, :].reshape(8, SUB, LANES)
            d0 = buf[2 + h, sub, :].reshape(8, SUB, LANES)
            p = (p0 + d0 * tail[None, :, lanes]).reshape(64, LANES)
            x = p * (st[z, pl.ds(r0 + SUB, 64), lanes] - st[z, sub, lanes])
            df = -(refs.k_f[z, sub, lanes] * x)
            di = refs.k_i[z, sub, lanes] * x
            dcand = refs.k_c[z, sub, lanes] * p
            df16 = df.astype(BF16)
            di16 = di.astype(BF16)
            refs.dpre[sub, h * width : h * width + LANES] = df16
            refs.dpre[sub, h * width + LANES : h * width + 2 * LANES] = di16
            refs.dpre[sub, h * width + 2 * LANES : h * width + 3 * LANES] = dcand.astype(BF16)
            sf, si = sums[h]
            out.append(
                (
                    sf + df16.astype(F32).reshape(8, SUB, LANES).sum(axis=0),
                    si + di16.astype(F32).reshape(8, SUB, LANES).sum(axis=0),
                )
            )
        return tuple(out)

    zero = jnp.zeros((SUB, LANES), F32)
    sums = lax.fori_loop(0, T // 64, grads, tuple((zero, zero) for _ in range(halves)))
    for h in range(halves):
        lanes = slice(h * LANES, (h + 1) * LANES)
        refs.fbg[z, :, lanes] = jnp.sum(sums[h][0], axis=0, keepdims=True)
        refs.ibg[z, :, lanes] = jnp.sum(sums[h][1], axis=0, keepdims=True)

    def back(i):
        rows = at(i, 256)
        add_planes(refs.oacc, rows, dot_t(refs.dpre[rows, :], refs.wmix[z]))

    loop(T // 256, back)


def norm_back(refs, T):
    n = T // SUB
    tmp = refs.buf
    D = refs.g1.shape[1]

    def body(i, total):
        rows = at(i, LANES)
        x = refs.tok_p[rows, :].astype(F32)
        d_in = load_planes(refs.oacc, rows, 0, D // LANES)
        r = lax.rsqrt(jnp.mean(x * x, axis=-1, keepdims=True) + EPS)
        nrm = x * r
        dn = d_in * refs.g1[...]
        mean = jnp.mean(dn * nrm, axis=-1, keepdims=True)
        out = refs.dfe[rows, :] + r * (dn - nrm * mean)
        scatter_rows(tmp, i * 16, n, out)
        return total + (d_in * nrm).reshape(16, SUB, D).sum(axis=0)

    total = lax.fori_loop(0, T // LANES, body, jnp.zeros((SUB, D), F32))
    refs.mgg[...] = jnp.sum(total, axis=0, keepdims=True)

    def emit(i):
        rows = at(i, LANES)
        for q in range(D // LANES):
            refs.tgrad[rows, q * LANES : (q + 1) * LANES] = tmp[q, rows, :].astype(BF16)

    loop(T // LANES, emit)


class Refs:
    def __init__(self, args):
        (
            self.tok, self.cot, self.wmix, self.wot, self.wup, self.wdt, self.g1, self.g2, self.fb, self.ib,
            self.block, self.tgrad, self.gmix, self.got, self.gup, self.gdt, self.fgg, self.mgg, self.fbg, self.ibg,
            self.tok_p, self.min, self.min_t, self.fin, self.fin_t, self.cot_p, self.cot_t, self.resid, self.oacc, self.dfe,
            self.pre, self.buf, self.dpre, self.slow, self.st, self.keep, self.k_f,
            self.k_i, self.k_c, self.gst, self.gsem,
        ) = args


def layer_kernel(*args):
    refs = Refs(args)
    T, D = refs.tok.shape
    Z = refs.wmix.shape[0]
    F = refs.wup.shape[0]
    gst, sem = refs.gst, refs.gsem
    cot_in(refs, T)
    norm_in(refs, T)
    loop(Z, lambda z: mixer_forward(refs, z, T))
    mix_out(refs, T)
    clear(refs.oacc, T)
    refs.dfe[...] = jnp.zeros_like(refs.dfe)

    def feed_step(f):
        feed(refs, f, T)
        gst[0, :, 0:C] = dot(refs.cot_t[...], refs.dpre[:, 0:C])
        gst[1, :, 0:C] = dot(refs.fin_t[...], refs.dpre[:, C : 2 * C])
        one = pltpu.make_async_copy(gst.at[0, :, 0:C], refs.gdt.at[f], sem.at[0])
        two = pltpu.make_async_copy(gst.at[1, :, 0:C], refs.gup.at[f], sem.at[1])
        one.start()
        two.start()
        one.wait()
        two.wait()

    loop(F, feed_step)
    feed_back(refs, T)
    clear(refs.oacc, T)

    def mixer_step(z):
        gst[0, :, 0:C] = dot(refs.fin_t[...], refs.slow[z])
        mixer_back(refs, z, T)
        gst[1, :, :] = dot(refs.min_t[...], refs.dpre[...])
        one = pltpu.make_async_copy(gst.at[0, :, 0:C], refs.got.at[z], sem.at[0])
        two = pltpu.make_async_copy(gst.at[1], refs.gmix.at[z], sem.at[1])
        one.start()
        two.start()
        one.wait()
        two.wait()

    loop(Z, mixer_step)
    norm_back(refs, T)


def layer(tok, cot, wmix, wot, wup, wdt, g1, g2, fb, ib):
    T, D = tok.shape
    Z, F = wmix.shape[0], wup.shape[0]
    sds = jax.ShapeDtypeStruct
    vm = pl.BlockSpec(memory_space=pltpu.VMEM)
    anyspec = pl.BlockSpec(memory_space=pl.ANY)
    out_shape = (
        sds((T, D), BF16), sds((T, D), BF16),
        sds((Z, D, 3 * C), F32), sds((Z, D, C), F32), sds((F, D, C), F32), sds((F, D, C), F32),
        sds((1, D), F32), sds((1, D), F32), sds((Z, 1, C), F32), sds((Z, 1, C), F32),
    )
    V = pltpu.VMEM
    scratch = [
        V((T, D), BF16), V((T, D), BF16), V((D, T), BF16), V((T, D), BF16), V((D, T), BF16),
        V((T, D), BF16), V((D, T), BF16), V((D // LANES, T, LANES), F32),
        V((D // LANES, T, LANES), F32), V((T, D), F32), V((3 * C // LANES, T, LANES), F32), V((4, T, LANES), F32),
        V((T, 3 * C), BF16), V((Z, T, C), BF16), V((Z, T + SUB, C), F32),
        V((Z, T, C), F32), V((Z, T, C), F32), V((Z, T, C), F32), V((Z, T, C), F32),
        V((2, D, 3 * C), F32), pltpu.SemaphoreType.DMA((2,)),
    ]
    return pl.pallas_call(
        layer_kernel,
        out_shape=out_shape,
        in_specs=[vm] * 10,
        out_specs=(vm, vm, anyspec, anyspec, anyspec, anyspec, vm, vm, vm, vm),
        scratch_shapes=scratch,
        compiler_params=pltpu.CompilerParams(vmem_limit_bytes=67043328),
        name="layer",
    )(tok, cot, wmix, wot, wup, wdt, g1, g2, fb, ib)


MESH = pl.DeviceIdType.MESH


def rcopy(src, dst, send, recv, device):
    return pltpu.make_async_remote_copy(
        src_ref=src, dst_ref=dst, send_sem=send, recv_sem=recv, device_id=device, device_id_type=MESH
    )


class Place:
    def __init__(self):
        self.g = lax.axis_index("grp")
        self.i = lax.axis_index("inner")
        self.y, self.x = self.g // 2, self.g % 2
        self.z, self.c = self.i // 2, self.i % 2
        self.me = self.g * 8 + self.i
        self.partner = (self.g, self.z * 2 + 1 - self.c)

    def flip(self, fx, fy):
        x = (self.x + fx) % 2
        y = (self.y + fy) % 2
        return y * 2 + x

    def near(self, z):
        e = z % 2
        return self.flip(1 - e, e)

    def far(self, z):
        e = z % 2
        return self.flip(e, 1 - e)

    def other(self, k):
        t = (self.me + k) % 32
        return (t // 8, t % 8)


def entry_barrier(place):
    barrier = pltpu.get_barrier_semaphore()

    def greet(k):
        pl.semaphore_signal(barrier, inc=1, device_id=place.other(k + 1), device_id_type=MESH)

    loop(31, greet)
    pl.semaphore_wait(barrier, 31)


def spread(values, start, count, total):
    lane = lax.broadcasted_iota(jnp.int32, (LANES, total), 1)
    row = lax.broadcasted_iota(jnp.int32, (LANES, total), 0)
    sel = jnp.where(row == start + lane % count, 1.0, 0.0).astype(BF16)
    picked = dot(values, sel)
    owner = lax.broadcasted_iota(jnp.int32, picked.shape, 0)
    spot = lax.broadcasted_iota(jnp.int32, picked.shape, 1)
    return jnp.sum(jnp.where(spot // count == owner, picked, 0.0), axis=0, keepdims=True)


def pack_vectors(mg, fb, ib, fg):
    parts = [mg, fb, ib, fg]
    used = sum(p.shape[0] for p in parts)
    rows = [p[...].astype(F32).reshape(1, p.shape[0]) for p in parts]
    return jnp.concatenate(rows + [jnp.zeros((1, LANES - used), F32)], axis=1)


def block_of(refs, a, g, i):
    if a == 0:
        return refs.wot.at[g, at(i, 64), :]
    if a == 1:
        return refs.wup.at[i, at(g, 128), :]
    return refs.wdt.at[pl.ds(2 * g, 2), at(i, 64), :]


def blocks_of(refs, a, i):
    if a == 0:
        return refs.wot.at[:, at(i, 64), :]
    if a == 1:
        return refs.wup.at[i]
    return refs.wdt.at[:, at(i, 64), :]


def mix_column(refs, z, c):
    return refs.wmix.at[z, :, at(c, 384)]


def gather_start(refs, p):
    local = []
    for k, w in enumerate((refs.fw, refs.iw, refs.cw)):
        spot = pl.ds(pl.multiple_of(p.c * 384 + k * 128, 128), 128)
        local.append(
            pltpu.make_async_copy(w, refs.wmix.at[p.z, at(p.g, 128), spot], refs.loc_s.at[k])
        )
    local.append(pltpu.make_async_copy(refs.ow, block_of(refs, 0, p.g, p.i), refs.loc_s.at[3]))
    local.append(pltpu.make_async_copy(refs.uw, block_of(refs, 1, p.g, p.i), refs.loc_s.at[4]))
    for k in range(2):
        local.append(
            pltpu.make_async_copy(
                refs.dw.at[:, k * 256 : (k + 1) * 256],
                refs.wdt.at[2 * p.g + k, at(p.i, 64), :],
                refs.loc_s.at[5 + k],
            )
        )
    for c in local:
        c.start()
    row = pack_vectors(refs.mg, refs.fbv, refs.ibv, refs.fg)
    refs.vstage[...] = row
    refs.vecs[p.me] = row
    entry_barrier(p)
    for c in local[:3]:
        c.wait()
    own = refs.wmix.at[p.z, at(p.g, 128), at(p.c, 384)]
    for k in range(1, 4):
        peer = p.flip(k % 2, k // 2)
        rcopy(own, own, refs.mxg_s.at[k - 1], refs.mxg_r.at[k - 1], (peer, p.i)).start()

    def vector(k):
        rcopy(refs.vstage, refs.vecs.at[p.me], refs.vec_s, refs.vec_r, p.other(k + 1)).start()

    loop(31, vector)
    for c in local[3:]:
        c.wait()
    for a in range(3):
        blk = block_of(refs, a, p.g, p.i)
        for k in range(1, 4):
            peer = (p.g, ((p.z + k) % 4) * 2 + p.c)
            rcopy(blk, blk, refs.ffz_s.at[a, k - 1], refs.ffz_r.at[a, p.z], peer).start()


def gather_vectors(refs, p):
    rows = refs.vecs.at[pl.ds(0, 31)]
    rcopy(rows, rows, refs.vec_s, refs.vec_r, p.partner).wait()
    v = refs.vecs[...].reshape(32, LANES).astype(BF16)
    refs.g1[...] = spread(v, 0, 16, 512)
    refs.g2[...] = spread(v, 80, 16, 512)
    fb = spread(v, 16, 32, 1024)
    ib = spread(v, 48, 32, 1024)
    for z in range(4):
        refs.fb[z] = fb[:, z * C : (z + 1) * C]
        refs.ib[z] = ib[:, z * C : (z + 1) * C]


def mix_exchange(refs, p, s):
    def send_partner(z):
        col = mix_column(refs, z, p.c)
        rcopy(col, col, refs.mxp_s.at[z], refs.mxp_r.at[z], p.partner).start()

    def wait_partner(z):
        col = mix_column(refs, z, 1 - p.c)
        rcopy(col, col, refs.mxp_s.at[z], refs.mxp_r.at[z], p.partner).wait_recv()

    def send_up(z):
        col = mix_column(refs, z, p.c)
        rcopy(col, col, refs.mxu_s.at[z], refs.mxz_r.at[z], (p.g, p.i + 2)).start()

    def send_down(z):
        col = mix_column(refs, z, p.c)
        rcopy(col, col, refs.mxd_s.at[z], refs.mxz_r.at[z], (p.g, p.i - 2)).start()

    def wait_line(z):
        col = mix_column(refs, z, p.c)
        rcopy(col, col, refs.mxp_s.at[z], refs.mxz_r.at[z], p.partner).wait_recv()

    @pl.when(s == 0)
    def _():
        for k in range(1, 4):
            peer = p.flip(k % 2, k // 2)
            blk = refs.wmix.at[p.z, at(peer, 128), at(p.c, 384)]
            rcopy(blk, blk, refs.mxg_s.at[k - 1], refs.mxg_r.at[k - 1], (peer, p.i)).wait()

        @pl.when(p.z < 3)
        def _():
            send_up(p.z)

        @pl.when(p.z > 0)
        def _():
            send_down(p.z)

        send_partner(p.z)
        wait_partner(p.z)

    below, above = p.z - s, p.z + s

    @pl.when((s > 0) & (below >= 0))
    def _():
        wait_line(below)

        @pl.when(p.z < 3)
        def _():
            send_up(below)

        send_partner(below)

    @pl.when((s > 0) & (above < 4))
    def _():
        wait_line(above)

        @pl.when(p.z > 0)
        def _():
            send_down(above)

        send_partner(above)

    @pl.when((s > 0) & (below >= 0))
    def _():
        wait_partner(below)

    @pl.when((s > 0) & (above < 4))
    def _():
        wait_partner(above)


def mix_drain(refs, p):
    for z in range(4):
        col = mix_column(refs, z, p.c)
        rcopy(col, col, refs.mxp_s.at[z], refs.mxp_r.at[z], p.partner).wait_send()

        @pl.when((z <= p.z) & (p.z < 3))
        def _():
            rcopy(col, col, refs.mxu_s.at[z], refs.mxz_r.at[z], p.partner).wait_send()

        @pl.when((z >= p.z) & (p.z > 0))
        def _():
            rcopy(col, col, refs.mxd_s.at[z], refs.mxz_r.at[z], p.partner).wait_send()


def feed_second(refs, p):
    for a in range(3):
        for z in range(4):
            blk = block_of(refs, a, p.g, z * 2 + p.c)

            @pl.when(p.z != z)
            def _():
                rcopy(blk, blk, refs.ffp_s.at[a, z], refs.ffz_r.at[a, z], p.partner).wait_recv()

            rcopy(blk, blk, refs.ff2_s.at[a, z], refs.ff2_r.at[a, z], (p.near(z), p.i)).start()


def feed_third(refs, p):
    for a in range(3):
        for z in range(4):
            mine = block_of(refs, a, p.g, z * 2 + p.c)
            near = block_of(refs, a, p.near(z), z * 2 + p.c)
            far = (p.far(z), p.i)
            rcopy(near, near, refs.ff2_s.at[a, z], refs.ff2_r.at[a, z], (p.near(z), p.i)).wait_recv()
            rcopy(mine, mine, refs.ff3_s.at[a, z, 0], refs.ff3_r.at[a, z, 0], far).start()
            rcopy(near, near, refs.ff3_s.at[a, z, 1], refs.ff3_r.at[a, z, 1], far).start()


def feed_fourth(refs, p):
    for a in range(3):
        for z in range(4):
            blk = block_of(refs, a, p.g, z * 2 + p.c)
            far = (p.far(z), p.i)
            for k in range(2):
                rcopy(blk, blk, refs.ff3_s.at[a, z, k], refs.ff3_r.at[a, z, k], far).wait_recv()
            full = blocks_of(refs, a, z * 2 + p.c)
            rcopy(full, full, refs.ffp_s.at[a, z], refs.ffp_r.at[a, z], p.partner).start()


def feed_last(refs, p):
    for a in range(3):
        for z in range(4):
            full = blocks_of(refs, a, z * 2 + 1 - p.c)
            rcopy(full, full, refs.ffp_s.at[a, z], refs.ffp_r.at[a, z], p.partner).wait_recv()


def feed_drain(refs, p):
    for a in range(3):
        for k in range(1, 4):
            blk = block_of(refs, a, p.g, p.i)
            rcopy(blk, blk, refs.ffz_s.at[a, k - 1], refs.ffz_r.at[a, p.z], p.partner).wait_send()
        for z in range(4):
            blk = block_of(refs, a, p.g, z * 2 + p.c)
            rcopy(blk, blk, refs.ff2_s.at[a, z], refs.ff2_r.at[a, z], p.partner).wait_send()
            for k in range(2):
                rcopy(blk, blk, refs.ff3_s.at[a, z, k], refs.ff3_r.at[a, z, k], p.partner).wait_send()
            full = blocks_of(refs, a, z * 2 + p.c)
            rcopy(full, full, refs.ffp_s.at[a, z], refs.ffp_r.at[a, z], p.partner).wait_send()


def slot_chunk(p, s):
    low = jnp.minimum(p.z, 3 - p.z)
    shift = jnp.where(s == 0, 1, jnp.where(s == 1, -1, 0))
    m = s + low * shift
    return jnp.where(p.z < 2, m, 3 - m)


def mixer_slots(refs, p, T):
    def slot(s):
        mix_exchange(refs, p, s)
        mixer_forward(refs, slot_chunk(p, s), T)

        @pl.when(s == 0)
        def _():
            feed_second(refs, p)

        @pl.when(s == 1)
        def _():
            feed_third(refs, p)

        @pl.when(s == 2)
        def _():
            feed_fourth(refs, p)

    loop(4, slot)
    mix_drain(refs, p)
    feed_last(refs, p)
    feed_drain(refs, p)


SHAPES = ((128, 256), (128, 256), (128, 384), (64, 256))
UP, DOWN, MIX, OUT = 0, 1, 2, 3
TINY = 1e-30
CLIP = 0.01
MATRICES = (
    (512, 1024), (512, 1024), (512, 1024), (1024, 512), (512, 2048), (2048, 512)
)
MATRIX_SLOTS = (1, 2, 3, 6, 8, 9)
VECTORS = ((0, 0, 16), (4, 16, 32), (5, 48, 32), (7, 80, 16))
COUNTS = (512, 524288, 524288, 524288, 1024, 1024, 524288, 512, 1048576, 1048576)


def spot(a, g, z):
    return (g, z) if a == DOWN else (z, g)


def rs_store(refs, a, g, z, value):
    refs.psend[a][(*spot(a, g, z),)] = value.astype(BF16)


def rs_role(p, g, z):
    e = z % 2
    y, x = g // 2, g % 2
    return (1 - e) * ((x + p.x) % 2) + e * ((y + p.y) % 2)


def rs_pair(refs, p, a, u):
    if a == OUT:
        src, dst = refs.psend[a], refs.precv[a]
    else:
        src, dst = refs.psend[a].at[u], refs.precv[a].at[u]
    return rcopy(src, dst, refs.rp_s.at[a, u], refs.rp_r.at[a, u], p.partner)


def rs_merge(refs, p, a, g, z, own):
    place = spot(a, g, z)
    v = own + refs.precv[a][place].astype(F32)
    role = rs_role(p, g, z)

    @pl.when(role == 1)
    def _():
        refs.psend[a][place] = v.astype(BF16)

    @pl.when(role == 0)
    def _():
        refs.precv[a][place] = v.astype(BF16)


def rs_group(p, z, k, sent):
    e = z % 2
    x = (1 - e) * ((p.x + sent) % 2) + e * k
    y = (1 - e) * k + e * ((p.y + sent) % 2)
    return y * 2 + x


def rs_first_copy(refs, p, a, z, k):
    g = rs_group(p, z, k, 1)
    return rcopy(
        refs.psend[a].at[spot(a, g, z)], refs.r1[a].at[z, k],
        refs.r1_s.at[a, z, k], refs.r1_r.at[a, z, k], (p.near(z), p.i),
    )


def rs_first_send(refs, p, a, z):
    for k in range(2):
        rs_first_copy(refs, p, a, z, k).start()


def rs_second(refs, p, a, z):
    e = z % 2
    mine = (1 - e) * p.y + e * p.x
    for k in range(2):
        rs_first_copy(refs, p, a, z, k).wait_recv()
    for k in range(2):
        place = spot(a, rs_group(p, z, k, 0), z)
        v = (refs.precv[a][place].astype(F32) + refs.r1[a][z, k].astype(F32)).astype(BF16)

        @pl.when(mine == k)
        def _():
            refs.precv[a][place] = v

        @pl.when(mine != k)
        def _():
            refs.psend[a][place] = v


def rs_second_copy(refs, p, a, z):
    e = z % 2
    other = 1 - ((1 - e) * p.y + e * p.x)
    place = spot(a, rs_group(p, z, other, 0), z)
    return rcopy(
        refs.psend[a].at[place], refs.r2[a].at[z], refs.r2_s.at[a, z], refs.r2_r.at[a, z],
        (p.far(z), p.i),
    )


def rs_third(refs, p, a, z):
    rs_second_copy(refs, p, a, z).wait_recv()
    place = spot(a, p.g, z)
    v = refs.precv[a][place].astype(F32) + refs.r2[a][z].astype(F32)

    @pl.when(z == p.z)
    def _():
        refs.fin_g[a][...] = v

    @pl.when(z != p.z)
    def _():
        refs.psend[a][place] = v.astype(BF16)


def rs_line(refs, p, a, z, owner):
    return rcopy(
        refs.psend[a].at[spot(a, p.g, z)], refs.r3[a].at[owner],
        refs.r3_s.at[a, z], refs.r3_r.at[a, owner], (p.g, z * 2 + p.c),
    )


def rs_third_send(refs, p, a, z):
    @pl.when(z != p.z)
    def _():
        rs_line(refs, p, a, z, p.z).start()


def rs_last(refs, p, a):
    for k in range(1, 4):
        z = (p.z + k) % 4
        rs_line(refs, p, a, z, z).wait_recv()
        refs.fin_g[a][...] += refs.r3[a][z].astype(F32)


def rs_drain(refs, p):
    def one(z):
        for a in range(4):
            for k in range(2):
                rs_first_copy(refs, p, a, z, k).wait_send()
            rs_second_copy(refs, p, a, z).wait_send()

            @pl.when(z != p.z)
            def _():
                rs_line(refs, p, a, z, p.z).wait_send()

    loop(4, one)


def own_row(x):
    return jnp.sum(x, axis=0, keepdims=True)


def lane_sum(x):
    folded = sum(x[:, k : k + LANES] for k in range(0, x.shape[1], LANES))
    return own_row(folded.T)


def wide(row):
    return jnp.concatenate([row, jnp.zeros((1, LANES - row.shape[1]), F32)], axis=1)


def cut(row):
    return [row[:, k : k + LANES] for k in range(0, row.shape[1], LANES)]


def stand(row):
    return jnp.broadcast_to(row, (LANES, LANES)).T


def scalars(values):
    lane = lax.broadcasted_iota(jnp.int32, (1, LANES), 1)
    out = jnp.zeros((1, LANES), F32)
    for k, v in enumerate(values):
        out = out + jnp.where(lane == k, v, 0.0)
    return out


def total(x):
    return jnp.sum(jnp.sum(x, axis=0, keepdims=True), axis=1, keepdims=True)


def segment(row, start, count):
    lane = lax.broadcasted_iota(jnp.int32, row.shape, 1)
    keep = (lane >= start) & (lane < start + count)
    return jnp.sum(jnp.where(keep, row, 0.0), axis=1, keepdims=True)


def gather_row(term, start, count):
    size = term.shape[1]
    owner = lax.broadcasted_iota(jnp.int32, (32, size), 0)
    spot = lax.broadcasted_iota(jnp.int32, (32, size), 1)
    masked = jnp.where(spot // count == owner, term, 0.0)
    lane = lax.broadcasted_iota(jnp.int32, (LANES, size), 0)
    from_spot = lax.broadcasted_iota(jnp.int32, (LANES, size), 1)
    sel = jnp.where(lane == start + from_spot % count, 1.0, 0.0).astype(BF16)
    out = jnp.zeros((32, LANES), F32)
    for _ in range(3):
        part = masked.astype(BF16)
        out = out + dot_t(part, sel)
        masked = masked - part.astype(F32)
    return out


def parameter_blocks(refs):
    return [
        refs.fw[...].astype(F32), refs.iw[...].astype(F32), refs.cw[...].astype(F32),
        refs.ow[...].astype(F32), refs.uw[...].astype(F32), refs.dw[...].astype(F32),
    ]


def old_rows(refs):
    rows = []
    for r in (refs.row_f, refs.row_i, refs.row_c, refs.row_o, refs.row_u, refs.row_d):
        rows += cut(r[...].reshape(1, r.shape[0]))
    return rows


def old_columns(refs):
    rows = []
    for r in (refs.col_f, refs.col_i, refs.col_c, refs.col_o, refs.col_u, refs.col_d):
        row = r[...].reshape(1, r.shape[0])
        rows += [wide(row)] if r.shape[0] < LANES else cut(row)
    return rows


ROW_PLACES = ((0, 1), (1, 2), (2, 3), (3, 5), (5, 6), (6, 10))
COLUMN_PLACES = ((0, 1), (1, 2), (2, 3), (3, 4), (4, 6), (6, 7))


def broadcast_row(src, box, send, recv, p):
    def one(k):
        rcopy(src, box.at[p.me], send, recv, p.other(k + 1)).start()

    loop(31, one)


def settle_row(box, send, recv, p):
    rows = box.at[pl.ds(0, 31)]
    rcopy(rows, rows, send, recv, p.partner).wait()


def vector_exchange(refs, p):
    rows = (
        gather_row(refs.mgg[...], 0, 16)
        + gather_row(jnp.concatenate([refs.fbg[z] for z in range(4)], axis=1), 16, 32)
        + gather_row(jnp.concatenate([refs.ibg[z] for z in range(4)], axis=1), 48, 32)
        + gather_row(refs.fgg[...], 80, 16)
    )
    refs.vout[...] = rows.reshape(32, 1, LANES)
    refs.vin[p.me] = refs.vout[p.me]

    def one(k):
        t = (p.me + k + 1) % 32
        rcopy(refs.vout.at[t], refs.vin.at[p.me], refs.vex_s, refs.vex_r, p.other(k + 1)).start()

    loop(31, one)


def gradient_blocks(refs):
    mix = refs.fin_g[MIX][...]
    down = refs.fin_g[DOWN][...]
    return [
        mix[:, 0:128], mix[:, 128:256], mix[:, 256:384], refs.fin_g[OUT][...], refs.fin_g[UP][...],
        jnp.concatenate([down[0:64], down[64:128]], axis=1),
    ]


def adafactor(refs, p):
    grads = gradient_blocks(refs)
    flipped = (False, False, False, True, False, True)
    row_parts, column_parts, totals = [], [], []
    for grad, flip in zip(grads, flipped):
        sq = grad * grad
        down, across = own_row(sq), lane_sum(sq)
        row_parts += cut(down) if flip else [across]
        column_parts += [wide(across)] if flip else cut(down)
        totals.append(jnp.sum(down, axis=1, keepdims=True))
    refs.rowst[...] = jnp.concatenate(row_parts + [jnp.zeros((6, LANES), F32)], axis=0)
    refs.colst[...] = jnp.concatenate(column_parts + [jnp.zeros((1, LANES), F32)], axis=0)
    weights = parameter_blocks(refs)
    params = pack_vectors(refs.mg, refs.fbv, refs.ibv, refs.fg)
    squares = [None] * 10
    for slot, w in zip(MATRIX_SLOTS, weights):
        squares[slot] = total(w * w)
    for slot, start, count in VECTORS:
        squares[slot] = segment(params * params, start, count)
    rows_old, columns_old = old_rows(refs), old_columns(refs)
    first = jnp.where(p.i == 0, 1.0, 0.0)
    row_sums = [first * total(jnp.concatenate(rows_old[a:b], axis=0)) for a, b in ROW_PLACES]
    refs.scal[...] = scalars(totals + squares + row_sums)
    refs.rowin[p.i] = refs.rowst[...]
    refs.colin[p.g] = refs.colst[...]
    refs.scin[p.me] = refs.scal[...]
    for k in range(1, 8):
        peer = (p.g, (p.i + k) % 8)
        rcopy(
            refs.rowst, refs.rowin.at[p.i], refs.row_s.at[k - 1], refs.row_r.at[k - 1], peer
        ).start()
    for k in range(1, 4):
        peer = ((p.g + k) % 4, p.i)
        rcopy(
            refs.colst, refs.colin.at[p.g], refs.col_s.at[k - 1], refs.col_r.at[k - 1], peer
        ).start()
    broadcast_row(refs.scal, refs.scin, refs.sc_s, refs.sc_r, p)
    vec_rows = refs.vin.at[pl.ds(0, 31)]
    rcopy(vec_rows, vec_rows, refs.vex_s, refs.vex_r, p.partner).wait()
    vector_grad = jnp.sum(refs.vin[...].reshape(32, LANES), axis=0, keepdims=True)
    seconds = pack_vectors(refs.sec_m, refs.sec_f, refs.sec_i, refs.sec_g)
    second = 0.5 * seconds + 0.5 * (vector_grad * vector_grad + TINY)
    vector_scaled = vector_grad * lax.rsqrt(second)
    for k in range(1, 8):
        rcopy(
            refs.rowst, refs.rowin.at[p.i], refs.row_s.at[k - 1], refs.row_r.at[k - 1], p.partner
        ).wait()
    for k in range(1, 4):
        rcopy(
            refs.colst, refs.colin.at[p.g], refs.col_s.at[k - 1], refs.col_r.at[k - 1], p.partner
        ).wait()
    settle_row(refs.scin, refs.sc_s, refs.sc_r, p)
    row_total = sum(refs.rowin[k] for k in range(8))
    column_total = sum(refs.colin[k] for k in range(4))
    sc = jnp.sum(refs.scin[...].reshape(32, LANES), axis=0, keepdims=True)
    rows_new, columns_new, scaled = [], [], []
    for k, (r, c) in enumerate(MATRICES):
        ra, rb = ROW_PLACES[k]
        ca, cb = COLUMN_PLACES[k]
        rows = [
            0.5 * rows_old[j] + 0.5 * (row_total[j : j + 1] / c + TINY) for j in range(ra, rb)
        ]
        columns = [
            0.5 * columns_old[j] + 0.5 * (column_total[j : j + 1] / r + TINY)
            for j in range(ca, cb)
        ]
        mean = 0.5 * sc[:, 16 + k : 17 + k] / r + 0.5 * (sc[:, k : k + 1] / (r * c) + TINY)
        lying, standing = (rows, columns) if flipped[k] else (columns, rows)
        tall = stand(standing[0])[0 : grads[k].shape[0]]
        lying = jnp.concatenate(lying, axis=1)
        tall = jnp.concatenate([tall] * (lying.shape[1] // LANES), axis=1)
        scaled.append(grads[k] * lax.rsqrt(tall * lying / mean))
        rows_new += rows
        columns_new += columns
    refs.rows_out[...] = jnp.concatenate(rows_new + [jnp.zeros((6, LANES), F32)], axis=0)
    refs.columns_out[...] = jnp.concatenate(columns_new + [jnp.zeros((1, LANES), F32)], axis=0)
    clips = [None] * 10
    for slot, s in zip(MATRIX_SLOTS, scaled):
        clips[slot] = total(s * s)
    for slot, start, count in VECTORS:
        clips[slot] = segment(vector_scaled * vector_scaled, start, count)
    refs.clip[...] = scalars(clips)
    refs.clin[p.me] = refs.clip[...]
    broadcast_row(refs.clip, refs.clin, refs.cl_s, refs.cl_r, p)
    settle_row(refs.clin, refs.cl_s, refs.cl_r, p)
    clip = jnp.sum(refs.clin[...].reshape(32, LANES), axis=0, keepdims=True)
    norms = [jnp.sqrt(clip[:, k : k + 1] / COUNTS[k]) for k in range(10)]
    steps = [
        -jnp.sqrt(sc[:, 6 + k : 7 + k] / COUNTS[k]) / jnp.maximum(CLIP, norms[k])
        for k in range(10)
    ]
    fresh = [w + steps[slot] * s for slot, w, s in zip(MATRIX_SLOTS, weights, scaled)]
    refs.grad_mix[...] = refs.fin_g[MIX][...]
    refs.grad_out[...] = grads[3]
    refs.grad_up[...] = grads[4]
    refs.grad_down[...] = grads[5]
    refs.new_mix[...] = jnp.concatenate(fresh[0:3], axis=1)
    refs.new_out[...] = fresh[3]
    refs.new_up[...] = fresh[4]
    refs.new_down[...] = fresh[5]
    lane = lax.broadcasted_iota(jnp.int32, (1, LANES), 1)
    step_row = jnp.zeros((1, LANES), F32)
    for slot, start, count in VECTORS:
        step_row = step_row + jnp.where((lane >= start) & (lane < start + count), steps[slot], 0.0)
    refs.vectors[...] = jnp.concatenate(
        [vector_grad, params + step_row * vector_scaled, second, scalars(norms)]
        + [jnp.zeros((4, LANES), F32)],
        axis=0,
    )


def finish_kernel(
    grad_mix, grad_out, grad_up, grad_down, new_mix, new_out, new_up, new_down,
    vectors, rows, columns,
    g_mg, g_f, g_i, g_c, g_fb, g_ib, g_o, g_fg, g_u, g_d,
    n_mg, n_f, n_i, n_c, n_fb, n_ib, n_o, n_fg, n_u, n_d,
    s_m, r_f, c_f, r_i, c_i, r_c, c_c, s_f, s_i, r_o, c_o, s_g, r_u, c_u, r_d, c_d, norms,
):
    for src, outs in ((grad_mix, (g_f, g_i, g_c)), (new_mix, (n_f, n_i, n_c))):
        for k, o in enumerate(outs):
            o[...] = src[:, k * 128 : (k + 1) * 128]
    for src, o in ((grad_out, g_o), (new_out, n_o), (grad_down, g_d), (new_down, n_d)):
        o[...] = src[...]
    g_u[...] = grad_up[...]
    n_u[...] = new_up[...]
    for row, outs in (
        (0, (g_mg, g_fb, g_ib, g_fg)), (1, (n_mg, n_fb, n_ib, n_fg)), (2, (s_m, s_f, s_i, s_g))
    ):
        for (_, start, count), o in zip(VECTORS, outs):
            o[...] = vectors[row, start : start + count]
    norms[...] = vectors[3, 0:10]
    for src, places, outs in (
        (rows, ROW_PLACES, (r_f, r_i, r_c, r_o, r_u, r_d)),
        (columns, COLUMN_PLACES, (c_f, c_i, c_c, c_o, c_u, c_d)),
    ):
        for (a, b), o in zip(places, outs):
            if b - a == 1:
                o[...] = src[a, 0 : o.shape[0]]
            else:
                for k in range(a, b):
                    o[(k - a) * LANES : (k - a + 1) * LANES] = src[k, :]


def finish(packed):
    sds = jax.ShapeDtypeStruct
    f = lambda *s: sds(s, F32)
    block = [f(16), f(128, 128), f(128, 128), f(128, 128), f(32), f(32), f(64, 256), f(16),
             f(128, 256), f(64, 512)]
    states = [f(16), f(128), f(128), f(128), f(128), f(128), f(128), f(32), f(32), f(256), f(64),
              f(16), f(128), f(256), f(512), f(64)]
    outs = tuple(block + block + states + [f(10)])
    vm = pl.BlockSpec(memory_space=pltpu.VMEM)
    return pl.pallas_call(
        finish_kernel,
        out_shape=outs,
        in_specs=[vm] * len(packed),
        out_specs=(vm,) * len(outs),
        name="finish",
    )(*packed)


class FusedRefs:
    def __init__(self, args):
        (
            self.tok_in, self.cot_in, self.fw, self.iw, self.cw, self.ow, self.uw, self.dw,
            self.mg, self.fbv, self.ibv, self.fg,
            self.sec_m, self.row_f, self.col_f, self.row_i, self.col_i, self.row_c, self.col_c,
            self.sec_f, self.sec_i, self.row_o, self.col_o, self.sec_g,
            self.row_u, self.col_u, self.row_d, self.col_d,
            self.block_out, self.tgrad_out,
            self.grad_mix, self.grad_out, self.grad_up, self.grad_down,
            self.new_mix, self.new_out, self.new_up, self.new_down,
            self.vectors, self.rows_out, self.columns_out,
            self.wmix, self.wot, self.wup, self.wdt, self.g1, self.g2, self.fb, self.ib,
            self.vecs, self.vstage, self.fgg, self.mgg, self.fbg, self.ibg,
            self.tok_p, self.fin, self.min_t, self.fin_t, self.cot_p, self.cot_t,
            self.resid, self.dfe,
            self.pre, self.buf, self.dpre, self.slow, self.st,
            self.keep, self.k_f, self.k_i, self.k_c,
            self.loc_s, self.mxg_s, self.mxg_r, self.mxu_s, self.mxd_s, self.mxz_r,
            self.mxp_s, self.mxp_r, self.vec_s, self.vec_r, self.ffz_s, self.ffz_r,
            self.ff2_s, self.ff2_r, self.ff3_s, self.ff3_r, self.ffp_s, self.ffp_r,
            self.vout, self.vin, self.rowst, self.rowin, self.colst, self.colin,
            self.scal, self.scin, self.clip, self.clin,
            self.rp_s, self.rp_r, self.r1_s, self.r1_r, self.r2_s, self.r2_r,
            self.r3_s, self.r3_r, self.vex_s, self.vex_r,
            self.row_s, self.row_r, self.col_s, self.col_r, self.sc_s, self.sc_r,
            self.cl_s, self.cl_r, self.io_s,
        ) = args[:119]
        rest = list(args[119:])
        self.psend, self.precv, self.r1, self.r2, self.r3, self.fin_g = (
            rest[4 * k : 4 * k + 4] for k in range(6)
        )
        self.io = self.dpre.at[:, 0:512]
        self.oacc = self.pre.at[pl.ds(4, 4)]
        self.tok = self.cot = self.block = self.tgrad = self.io
        self.min = self.fin


def halves_of(refs, plane, rows):
    size = rows.size
    low = refs.pre[plane, rows, :]
    high = refs.pre[plane, pl.ds(rows.start + 512, size), :]
    return jnp.concatenate([low, high], axis=1)


def put_halves(refs, plane, value):
    refs.pre[plane, 0:512, :] = value[:, 0:LANES]
    refs.pre[plane, 512:1024, :] = value[:, LANES : 2 * LANES]


def line_rows(z, c):
    return pl.ds(pl.multiple_of((z * 2 + c) * 64, 64), 64)


def put_feed_grads(refs, p, f):
    z, h = f // 2, f % 2
    up = dot(refs.fin_t[...], refs.dpre[:, C : 2 * C])

    @pl.when(h == p.c)
    def _():
        put_halves(refs, 0, up)

    @pl.when(h != p.c)
    def _():
        for g in range(4):
            refs.psend[UP][z, g] = up[g * 128 : (g + 1) * 128].astype(BF16)

    put_halves(refs, 1 + h, dot(refs.cot_t[...], refs.dpre[:, 0:C]))
    half = pl.ds(pl.multiple_of(h * 64, 64), 64)
    for zz in range(4):
        part = halves_of(refs, 1 + h, line_rows(zz, 1 - p.c))
        refs.psend[DOWN][z, zz, half, :] = part.astype(BF16)


def merge_up(refs, p, z):
    rs_pair(refs, p, UP, z).wait()
    for g in range(4):
        rs_merge(refs, p, UP, g, z, halves_of(refs, 0, pl.ds(g * 128, 128)))


def merge_down(refs, p, g):
    rs_pair(refs, p, DOWN, g).wait()
    for z in range(4):
        own = jnp.concatenate(
            [halves_of(refs, 1 + h, line_rows(z, p.c)) for h in range(2)], axis=0
        )
        rs_merge_at(refs, p, DOWN, g, z, own)


def rs_merge_at(refs, p, a, g, z, own):
    e = z % 2
    y, x = g // 2, g % 2
    role = (1 - e) * ((x + p.x) % 2) + e * ((y + p.y) % 2)
    place = spot(a, g, z)
    v = (own + refs.precv[a][place].astype(F32)).astype(BF16)

    @pl.when(role == 1)
    def _():
        refs.psend[a][place] = v

    @pl.when(role == 0)
    def _():
        refs.precv[a][place] = v


def put_out_grads(refs, p):
    def one(g):
        put_halves(refs, g, dot(refs.fin_t[...], refs.slow[g]))
        for z in range(4):
            part = halves_of(refs, g, line_rows(z, 1 - p.c))
            refs.psend[OUT][z, g] = part.astype(BF16)

    loop(4, one)


def merge_out(refs, p):
    rs_pair(refs, p, OUT, 0).wait()

    def one(z):
        for g in range(4):
            rs_merge(refs, p, OUT, g, z, halves_of(refs, g, line_rows(z, p.c)))

    loop(4, one)


def mix_part(refs, g, c):
    cols = []
    for j in range(3):
        q = 3 * c + j
        rows = pl.ds(pl.multiple_of((q % 2) * 512 + g * 128, 128), 128)
        cols.append(refs.pre[q // 2, rows, :])
    return jnp.concatenate(cols, axis=1)


def put_mix_grads(refs, p, z):
    for j in range(3):
        put_halves(refs, j, dot(refs.min_t[...], refs.dpre[:, j * C : (j + 1) * C]))
    for g in range(4):
        refs.psend[MIX][z, g] = mix_part(refs, g, 1 - p.c).astype(BF16)


def merge_mix(refs, p, z):
    rs_pair(refs, p, MIX, z).wait()
    for g in range(4):
        rs_merge(refs, p, MIX, g, z, mix_part(refs, g, p.c))


def all_z(body):
    loop(4, body)


def second(refs, p, a, z):
    rs_second(refs, p, a, z)
    rs_second_copy(refs, p, a, z).start()


def third(refs, p, a, z):
    rs_third(refs, p, a, z)
    rs_third_send(refs, p, a, z)


def feed_tick(refs, p, f):
    @pl.when((f % 2 == 0) & (f >= 2))
    def _():
        merge_up(refs, p, f // 2 - 1)
        merge_down(refs, p, f // 2 - 1)
        rs_first_send(refs, p, UP, f // 2 - 1)

    @pl.when((f % 2 == 0) & (f >= 4))
    def _():
        second(refs, p, UP, f // 2 - 2)

    @pl.when((f % 2 == 0) & (f >= 6))
    def _():
        third(refs, p, UP, f // 2 - 3)


def fused_kernel(*args):
    refs = FusedRefs(args)
    refs.fin_grad = refs.fin_g
    T, D = refs.tok_p.shape
    p = Place()
    load = pltpu.make_async_copy(refs.cot_in, refs.io, refs.io_s)
    load.start()
    gather_start(refs, p)
    load.wait()
    cot_in(refs, T)
    load = pltpu.make_async_copy(refs.tok_in, refs.io, refs.io_s)
    load.start()
    gather_vectors(refs, p)
    load.wait()
    norm_in(refs, T)
    mixer_slots(refs, p, T)
    mix_out(refs, T)
    clear(refs.oacc, T)
    refs.dfe[...] = jnp.zeros_like(refs.dfe)

    def feed_step(f):
        feed(refs, f, T)
        feed_tick(refs, p, f)
        put_feed_grads(refs, p, f)

        @pl.when(f % 2 == 1)
        def _():
            rs_pair(refs, p, UP, f // 2).start()
            rs_pair(refs, p, DOWN, f // 2).start()

    loop(8, feed_step)
    feed_back(refs, T)
    store = pltpu.make_async_copy(refs.io, refs.block_out, refs.io_s)
    store.start()
    merge_up(refs, p, 3)
    merge_down(refs, p, 3)
    rs_first_send(refs, p, UP, 3)
    all_z(lambda z: rs_first_send(refs, p, DOWN, z))
    second(refs, p, UP, 2)
    third(refs, p, UP, 1)
    put_out_grads(refs, p)
    rs_pair(refs, p, OUT, 0).start()
    clear(refs.oacc, T)
    store.wait()

    def chunk(n):
        return (p.z + 1 + n) % 4

    def mixer_step(n):
        z = chunk(n)
        mixer_back(refs, z, T)

        @pl.when(n == 0)
        def _():
            merge_out(refs, p)
            all_z(lambda z: rs_first_send(refs, p, OUT, z))
            all_z(lambda z: second(refs, p, DOWN, z))
            second(refs, p, UP, 3)
            third(refs, p, UP, 2)

        @pl.when(n >= 1)
        def _():
            merge_mix(refs, p, chunk(n - 1))
            rs_first_send(refs, p, MIX, chunk(n - 1))

        @pl.when(n == 1)
        def _():
            all_z(lambda z: second(refs, p, OUT, z))
            all_z(lambda z: third(refs, p, DOWN, z))
            third(refs, p, UP, 3)

        @pl.when(n >= 2)
        def _():
            second(refs, p, MIX, chunk(n - 2))

        @pl.when(n == 2)
        def _():
            all_z(lambda z: third(refs, p, OUT, z))

        @pl.when(n == 3)
        def _():
            third(refs, p, MIX, chunk(0))

        put_mix_grads(refs, p, z)
        rs_pair(refs, p, MIX, z).start()

    loop(4, mixer_step)
    norm_back(refs, T)
    store = pltpu.make_async_copy(refs.io, refs.tgrad_out, refs.io_s)
    store.start()
    merge_mix(refs, p, chunk(3))
    rs_first_send(refs, p, MIX, chunk(3))
    vector_exchange(refs, p)
    second(refs, p, MIX, chunk(2))
    third(refs, p, MIX, chunk(1))
    for a in (UP, DOWN, OUT):
        rs_last(refs, p, a)
    second(refs, p, MIX, chunk(3))
    third(refs, p, MIX, chunk(2))
    third(refs, p, MIX, chunk(3))
    rs_last(refs, p, MIX)
    rs_drain(refs, p)
    adafactor(refs, p)
    store.wait()


def fused(*args):
    T, D = args[0].shape
    Z, F = 4, 8
    sds = jax.ShapeDtypeStruct
    vm = pl.BlockSpec(memory_space=pltpu.VMEM)
    anyspec = pl.BlockSpec(memory_space=pl.ANY)
    V = pltpu.VMEM
    S = pltpu.SemaphoreType.DMA
    outs = (
        sds((T, D), BF16), sds((T, D), BF16),
        sds((128, 384), F32), sds((64, 256), F32), sds((128, 256), F32), sds((64, 512), F32),
        sds((128, 384), F32), sds((64, 256), F32), sds((128, 256), F32), sds((64, 512), F32),
        sds((8, LANES), F32), sds((16, LANES), F32), sds((8, LANES), F32),
    )
    row = V((1, LANES), F32)
    box = V((32, 1, LANES), F32)
    scratch = [
        V((Z, D, 3 * C), BF16), V((Z, D, C), BF16), V((F, D, C), BF16), V((F, D, C), BF16),
        V((1, D), F32), V((1, D), F32), V((Z, 1, C), F32), V((Z, 1, C), F32),
        box, row, V((1, D), F32), V((1, D), F32), V((Z, 1, C), F32), V((Z, 1, C), F32),
        V((T, D), BF16), V((T, D), BF16), V((D, T), BF16), V((D, T), BF16),
        V((T, D), BF16), V((D, T), BF16),
        V((D // LANES, T, LANES), F32), V((T, D), F32),
        V((8, T, LANES), F32), V((4, T, LANES), F32),
        V((T, 3 * C), BF16), V((Z, T, C), BF16), V((Z, T + SUB, C), F32),
        V((Z, T, C), F32), V((Z, T, C), F32), V((Z, T, C), F32), V((Z, T, C), F32),
        S((7,)), S((3,)), S((3,)), S((4,)), S((4,)), S((4,)),
        S((4,)), S((4,)), S(()), S(()), S((3, 3)), S((3, 4)),
        S((3, 4)), S((3, 4)), S((3, 4, 2)), S((3, 4, 2)), S((3, 4)), S((3, 4)),
        box, box, V((16, LANES), F32), V((8, 16, LANES), F32),
        V((8, LANES), F32), V((4, 8, LANES), F32), row, box, row, box,
        S((4, 4)), S((4, 4)), S((4, 4, 2)), S((4, 4, 2)), S((4, 4)), S((4, 4)),
        S((4, 4)), S((4, 4)), S(()), S(()),
        S((7,)), S((7,)), S((3,)), S((3,)), S(()), S(()), S(()), S(()), S(()),
    ]
    scratch += (
        [V((4, 4) + s, BF16) for s in SHAPES] * 2
        + [V((4, 2) + s, BF16) for s in SHAPES]
        + [V((4,) + s, BF16) for s in SHAPES] * 2
        + [V(s, F32) for s in SHAPES]
    )
    return pl.pallas_call(
        fused_kernel,
        out_shape=outs,
        in_specs=[anyspec, anyspec] + [vm] * (len(args) - 2),
        out_specs=(anyspec, anyspec) + (vm,) * (len(outs) - 2),
        scratch_shapes=scratch,
        compiler_params=pltpu.CompilerParams(
            vmem_limit_bytes=67043328, collective_id=0, has_side_effects=True
        ),
        name="fused",
    )(*args)


def gathered_layer(tok, cot, mix, ow, uw, dw, mg, fb, ib, fg):
    def whole(w):
        w = lax.all_gather(w, "inner", axis=1, tiled=True)
        return lax.all_gather(w, "grp", axis=0, tiled=True)

    def vec(v):
        return lax.all_gather(v, ("grp", "inner"), axis=0, tiled=True).astype(F32)

    width = tok.shape[1]
    inners = lax.axis_size("inner")
    Z, F = mix[0].shape[1] * inners // C, uw.shape[1] * inners // C
    gates = [whole(w).reshape(width, Z, C // LANES, 1, LANES) for w in mix]
    wmix = jnp.concatenate(gates, axis=3).reshape(width, Z, 3 * C).transpose(1, 0, 2)
    wot = whole(ow).reshape(Z, C, width).transpose(0, 2, 1)
    wup = whole(uw).reshape(width, F, C).transpose(1, 0, 2)
    wdt = whole(dw).reshape(F, C, width).transpose(0, 2, 1)
    return layer(
        tok, cot, wmix, wot, wup, wdt,
        vec(mg).reshape(1, width), vec(fg).reshape(1, width),
        vec(fb).reshape(Z, 1, C), vec(ib).reshape(Z, 1, C),
    )


def body(
    tokens,
    cotangent,
    mixer_gain,
    forget_weight,
    input_gate_weight,
    candidate_weight,
    forget_bias,
    input_bias,
    output_weight,
    feed_norm_gain,
    up_weight,
    down_weight,
    mixer_second,
    forget_rows,
    forget_columns,
    input_rows,
    input_columns,
    candidate_rows,
    candidate_columns,
    forget_second,
    input_second,
    output_rows,
    output_columns,
    feed_second,
    up_rows,
    up_columns,
    down_rows,
    down_columns,
):
    groups = lax.axis_size("grp")
    inners = lax.axis_size("inner")
    seqs, length, width = tokens.shape
    hidden = forget_weight.shape[1] * inners
    ff = up_weight.shape[1] * inners
    paired = (groups, inners) == (4, 8) and (length, width, hidden, ff) == (1024, 512, 1024, 2048)
    Z, F = hidden // C, ff // C
    if paired:
        block_output, tokens_grad, *packed = fused(
            tokens.reshape(length, width), cotangent.reshape(length, width),
            forget_weight, input_gate_weight, candidate_weight,
            output_weight.T, up_weight, down_weight.T,
            mixer_gain, forget_bias, input_bias, feed_norm_gain,
            mixer_second, forget_rows, forget_columns, input_rows, input_columns,
            candidate_rows, candidate_columns, forget_second, input_second,
            output_rows, output_columns, feed_second,
            up_rows, up_columns, down_rows, down_columns,
        )
        done = list(finish(packed))
        for k in (6, 9, 16, 19):
            done[k] = done[k].T
        return (block_output.reshape(tokens.shape), tokens_grad.reshape(tokens.shape), *done)
    results = gathered_layer(
        tokens.reshape(length, width), cotangent.reshape(length, width),
        (forget_weight, input_gate_weight, candidate_weight),
        output_weight, up_weight, down_weight,
        mixer_gain, forget_bias, input_bias, feed_norm_gain,
    )
    block_output, tokens_grad, gmix, got, gup, gdt, fgg, mgg, fbg, ibg = results
    block_output = block_output.reshape(tokens.shape)
    tokens_grad = tokens_grad.reshape(tokens.shape)
    split = gmix.transpose(1, 0, 2).reshape(width, Z, C // LANES, 3, LANES)
    forget_term, input_term, cand_term = [
        split[:, :, :, k].reshape(width, hidden) for k in range(3)
    ]
    output_term = got.transpose(0, 2, 1).reshape(hidden, width)
    up_term = gup.transpose(1, 0, 2).reshape(width, ff)
    down_term = gdt.transpose(0, 2, 1).reshape(ff, width)
    gain_first_term, gain_second_term = mgg.reshape(-1), fgg.reshape(-1)
    fbias_term, ibias_term = fbg.reshape(-1), ibg.reshape(-1)
    part = (
        lax.psum_scatter(
            gain_first_term.reshape(groups, -1), "inner", scatter_dimension=1, tiled=True
        ),
        lax.psum_scatter(forget_term, "inner", scatter_dimension=1, tiled=True),
        lax.psum_scatter(input_term, "inner", scatter_dimension=1, tiled=True),
        lax.psum_scatter(cand_term, "inner", scatter_dimension=1, tiled=True),
        lax.psum_scatter(fbias_term.reshape(groups, -1), "inner", scatter_dimension=1, tiled=True),
        lax.psum_scatter(ibias_term.reshape(groups, -1), "inner", scatter_dimension=1, tiled=True),
        lax.psum_scatter(output_term, "inner", scatter_dimension=1, tiled=True),
        lax.psum_scatter(
            gain_second_term.reshape(groups, -1), "inner", scatter_dimension=1, tiled=True
        ),
        lax.psum_scatter(up_term, "inner", scatter_dimension=1, tiled=True),
        lax.psum_scatter(down_term, "inner", scatter_dimension=1, tiled=True),
    )
    mine = (
        lax.psum_scatter(part[0], "grp", scatter_dimension=0, tiled=True),
        lax.psum_scatter(part[1], "grp", scatter_dimension=0, tiled=True),
        lax.psum_scatter(part[2], "grp", scatter_dimension=0, tiled=True),
        lax.psum_scatter(part[3], "grp", scatter_dimension=0, tiled=True),
        lax.psum_scatter(part[4], "grp", scatter_dimension=0, tiled=True),
        lax.psum_scatter(part[5], "grp", scatter_dimension=0, tiled=True),
        lax.psum_scatter(part[6], "grp", scatter_dimension=0, tiled=True),
        lax.psum_scatter(part[7], "grp", scatter_dimension=0, tiled=True),
        lax.psum_scatter(part[8], "grp", scatter_dimension=0, tiled=True),
        lax.psum_scatter(part[9], "grp", scatter_dimension=0, tiled=True),
    )
    params = [
        mixer_gain,
        forget_weight,
        input_gate_weight,
        candidate_weight,
        forget_bias,
        input_bias,
        output_weight,
        feed_norm_gain,
        up_weight,
        down_weight,
    ]
    locals_f = [p.astype(jnp.float32) for p in params]
    grads = [
        mine[0].reshape(-1),
        mine[1],
        mine[2],
        mine[3],
        mine[4].reshape(-1),
        mine[5].reshape(-1),
        mine[6],
        mine[7].reshape(-1),
        mine[8],
        mine[9],
    ]
    matrix_slots = [1, 2, 3, 6, 8, 9]
    vector_slots = [0, 4, 5, 7]
    rows_old = [forget_rows, input_rows, candidate_rows, output_rows, up_rows, down_rows]
    columns_old = [
        forget_columns,
        input_columns,
        candidate_columns,
        output_columns,
        up_columns,
        down_columns,
    ]
    seconds_old = [mixer_second, forget_second, input_second, feed_second]
    counts = [params[k].size * groups * inners for k in range(10)]
    first_inner = (lax.axis_index("inner") == 0).astype(jnp.float32)
    scales = lax.psum(
        jnp.stack(
            [jnp.sum(w * w) for w in locals_f] + [jnp.sum(r) * first_inner for r in rows_old]
        ),
        ("grp", "inner"),
    )
    mats = [grads[k] for k in matrix_slots]
    row_parts = [jnp.sum(g * g, axis=1) for g in mats]
    column_parts = [jnp.sum(g * g, axis=0) for g in mats]
    row_totals = lax.psum(
        (row_parts[0], row_parts[1], row_parts[2], row_parts[3], row_parts[4], row_parts[5]),
        "inner",
    )
    column_totals = lax.psum(
        (
            column_parts[0],
            column_parts[1],
            column_parts[2],
            column_parts[3],
            column_parts[4],
            column_parts[5],
        ),
        "grp",
    )
    grand = lax.psum(jnp.stack([jnp.sum(v) for v in row_totals]), "grp")
    scaled_all = [None] * 10
    new_states = [None] * 16
    state_places = {1: (1, 2), 2: (3, 4), 3: (5, 6), 6: (9, 10), 8: (12, 13), 9: (14, 15)}
    second_places = {0: 0, 4: 7, 5: 8, 7: 11}
    for k in range(6):
        slot = matrix_slots[k]
        grad = mats[k]
        full_rows = grad.shape[0] * groups
        full_columns = grad.shape[1] * inners
        rows = 0.5 * rows_old[k] + 0.5 * (row_totals[k] / full_columns + TINY)
        columns = 0.5 * columns_old[k] + 0.5 * (column_totals[k] / full_rows + TINY)
        row_mean = 0.5 * scales[10 + k] / full_rows + 0.5 * (
            grand[k] / (full_rows * full_columns) + TINY
        )
        scaled_all[slot] = grad * lax.rsqrt(rows[:, None] * columns[None, :] / row_mean)
        new_states[state_places[slot][0]] = rows
        new_states[state_places[slot][1]] = columns
    for k in range(4):
        slot = vector_slots[k]
        grad = grads[slot]
        second = 0.5 * seconds_old[k] + 0.5 * (grad * grad + TINY)
        scaled_all[slot] = grad * lax.rsqrt(second)
        new_states[second_places[slot]] = second
    clip = lax.psum(jnp.stack([jnp.sum(s * s) for s in scaled_all]), ("grp", "inner"))
    count_array = jnp.array(counts, jnp.float32)
    update_norms = jnp.sqrt(clip / count_array)
    fresh = [
        locals_f[k]
        + -jnp.sqrt(scales[k] / counts[k]) * scaled_all[k] / jnp.maximum(CLIP, update_norms[k])
        for k in range(10)
    ]
    return (
        block_output,
        tokens_grad,
        grads[0],
        grads[1],
        grads[2],
        grads[3],
        grads[4],
        grads[5],
        grads[6],
        grads[7],
        grads[8],
        grads[9],
        fresh[0],
        fresh[1],
        fresh[2],
        fresh[3],
        fresh[4],
        fresh[5],
        fresh[6],
        fresh[7],
        fresh[8],
        fresh[9],
        new_states[0],
        new_states[1],
        new_states[2],
        new_states[3],
        new_states[4],
        new_states[5],
        new_states[6],
        new_states[7],
        new_states[8],
        new_states[9],
        new_states[10],
        new_states[11],
        new_states[12],
        new_states[13],
        new_states[14],
        new_states[15],
        update_norms,
    )


def solution(mesh):
    return jax.shard_map(
        body,
        mesh=mesh,
        in_specs=(
            P(("grp", "inner"), None, None),
            P(("grp", "inner"), None, None),
            P(("grp", "inner")),
            P("grp", "inner"),
            P("grp", "inner"),
            P("grp", "inner"),
            P(("grp", "inner")),
            P(("grp", "inner")),
            P("grp", "inner"),
            P(("grp", "inner")),
            P("grp", "inner"),
            P("grp", "inner"),
            P(("grp", "inner")),
            P("grp"),
            P("inner"),
            P("grp"),
            P("inner"),
            P("grp"),
            P("inner"),
            P(("grp", "inner")),
            P(("grp", "inner")),
            P("grp"),
            P("inner"),
            P(("grp", "inner")),
            P("grp"),
            P("inner"),
            P("grp"),
            P("inner"),
        ),
        out_specs=(
            P(("grp", "inner"), None, None),
            P(("grp", "inner"), None, None),
            P(("grp", "inner")),
            P("grp", "inner"),
            P("grp", "inner"),
            P("grp", "inner"),
            P(("grp", "inner")),
            P(("grp", "inner")),
            P("grp", "inner"),
            P(("grp", "inner")),
            P("grp", "inner"),
            P("grp", "inner"),
            P(("grp", "inner")),
            P("grp", "inner"),
            P("grp", "inner"),
            P("grp", "inner"),
            P(("grp", "inner")),
            P(("grp", "inner")),
            P("grp", "inner"),
            P(("grp", "inner")),
            P("grp", "inner"),
            P("grp", "inner"),
            P(("grp", "inner")),
            P("grp"),
            P("inner"),
            P("grp"),
            P("inner"),
            P("grp"),
            P("inner"),
            P(("grp", "inner")),
            P(("grp", "inner")),
            P("grp"),
            P("inner"),
            P(("grp", "inner")),
            P("grp"),
            P("inner"),
            P("grp"),
            P("inner"),
            P(),
        ),
        check_vma=False,
    )
```

```python
import functools
import math
import jax
import jax.numpy as jnp
from jax import lax
from jax.experimental import pallas as pl
from jax.sharding import PartitionSpec as P
from jax.experimental.pallas import tpu as pltpu

EPS = 1e-06
F32 = jnp.float32
BF16 = jnp.bfloat16
C = 256
LANES = 128
SUB = 8
ERFC = (
    0.2256758669, 0.2256693636, 0.2078460312, 0.1685204197, 0.1415057621,
    -0.005753053848, 0.1692475449, -0.182997133, 0.05028532412,
)


def dot(a, b):
    return jnp.dot(a, b, preferred_element_type=F32)


def dot_t(a, b):
    return lax.dot_general(a, b, (((1,), (1,)), ((), ())), preferred_element_type=F32)


def loop(steps, body):
    def run(i, carry):
        body(i)
        return carry

    lax.fori_loop(0, steps, run, 0)


def at(i, size):
    return pl.ds(pl.multiple_of(i * size, size), size)


def gelu_parts(x):
    ax = jnp.abs(x)
    e = jnp.exp(-0.5 * (x * x))
    t = 1.0 / (1.0 + (0.4 * math.sqrt(0.5)) * ax)
    poly = jnp.full_like(t, ERFC[-1])
    for c in ERFC[-2::-1]:
        poly = poly * t + c
    half = 0.5 * (poly * t * e)
    cdf = jnp.where(x >= 0, 1.0 - half, half)
    return x * cdf, cdf + (x * e) * (1.0 / math.sqrt(2.0 * math.pi))


def strided(ref, j, n):
    return ref[pl.ds(j, SUB, stride=n), :]


def gather_rows(tmp, j0, n, D):
    columns = [
        jnp.concatenate([tmp[q, pl.ds(j0 + jj, SUB, stride=n), :] for jj in range(16)], axis=0)
        for q in range(D // LANES)
    ]
    return jnp.concatenate(columns, axis=1)


def scatter_rows(tmp, j0, n, out):
    for q in range(out.shape[1] // LANES):
        for jj in range(16):
            tmp[q, pl.ds(j0 + jj, SUB, stride=n), :] = out[
                jj * SUB : (jj + 1) * SUB, q * LANES : (q + 1) * LANES
            ]


def load_planes(ref, rows, start=0, count=None):
    count = ref.shape[0] if count is None else count
    return jnp.concatenate([ref[q, rows, :] for q in range(start, start + count)], axis=1)


def store_planes(ref, rows, value, start=0):
    for q in range(value.shape[1] // LANES):
        ref[start + q, rows, :] = value[:, q * LANES : (q + 1) * LANES]


def add_planes(ref, rows, value):
    for q in range(value.shape[1] // LANES):
        ref[q, rows, :] += value[:, q * LANES : (q + 1) * LANES]


def clear(ref, T):
    for q in range(4):
        ref[q, 0:T, :] = jnp.zeros((T, LANES), F32)


def norm_in(refs, T):
    n = T // SUB
    tmp, g1 = refs.buf, refs.g1
    D = g1.shape[1]

    def widen(i):
        rows = at(i, LANES)
        wide = refs.tok[rows, :].astype(F32)
        for q in range(D // LANES):
            tmp[q, rows, :] = wide[:, q * LANES : (q + 1) * LANES]

    loop(T // LANES, widen)

    def place(i):
        x = gather_rows(tmp, i * 16, n, D)
        y = x * lax.rsqrt(jnp.mean(x * x, axis=-1, keepdims=True) + EPS) * g1[...]
        rows = at(i, LANES)
        refs.tok_p[rows, :] = x.astype(BF16)
        refs.min[rows, :] = y.astype(BF16)
        refs.min_t[:, rows] = y.T.astype(BF16)

    loop(T // LANES, place)


def cot_in(refs, T):
    n = T // SUB
    tmp = refs.buf
    D = refs.g1.shape[1]

    def widen(i):
        rows = at(i, LANES)
        wide = refs.cot[rows, :].astype(F32)
        for q in range(D // LANES):
            tmp[q, rows, :] = wide[:, q * LANES : (q + 1) * LANES]

    loop(T // LANES, widen)

    def place(i):
        x = gather_rows(tmp, i * 16, n, D)
        rows = at(i, LANES)
        refs.cot_p[rows, :] = x.astype(BF16)
        refs.cot_t[:, rows] = x.T.astype(BF16)

    loop(T // LANES, place)


def mixer_forward(refs, z, T, hook=None):
    pre, ac, st = refs.pre, refs.buf, refs.st
    halves = C // LANES
    width = 3 * LANES

    def project(i):
        rows = at(i, 256)
        out = dot(refs.min[rows, :], refs.wmix[z])
        for q in range(3 * halves):
            pre[q, rows, :] = out[:, q * LANES : (q + 1) * LANES]

    loop(T // 256, project)
    fb = refs.fb[z]
    ib = refs.ib[z]

    def gates(i, carry):
        r0 = pl.multiple_of(i * 64, 64)
        out = []
        for h in range(halves):
            a, b = carry[h]
            lanes = slice(h * LANES, (h + 1) * LANES)
            pf = pre[3 * h, pl.ds(r0, 64), :] + fb[:, lanes]
            pi = pre[3 * h + 1, pl.ds(r0, 64), :] + ib[:, lanes]
            pc = pre[3 * h + 2, pl.ds(r0, 64), :]
            m = jnp.minimum(jnp.minimum(pf, pi), 0.0)
            e0 = jnp.exp(m)
            ef = jnp.exp(m - pf)
            ei = jnp.exp(m - pi)
            nk = e0 + ei
            na = e0 + ef
            inv = 1.0 / (nk + na)
            keep = nk * inv
            admit = na * inv
            not_f = 1.0 / (1.0 + jnp.exp(pf))
            not_i = 1.0 / (1.0 + jnp.exp(pi))
            ec = jnp.exp(jnp.minimum(pc, 0.0))
            sg = ec / (1.0 + ec)
            positive = pc >= 0
            value = jnp.where(positive, pc + 0.5, sg)
            slope = jnp.where(positive, 1.0, sg * (1.0 - sg))
            refs.keep[z, pl.ds(r0, 64), lanes] = keep
            refs.k_f[z, pl.ds(r0, 64), lanes] = keep * not_f
            refs.k_i[z, pl.ds(r0, 64), lanes] = keep * not_i
            refs.k_c[z, pl.ds(r0, 64), lanes] = admit * slope
            inflow = admit * value
            alist, blist = [], []
            for j in range(8):
                kj = keep[j * SUB : (j + 1) * SUB]
                b = kj * b + inflow[j * SUB : (j + 1) * SUB]
                a = kj * a
                alist.append(a)
                blist.append(b)
            ac[h, pl.ds(r0, 64), :] = jnp.concatenate(alist, axis=0)
            st[z, pl.ds(r0 + SUB, 64), lanes] = jnp.concatenate(blist, axis=0)
            out.append((a, b))
        return tuple(out)

    one = jnp.ones((SUB, LANES), F32)
    zero = jnp.zeros((SUB, LANES), F32)
    if hook is not None:
        hook(1)
    ends = lax.fori_loop(0, T // 64, gates, tuple((one, zero) for _ in range(halves)))
    if hook is not None:
        hook(2)
    for h in range(halves):
        a, b = ends[h]
        rows = [jnp.zeros((1, LANES), F32)]
        for s in range(SUB - 1):
            rows.append(a[s : s + 1] * rows[-1] + b[s : s + 1])
        st[z, 0:SUB, h * LANES : (h + 1) * LANES] = jnp.concatenate(rows, axis=0)
    first = st[z, 0:SUB, :]

    def finish(i):
        r0 = pl.multiple_of(i * 64, 64)
        a = load_planes(ac, pl.ds(r0, 64), 0, 2).reshape(8, SUB, C)
        b = st[z, pl.ds(r0 + SUB, 64), :].reshape(8, SUB, C)
        s = (b + a * first[None]).reshape(64, C)
        st[z, pl.ds(r0 + SUB, 64), :] = s
        refs.slow[z, pl.ds(r0, 64), :] = s.astype(BF16)

    loop(T // 64, finish)


def mix_out(refs, T):
    Z = refs.wot.shape[0]

    def body(i):
        rows = at(i, 256)
        acc = refs.tok_p[rows, :].astype(F32)
        for z in range(Z):
            acc = acc + dot_t(refs.slow[z, rows, :], refs.wot[z])
        store_planes(refs.resid, rows, acc)
        for k in range(2):
            x = acc[k * LANES : (k + 1) * LANES]
            y = x * lax.rsqrt(jnp.mean(x * x, axis=-1, keepdims=True) + EPS) * refs.g2[...]
            sub = pl.ds(pl.multiple_of(i * 256 + k * LANES, LANES), LANES)
            refs.fin[sub, :] = y.astype(BF16)
            refs.fin_t[:, sub] = y.T.astype(BF16)

    loop(T // 256, body)


def feed(refs, f, T):
    wup, wdt = refs.wup, refs.wdt

    def body(i):
        rows = at(i, 256)
        store_planes(refs.buf, rows, dot(refs.fin[rows, :], wup[f]))
        store_planes(refs.buf, rows, dot(refs.cot_p[rows, :], wdt[f]), 2)
        for k in range(4):
            sub = pl.ds(pl.multiple_of(i * 256 + k * 64, 64), 64)
            act, slope = gelu_parts(load_planes(refs.buf, sub, 0, 2))
            refs.dpre[sub, 0:C] = act.astype(BF16)
            refs.dpre[sub, C : 2 * C] = (load_planes(refs.buf, sub, 2, 2) * slope).astype(BF16)
        add_planes(refs.oacc, rows, dot_t(refs.dpre[rows, 0:C], wdt[f]))
        refs.dfe[rows, :] += dot_t(refs.dpre[rows, C : 2 * C], wup[f])

    loop(T // 256, body)


def feed_back(refs, T):
    n = T // SUB
    tmp = refs.buf
    D = refs.g1.shape[1]

    def body(i, total):
        rows = at(i, LANES)
        x = load_planes(refs.resid, rows)
        df = refs.dfe[rows, :]
        out = x + load_planes(refs.oacc, rows, 0, D // LANES)
        scatter_rows(tmp, i * 16, n, out)
        r = lax.rsqrt(jnp.mean(x * x, axis=-1, keepdims=True) + EPS)
        nrm = x * r
        dn = df * refs.g2[...]
        mean = jnp.mean(dn * nrm, axis=-1, keepdims=True)
        dres = refs.cot_p[rows, :].astype(F32) + r * (dn - nrm * mean)
        refs.dfe[rows, :] = dres
        refs.fin[rows, :] = dres.astype(BF16)
        refs.fin_t[:, rows] = dres.T.astype(BF16)
        return total + (df * nrm).reshape(16, SUB, D).sum(axis=0)

    total = lax.fori_loop(0, T // LANES, body, jnp.zeros((SUB, D), F32))
    refs.fgg[...] = jnp.sum(total, axis=0, keepdims=True)

    def emit(i):
        rows = at(i, LANES)
        for q in range(D // LANES):
            refs.block[rows, q * LANES : (q + 1) * LANES] = tmp[q, rows, :].astype(BF16)

    loop(T // LANES, emit)


def mixer_back(refs, z, T):
    buf, st = refs.buf, refs.st
    halves = C // LANES
    width = 3 * LANES

    def project(i):
        rows = at(i, 256)
        store_planes(buf, rows, dot(refs.fin[rows, :], refs.wot[z]))

    loop(T // 256, project)
    steps = T // 64

    def local(i, carry):
        r0 = pl.multiple_of((steps - 1 - i) * 64, 64)
        d = load_planes(buf, pl.ds(r0, 64), 0, 2)
        k = refs.keep[z, pl.ds(r0, 64), :]
        e, dk = carry
        plist, dlist = [None] * 8, [None] * 8
        for j in range(7, -1, -1):
            kj = k[j * SUB : (j + 1) * SUB]
            p = d[j * SUB : (j + 1) * SUB] + e
            plist[j] = p
            dlist[j] = dk
            e = kj * p
            dk = kj * dk
        store_planes(buf, pl.ds(r0, 64), jnp.concatenate(plist, axis=0))
        store_planes(buf, pl.ds(r0, 64), jnp.concatenate(dlist, axis=0), 2)
        return e, dk

    e, dk = lax.fori_loop(0, steps, local, (jnp.zeros((SUB, C), F32), jnp.ones((SUB, C), F32)))
    rows = [jnp.zeros((1, C), F32)]
    for s in range(SUB - 1, 0, -1):
        rows.insert(0, e[s : s + 1] + dk[s : s + 1] * rows[0])
    tail = jnp.concatenate(rows, axis=0)

    def grads(i, sums):
        r0 = pl.multiple_of(i * 64, 64)
        out = []
        for h in range(halves):
            lanes = slice(h * LANES, (h + 1) * LANES)
            sub = pl.ds(r0, 64)
            p0 = buf[h, sub, :].reshape(8, SUB, LANES)
            d0 = buf[2 + h, sub, :].reshape(8, SUB, LANES)
            p = (p0 + d0 * tail[None, :, lanes]).reshape(64, LANES)
            x = p * (st[z, pl.ds(r0 + SUB, 64), lanes] - st[z, sub, lanes])
            df = -(refs.k_f[z, sub, lanes] * x)
            di = refs.k_i[z, sub, lanes] * x
            dcand = refs.k_c[z, sub, lanes] * p
            df16 = df.astype(BF16)
            di16 = di.astype(BF16)
            refs.dpre[sub, h * width : h * width + LANES] = df16
            refs.dpre[sub, h * width + LANES : h * width + 2 * LANES] = di16
            refs.dpre[sub, h * width + 2 * LANES : h * width + 3 * LANES] = dcand.astype(BF16)
            sf, si = sums[h]
            out.append(
                (
                    sf + df16.astype(F32).reshape(8, SUB, LANES).sum(axis=0),
                    si + di16.astype(F32).reshape(8, SUB, LANES).sum(axis=0),
                )
            )
        return tuple(out)

    zero = jnp.zeros((SUB, LANES), F32)
    sums = lax.fori_loop(0, T // 64, grads, tuple((zero, zero) for _ in range(halves)))
    for h in range(halves):
        lanes = slice(h * LANES, (h + 1) * LANES)
        refs.fbg[z, :, lanes] = jnp.sum(sums[h][0], axis=0, keepdims=True)
        refs.ibg[z, :, lanes] = jnp.sum(sums[h][1], axis=0, keepdims=True)

    def back(i):
        rows = at(i, 256)
        add_planes(refs.oacc, rows, dot_t(refs.dpre[rows, :], refs.wmix[z]))

    loop(T // 256, back)


def norm_back(refs, T):
    n = T // SUB
    tmp = refs.buf
    D = refs.g1.shape[1]

    def body(i, total):
        rows = at(i, LANES)
        x = refs.tok_p[rows, :].astype(F32)
        d_in = load_planes(refs.oacc, rows, 0, D // LANES)
        r = lax.rsqrt(jnp.mean(x * x, axis=-1, keepdims=True) + EPS)
        nrm = x * r
        dn = d_in * refs.g1[...]
        mean = jnp.mean(dn * nrm, axis=-1, keepdims=True)
        out = refs.dfe[rows, :] + r * (dn - nrm * mean)
        scatter_rows(tmp, i * 16, n, out)
        return total + (d_in * nrm).reshape(16, SUB, D).sum(axis=0)

    total = lax.fori_loop(0, T // LANES, body, jnp.zeros((SUB, D), F32))
    refs.mgg[...] = jnp.sum(total, axis=0, keepdims=True)

    def emit(i):
        rows = at(i, LANES)
        for q in range(D // LANES):
            refs.tgrad[rows, q * LANES : (q + 1) * LANES] = tmp[q, rows, :].astype(BF16)

    loop(T // LANES, emit)


class Refs:
    def __init__(self, args):
        (
            self.tok, self.cot, self.wmix, self.wot, self.wup, self.wdt, self.g1, self.g2, self.fb, self.ib,
            self.block, self.tgrad, self.gmix, self.got, self.gup, self.gdt, self.fgg, self.mgg, self.fbg, self.ibg,
            self.tok_p, self.min, self.min_t, self.fin, self.fin_t, self.cot_p, self.cot_t, self.resid, self.oacc, self.dfe,
            self.pre, self.buf, self.dpre, self.slow, self.st, self.keep, self.k_f,
            self.k_i, self.k_c, self.gst, self.gsem,
        ) = args


def layer_kernel(*args):
    refs = Refs(args)
    T, D = refs.tok.shape
    Z = refs.wmix.shape[0]
    F = refs.wup.shape[0]
    gst, sem = refs.gst, refs.gsem
    cot_in(refs, T)
    norm_in(refs, T)
    loop(Z, lambda z: mixer_forward(refs, z, T))
    mix_out(refs, T)
    clear(refs.oacc, T)
    refs.dfe[...] = jnp.zeros_like(refs.dfe)

    def feed_step(f):
        feed(refs, f, T)
        gst[0, :, 0:C] = dot(refs.cot_t[...], refs.dpre[:, 0:C])
        gst[1, :, 0:C] = dot(refs.fin_t[...], refs.dpre[:, C : 2 * C])
        one = pltpu.make_async_copy(gst.at[0, :, 0:C], refs.gdt.at[f], sem.at[0])
        two = pltpu.make_async_copy(gst.at[1, :, 0:C], refs.gup.at[f], sem.at[1])
        one.start()
        two.start()
        one.wait()
        two.wait()

    loop(F, feed_step)
    feed_back(refs, T)
    clear(refs.oacc, T)

    def mixer_step(z):
        gst[0, :, 0:C] = dot(refs.fin_t[...], refs.slow[z])
        mixer_back(refs, z, T)
        gst[1, :, :] = dot(refs.min_t[...], refs.dpre[...])
        one = pltpu.make_async_copy(gst.at[0, :, 0:C], refs.got.at[z], sem.at[0])
        two = pltpu.make_async_copy(gst.at[1], refs.gmix.at[z], sem.at[1])
        one.start()
        two.start()
        one.wait()
        two.wait()

    loop(Z, mixer_step)
    norm_back(refs, T)


def layer(tok, cot, wmix, wot, wup, wdt, g1, g2, fb, ib):
    T, D = tok.shape
    Z, F = wmix.shape[0], wup.shape[0]
    sds = jax.ShapeDtypeStruct
    vm = pl.BlockSpec(memory_space=pltpu.VMEM)
    anyspec = pl.BlockSpec(memory_space=pl.ANY)
    out_shape = (
        sds((T, D), BF16), sds((T, D), BF16),
        sds((Z, D, 3 * C), F32), sds((Z, D, C), F32), sds((F, D, C), F32), sds((F, D, C), F32),
        sds((1, D), F32), sds((1, D), F32), sds((Z, 1, C), F32), sds((Z, 1, C), F32),
    )
    V = pltpu.VMEM
    scratch = [
        V((T, D), BF16), V((T, D), BF16), V((D, T), BF16), V((T, D), BF16), V((D, T), BF16),
        V((T, D), BF16), V((D, T), BF16), V((D // LANES, T, LANES), F32),
        V((D // LANES, T, LANES), F32), V((T, D), F32), V((3 * C // LANES, T, LANES), F32), V((4, T, LANES), F32),
        V((T, 3 * C), BF16), V((Z, T, C), BF16), V((Z, T + SUB, C), F32),
        V((Z, T, C), F32), V((Z, T, C), F32), V((Z, T, C), F32), V((Z, T, C), F32),
        V((2, D, 3 * C), F32), pltpu.SemaphoreType.DMA((2,)),
    ]
    return pl.pallas_call(
        layer_kernel,
        out_shape=out_shape,
        in_specs=[vm] * 10,
        out_specs=(vm, vm, anyspec, anyspec, anyspec, anyspec, vm, vm, vm, vm),
        scratch_shapes=scratch,
        compiler_params=pltpu.CompilerParams(vmem_limit_bytes=67043328),
        name="layer",
    )(tok, cot, wmix, wot, wup, wdt, g1, g2, fb, ib)


MESH = pl.DeviceIdType.MESH


def rcopy(src, dst, send, recv, device):
    return pltpu.make_async_remote_copy(
        src_ref=src, dst_ref=dst, send_sem=send, recv_sem=recv, device_id=device, device_id_type=MESH
    )


class Place:
    def __init__(self):
        self.g = lax.axis_index("grp")
        self.i = lax.axis_index("inner")
        self.y, self.x = self.g // 2, self.g % 2
        self.z, self.c = self.i // 2, self.i % 2
        self.me = self.g * 8 + self.i
        self.partner = (self.g, self.z * 2 + 1 - self.c)

    def flip(self, fx, fy):
        x = (self.x + fx) % 2
        y = (self.y + fy) % 2
        return y * 2 + x

    def near(self, z):
        e = z % 2
        return self.flip(1 - e, e)

    def far(self, z):
        e = z % 2
        return self.flip(e, 1 - e)

    def other(self, k):
        t = (self.me + k) % 32
        return (t // 8, t % 8)


def entry_barrier(place):
    barrier = pltpu.get_barrier_semaphore()

    def greet(k):
        pl.semaphore_signal(barrier, inc=1, device_id=place.other(k + 1), device_id_type=MESH)

    loop(31, greet)
    pl.semaphore_wait(barrier, 31)


def spread(values, start, count, total):
    lane = lax.broadcasted_iota(jnp.int32, (LANES, total), 1)
    row = lax.broadcasted_iota(jnp.int32, (LANES, total), 0)
    sel = jnp.where(row == start + lane % count, 1.0, 0.0).astype(BF16)
    picked = dot(values, sel)
    owner = lax.broadcasted_iota(jnp.int32, picked.shape, 0)
    spot = lax.broadcasted_iota(jnp.int32, picked.shape, 1)
    return jnp.sum(jnp.where(spot // count == owner, picked, 0.0), axis=0, keepdims=True)


def pack_vectors(mg, fb, ib, fg):
    parts = [mg, fb, ib, fg]
    used = sum(p.shape[0] for p in parts)
    rows = [p[...].astype(F32).reshape(1, p.shape[0]) for p in parts]
    return jnp.concatenate(rows + [jnp.zeros((1, LANES - used), F32)], axis=1)


FIRST = (3, 0)
LATER = (1, 2)


def block_of(refs, a, g, i):
    if a == 0:
        return refs.wot.at[g, at(i, 64), :]
    if a == 1:
        return refs.wup.at[i, at(g, 128), :]
    if a == 2:
        return refs.wdt.at[pl.ds(2 * g, 2), at(i, 64), :]
    return refs.wmix.at[i // 2, at(g, 128), at(i % 2, 384)]


def blocks_of(refs, a, i):
    if a == 0:
        return refs.wot.at[:, at(i, 64), :]
    if a == 1:
        return refs.wup.at[i]
    if a == 2:
        return refs.wdt.at[:, at(i, 64), :]
    return refs.wmix.at[i // 2, :, at(i % 2, 384)]


def line_send(refs, p, a):
    blk = block_of(refs, a, p.g, p.i)
    for s in range(1, 4):
        peer = (p.g, slot_chunk(p, s) * 2 + p.c)
        rcopy(blk, blk, refs.gz_s.at[a, s - 1], refs.gz_r.at[a, p.z], peer).start()


def near_of(p, a, z):
    return p.near(z + (a in LATER))


def far_of(p, a, z):
    return p.far(z + (a in LATER))


def line_wait(refs, p, a, z):
    @pl.when(z != p.z)
    def _():
        blk = block_of(refs, a, p.g, z * 2 + p.c)
        rcopy(blk, blk, refs.gp_s.at[a, z, 0], refs.gz_r.at[a, z], p.partner).wait_recv()


def near_send(refs, p, a, z):
    blk = block_of(refs, a, p.g, z * 2 + p.c)
    near, far = (near_of(p, a, z), p.i), (far_of(p, a, z), p.i)
    rcopy(blk, blk, refs.gn_s.at[a, z], refs.gn_r.at[a, z], near).start()
    rcopy(blk, blk, refs.gf_s.at[a, z, 0], refs.gf_r.at[a, z, 0], far).start()


def far_send(refs, p, a, z):
    near = block_of(refs, a, near_of(p, a, z), z * 2 + p.c)
    far = (far_of(p, a, z), p.i)
    rcopy(near, near, refs.gn_s.at[a, z], refs.gn_r.at[a, z], p.partner).wait_recv()
    rcopy(near, near, refs.gf_s.at[a, z, 1], refs.gf_r.at[a, z, 1], far).start()


def far_wait(refs, p, a, z, k):
    blk = block_of(refs, a, p.g, z * 2 + p.c)
    rcopy(blk, blk, refs.gf_s.at[a, z, k], refs.gf_r.at[a, z, k], p.partner).wait_recv()


def pair_copy(refs, p, a, z, c):
    full = blocks_of(refs, a, z * 2 + c)
    return rcopy(full, full, refs.gp_s.at[a, z, 0], refs.gp_r.at[a, z, 0], p.partner)


def first_step(refs, p, kind, s):
    for a in FIRST:
        z = slot_chunk(p, s)
        if kind == "n":
            line_wait(refs, p, a, z)
            near_send(refs, p, a, z)
        elif kind == "f":
            far_send(refs, p, a, z)
        elif kind == "p":
            far_wait(refs, p, a, z, 0)
            far_wait(refs, p, a, z, 1)
            pair_copy(refs, p, a, z, p.c).start()
        else:
            pair_copy(refs, p, a, z, 1 - p.c).wait_recv()


def up_step(refs, p, kind, m):
    if kind == "n":

        @pl.when(p.z != m)
        def _():
            line_wait(refs, p, 1, m)
            near_send(refs, p, 1, m)
    elif kind == "f":
        far_send(refs, p, 1, m)
    elif kind == "p":
        far_wait(refs, p, 1, m, 0)
        far_wait(refs, p, 1, m, 1)
        pair_copy(refs, p, 1, m, p.c).start()
    else:
        pair_copy(refs, p, 1, m, 1 - p.c).wait_recv()


def up_own(refs, p, phase):
    inner = (p.z + 1) // 2 % 2

    @pl.when(inner == phase)
    def _():
        near_send(refs, p, 1, p.z)


def down_pair(refs, p, z, phase, k, c):
    g = (1 + k) if phase else 3 * k
    blk = block_of(refs, 2, g, z * 2 + c)
    return rcopy(blk, blk, refs.gp_s.at[2, z, phase * 2 + k], refs.gp_r.at[2, z, phase * 2 + k], p.partner)


def down_step(refs, p, kind, phase, s):
    z = slot_chunk(p, s)
    active = (p.x + p.y) % 2 == phase
    idle = (p.x + p.y) % 2 != phase
    if kind == "n":

        @pl.when(active)
        def _():
            line_wait(refs, p, 2, z)
            near_send(refs, p, 2, z)
    elif kind == "f":

        @pl.when(idle)
        def _():
            far_send(refs, p, 2, z)
    elif kind == "p":

        @pl.when(active)
        def _():
            far_wait(refs, p, 2, z, 1)

        @pl.when(idle)
        def _():
            far_wait(refs, p, 2, z, 0)

        for k in range(2):
            down_pair(refs, p, z, phase, k, p.c).start()
    else:
        for k in range(2):
            down_pair(refs, p, z, phase, k, 1 - p.c).wait_recv()


def gather_drain(refs, p):
    for a in range(4):
        blk = block_of(refs, a, p.g, p.i)
        for k in range(3):
            rcopy(blk, blk, refs.gz_s.at[a, k], refs.gz_r.at[a, p.z], p.partner).wait_send()
        for z in range(4):
            blk = block_of(refs, a, p.g, z * 2 + p.c)
            rcopy(blk, blk, refs.gn_s.at[a, z], refs.gn_r.at[a, z], p.partner).wait_send()
            for k in range(2):
                rcopy(blk, blk, refs.gf_s.at[a, z, k], refs.gf_r.at[a, z, k], p.partner).wait_send()
            if a == 2:
                for k in range(4):
                    down_pair(refs, p, z, k // 2, k % 2, p.c).wait_send()
            else:
                pair_copy(refs, p, a, z, p.c).wait_send()


def gather_hook(refs, p, actions):
    for action in actions.split():
        kind, number = action[1], int(action[-1])
        if action[0] == "M":
            first_step(refs, p, kind, number)
        elif action[0] == "U":
            up_step(refs, p, kind, number)
        else:
            down_step(refs, p, kind, int(action[2]), number)


def gather_start(refs, p):
    local = []
    for k, w in enumerate((refs.fw, refs.iw, refs.cw)):
        spot = pl.ds(pl.multiple_of(p.c * 384 + k * 128, 128), 128)
        local.append(
            pltpu.make_async_copy(w, refs.wmix.at[p.z, at(p.g, 128), spot], refs.loc_s.at[k])
        )
    local.append(pltpu.make_async_copy(refs.ow, block_of(refs, 0, p.g, p.i), refs.loc_s.at[3]))
    local.append(pltpu.make_async_copy(refs.uw, block_of(refs, 1, p.g, p.i), refs.loc_s.at[4]))
    for k in range(2):
        local.append(
            pltpu.make_async_copy(
                refs.dw.at[:, k * 256 : (k + 1) * 256],
                refs.wdt.at[2 * p.g + k, at(p.i, 64), :],
                refs.loc_s.at[5 + k],
            )
        )
    for c in local:
        c.start()
    row = pack_vectors(refs.mg, refs.fbv, refs.ibv, refs.fg)
    refs.vstage[...] = row
    refs.vecs[p.me] = row
    for c in local:
        c.wait()
    entry_barrier(p)

    def vector(k):
        rcopy(refs.vstage, refs.vecs.at[p.me], refs.vec_s, refs.vec_r, p.other(k + 1)).start()

    for a in FIRST:
        near_send(refs, p, a, p.z)
    up_own(refs, p, 0)
    down_step(refs, p, "n", 0, 0)
    loop(31, vector)
    for a in FIRST:
        line_send(refs, p, a)
    inner = (p.z + 1) // 2 % 2

    @pl.when(inner == 0)
    def _():
        line_send(refs, p, 1)

    line_send(refs, p, 2)

    @pl.when(inner == 1)
    def _():
        line_send(refs, p, 1)


def gather_vectors(refs, p):
    rows = refs.vecs.at[pl.ds(0, 31)]
    rcopy(rows, rows, refs.vec_s, refs.vec_r, p.partner).wait()
    v = refs.vecs[...].reshape(32, LANES).astype(BF16)
    refs.g1[...] = spread(v, 0, 16, 512)
    refs.g2[...] = spread(v, 80, 16, 512)
    fb = spread(v, 16, 32, 1024)
    ib = spread(v, 48, 32, 1024)
    for z in range(4):
        refs.fb[z] = fb[:, z * C : (z + 1) * C]
        refs.ib[z] = ib[:, z * C : (z + 1) * C]


def slot_chunk(p, s):
    low = jnp.minimum(p.z, 3 - p.z)
    shift = jnp.where(s == 0, 1, jnp.where(s == 1, -1, 0))
    m = s + low * shift
    return jnp.where(p.z < 2, m, 3 - m)


SLOT_HOOKS = (
    ("", "Mf2 Dn01", "Mp1 Mf3 Un0 Un3"),
    ("Md1", "Mp2 Df00 Df01", "Dn02 Dn03 Uf0 Uf3"),
    ("Md2", "Mp3", "Df02 Df03 Dp00 Dp01"),
    ("Md3", "Un1 Un2 Dn10 Dn11 Dn12 Dn13", "Dp02 Dp03 Up0 Up3"),
)


def mixer_slots(refs, p, T):
    def hook(s, j):
        for k in range(4):

            @pl.when(s == k)
            def _():
                gather_hook(refs, p, SLOT_HOOKS[k][j])

    def slot(s):
        hook(s, 0)
        mixer_forward(refs, slot_chunk(p, s), T, lambda j: hook(s, j))

    loop(4, slot)


SHAPES = ((128, 256), (128, 256), (128, 384), (64, 256))
UP, DOWN, MIX, OUT = 0, 1, 2, 3
TINY = 1e-30
CLIP = 0.01
MATRICES = (
    (512, 1024), (512, 1024), (512, 1024), (1024, 512), (512, 2048), (2048, 512)
)
MATRIX_SLOTS = (1, 2, 3, 6, 8, 9)
VECTORS = ((0, 0, 16), (4, 16, 32), (5, 48, 32), (7, 80, 16))
COUNTS = (512, 524288, 524288, 524288, 1024, 1024, 524288, 512, 1048576, 1048576)


def spot(a, g, z):
    return (g, z) if a == DOWN else (z, g)


def rs_store(refs, a, g, z, value):
    refs.psend[a][(*spot(a, g, z),)] = value.astype(BF16)


def rs_role(p, g, z):
    e = z % 2
    y, x = g // 2, g % 2
    return (1 - e) * ((x + p.x) % 2) + e * ((y + p.y) % 2)


def rs_pair(refs, p, a, u):
    if a == OUT:
        src, dst = refs.psend[a], refs.precv[a]
    else:
        src, dst = refs.psend[a].at[u], refs.precv[a].at[u]
    return rcopy(src, dst, refs.rp_s.at[a, u], refs.rp_r.at[a, u], p.partner)


def rs_merge(refs, p, a, g, z, own):
    place = spot(a, g, z)
    v = own + refs.precv[a][place].astype(F32)
    role = rs_role(p, g, z)

    @pl.when(role == 1)
    def _():
        refs.psend[a][place] = v.astype(BF16)

    @pl.when(role == 0)
    def _():
        refs.precv[a][place] = v.astype(BF16)


def rs_group(p, z, k, sent):
    e = z % 2
    x = (1 - e) * ((p.x + sent) % 2) + e * k
    y = (1 - e) * k + e * ((p.y + sent) % 2)
    return y * 2 + x


def rs_first_copy(refs, p, a, z, k):
    g = rs_group(p, z, k, 1)
    return rcopy(
        refs.psend[a].at[spot(a, g, z)], refs.r1[a].at[z, k],
        refs.r1_s.at[a, z, k], refs.r1_r.at[a, z, k], (p.near(z), p.i),
    )


def rs_first_send(refs, p, a, z):
    for k in range(2):
        rs_first_copy(refs, p, a, z, k).start()


def rs_second(refs, p, a, z):
    e = z % 2
    mine = (1 - e) * p.y + e * p.x
    for k in range(2):
        rs_first_copy(refs, p, a, z, k).wait_recv()
    for k in range(2):
        place = spot(a, rs_group(p, z, k, 0), z)
        v = (refs.precv[a][place].astype(F32) + refs.r1[a][z, k].astype(F32)).astype(BF16)

        @pl.when(mine == k)
        def _():
            refs.precv[a][place] = v

        @pl.when(mine != k)
        def _():
            refs.psend[a][place] = v


def rs_second_copy(refs, p, a, z):
    e = z % 2
    other = 1 - ((1 - e) * p.y + e * p.x)
    place = spot(a, rs_group(p, z, other, 0), z)
    return rcopy(
        refs.psend[a].at[place], refs.r2[a].at[z], refs.r2_s.at[a, z], refs.r2_r.at[a, z],
        (p.far(z), p.i),
    )


def rs_third(refs, p, a, z):
    rs_second_copy(refs, p, a, z).wait_recv()
    place = spot(a, p.g, z)
    v = refs.precv[a][place].astype(F32) + refs.r2[a][z].astype(F32)

    @pl.when(z == p.z)
    def _():
        refs.fin_g[a][...] = v

    @pl.when(z != p.z)
    def _():
        refs.psend[a][place] = v.astype(BF16)


def rs_line(refs, p, a, z, owner):
    return rcopy(
        refs.psend[a].at[spot(a, p.g, z)], refs.r3[a].at[owner],
        refs.r3_s.at[a, z], refs.r3_r.at[a, owner], (p.g, z * 2 + p.c),
    )


def rs_third_send(refs, p, a, z):
    @pl.when(z != p.z)
    def _():
        rs_line(refs, p, a, z, p.z).start()


def rs_last(refs, p, a):
    for k in range(1, 4):
        z = (p.z + k) % 4
        rs_line(refs, p, a, z, z).wait_recv()
        refs.fin_g[a][...] += refs.r3[a][z].astype(F32)


def rs_drain(refs, p):
    def one(z):
        for a in range(4):
            for k in range(2):
                rs_first_copy(refs, p, a, z, k).wait_send()
            rs_second_copy(refs, p, a, z).wait_send()

            @pl.when(z != p.z)
            def _():
                rs_line(refs, p, a, z, p.z).wait_send()

    loop(4, one)


def own_row(x):
    return jnp.sum(x, axis=0, keepdims=True)


def lane_sum(x):
    folded = sum(x[:, k : k + LANES] for k in range(0, x.shape[1], LANES))
    return own_row(folded.T)


def wide(row):
    return jnp.concatenate([row, jnp.zeros((1, LANES - row.shape[1]), F32)], axis=1)


def cut(row):
    return [row[:, k : k + LANES] for k in range(0, row.shape[1], LANES)]


def stand(row):
    return jnp.broadcast_to(row, (LANES, LANES)).T


def scalars(values):
    lane = lax.broadcasted_iota(jnp.int32, (1, LANES), 1)
    out = jnp.zeros((1, LANES), F32)
    for k, v in enumerate(values):
        out = out + jnp.where(lane == k, v, 0.0)
    return out


def total(x):
    return jnp.sum(jnp.sum(x, axis=0, keepdims=True), axis=1, keepdims=True)


def segment(row, start, count):
    lane = lax.broadcasted_iota(jnp.int32, row.shape, 1)
    keep = (lane >= start) & (lane < start + count)
    return jnp.sum(jnp.where(keep, row, 0.0), axis=1, keepdims=True)


def gather_row(term, start, count):
    size = term.shape[1]
    owner = lax.broadcasted_iota(jnp.int32, (32, size), 0)
    spot = lax.broadcasted_iota(jnp.int32, (32, size), 1)
    masked = jnp.where(spot // count == owner, term, 0.0)
    lane = lax.broadcasted_iota(jnp.int32, (LANES, size), 0)
    from_spot = lax.broadcasted_iota(jnp.int32, (LANES, size), 1)
    sel = jnp.where(lane == start + from_spot % count, 1.0, 0.0).astype(BF16)
    out = jnp.zeros((32, LANES), F32)
    for _ in range(3):
        part = masked.astype(BF16)
        out = out + dot_t(part, sel)
        masked = masked - part.astype(F32)
    return out


def parameter_blocks(refs):
    return [
        refs.fw[...].astype(F32), refs.iw[...].astype(F32), refs.cw[...].astype(F32),
        refs.ow[...].astype(F32), refs.uw[...].astype(F32), refs.dw[...].astype(F32),
    ]


def old_rows(refs):
    rows = []
    for r in (refs.row_f, refs.row_i, refs.row_c, refs.row_o, refs.row_u, refs.row_d):
        rows += cut(r[...].reshape(1, r.shape[0]))
    return rows


def old_columns(refs):
    rows = []
    for r in (refs.col_f, refs.col_i, refs.col_c, refs.col_o, refs.col_u, refs.col_d):
        row = r[...].reshape(1, r.shape[0])
        rows += [wide(row)] if r.shape[0] < LANES else cut(row)
    return rows


ROW_PLACES = ((0, 1), (1, 2), (2, 3), (3, 5), (5, 6), (6, 10))
COLUMN_PLACES = ((0, 1), (1, 2), (2, 3), (3, 4), (4, 6), (6, 7))


def broadcast_row(src, box, send, recv, p):
    def one(k):
        rcopy(src, box.at[p.me], send, recv, p.other(k + 1)).start()

    loop(31, one)


def settle_row(box, send, recv, p):
    rows = box.at[pl.ds(0, 31)]
    rcopy(rows, rows, send, recv, p.partner).wait()


def vector_exchange(refs, p):
    rows = (
        gather_row(refs.mgg[...], 0, 16)
        + gather_row(jnp.concatenate([refs.fbg[z] for z in range(4)], axis=1), 16, 32)
        + gather_row(jnp.concatenate([refs.ibg[z] for z in range(4)], axis=1), 48, 32)
        + gather_row(refs.fgg[...], 80, 16)
    )
    refs.vout[...] = rows.reshape(32, 1, LANES)
    refs.vin[p.me] = refs.vout[p.me]

    def one(k):
        t = (p.me + k + 1) % 32
        rcopy(refs.vout.at[t], refs.vin.at[p.me], refs.vex_s, refs.vex_r, p.other(k + 1)).start()

    loop(31, one)


def gradient_blocks(refs):
    mix = refs.fin_g[MIX][...]
    down = refs.fin_g[DOWN][...]
    return [
        mix[:, 0:128], mix[:, 128:256], mix[:, 256:384], refs.fin_g[OUT][...], refs.fin_g[UP][...],
        jnp.concatenate([down[0:64], down[64:128]], axis=1),
    ]


def adafactor(refs, p):
    grads = gradient_blocks(refs)
    flipped = (False, False, False, True, False, True)
    row_parts, column_parts, totals = [], [], []
    for grad, flip in zip(grads, flipped):
        sq = grad * grad
        down, across = own_row(sq), lane_sum(sq)
        row_parts += cut(down) if flip else [across]
        column_parts += [wide(across)] if flip else cut(down)
        totals.append(jnp.sum(down, axis=1, keepdims=True))
    refs.rowst[...] = jnp.concatenate(row_parts + [jnp.zeros((6, LANES), F32)], axis=0)
    refs.colst[...] = jnp.concatenate(column_parts + [jnp.zeros((1, LANES), F32)], axis=0)
    weights = parameter_blocks(refs)
    params = pack_vectors(refs.mg, refs.fbv, refs.ibv, refs.fg)
    squares = [None] * 10
    for slot, w in zip(MATRIX_SLOTS, weights):
        squares[slot] = total(w * w)
    for slot, start, count in VECTORS:
        squares[slot] = segment(params * params, start, count)
    rows_old, columns_old = old_rows(refs), old_columns(refs)
    first = jnp.where(p.i == 0, 1.0, 0.0)
    row_sums = [first * total(jnp.concatenate(rows_old[a:b], axis=0)) for a, b in ROW_PLACES]
    refs.scal[...] = scalars(totals + squares + row_sums)
    refs.rowin[p.i] = refs.rowst[...]
    refs.colin[p.g] = refs.colst[...]
    refs.scin[p.me] = refs.scal[...]
    for k in range(1, 8):
        peer = (p.g, (p.i + k) % 8)
        rcopy(
            refs.rowst, refs.rowin.at[p.i], refs.row_s.at[k - 1], refs.row_r.at[k - 1], peer
        ).start()
    for k in range(1, 4):
        peer = ((p.g + k) % 4, p.i)
        rcopy(
            refs.colst, refs.colin.at[p.g], refs.col_s.at[k - 1], refs.col_r.at[k - 1], peer
        ).start()
    broadcast_row(refs.scal, refs.scin, refs.sc_s, refs.sc_r, p)
    vec_rows = refs.vin.at[pl.ds(0, 31)]
    rcopy(vec_rows, vec_rows, refs.vex_s, refs.vex_r, p.partner).wait()
    vector_grad = jnp.sum(refs.vin[...].reshape(32, LANES), axis=0, keepdims=True)
    seconds = pack_vectors(refs.sec_m, refs.sec_f, refs.sec_i, refs.sec_g)
    second = 0.5 * seconds + 0.5 * (vector_grad * vector_grad + TINY)
    vector_scaled = vector_grad * lax.rsqrt(second)
    for k in range(1, 8):
        rcopy(
            refs.rowst, refs.rowin.at[p.i], refs.row_s.at[k - 1], refs.row_r.at[k - 1], p.partner
        ).wait()
    for k in range(1, 4):
        rcopy(
            refs.colst, refs.colin.at[p.g], refs.col_s.at[k - 1], refs.col_r.at[k - 1], p.partner
        ).wait()
    settle_row(refs.scin, refs.sc_s, refs.sc_r, p)
    row_total = sum(refs.rowin[k] for k in range(8))
    column_total = sum(refs.colin[k] for k in range(4))
    sc = jnp.sum(refs.scin[...].reshape(32, LANES), axis=0, keepdims=True)
    rows_new, columns_new, scaled = [], [], []
    for k, (r, c) in enumerate(MATRICES):
        ra, rb = ROW_PLACES[k]
        ca, cb = COLUMN_PLACES[k]
        rows = [
            0.5 * rows_old[j] + 0.5 * (row_total[j : j + 1] / c + TINY) for j in range(ra, rb)
        ]
        columns = [
            0.5 * columns_old[j] + 0.5 * (column_total[j : j + 1] / r + TINY)
            for j in range(ca, cb)
        ]
        mean = 0.5 * sc[:, 16 + k : 17 + k] / r + 0.5 * (sc[:, k : k + 1] / (r * c) + TINY)
        lying, standing = (rows, columns) if flipped[k] else (columns, rows)
        tall = stand(standing[0])[0 : grads[k].shape[0]]
        lying = jnp.concatenate(lying, axis=1)
        tall = jnp.concatenate([tall] * (lying.shape[1] // LANES), axis=1)
        scaled.append(grads[k] * lax.rsqrt(tall * lying / mean))
        rows_new += rows
        columns_new += columns
    refs.rows_out[...] = jnp.concatenate(rows_new + [jnp.zeros((6, LANES), F32)], axis=0)
    refs.columns_out[...] = jnp.concatenate(columns_new + [jnp.zeros((1, LANES), F32)], axis=0)
    clips = [None] * 10
    for slot, s in zip(MATRIX_SLOTS, scaled):
        clips[slot] = total(s * s)
    for slot, start, count in VECTORS:
        clips[slot] = segment(vector_scaled * vector_scaled, start, count)
    refs.clip[...] = scalars(clips)
    refs.clin[p.me] = refs.clip[...]
    broadcast_row(refs.clip, refs.clin, refs.cl_s, refs.cl_r, p)
    settle_row(refs.clin, refs.cl_s, refs.cl_r, p)
    clip = jnp.sum(refs.clin[...].reshape(32, LANES), axis=0, keepdims=True)
    norms = [jnp.sqrt(clip[:, k : k + 1] / COUNTS[k]) for k in range(10)]
    steps = [
        -jnp.sqrt(sc[:, 6 + k : 7 + k] / COUNTS[k]) / jnp.maximum(CLIP, norms[k])
        for k in range(10)
    ]
    fresh = [w + steps[slot] * s for slot, w, s in zip(MATRIX_SLOTS, weights, scaled)]
    refs.grad_mix[...] = refs.fin_g[MIX][...]
    refs.grad_out[...] = grads[3]
    refs.grad_up[...] = grads[4]
    refs.grad_down[...] = grads[5]
    refs.new_mix[...] = jnp.concatenate(fresh[0:3], axis=1)
    refs.new_out[...] = fresh[3]
    refs.new_up[...] = fresh[4]
    refs.new_down[...] = fresh[5]
    lane = lax.broadcasted_iota(jnp.int32, (1, LANES), 1)
    step_row = jnp.zeros((1, LANES), F32)
    for slot, start, count in VECTORS:
        step_row = step_row + jnp.where((lane >= start) & (lane < start + count), steps[slot], 0.0)
    refs.vectors[...] = jnp.concatenate(
        [vector_grad, params + step_row * vector_scaled, second, scalars(norms)]
        + [jnp.zeros((4, LANES), F32)],
        axis=0,
    )


def finish_kernel(
    grad_mix, grad_out, grad_up, grad_down, new_mix, new_out, new_up, new_down,
    vectors, rows, columns,
    g_mg, g_f, g_i, g_c, g_fb, g_ib, g_o, g_fg, g_u, g_d,
    n_mg, n_f, n_i, n_c, n_fb, n_ib, n_o, n_fg, n_u, n_d,
    s_m, r_f, c_f, r_i, c_i, r_c, c_c, s_f, s_i, r_o, c_o, s_g, r_u, c_u, r_d, c_d, norms,
):
    for src, outs in ((grad_mix, (g_f, g_i, g_c)), (new_mix, (n_f, n_i, n_c))):
        for k, o in enumerate(outs):
            o[...] = src[:, k * 128 : (k + 1) * 128]
    for src, o in ((grad_out, g_o), (new_out, n_o), (grad_down, g_d), (new_down, n_d)):
        o[...] = src[...]
    g_u[...] = grad_up[...]
    n_u[...] = new_up[...]
    for row, outs in (
        (0, (g_mg, g_fb, g_ib, g_fg)), (1, (n_mg, n_fb, n_ib, n_fg)), (2, (s_m, s_f, s_i, s_g))
    ):
        for (_, start, count), o in zip(VECTORS, outs):
            o[...] = vectors[row, start : start + count]
    norms[...] = vectors[3, 0:10]
    for src, places, outs in (
        (rows, ROW_PLACES, (r_f, r_i, r_c, r_o, r_u, r_d)),
        (columns, COLUMN_PLACES, (c_f, c_i, c_c, c_o, c_u, c_d)),
    ):
        for (a, b), o in zip(places, outs):
            if b - a == 1:
                o[...] = src[a, 0 : o.shape[0]]
            else:
                for k in range(a, b):
                    o[(k - a) * LANES : (k - a + 1) * LANES] = src[k, :]


def finish(packed):
    sds = jax.ShapeDtypeStruct
    f = lambda *s: sds(s, F32)
    block = [f(16), f(128, 128), f(128, 128), f(128, 128), f(32), f(32), f(64, 256), f(16),
             f(128, 256), f(64, 512)]
    states = [f(16), f(128), f(128), f(128), f(128), f(128), f(128), f(32), f(32), f(256), f(64),
              f(16), f(128), f(256), f(512), f(64)]
    outs = tuple(block + block + states + [f(10)])
    vm = pl.BlockSpec(memory_space=pltpu.VMEM)
    return pl.pallas_call(
        finish_kernel,
        out_shape=outs,
        in_specs=[vm] * len(packed),
        out_specs=(vm,) * len(outs),
        name="finish",
    )(*packed)


class FusedRefs:
    def __init__(self, args):
        (
            self.tok_in, self.cot_in, self.fw, self.iw, self.cw, self.ow, self.uw, self.dw,
            self.mg, self.fbv, self.ibv, self.fg,
            self.sec_m, self.row_f, self.col_f, self.row_i, self.col_i, self.row_c, self.col_c,
            self.sec_f, self.sec_i, self.row_o, self.col_o, self.sec_g,
            self.row_u, self.col_u, self.row_d, self.col_d,
            self.block_out, self.tgrad_out,
            self.grad_mix, self.grad_out, self.grad_up, self.grad_down,
            self.new_mix, self.new_out, self.new_up, self.new_down,
            self.vectors, self.rows_out, self.columns_out,
            self.wmix, self.wot, self.wup, self.wdt, self.g1, self.g2, self.fb, self.ib,
            self.vecs, self.vstage, self.fgg, self.mgg, self.fbg, self.ibg,
            self.tok_p, self.fin, self.min_t, self.fin_t, self.cot_p, self.cot_t,
            self.resid, self.dfe,
            self.pre, self.buf, self.dpre, self.slow, self.st,
            self.keep, self.k_f, self.k_i, self.k_c,
            self.loc_s, self.vec_s, self.vec_r, self.gz_s, self.gz_r,
            self.gn_s, self.gn_r, self.gf_s, self.gf_r, self.gp_s, self.gp_r,
            self.vout, self.vin, self.rowst, self.rowin, self.colst, self.colin,
            self.scal, self.scin, self.clip, self.clin,
            self.rp_s, self.rp_r, self.r1_s, self.r1_r, self.r2_s, self.r2_r,
            self.r3_s, self.r3_r, self.vex_s, self.vex_r,
            self.row_s, self.row_r, self.col_s, self.col_r, self.sc_s, self.sc_r,
            self.cl_s, self.cl_r, self.io_s,
        ) = args[:112]
        rest = list(args[112:])
        self.psend, self.precv, self.r1, self.r2, self.r3, self.fin_g = (
            rest[4 * k : 4 * k + 4] for k in range(6)
        )
        self.io = self.dpre.at[:, 0:512]
        self.oacc = self.pre.at[pl.ds(4, 4)]
        self.tok = self.cot = self.block = self.tgrad = self.io
        self.min = self.fin


def halves_of(refs, plane, rows):
    size = rows.size
    low = refs.pre[plane, rows, :]
    high = refs.pre[plane, pl.ds(rows.start + 512, size), :]
    return jnp.concatenate([low, high], axis=1)


def put_halves(refs, plane, value):
    refs.pre[plane, 0:512, :] = value[:, 0:LANES]
    refs.pre[plane, 512:1024, :] = value[:, LANES : 2 * LANES]


def line_rows(z, c):
    return pl.ds(pl.multiple_of((z * 2 + c) * 64, 64), 64)


def put_feed_grads(refs, p, f):
    z, h = f // 2, f % 2
    up = dot(refs.fin_t[...], refs.dpre[:, C : 2 * C])

    @pl.when(h == p.c)
    def _():
        put_halves(refs, 0, up)

    @pl.when(h != p.c)
    def _():
        for g in range(4):
            refs.psend[UP][z, g] = up[g * 128 : (g + 1) * 128].astype(BF16)

    put_halves(refs, 1 + h, dot(refs.cot_t[...], refs.dpre[:, 0:C]))
    half = pl.ds(pl.multiple_of(h * 64, 64), 64)
    for zz in range(4):
        part = halves_of(refs, 1 + h, line_rows(zz, 1 - p.c))
        refs.psend[DOWN][z, zz, half, :] = part.astype(BF16)


def merge_up(refs, p, z):
    rs_pair(refs, p, UP, z).wait()
    for g in range(4):
        rs_merge(refs, p, UP, g, z, halves_of(refs, 0, pl.ds(g * 128, 128)))


def merge_down(refs, p, g):
    rs_pair(refs, p, DOWN, g).wait()
    for z in range(4):
        own = jnp.concatenate(
            [halves_of(refs, 1 + h, line_rows(z, p.c)) for h in range(2)], axis=0
        )
        rs_merge_at(refs, p, DOWN, g, z, own)


def rs_merge_at(refs, p, a, g, z, own):
    e = z % 2
    y, x = g // 2, g % 2
    role = (1 - e) * ((x + p.x) % 2) + e * ((y + p.y) % 2)
    place = spot(a, g, z)
    v = (own + refs.precv[a][place].astype(F32)).astype(BF16)

    @pl.when(role == 1)
    def _():
        refs.psend[a][place] = v

    @pl.when(role == 0)
    def _():
        refs.precv[a][place] = v


def put_out_grads(refs, p):
    def one(g):
        put_halves(refs, g, dot(refs.fin_t[...], refs.slow[g]))
        for z in range(4):
            part = halves_of(refs, g, line_rows(z, 1 - p.c))
            refs.psend[OUT][z, g] = part.astype(BF16)

    loop(4, one)


def merge_out(refs, p):
    rs_pair(refs, p, OUT, 0).wait()

    def one(z):
        for g in range(4):
            rs_merge(refs, p, OUT, g, z, halves_of(refs, g, line_rows(z, p.c)))

    loop(4, one)


def mix_part(refs, g, c):
    cols = []
    for j in range(3):
        q = 3 * c + j
        rows = pl.ds(pl.multiple_of((q % 2) * 512 + g * 128, 128), 128)
        cols.append(refs.pre[q // 2, rows, :])
    return jnp.concatenate(cols, axis=1)


def put_mix_grads(refs, p, z):
    for j in range(3):
        put_halves(refs, j, dot(refs.min_t[...], refs.dpre[:, j * C : (j + 1) * C]))
    for g in range(4):
        refs.psend[MIX][z, g] = mix_part(refs, g, 1 - p.c).astype(BF16)


def merge_mix(refs, p, z):
    rs_pair(refs, p, MIX, z).wait()
    for g in range(4):
        rs_merge(refs, p, MIX, g, z, mix_part(refs, g, p.c))


def all_z(body):
    loop(4, body)


def second(refs, p, a, z):
    rs_second(refs, p, a, z)
    rs_second_copy(refs, p, a, z).start()


def third(refs, p, a, z):
    rs_third(refs, p, a, z)
    rs_third_send(refs, p, a, z)


def feed_order(k):
    return jnp.where(k == 1, 3, jnp.where(k >= 2, k - 1, 0))


def feed_tick(refs, p, f):
    @pl.when((f % 2 == 0) & (f >= 2))
    def _():
        last = feed_order(f // 2 - 1)
        merge_up(refs, p, last)
        merge_down(refs, p, last)
        rs_first_send(refs, p, UP, last)

    @pl.when((f % 2 == 0) & (f >= 4))
    def _():
        second(refs, p, UP, feed_order(f // 2 - 2))

    @pl.when((f % 2 == 0) & (f >= 6))
    def _():
        third(refs, p, UP, feed_order(f // 2 - 3))


def fused_kernel(*args):
    refs = FusedRefs(args)
    refs.fin_grad = refs.fin_g
    T, D = refs.tok_p.shape
    p = Place()
    load = pltpu.make_async_copy(refs.cot_in, refs.io, refs.io_s)
    load.start()
    gather_start(refs, p)
    load.wait()
    cot_in(refs, T)
    load = pltpu.make_async_copy(refs.tok_in, refs.io, refs.io_s)
    load.start()
    gather_vectors(refs, p)
    load.wait()
    norm_in(refs, T)
    gather_hook(refs, p, "Mf0 Mn1 Mn2 Mf1 Mp0 Mn3 Md0")
    mixer_slots(refs, p, T)
    up_own(refs, p, 1)
    mix_out(refs, T)
    gather_hook(refs, p, "Ud0 Ud3 Dd00 Dd01 Dd02 Dd03")
    clear(refs.oacc, T)
    refs.dfe[...] = jnp.zeros_like(refs.dfe)

    def feed_step(f):
        @pl.when(f == 4)
        def _():
            gather_hook(refs, p, "Ud1 Ud2 Dd10 Dd11 Dd12 Dd13")

        feed(refs, feed_order(f // 2) * 2 + f % 2, T)

        @pl.when(f == 0)
        def _():
            gather_hook(refs, p, "Uf1 Uf2 Df10 Df11 Df12 Df13")

        @pl.when(f == 1)
        def _():
            gather_hook(refs, p, "Up1 Up2 Dp10 Dp11 Dp12 Dp13")

        feed_tick(refs, p, f)
        put_feed_grads(refs, p, feed_order(f // 2) * 2 + f % 2)

        @pl.when(f % 2 == 1)
        def _():
            rs_pair(refs, p, UP, feed_order(f // 2)).start()
            rs_pair(refs, p, DOWN, feed_order(f // 2)).start()

    loop(8, feed_step)
    feed_back(refs, T)
    store = pltpu.make_async_copy(refs.io, refs.block_out, refs.io_s)
    store.start()
    gather_drain(refs, p)
    merge_up(refs, p, 2)
    merge_down(refs, p, 2)
    rs_first_send(refs, p, UP, 2)
    all_z(lambda z: rs_first_send(refs, p, DOWN, z))
    second(refs, p, UP, 1)
    third(refs, p, UP, 3)
    put_out_grads(refs, p)
    rs_pair(refs, p, OUT, 0).start()
    clear(refs.oacc, T)
    store.wait()

    def chunk(n):
        return (p.z + 1 + n) % 4

    def mixer_step(n):
        z = chunk(n)
        mixer_back(refs, z, T)

        @pl.when(n == 0)
        def _():
            merge_out(refs, p)
            all_z(lambda z: rs_first_send(refs, p, OUT, z))
            all_z(lambda z: second(refs, p, DOWN, z))
            second(refs, p, UP, 2)
            third(refs, p, UP, 1)

        @pl.when(n >= 1)
        def _():
            merge_mix(refs, p, chunk(n - 1))
            rs_first_send(refs, p, MIX, chunk(n - 1))

        @pl.when(n == 1)
        def _():
            all_z(lambda z: second(refs, p, OUT, z))
            all_z(lambda z: third(refs, p, DOWN, z))
            third(refs, p, UP, 2)

        @pl.when(n >= 2)
        def _():
            second(refs, p, MIX, chunk(n - 2))

        @pl.when(n == 2)
        def _():
            all_z(lambda z: third(refs, p, OUT, z))

        @pl.when(n == 3)
        def _():
            third(refs, p, MIX, chunk(0))

        put_mix_grads(refs, p, z)
        rs_pair(refs, p, MIX, z).start()

    loop(4, mixer_step)
    norm_back(refs, T)
    store = pltpu.make_async_copy(refs.io, refs.tgrad_out, refs.io_s)
    store.start()
    merge_mix(refs, p, chunk(3))
    rs_first_send(refs, p, MIX, chunk(3))
    vector_exchange(refs, p)
    second(refs, p, MIX, chunk(2))
    third(refs, p, MIX, chunk(1))
    for a in (UP, DOWN, OUT):
        rs_last(refs, p, a)
    second(refs, p, MIX, chunk(3))
    third(refs, p, MIX, chunk(2))
    third(refs, p, MIX, chunk(3))
    rs_last(refs, p, MIX)
    rs_drain(refs, p)
    adafactor(refs, p)
    store.wait()


def fused(*args):
    T, D = args[0].shape
    Z, F = 4, 8
    sds = jax.ShapeDtypeStruct
    vm = pl.BlockSpec(memory_space=pltpu.VMEM)
    anyspec = pl.BlockSpec(memory_space=pl.ANY)
    V = pltpu.VMEM
    S = pltpu.SemaphoreType.DMA
    outs = (
        sds((T, D), BF16), sds((T, D), BF16),
        sds((128, 384), F32), sds((64, 256), F32), sds((128, 256), F32), sds((64, 512), F32),
        sds((128, 384), F32), sds((64, 256), F32), sds((128, 256), F32), sds((64, 512), F32),
        sds((8, LANES), F32), sds((16, LANES), F32), sds((8, LANES), F32),
    )
    row = V((1, LANES), F32)
    box = V((32, 1, LANES), F32)
    scratch = [
        V((Z, D, 3 * C), BF16), V((Z, D, C), BF16), V((F, D, C), BF16), V((F, D, C), BF16),
        V((1, D), F32), V((1, D), F32), V((Z, 1, C), F32), V((Z, 1, C), F32),
        box, row, V((1, D), F32), V((1, D), F32), V((Z, 1, C), F32), V((Z, 1, C), F32),
        V((T, D), BF16), V((T, D), BF16), V((D, T), BF16), V((D, T), BF16),
        V((T, D), BF16), V((D, T), BF16),
        V((D // LANES, T, LANES), F32), V((T, D), F32),
        V((8, T, LANES), F32), V((4, T, LANES), F32),
        V((T, 3 * C), BF16), V((Z, T, C), BF16), V((Z, T + SUB, C), F32),
        V((Z, T, C), F32), V((Z, T, C), F32), V((Z, T, C), F32), V((Z, T, C), F32),
        S((7,)), S(()), S(()), S((4, 3)), S((4, 4)),
        S((4, 4)), S((4, 4)), S((4, 4, 2)), S((4, 4, 2)), S((4, 4, 4)), S((4, 4, 4)),
        box, box, V((16, LANES), F32), V((8, 16, LANES), F32),
        V((8, LANES), F32), V((4, 8, LANES), F32), row, box, row, box,
        S((4, 4)), S((4, 4)), S((4, 4, 2)), S((4, 4, 2)), S((4, 4)), S((4, 4)),
        S((4, 4)), S((4, 4)), S(()), S(()),
        S((7,)), S((7,)), S((3,)), S((3,)), S(()), S(()), S(()), S(()), S(()),
    ]
    scratch += (
        [V((4, 4) + s, BF16) for s in SHAPES] * 2
        + [V((4, 2) + s, BF16) for s in SHAPES]
        + [V((4,) + s, BF16) for s in SHAPES] * 2
        + [V(s, F32) for s in SHAPES]
    )
    return pl.pallas_call(
        fused_kernel,
        out_shape=outs,
        in_specs=[anyspec, anyspec] + [vm] * (len(args) - 2),
        out_specs=(anyspec, anyspec) + (vm,) * (len(outs) - 2),
        scratch_shapes=scratch,
        compiler_params=pltpu.CompilerParams(
            vmem_limit_bytes=67043328, collective_id=0, has_side_effects=True
        ),
        name="fused",
    )(*args)


def gathered_layer(tok, cot, mix, ow, uw, dw, mg, fb, ib, fg):
    def whole(w):
        w = lax.all_gather(w, "inner", axis=1, tiled=True)
        return lax.all_gather(w, "grp", axis=0, tiled=True)

    def vec(v):
        return lax.all_gather(v, ("grp", "inner"), axis=0, tiled=True).astype(F32)

    width = tok.shape[1]
    inners = lax.axis_size("inner")
    Z, F = mix[0].shape[1] * inners // C, uw.shape[1] * inners // C
    gates = [whole(w).reshape(width, Z, C // LANES, 1, LANES) for w in mix]
    wmix = jnp.concatenate(gates, axis=3).reshape(width, Z, 3 * C).transpose(1, 0, 2)
    wot = whole(ow).reshape(Z, C, width).transpose(0, 2, 1)
    wup = whole(uw).reshape(width, F, C).transpose(1, 0, 2)
    wdt = whole(dw).reshape(F, C, width).transpose(0, 2, 1)
    return layer(
        tok, cot, wmix, wot, wup, wdt,
        vec(mg).reshape(1, width), vec(fg).reshape(1, width),
        vec(fb).reshape(Z, 1, C), vec(ib).reshape(Z, 1, C),
    )


def body(
    tokens,
    cotangent,
    mixer_gain,
    forget_weight,
    input_gate_weight,
    candidate_weight,
    forget_bias,
    input_bias,
    output_weight,
    feed_norm_gain,
    up_weight,
    down_weight,
    mixer_second,
    forget_rows,
    forget_columns,
    input_rows,
    input_columns,
    candidate_rows,
    candidate_columns,
    forget_second,
    input_second,
    output_rows,
    output_columns,
    feed_second,
    up_rows,
    up_columns,
    down_rows,
    down_columns,
):
    groups = lax.axis_size("grp")
    inners = lax.axis_size("inner")
    seqs, length, width = tokens.shape
    hidden = forget_weight.shape[1] * inners
    ff = up_weight.shape[1] * inners
    paired = (groups, inners) == (4, 8) and (length, width, hidden, ff) == (1024, 512, 1024, 2048)
    Z, F = hidden // C, ff // C
    if paired:
        block_output, tokens_grad, *packed = fused(
            tokens.reshape(length, width), cotangent.reshape(length, width),
            forget_weight, input_gate_weight, candidate_weight,
            output_weight.T, up_weight, down_weight.T,
            mixer_gain, forget_bias, input_bias, feed_norm_gain,
            mixer_second, forget_rows, forget_columns, input_rows, input_columns,
            candidate_rows, candidate_columns, forget_second, input_second,
            output_rows, output_columns, feed_second,
            up_rows, up_columns, down_rows, down_columns,
        )
        done = list(finish(packed))
        for k in (6, 9, 16, 19):
            done[k] = done[k].T
        return (block_output.reshape(tokens.shape), tokens_grad.reshape(tokens.shape), *done)
    results = gathered_layer(
        tokens.reshape(length, width), cotangent.reshape(length, width),
        (forget_weight, input_gate_weight, candidate_weight),
        output_weight, up_weight, down_weight,
        mixer_gain, forget_bias, input_bias, feed_norm_gain,
    )
    block_output, tokens_grad, gmix, got, gup, gdt, fgg, mgg, fbg, ibg = results
    block_output = block_output.reshape(tokens.shape)
    tokens_grad = tokens_grad.reshape(tokens.shape)
    split = gmix.transpose(1, 0, 2).reshape(width, Z, C // LANES, 3, LANES)
    forget_term, input_term, cand_term = [
        split[:, :, :, k].reshape(width, hidden) for k in range(3)
    ]
    output_term = got.transpose(0, 2, 1).reshape(hidden, width)
    up_term = gup.transpose(1, 0, 2).reshape(width, ff)
    down_term = gdt.transpose(0, 2, 1).reshape(ff, width)
    gain_first_term, gain_second_term = mgg.reshape(-1), fgg.reshape(-1)
    fbias_term, ibias_term = fbg.reshape(-1), ibg.reshape(-1)
    part = (
        lax.psum_scatter(
            gain_first_term.reshape(groups, -1), "inner", scatter_dimension=1, tiled=True
        ),
        lax.psum_scatter(forget_term, "inner", scatter_dimension=1, tiled=True),
        lax.psum_scatter(input_term, "inner", scatter_dimension=1, tiled=True),
        lax.psum_scatter(cand_term, "inner", scatter_dimension=1, tiled=True),
        lax.psum_scatter(fbias_term.reshape(groups, -1), "inner", scatter_dimension=1, tiled=True),
        lax.psum_scatter(ibias_term.reshape(groups, -1), "inner", scatter_dimension=1, tiled=True),
        lax.psum_scatter(output_term, "inner", scatter_dimension=1, tiled=True),
        lax.psum_scatter(
            gain_second_term.reshape(groups, -1), "inner", scatter_dimension=1, tiled=True
        ),
        lax.psum_scatter(up_term, "inner", scatter_dimension=1, tiled=True),
        lax.psum_scatter(down_term, "inner", scatter_dimension=1, tiled=True),
    )
    mine = (
        lax.psum_scatter(part[0], "grp", scatter_dimension=0, tiled=True),
        lax.psum_scatter(part[1], "grp", scatter_dimension=0, tiled=True),
        lax.psum_scatter(part[2], "grp", scatter_dimension=0, tiled=True),
        lax.psum_scatter(part[3], "grp", scatter_dimension=0, tiled=True),
        lax.psum_scatter(part[4], "grp", scatter_dimension=0, tiled=True),
        lax.psum_scatter(part[5], "grp", scatter_dimension=0, tiled=True),
        lax.psum_scatter(part[6], "grp", scatter_dimension=0, tiled=True),
        lax.psum_scatter(part[7], "grp", scatter_dimension=0, tiled=True),
        lax.psum_scatter(part[8], "grp", scatter_dimension=0, tiled=True),
        lax.psum_scatter(part[9], "grp", scatter_dimension=0, tiled=True),
    )
    params = [
        mixer_gain,
        forget_weight,
        input_gate_weight,
        candidate_weight,
        forget_bias,
        input_bias,
        output_weight,
        feed_norm_gain,
        up_weight,
        down_weight,
    ]
    locals_f = [p.astype(jnp.float32) for p in params]
    grads = [
        mine[0].reshape(-1),
        mine[1],
        mine[2],
        mine[3],
        mine[4].reshape(-1),
        mine[5].reshape(-1),
        mine[6],
        mine[7].reshape(-1),
        mine[8],
        mine[9],
    ]
    matrix_slots = [1, 2, 3, 6, 8, 9]
    vector_slots = [0, 4, 5, 7]
    rows_old = [forget_rows, input_rows, candidate_rows, output_rows, up_rows, down_rows]
    columns_old = [
        forget_columns,
        input_columns,
        candidate_columns,
        output_columns,
        up_columns,
        down_columns,
    ]
    seconds_old = [mixer_second, forget_second, input_second, feed_second]
    counts = [params[k].size * groups * inners for k in range(10)]
    first_inner = (lax.axis_index("inner") == 0).astype(jnp.float32)
    scales = lax.psum(
        jnp.stack(
            [jnp.sum(w * w) for w in locals_f] + [jnp.sum(r) * first_inner for r in rows_old]
        ),
        ("grp", "inner"),
    )
    mats = [grads[k] for k in matrix_slots]
    row_parts = [jnp.sum(g * g, axis=1) for g in mats]
    column_parts = [jnp.sum(g * g, axis=0) for g in mats]
    row_totals = lax.psum(
        (row_parts[0], row_parts[1], row_parts[2], row_parts[3], row_parts[4], row_parts[5]),
        "inner",
    )
    column_totals = lax.psum(
        (
            column_parts[0],
            column_parts[1],
            column_parts[2],
            column_parts[3],
            column_parts[4],
            column_parts[5],
        ),
        "grp",
    )
    grand = lax.psum(jnp.stack([jnp.sum(v) for v in row_totals]), "grp")
    scaled_all = [None] * 10
    new_states = [None] * 16
    state_places = {1: (1, 2), 2: (3, 4), 3: (5, 6), 6: (9, 10), 8: (12, 13), 9: (14, 15)}
    second_places = {0: 0, 4: 7, 5: 8, 7: 11}
    for k in range(6):
        slot = matrix_slots[k]
        grad = mats[k]
        full_rows = grad.shape[0] * groups
        full_columns = grad.shape[1] * inners
        rows = 0.5 * rows_old[k] + 0.5 * (row_totals[k] / full_columns + TINY)
        columns = 0.5 * columns_old[k] + 0.5 * (column_totals[k] / full_rows + TINY)
        row_mean = 0.5 * scales[10 + k] / full_rows + 0.5 * (
            grand[k] / (full_rows * full_columns) + TINY
        )
        scaled_all[slot] = grad * lax.rsqrt(rows[:, None] * columns[None, :] / row_mean)
        new_states[state_places[slot][0]] = rows
        new_states[state_places[slot][1]] = columns
    for k in range(4):
        slot = vector_slots[k]
        grad = grads[slot]
        second = 0.5 * seconds_old[k] + 0.5 * (grad * grad + TINY)
        scaled_all[slot] = grad * lax.rsqrt(second)
        new_states[second_places[slot]] = second
    clip = lax.psum(jnp.stack([jnp.sum(s * s) for s in scaled_all]), ("grp", "inner"))
    count_array = jnp.array(counts, jnp.float32)
    update_norms = jnp.sqrt(clip / count_array)
    fresh = [
        locals_f[k]
        + -jnp.sqrt(scales[k] / counts[k]) * scaled_all[k] / jnp.maximum(CLIP, update_norms[k])
        for k in range(10)
    ]
    return (
        block_output,
        tokens_grad,
        grads[0],
        grads[1],
        grads[2],
        grads[3],
        grads[4],
        grads[5],
        grads[6],
        grads[7],
        grads[8],
        grads[9],
        fresh[0],
        fresh[1],
        fresh[2],
        fresh[3],
        fresh[4],
        fresh[5],
        fresh[6],
        fresh[7],
        fresh[8],
        fresh[9],
        new_states[0],
        new_states[1],
        new_states[2],
        new_states[3],
        new_states[4],
        new_states[5],
        new_states[6],
        new_states[7],
        new_states[8],
        new_states[9],
        new_states[10],
        new_states[11],
        new_states[12],
        new_states[13],
        new_states[14],
        new_states[15],
        update_norms,
    )


def solution(mesh):
    return jax.shard_map(
        body,
        mesh=mesh,
        in_specs=(
            P(("grp", "inner"), None, None),
            P(("grp", "inner"), None, None),
            P(("grp", "inner")),
            P("grp", "inner"),
            P("grp", "inner"),
            P("grp", "inner"),
            P(("grp", "inner")),
            P(("grp", "inner")),
            P("grp", "inner"),
            P(("grp", "inner")),
            P("grp", "inner"),
            P("grp", "inner"),
            P(("grp", "inner")),
            P("grp"),
            P("inner"),
            P("grp"),
            P("inner"),
            P("grp"),
            P("inner"),
            P(("grp", "inner")),
            P(("grp", "inner")),
            P("grp"),
            P("inner"),
            P(("grp", "inner")),
            P("grp"),
            P("inner"),
            P("grp"),
            P("inner"),
        ),
        out_specs=(
            P(("grp", "inner"), None, None),
            P(("grp", "inner"), None, None),
            P(("grp", "inner")),
            P("grp", "inner"),
            P("grp", "inner"),
            P("grp", "inner"),
            P(("grp", "inner")),
            P(("grp", "inner")),
            P("grp", "inner"),
            P(("grp", "inner")),
            P("grp", "inner"),
            P("grp", "inner"),
            P(("grp", "inner")),
            P("grp", "inner"),
            P("grp", "inner"),
            P("grp", "inner"),
            P(("grp", "inner")),
            P(("grp", "inner")),
            P("grp", "inner"),
            P(("grp", "inner")),
            P("grp", "inner"),
            P("grp", "inner"),
            P(("grp", "inner")),
            P("grp"),
            P("inner"),
            P("grp"),
            P("inner"),
            P("grp"),
            P("inner"),
            P(("grp", "inner")),
            P(("grp", "inner")),
            P("grp"),
            P("inner"),
            P(("grp", "inner")),
            P("grp"),
            P("inner"),
            P("grp"),
            P("inner"),
            P(),
        ),
        check_vma=False,
    )
```

```python
import functools
import math
import jax
import jax.numpy as jnp
from jax import lax
from jax.experimental import pallas as pl
from jax.sharding import PartitionSpec as P
from jax.experimental.pallas import tpu as pltpu

EPS = 1e-06
F32 = jnp.float32
BF16 = jnp.bfloat16
C = 256
LANES = 128
SUB = 8
ERFC = (
    0.2256758669, 0.2256693636, 0.2078460312, 0.1685204197, 0.1415057621,
    -0.005753053848, 0.1692475449, -0.182997133, 0.05028532412,
)


def dot(a, b):
    return jnp.dot(a, b, preferred_element_type=F32)


def dot_t(a, b):
    return lax.dot_general(a, b, (((1,), (1,)), ((), ())), preferred_element_type=F32)


def loop(steps, body):
    def run(i, carry):
        body(i)
        return carry

    lax.fori_loop(0, steps, run, 0)


def at(i, size):
    return pl.ds(pl.multiple_of(i * size, size), size)


def gelu_parts(x):
    e = jnp.exp2((x * x) * (-0.5 / math.log(2.0)))
    t = 1.0 / (1.0 + (0.4 * math.sqrt(0.5)) * jnp.abs(x))
    poly = jnp.full_like(t, 0.5 * ERFC[-1])
    for c in ERFC[-2::-1]:
        poly = poly * t + 0.5 * c
    half = poly * (t * e)
    cdf = jnp.where(x >= 0, 1.0 - half, half)
    return x * cdf, cdf + (x * e) * (1.0 / math.sqrt(2.0 * math.pi))


def gather_rows(tmp, j0, n, D):
    columns = [
        jnp.concatenate([tmp[q, pl.ds(j0 + jj, SUB, stride=n), :] for jj in range(16)], axis=0)
        for q in range(D // LANES)
    ]
    return jnp.concatenate(columns, axis=1)


def scatter_rows(tmp, j0, n, out):
    for q in range(out.shape[1] // LANES):
        for jj in range(16):
            tmp[q, pl.ds(j0 + jj, SUB, stride=n), :] = out[
                jj * SUB : (jj + 1) * SUB, q * LANES : (q + 1) * LANES
            ]


LOG2E = 1.0 / math.log(2.0)


def load_planes(ref, rows, start=0, count=None):
    count = ref.shape[0] if count is None else count
    return jnp.concatenate([ref[q, rows, :] for q in range(start, start + count)], axis=1)


def store_planes(ref, rows, value, start=0):
    for q in range(value.shape[1] // LANES):
        ref[start + q, rows, :] = value[:, q * LANES : (q + 1) * LANES]


def add_planes(ref, rows, value):
    for q in range(value.shape[1] // LANES):
        ref[q, rows, :] += value[:, q * LANES : (q + 1) * LANES]


def clear(ref, T):
    for q in range(4):
        ref[q, 0:T, :] = jnp.zeros((T, LANES), F32)


def norm_in(refs, T):
    n = T // SUB
    tmp, g1 = refs.buf, refs.g1
    D = g1.shape[1]

    def widen(i):
        rows = at(i, LANES)
        wide = refs.tok[rows, :].astype(F32)
        for q in range(D // LANES):
            tmp[q, rows, :] = wide[:, q * LANES : (q + 1) * LANES]

    loop(T // LANES, widen)

    def place(i):
        x = gather_rows(tmp, i * 16, n, D)
        y = x * lax.rsqrt(jnp.mean(x * x, axis=-1, keepdims=True) + EPS) * g1[...]
        rows = at(i, LANES)
        refs.tok_p[rows, :] = x.astype(BF16)
        refs.min[rows, :] = y.astype(BF16)
        refs.min_t[:, rows] = y.T.astype(BF16)

    loop(T // LANES, place)


def cot_in(refs, T):
    n = T // SUB
    tmp = refs.buf
    D = refs.g1.shape[1]

    def widen(i):
        rows = at(i, LANES)
        wide = refs.cot[rows, :].astype(F32)
        for q in range(D // LANES):
            tmp[q, rows, :] = wide[:, q * LANES : (q + 1) * LANES]

    loop(T // LANES, widen)

    def place(i):
        x = gather_rows(tmp, i * 16, n, D)
        rows = at(i, LANES)
        refs.cot_p[rows, :] = x.astype(BF16)
        refs.cot_t[:, rows] = x.T.astype(BF16)

    loop(T // LANES, place)


def mixer_forward(refs, z, T, hook=None):
    pre, ac, st = refs.pre, refs.buf, refs.st
    halves = C // LANES
    width = 3 * LANES

    def project(i):
        rows = at(i, 256)
        out = dot(refs.min[rows, :], refs.wmix[z])
        for q in range(3 * halves):
            pre[q, rows, :] = out[:, q * LANES : (q + 1) * LANES]

    loop(T // 256, project)
    fb = refs.fb[z]
    ib = refs.ib[z]

    def gates(i, carry):
        r0 = pl.multiple_of(i * 64, 64)
        out = []
        for h in range(halves):
            a, b = carry[h]
            lanes = slice(h * LANES, (h + 1) * LANES)
            pf = pre[3 * h, pl.ds(r0, 64), :] + fb[:, lanes]
            pi = pre[3 * h + 1, pl.ds(r0, 64), :] + ib[:, lanes]
            pc = pre[3 * h + 2, pl.ds(r0, 64), :]
            pf, pi = pf * LOG2E, pi * LOG2E
            m = jnp.minimum(jnp.minimum(pf, pi), 0.0)
            e0 = jnp.exp2(m)
            ef = jnp.exp2(m - pf)
            ei = jnp.exp2(m - pi)
            nk = e0 + ei
            na = e0 + ef
            both = nk + na
            floor = jnp.maximum(na, 1e-37)
            rec = 1.0 / (both * floor)
            inv = rec * floor
            keep = nk * inv
            admit = na * inv
            ec = jnp.exp(jnp.minimum(pc, 0.0))
            sg = ec / (1.0 + ec)
            positive = pc >= 0
            value = jnp.where(positive, pc + 0.5, sg)
            slope = jnp.where(positive, 1.0, sg * (1.0 - sg))
            refs.keep[z, pl.ds(r0, 64), lanes] = keep
            refs.k_f[z, pl.ds(r0, 64), lanes] = keep * (ef * (rec * both))
            refs.k_i[z, pl.ds(r0, 64), lanes] = ei * inv
            refs.k_c[z, pl.ds(r0, 64), lanes] = admit * slope
            inflow = admit * value
            alist, blist = [], []
            for j in range(8):
                kj = keep[j * SUB : (j + 1) * SUB]
                b = kj * b + inflow[j * SUB : (j + 1) * SUB]
                a = kj * a
                alist.append(a)
                blist.append(b)
            ac[h, pl.ds(r0, 64), :] = jnp.concatenate(alist, axis=0)
            st[z, pl.ds(r0 + SUB, 64), lanes] = jnp.concatenate(blist, axis=0)
            out.append((a, b))
        return tuple(out)

    one = jnp.ones((SUB, LANES), F32)
    zero = jnp.zeros((SUB, LANES), F32)
    if hook is not None:
        hook(1)
    ends = lax.fori_loop(0, T // 64, gates, tuple((one, zero) for _ in range(halves)))
    if hook is not None:
        hook(2)
    for h in range(halves):
        a, b = ends[h]
        rows = [jnp.zeros((1, LANES), F32)]
        for s in range(SUB - 1):
            rows.append(a[s : s + 1] * rows[-1] + b[s : s + 1])
        st[z, 0:SUB, h * LANES : (h + 1) * LANES] = jnp.concatenate(rows, axis=0)
    first = st[z, 0:SUB, :]

    def finish(i):
        r0 = pl.multiple_of(i * 64, 64)
        a = load_planes(ac, pl.ds(r0, 64), 0, 2).reshape(8, SUB, C)
        b = st[z, pl.ds(r0 + SUB, 64), :].reshape(8, SUB, C)
        s = (b + a * first[None]).reshape(64, C)
        st[z, pl.ds(r0 + SUB, 64), :] = s
        refs.slow[z, pl.ds(r0, 64), :] = s.astype(BF16)

    loop(T // 64, finish)


def mix_out(refs, T):
    Z = refs.wot.shape[0]

    def body(i):
        rows = at(i, 256)
        acc = refs.tok_p[rows, :].astype(F32)
        for z in range(Z):
            acc = acc + dot_t(refs.slow[z, rows, :], refs.wot[z])
        store_planes(refs.resid, rows, acc)
        for k in range(2):
            x = acc[k * LANES : (k + 1) * LANES]
            y = x * lax.rsqrt(jnp.mean(x * x, axis=-1, keepdims=True) + EPS) * refs.g2[...]
            sub = pl.ds(pl.multiple_of(i * 256 + k * LANES, LANES), LANES)
            refs.fin[sub, :] = y.astype(BF16)
            refs.fin_t[:, sub] = y.T.astype(BF16)

    loop(T // 256, body)


def feed(refs, f, T):
    wup, wdt = refs.wup, refs.wdt
    size = 256
    tiles = T // size

    def project(i):
        rows = slice(i * size, (i + 1) * size)
        store_planes(refs.buf, rows, dot(refs.fin[rows, :], wup[f]))
        store_planes(refs.buf, rows, dot(refs.cot_p[rows, :], wdt[f]), 2)

    def activate(i):
        for k in range(size // 32):
            rows = slice(i * size + k * 32, i * size + (k + 1) * 32)
            for q in range(C // LANES):
                act, slope = gelu_parts(refs.buf[q, rows, :])
                lanes = slice(q * LANES, (q + 1) * LANES)
                refs.dpre[rows, lanes] = act.astype(BF16)
                lanes = slice(C + q * LANES, C + (q + 1) * LANES)
                refs.dpre[rows, lanes] = (refs.buf[2 + q, rows, :] * slope).astype(BF16)

    def add(i):
        rows = slice(i * size, (i + 1) * size)
        add_planes(refs.oacc, rows, dot_t(refs.dpre[rows, 0:C], wdt[f]))
        refs.dfe[rows, :] += dot_t(refs.dpre[rows, C : 2 * C], wup[f])

    for i in range(tiles + 2):
        if i < tiles:
            project(i)
        if 1 <= i < tiles + 1:
            activate(i - 1)
        if i >= 2:
            add(i - 2)


def feed_back(refs, T):
    n = T // SUB
    tmp = refs.buf
    D = refs.g1.shape[1]

    def body(i, total):
        rows = at(i, LANES)
        x = load_planes(refs.resid, rows)
        df = refs.dfe[rows, :]
        out = x + load_planes(refs.oacc, rows, 0, D // LANES)
        scatter_rows(tmp, i * 16, n, out)
        r = lax.rsqrt(jnp.mean(x * x, axis=-1, keepdims=True) + EPS)
        nrm = x * r
        dn = df * refs.g2[...]
        mean = jnp.mean(dn * nrm, axis=-1, keepdims=True)
        dres = refs.cot_p[rows, :].astype(F32) + r * (dn - nrm * mean)
        refs.dfe[rows, :] = dres
        refs.fin[rows, :] = dres.astype(BF16)
        refs.fin_t[:, rows] = dres.T.astype(BF16)
        return total + (df * nrm).reshape(16, SUB, D).sum(axis=0)

    total = lax.fori_loop(0, T // LANES, body, jnp.zeros((SUB, D), F32))
    refs.fgg[...] = jnp.sum(total, axis=0, keepdims=True)

    def emit(i):
        rows = at(i, LANES)
        for q in range(D // LANES):
            refs.block[rows, q * LANES : (q + 1) * LANES] = tmp[q, rows, :].astype(BF16)

    loop(T // LANES, emit)


def mixer_back(refs, z, T):
    buf, st = refs.buf, refs.st
    halves = C // LANES
    width = 3 * LANES

    def project(i):
        rows = at(i, 256)
        store_planes(buf, rows, dot(refs.fin[rows, :], refs.wot[z]))

    loop(T // 256, project)
    steps = T // 64

    def local(i, carry):
        r0 = pl.multiple_of((steps - 1 - i) * 64, 64)
        d = load_planes(buf, pl.ds(r0, 64), 0, 2)
        k = refs.keep[z, pl.ds(r0, 64), :]
        e, dk = carry
        plist, dlist = [None] * 8, [None] * 8
        for j in range(7, -1, -1):
            kj = k[j * SUB : (j + 1) * SUB]
            p = d[j * SUB : (j + 1) * SUB] + e
            plist[j] = p
            dlist[j] = dk
            e = kj * p
            dk = kj * dk
        store_planes(buf, pl.ds(r0, 64), jnp.concatenate(plist, axis=0))
        store_planes(buf, pl.ds(r0, 64), jnp.concatenate(dlist, axis=0), 2)
        return e, dk

    e, dk = lax.fori_loop(0, steps, local, (jnp.zeros((SUB, C), F32), jnp.ones((SUB, C), F32)))
    rows = [jnp.zeros((1, C), F32)]
    for s in range(SUB - 1, 0, -1):
        rows.insert(0, e[s : s + 1] + dk[s : s + 1] * rows[0])
    tail = jnp.concatenate(rows, axis=0)

    def grads(i, sums):
        r0 = pl.multiple_of(i * 64, 64)
        out = []
        for h in range(halves):
            lanes = slice(h * LANES, (h + 1) * LANES)
            sub = pl.ds(r0, 64)
            p0 = buf[h, sub, :].reshape(8, SUB, LANES)
            d0 = buf[2 + h, sub, :].reshape(8, SUB, LANES)
            p = (p0 + d0 * tail[None, :, lanes]).reshape(64, LANES)
            x = p * (st[z, pl.ds(r0 + SUB, 64), lanes] - st[z, sub, lanes])
            df = -(refs.k_f[z, sub, lanes] * x)
            di = refs.k_i[z, sub, lanes] * x
            dcand = refs.k_c[z, sub, lanes] * p
            df16 = df.astype(BF16)
            di16 = di.astype(BF16)
            refs.dpre[sub, h * width : h * width + LANES] = df16
            refs.dpre[sub, h * width + LANES : h * width + 2 * LANES] = di16
            refs.dpre[sub, h * width + 2 * LANES : h * width + 3 * LANES] = dcand.astype(BF16)
            sf, si = sums[h]
            out.append(
                (
                    sf + df16.astype(F32).reshape(8, SUB, LANES).sum(axis=0),
                    si + di16.astype(F32).reshape(8, SUB, LANES).sum(axis=0),
                )
            )
        return tuple(out)

    zero = jnp.zeros((SUB, LANES), F32)
    sums = lax.fori_loop(0, T // 64, grads, tuple((zero, zero) for _ in range(halves)))
    for h in range(halves):
        lanes = slice(h * LANES, (h + 1) * LANES)
        refs.fbg[z, :, lanes] = jnp.sum(sums[h][0], axis=0, keepdims=True)
        refs.ibg[z, :, lanes] = jnp.sum(sums[h][1], axis=0, keepdims=True)

    def back(i):
        rows = at(i, 256)
        add_planes(refs.oacc, rows, dot_t(refs.dpre[rows, :], refs.wmix[z]))

    loop(T // 256, back)


def norm_back(refs, T):
    n = T // SUB
    tmp = refs.buf
    D = refs.g1.shape[1]

    def body(i, total):
        rows = at(i, LANES)
        x = refs.tok_p[rows, :].astype(F32)
        d_in = load_planes(refs.oacc, rows, 0, D // LANES)
        r = lax.rsqrt(jnp.mean(x * x, axis=-1, keepdims=True) + EPS)
        nrm = x * r
        dn = d_in * refs.g1[...]
        mean = jnp.mean(dn * nrm, axis=-1, keepdims=True)
        out = refs.dfe[rows, :] + r * (dn - nrm * mean)
        scatter_rows(tmp, i * 16, n, out)
        return total + (d_in * nrm).reshape(16, SUB, D).sum(axis=0)

    total = lax.fori_loop(0, T // LANES, body, jnp.zeros((SUB, D), F32))
    refs.mgg[...] = jnp.sum(total, axis=0, keepdims=True)

    def emit(i):
        rows = at(i, LANES)
        for q in range(D // LANES):
            refs.tgrad[rows, q * LANES : (q + 1) * LANES] = tmp[q, rows, :].astype(BF16)

    loop(T // LANES, emit)


class Refs:
    def __init__(self, args):
        (
            self.tok, self.cot, self.wmix, self.wot, self.wup, self.wdt, self.g1, self.g2, self.fb, self.ib,
            self.block, self.tgrad, self.gmix, self.got, self.gup, self.gdt, self.fgg, self.mgg, self.fbg, self.ibg,
            self.tok_p, self.min, self.min_t, self.fin, self.fin_t, self.cot_p, self.cot_t, self.resid, self.oacc, self.dfe,
            self.pre, self.buf, self.dpre, self.slow, self.st, self.keep, self.k_f,
            self.k_i, self.k_c, self.gst, self.gsem,
        ) = args


def layer_kernel(*args):
    refs = Refs(args)
    T, D = refs.tok.shape
    Z = refs.wmix.shape[0]
    F = refs.wup.shape[0]
    gst, sem = refs.gst, refs.gsem
    cot_in(refs, T)
    norm_in(refs, T)
    loop(Z, lambda z: mixer_forward(refs, z, T))
    mix_out(refs, T)
    clear(refs.oacc, T)
    refs.dfe[...] = jnp.zeros_like(refs.dfe)

    def feed_step(f):
        feed(refs, f, T)
        gst[0, :, 0:C] = dot(refs.cot_t[...], refs.dpre[:, 0:C])
        gst[1, :, 0:C] = dot(refs.fin_t[...], refs.dpre[:, C : 2 * C])
        one = pltpu.make_async_copy(gst.at[0, :, 0:C], refs.gdt.at[f], sem.at[0])
        two = pltpu.make_async_copy(gst.at[1, :, 0:C], refs.gup.at[f], sem.at[1])
        one.start()
        two.start()
        one.wait()
        two.wait()

    loop(F, feed_step)
    feed_back(refs, T)
    clear(refs.oacc, T)

    def mixer_step(z):
        gst[0, :, 0:C] = dot(refs.fin_t[...], refs.slow[z])
        mixer_back(refs, z, T)
        gst[1, :, :] = dot(refs.min_t[...], refs.dpre[...])
        one = pltpu.make_async_copy(gst.at[0, :, 0:C], refs.got.at[z], sem.at[0])
        two = pltpu.make_async_copy(gst.at[1], refs.gmix.at[z], sem.at[1])
        one.start()
        two.start()
        one.wait()
        two.wait()

    loop(Z, mixer_step)
    norm_back(refs, T)


def layer(tok, cot, wmix, wot, wup, wdt, g1, g2, fb, ib):
    T, D = tok.shape
    Z, F = wmix.shape[0], wup.shape[0]
    sds = jax.ShapeDtypeStruct
    vm = pl.BlockSpec(memory_space=pltpu.VMEM)
    anyspec = pl.BlockSpec(memory_space=pl.ANY)
    out_shape = (
        sds((T, D), BF16), sds((T, D), BF16),
        sds((Z, D, 3 * C), F32), sds((Z, D, C), F32), sds((F, D, C), F32), sds((F, D, C), F32),
        sds((1, D), F32), sds((1, D), F32), sds((Z, 1, C), F32), sds((Z, 1, C), F32),
    )
    V = pltpu.VMEM
    scratch = [
        V((T, D), BF16), V((T, D), BF16), V((D, T), BF16), V((T, D), BF16), V((D, T), BF16),
        V((T, D), BF16), V((D, T), BF16), V((D // LANES, T, LANES), F32),
        V((D // LANES, T, LANES), F32), V((T, D), F32), V((3 * C // LANES, T, LANES), F32), V((4, T, LANES), F32),
        V((T, 3 * C), BF16), V((Z, T, C), BF16), V((Z, T + SUB, C), F32),
        V((Z, T, C), F32), V((Z, T, C), F32), V((Z, T, C), F32), V((Z, T, C), F32),
        V((2, D, 3 * C), F32), pltpu.SemaphoreType.DMA((2,)),
    ]
    return pl.pallas_call(
        layer_kernel,
        out_shape=out_shape,
        in_specs=[vm] * 10,
        out_specs=(vm, vm, anyspec, anyspec, anyspec, anyspec, vm, vm, vm, vm),
        scratch_shapes=scratch,
        compiler_params=pltpu.CompilerParams(vmem_limit_bytes=67043328),
        name="layer",
    )(tok, cot, wmix, wot, wup, wdt, g1, g2, fb, ib)


MESH = pl.DeviceIdType.MESH


def rcopy(src, dst, send, recv, device):
    return pltpu.make_async_remote_copy(
        src_ref=src, dst_ref=dst, send_sem=send, recv_sem=recv, device_id=device, device_id_type=MESH
    )


class Place:
    def __init__(self):
        self.g = lax.axis_index("grp")
        self.i = lax.axis_index("inner")
        self.y, self.x = self.g // 2, self.g % 2
        self.z, self.c = self.i // 2, self.i % 2
        self.me = self.g * 8 + self.i
        self.partner = (self.g, self.z * 2 + 1 - self.c)

    def flip(self, fx, fy):
        x = (self.x + fx) % 2
        y = (self.y + fy) % 2
        return y * 2 + x

    def near(self, z):
        e = z % 2
        return self.flip(1 - e, e)

    def far(self, z):
        e = z % 2
        return self.flip(e, 1 - e)

    def other(self, k):
        t = (self.me + k) % 32
        return (t // 8, t % 8)


def entry_barrier(place):
    barrier = pltpu.get_barrier_semaphore()

    def greet(k):
        pl.semaphore_signal(barrier, inc=1, device_id=place.other(k + 1), device_id_type=MESH)

    loop(31, greet)
    pl.semaphore_wait(barrier, 31)


def spread(values, start, count, total):
    lane = lax.broadcasted_iota(jnp.int32, (LANES, total), 1)
    row = lax.broadcasted_iota(jnp.int32, (LANES, total), 0)
    sel = jnp.where(row == start + lane % count, 1.0, 0.0).astype(BF16)
    picked = dot(values, sel)
    owner = lax.broadcasted_iota(jnp.int32, picked.shape, 0)
    spot = lax.broadcasted_iota(jnp.int32, picked.shape, 1)
    return jnp.sum(jnp.where(spot // count == owner, picked, 0.0), axis=0, keepdims=True)


def pack_vectors(mg, fb, ib, fg):
    parts = [mg, fb, ib, fg]
    used = sum(p.shape[0] for p in parts)
    rows = [p[...].astype(F32).reshape(1, p.shape[0]) for p in parts]
    return jnp.concatenate(rows + [jnp.zeros((1, LANES - used), F32)], axis=1)


FIRST = (3, 0)
LATER = (1, 2)


def block_of(refs, a, g, i):
    if a == 0:
        return refs.wot.at[g, at(i, 64), :]
    if a == 1:
        return refs.wup.at[i, at(g, 128), :]
    if a == 2:
        return refs.wdt.at[pl.ds(2 * g, 2), at(i, 64), :]
    return refs.wmix.at[i // 2, at(g, 128), at(i % 2, 384)]


def blocks_of(refs, a, i):
    if a == 0:
        return refs.wot.at[:, at(i, 64), :]
    if a == 1:
        return refs.wup.at[i]
    if a == 2:
        return refs.wdt.at[:, at(i, 64), :]
    return refs.wmix.at[i // 2, :, at(i % 2, 384)]


def line_send(refs, p, a):
    blk = block_of(refs, a, p.g, p.i)
    for s in range(1, 4):
        peer = (p.g, slot_chunk(p, s) * 2 + p.c)
        rcopy(blk, blk, refs.gz_s.at[a, s - 1], refs.gz_r.at[a, p.z], peer).start()


def near_of(p, a, z):
    return p.near(z + (a in LATER))


def far_of(p, a, z):
    return p.far(z + (a in LATER))


def line_wait(refs, p, a, z):
    @pl.when(z != p.z)
    def _():
        blk = block_of(refs, a, p.g, z * 2 + p.c)
        rcopy(blk, blk, refs.gp_s.at[a, z, 0], refs.gz_r.at[a, z], p.partner).wait_recv()


def near_send(refs, p, a, z):
    blk = block_of(refs, a, p.g, z * 2 + p.c)
    near, far = (near_of(p, a, z), p.i), (far_of(p, a, z), p.i)
    rcopy(blk, blk, refs.gn_s.at[a, z], refs.gn_r.at[a, z], near).start()
    rcopy(blk, blk, refs.gf_s.at[a, z, 0], refs.gf_r.at[a, z, 0], far).start()


def far_send(refs, p, a, z):
    near = block_of(refs, a, near_of(p, a, z), z * 2 + p.c)
    far = (far_of(p, a, z), p.i)
    rcopy(near, near, refs.gn_s.at[a, z], refs.gn_r.at[a, z], p.partner).wait_recv()
    rcopy(near, near, refs.gf_s.at[a, z, 1], refs.gf_r.at[a, z, 1], far).start()


def far_wait(refs, p, a, z, k):
    blk = block_of(refs, a, p.g, z * 2 + p.c)
    rcopy(blk, blk, refs.gf_s.at[a, z, k], refs.gf_r.at[a, z, k], p.partner).wait_recv()


def pair_copy(refs, p, a, z, c):
    full = blocks_of(refs, a, z * 2 + c)
    return rcopy(full, full, refs.gp_s.at[a, z, 0], refs.gp_r.at[a, z, 0], p.partner)


def first_step(refs, p, kind, s):
    for a in FIRST:
        z = slot_chunk(p, s)
        if kind == "n":
            line_wait(refs, p, a, z)
            near_send(refs, p, a, z)
        elif kind == "f":
            far_send(refs, p, a, z)
        elif kind == "p":
            far_wait(refs, p, a, z, 0)
            far_wait(refs, p, a, z, 1)
            pair_copy(refs, p, a, z, p.c).start()
        else:
            pair_copy(refs, p, a, z, 1 - p.c).wait_recv()


def up_step(refs, p, kind, m):
    if kind == "n":

        @pl.when(p.z != m)
        def _():
            line_wait(refs, p, 1, m)
            near_send(refs, p, 1, m)
    elif kind == "f":
        far_send(refs, p, 1, m)
    elif kind == "p":
        far_wait(refs, p, 1, m, 0)
        far_wait(refs, p, 1, m, 1)
        pair_copy(refs, p, 1, m, p.c).start()
    else:
        pair_copy(refs, p, 1, m, 1 - p.c).wait_recv()


def up_own(refs, p, phase):
    inner = (p.z + 1) // 2 % 2

    @pl.when(inner == phase)
    def _():
        near_send(refs, p, 1, p.z)


def down_pair(refs, p, z, phase, k, c):
    g = (1 + k) if phase else 3 * k
    blk = block_of(refs, 2, g, z * 2 + c)
    return rcopy(blk, blk, refs.gp_s.at[2, z, phase * 2 + k], refs.gp_r.at[2, z, phase * 2 + k], p.partner)


def down_step(refs, p, kind, phase, s):
    z = slot_chunk(p, s)
    active = (p.x + p.y) % 2 == phase
    idle = (p.x + p.y) % 2 != phase
    if kind == "n":

        @pl.when(active)
        def _():
            line_wait(refs, p, 2, z)
            near_send(refs, p, 2, z)
    elif kind == "f":

        @pl.when(idle)
        def _():
            far_send(refs, p, 2, z)
    elif kind == "p":

        @pl.when(active)
        def _():
            far_wait(refs, p, 2, z, 1)

        @pl.when(idle)
        def _():
            far_wait(refs, p, 2, z, 0)

        for k in range(2):
            down_pair(refs, p, z, phase, k, p.c).start()
    else:
        for k in range(2):
            down_pair(refs, p, z, phase, k, 1 - p.c).wait_recv()


def gather_drain(refs, p):
    for a in range(4):
        blk = block_of(refs, a, p.g, p.i)
        for k in range(3):
            rcopy(blk, blk, refs.gz_s.at[a, k], refs.gz_r.at[a, p.z], p.partner).wait_send()
        for z in range(4):
            blk = block_of(refs, a, p.g, z * 2 + p.c)
            rcopy(blk, blk, refs.gn_s.at[a, z], refs.gn_r.at[a, z], p.partner).wait_send()
            for k in range(2):
                rcopy(blk, blk, refs.gf_s.at[a, z, k], refs.gf_r.at[a, z, k], p.partner).wait_send()
            if a == 2:
                for k in range(4):
                    down_pair(refs, p, z, k // 2, k % 2, p.c).wait_send()
            else:
                pair_copy(refs, p, a, z, p.c).wait_send()


def gather_hook(refs, p, actions):
    for action in actions.split():
        kind, number = action[1], int(action[-1])
        if action[0] == "M":
            first_step(refs, p, kind, number)
        elif action[0] == "U":
            up_step(refs, p, kind, number)
        else:
            down_step(refs, p, kind, int(action[2]), number)


def gather_start(refs, p):
    local = []
    for k, w in enumerate((refs.fw, refs.iw, refs.cw)):
        spot = pl.ds(pl.multiple_of(p.c * 384 + k * 128, 128), 128)
        local.append(
            pltpu.make_async_copy(w, refs.wmix.at[p.z, at(p.g, 128), spot], refs.loc_s.at[k])
        )
    local.append(pltpu.make_async_copy(refs.ow, block_of(refs, 0, p.g, p.i), refs.loc_s.at[3]))
    local.append(pltpu.make_async_copy(refs.uw, block_of(refs, 1, p.g, p.i), refs.loc_s.at[4]))
    for k in range(2):
        local.append(
            pltpu.make_async_copy(
                refs.dw.at[:, k * 256 : (k + 1) * 256],
                refs.wdt.at[2 * p.g + k, at(p.i, 64), :],
                refs.loc_s.at[5 + k],
            )
        )
    for c in local:
        c.start()
    row = pack_vectors(refs.mg, refs.fbv, refs.ibv, refs.fg)
    refs.vstage[...] = row
    refs.vecs[p.me] = row
    for c in local:
        c.wait()
    entry_barrier(p)

    def vector(k):
        rcopy(refs.vstage, refs.vecs.at[p.me], refs.vec_s, refs.vec_r, p.other(k + 1)).start()

    for a in FIRST:
        near_send(refs, p, a, p.z)
    up_own(refs, p, 0)
    down_step(refs, p, "n", 0, 0)
    loop(31, vector)
    for a in FIRST:
        line_send(refs, p, a)
    inner = (p.z + 1) // 2 % 2

    @pl.when(inner == 0)
    def _():
        line_send(refs, p, 1)

    line_send(refs, p, 2)

    @pl.when(inner == 1)
    def _():
        line_send(refs, p, 1)


def gather_vectors(refs, p):
    rows = refs.vecs.at[pl.ds(0, 31)]
    rcopy(rows, rows, refs.vec_s, refs.vec_r, p.partner).wait()
    v = refs.vecs[...].reshape(32, LANES).astype(BF16)
    refs.g1[...] = spread(v, 0, 16, 512)
    refs.g2[...] = spread(v, 80, 16, 512)
    fb = spread(v, 16, 32, 1024)
    ib = spread(v, 48, 32, 1024)
    for z in range(4):
        refs.fb[z] = fb[:, z * C : (z + 1) * C]
        refs.ib[z] = ib[:, z * C : (z + 1) * C]


def slot_chunk(p, s):
    low = jnp.minimum(p.z, 3 - p.z)
    shift = jnp.where(s == 0, 1, jnp.where(s == 1, -1, 0))
    m = s + low * shift
    return jnp.where(p.z < 2, m, 3 - m)


SLOT_HOOKS = (
    ("", "Mf2 Dn01", "Mp1 Mf3 Un0 Un3"),
    ("Md1", "Mp2 Df00 Df01", "Dn02 Dn03 Uf0 Uf3"),
    ("Md2", "Mp3", "Df02 Df03 Dp00 Dp01"),
    ("Md3", "Un1 Un2 Dn10 Dn11 Dn12 Dn13", "Dp02 Dp03 Up0 Up3"),
)


def mixer_slots(refs, p, T):
    def hook(s, j):
        for k in range(4):

            @pl.when(s == k)
            def _():
                gather_hook(refs, p, SLOT_HOOKS[k][j])

    def slot(s):
        hook(s, 0)
        mixer_forward(refs, slot_chunk(p, s), T, lambda j: hook(s, j))

    loop(4, slot)


SHAPES = ((128, 256), (128, 256), (128, 384), (64, 256))
UP, DOWN, MIX, OUT = 0, 1, 2, 3
TINY = 1e-30
CLIP = 0.01
MATRICES = (
    (512, 1024), (512, 1024), (512, 1024), (1024, 512), (512, 2048), (2048, 512)
)
MATRIX_SLOTS = (1, 2, 3, 6, 8, 9)
VECTORS = ((0, 0, 16), (4, 16, 32), (5, 48, 32), (7, 80, 16))
COUNTS = (512, 524288, 524288, 524288, 1024, 1024, 524288, 512, 1048576, 1048576)


def spot(a, g, z):
    return (g, z) if a == DOWN else (z, g)


def rs_store(refs, a, g, z, value):
    refs.psend[a][(*spot(a, g, z),)] = value.astype(BF16)


def rs_role(p, g, z):
    e = z % 2
    y, x = g // 2, g % 2
    return (1 - e) * ((x + p.x) % 2) + e * ((y + p.y) % 2)


def rs_pair(refs, p, a, u):
    if a == OUT:
        src, dst = refs.psend[a], refs.precv[a]
    else:
        src, dst = refs.psend[a].at[u], refs.precv[a].at[u]
    return rcopy(src, dst, refs.rp_s.at[a, u], refs.rp_r.at[a, u], p.partner)


def rs_merge(refs, p, a, g, z, own):
    place = spot(a, g, z)
    v = own + refs.precv[a][place].astype(F32)
    role = rs_role(p, g, z)

    @pl.when(role == 1)
    def _():
        refs.psend[a][place] = v.astype(BF16)

    @pl.when(role == 0)
    def _():
        refs.precv[a][place] = v.astype(BF16)


def rs_group(p, z, k, sent):
    e = z % 2
    x = (1 - e) * ((p.x + sent) % 2) + e * k
    y = (1 - e) * k + e * ((p.y + sent) % 2)
    return y * 2 + x


def rs_first_copy(refs, p, a, z, k):
    g = rs_group(p, z, k, 1)
    return rcopy(
        refs.psend[a].at[spot(a, g, z)], refs.r1[a].at[z, k],
        refs.r1_s.at[a, z, k], refs.r1_r.at[a, z, k], (p.near(z), p.i),
    )


def rs_first_send(refs, p, a, z):
    for k in range(2):
        rs_first_copy(refs, p, a, z, k).start()


def rs_second(refs, p, a, z):
    e = z % 2
    mine = (1 - e) * p.y + e * p.x
    for k in range(2):
        rs_first_copy(refs, p, a, z, k).wait_recv()
    for k in range(2):
        place = spot(a, rs_group(p, z, k, 0), z)
        v = (refs.precv[a][place].astype(F32) + refs.r1[a][z, k].astype(F32)).astype(BF16)

        @pl.when(mine == k)
        def _():
            refs.precv[a][place] = v

        @pl.when(mine != k)
        def _():
            refs.psend[a][place] = v


def rs_second_copy(refs, p, a, z):
    e = z % 2
    other = 1 - ((1 - e) * p.y + e * p.x)
    place = spot(a, rs_group(p, z, other, 0), z)
    return rcopy(
        refs.psend[a].at[place], refs.r2[a].at[z], refs.r2_s.at[a, z], refs.r2_r.at[a, z],
        (p.far(z), p.i),
    )


def rs_third(refs, p, a, z):
    rs_second_copy(refs, p, a, z).wait_recv()
    place = spot(a, p.g, z)
    v = refs.precv[a][place].astype(F32) + refs.r2[a][z].astype(F32)

    @pl.when(z == p.z)
    def _():
        refs.fin_g[a][...] = v

    @pl.when(z != p.z)
    def _():
        refs.psend[a][place] = v.astype(BF16)


def rs_line(refs, p, a, z, owner):
    return rcopy(
        refs.psend[a].at[spot(a, p.g, z)], refs.r3[a].at[owner],
        refs.r3_s.at[a, z], refs.r3_r.at[a, owner], (p.g, z * 2 + p.c),
    )


def rs_third_send(refs, p, a, z):
    @pl.when(z != p.z)
    def _():
        rs_line(refs, p, a, z, p.z).start()


def rs_last(refs, p, a):
    for k in range(1, 4):
        z = (p.z + k) % 4
        rs_line(refs, p, a, z, z).wait_recv()
        refs.fin_g[a][...] += refs.r3[a][z].astype(F32)


def rs_drain(refs, p):
    def one(z):
        for a in range(4):
            for k in range(2):
                rs_first_copy(refs, p, a, z, k).wait_send()
            rs_second_copy(refs, p, a, z).wait_send()

            @pl.when(z != p.z)
            def _():
                rs_line(refs, p, a, z, p.z).wait_send()

    loop(4, one)


def own_row(x):
    return jnp.sum(x, axis=0, keepdims=True)


def lane_sum(x):
    folded = sum(x[:, k : k + LANES] for k in range(0, x.shape[1], LANES))
    return own_row(folded.T)


def wide(row):
    return jnp.concatenate([row, jnp.zeros((1, LANES - row.shape[1]), F32)], axis=1)


def cut(row):
    return [row[:, k : k + LANES] for k in range(0, row.shape[1], LANES)]


def stand(row):
    return jnp.broadcast_to(row, (LANES, LANES)).T


def scalars(values):
    lane = lax.broadcasted_iota(jnp.int32, (1, LANES), 1)
    out = jnp.zeros((1, LANES), F32)
    for k, v in enumerate(values):
        out = out + jnp.where(lane == k, v, 0.0)
    return out


def total(x):
    return jnp.sum(jnp.sum(x, axis=0, keepdims=True), axis=1, keepdims=True)


def segment(row, start, count):
    lane = lax.broadcasted_iota(jnp.int32, row.shape, 1)
    keep = (lane >= start) & (lane < start + count)
    return jnp.sum(jnp.where(keep, row, 0.0), axis=1, keepdims=True)


def gather_row(term, start, count):
    size = term.shape[1]
    owner = lax.broadcasted_iota(jnp.int32, (32, size), 0)
    spot = lax.broadcasted_iota(jnp.int32, (32, size), 1)
    masked = jnp.where(spot // count == owner, term, 0.0)
    lane = lax.broadcasted_iota(jnp.int32, (LANES, size), 0)
    from_spot = lax.broadcasted_iota(jnp.int32, (LANES, size), 1)
    sel = jnp.where(lane == start + from_spot % count, 1.0, 0.0).astype(BF16)
    out = jnp.zeros((32, LANES), F32)
    for _ in range(3):
        part = masked.astype(BF16)
        out = out + dot_t(part, sel)
        masked = masked - part.astype(F32)
    return out


def parameter_blocks(refs):
    return [
        refs.fw[...].astype(F32), refs.iw[...].astype(F32), refs.cw[...].astype(F32),
        refs.ow[...].astype(F32), refs.uw[...].astype(F32), refs.dw[...].astype(F32),
    ]


def old_rows(refs):
    rows = []
    for r in (refs.row_f, refs.row_i, refs.row_c, refs.row_o, refs.row_u, refs.row_d):
        rows += cut(r[...].reshape(1, r.shape[0]))
    return rows


def old_columns(refs):
    rows = []
    for r in (refs.col_f, refs.col_i, refs.col_c, refs.col_o, refs.col_u, refs.col_d):
        row = r[...].reshape(1, r.shape[0])
        rows += [wide(row)] if r.shape[0] < LANES else cut(row)
    return rows


ROW_PLACES = ((0, 1), (1, 2), (2, 3), (3, 5), (5, 6), (6, 10))
COLUMN_PLACES = ((0, 1), (1, 2), (2, 3), (3, 4), (4, 6), (6, 7))


def broadcast_row(src, box, send, recv, p):
    def one(k):
        rcopy(src, box.at[p.me], send, recv, p.other(k + 1)).start()

    loop(31, one)


def settle_row(box, send, recv, p):
    rows = box.at[pl.ds(0, 31)]
    rcopy(rows, rows, send, recv, p.partner).wait()


def vector_exchange(refs, p):
    rows = (
        gather_row(refs.mgg[...], 0, 16)
        + gather_row(jnp.concatenate([refs.fbg[z] for z in range(4)], axis=1), 16, 32)
        + gather_row(jnp.concatenate([refs.ibg[z] for z in range(4)], axis=1), 48, 32)
        + gather_row(refs.fgg[...], 80, 16)
    )
    refs.vout[...] = rows.reshape(32, 1, LANES)
    refs.vin[p.me] = refs.vout[p.me]

    def one(k):
        t = (p.me + k + 1) % 32
        rcopy(refs.vout.at[t], refs.vin.at[p.me], refs.vex_s, refs.vex_r, p.other(k + 1)).start()

    loop(31, one)


def gradient_blocks(refs):
    mix = refs.fin_g[MIX][...]
    down = refs.fin_g[DOWN][...]
    return [
        mix[:, 0:128], mix[:, 128:256], mix[:, 256:384], refs.fin_g[OUT][...], refs.fin_g[UP][...],
        jnp.concatenate([down[0:64], down[64:128]], axis=1),
    ]


def adafactor(refs, p):
    grads = gradient_blocks(refs)
    flipped = (False, False, False, True, False, True)
    row_parts, column_parts, totals = [], [], []
    for grad, flip in zip(grads, flipped):
        sq = grad * grad
        down, across = own_row(sq), lane_sum(sq)
        row_parts += cut(down) if flip else [across]
        column_parts += [wide(across)] if flip else cut(down)
        totals.append(jnp.sum(down, axis=1, keepdims=True))
    refs.rowst[...] = jnp.concatenate(row_parts + [jnp.zeros((6, LANES), F32)], axis=0)
    refs.colst[...] = jnp.concatenate(column_parts + [jnp.zeros((1, LANES), F32)], axis=0)
    weights = parameter_blocks(refs)
    params = pack_vectors(refs.mg, refs.fbv, refs.ibv, refs.fg)
    squares = [None] * 10
    for slot, w in zip(MATRIX_SLOTS, weights):
        squares[slot] = total(w * w)
    for slot, start, count in VECTORS:
        squares[slot] = segment(params * params, start, count)
    rows_old, columns_old = old_rows(refs), old_columns(refs)
    first = jnp.where(p.i == 0, 1.0, 0.0)
    row_sums = [first * total(jnp.concatenate(rows_old[a:b], axis=0)) for a, b in ROW_PLACES]
    refs.scal[...] = scalars(totals + squares + row_sums)
    refs.rowin[p.i] = refs.rowst[...]
    refs.colin[p.g] = refs.colst[...]
    refs.scin[p.me] = refs.scal[...]
    for k in range(1, 8):
        peer = (p.g, (p.i + k) % 8)
        rcopy(
            refs.rowst, refs.rowin.at[p.i], refs.row_s.at[k - 1], refs.row_r.at[k - 1], peer
        ).start()
    for k in range(1, 4):
        peer = ((p.g + k) % 4, p.i)
        rcopy(
            refs.colst, refs.colin.at[p.g], refs.col_s.at[k - 1], refs.col_r.at[k - 1], peer
        ).start()
    broadcast_row(refs.scal, refs.scin, refs.sc_s, refs.sc_r, p)
    vec_rows = refs.vin.at[pl.ds(0, 31)]
    rcopy(vec_rows, vec_rows, refs.vex_s, refs.vex_r, p.partner).wait()
    vector_grad = jnp.sum(refs.vin[...].reshape(32, LANES), axis=0, keepdims=True)
    seconds = pack_vectors(refs.sec_m, refs.sec_f, refs.sec_i, refs.sec_g)
    second = 0.5 * seconds + 0.5 * (vector_grad * vector_grad + TINY)
    vector_scaled = vector_grad * lax.rsqrt(second)
    for k in range(1, 8):
        rcopy(
            refs.rowst, refs.rowin.at[p.i], refs.row_s.at[k - 1], refs.row_r.at[k - 1], p.partner
        ).wait()
    for k in range(1, 4):
        rcopy(
            refs.colst, refs.colin.at[p.g], refs.col_s.at[k - 1], refs.col_r.at[k - 1], p.partner
        ).wait()
    settle_row(refs.scin, refs.sc_s, refs.sc_r, p)
    row_total = sum(refs.rowin[k] for k in range(8))
    column_total = sum(refs.colin[k] for k in range(4))
    sc = jnp.sum(refs.scin[...].reshape(32, LANES), axis=0, keepdims=True)
    rows_new, columns_new, scaled = [], [], []
    for k, (r, c) in enumerate(MATRICES):
        ra, rb = ROW_PLACES[k]
        ca, cb = COLUMN_PLACES[k]
        rows = [
            0.5 * rows_old[j] + 0.5 * (row_total[j : j + 1] / c + TINY) for j in range(ra, rb)
        ]
        columns = [
            0.5 * columns_old[j] + 0.5 * (column_total[j : j + 1] / r + TINY)
            for j in range(ca, cb)
        ]
        mean = 0.5 * sc[:, 16 + k : 17 + k] / r + 0.5 * (sc[:, k : k + 1] / (r * c) + TINY)
        lying, standing = (rows, columns) if flipped[k] else (columns, rows)
        tall = stand(standing[0])[0 : grads[k].shape[0]]
        lying = jnp.concatenate(lying, axis=1)
        tall = jnp.concatenate([tall] * (lying.shape[1] // LANES), axis=1)
        scaled.append(grads[k] * lax.rsqrt(tall * lying / mean))
        rows_new += rows
        columns_new += columns
    refs.rows_out[...] = jnp.concatenate(rows_new + [jnp.zeros((6, LANES), F32)], axis=0)
    refs.columns_out[...] = jnp.concatenate(columns_new + [jnp.zeros((1, LANES), F32)], axis=0)
    clips = [None] * 10
    for slot, s in zip(MATRIX_SLOTS, scaled):
        clips[slot] = total(s * s)
    for slot, start, count in VECTORS:
        clips[slot] = segment(vector_scaled * vector_scaled, start, count)
    refs.clip[...] = scalars(clips)
    refs.clin[p.me] = refs.clip[...]
    broadcast_row(refs.clip, refs.clin, refs.cl_s, refs.cl_r, p)
    settle_row(refs.clin, refs.cl_s, refs.cl_r, p)
    clip = jnp.sum(refs.clin[...].reshape(32, LANES), axis=0, keepdims=True)
    norms = [jnp.sqrt(clip[:, k : k + 1] / COUNTS[k]) for k in range(10)]
    steps = [
        -jnp.sqrt(sc[:, 6 + k : 7 + k] / COUNTS[k]) / jnp.maximum(CLIP, norms[k])
        for k in range(10)
    ]
    fresh = [w + steps[slot] * s for slot, w, s in zip(MATRIX_SLOTS, weights, scaled)]
    refs.grad_mix[...] = refs.fin_g[MIX][...]
    refs.grad_out[...] = grads[3]
    refs.grad_up[...] = grads[4]
    refs.grad_down[...] = grads[5]
    refs.new_mix[...] = jnp.concatenate(fresh[0:3], axis=1)
    refs.new_out[...] = fresh[3]
    refs.new_up[...] = fresh[4]
    refs.new_down[...] = fresh[5]
    lane = lax.broadcasted_iota(jnp.int32, (1, LANES), 1)
    step_row = jnp.zeros((1, LANES), F32)
    for slot, start, count in VECTORS:
        step_row = step_row + jnp.where((lane >= start) & (lane < start + count), steps[slot], 0.0)
    refs.vectors[...] = jnp.concatenate(
        [vector_grad, params + step_row * vector_scaled, second, scalars(norms)]
        + [jnp.zeros((4, LANES), F32)],
        axis=0,
    )


def finish_kernel(
    grad_mix, grad_out, grad_up, grad_down, new_mix, new_out, new_up, new_down,
    vectors, rows, columns,
    g_mg, g_f, g_i, g_c, g_fb, g_ib, g_o, g_fg, g_u, g_d,
    n_mg, n_f, n_i, n_c, n_fb, n_ib, n_o, n_fg, n_u, n_d,
    s_m, r_f, c_f, r_i, c_i, r_c, c_c, s_f, s_i, r_o, c_o, s_g, r_u, c_u, r_d, c_d, norms,
):
    for src, outs in ((grad_mix, (g_f, g_i, g_c)), (new_mix, (n_f, n_i, n_c))):
        for k, o in enumerate(outs):
            o[...] = src[:, k * 128 : (k + 1) * 128]
    for src, o in ((grad_out, g_o), (new_out, n_o), (grad_down, g_d), (new_down, n_d)):
        o[...] = src[...]
    g_u[...] = grad_up[...]
    n_u[...] = new_up[...]
    for row, outs in (
        (0, (g_mg, g_fb, g_ib, g_fg)), (1, (n_mg, n_fb, n_ib, n_fg)), (2, (s_m, s_f, s_i, s_g))
    ):
        for (_, start, count), o in zip(VECTORS, outs):
            o[...] = vectors[row, start : start + count]
    norms[...] = vectors[3, 0:10]
    for src, places, outs in (
        (rows, ROW_PLACES, (r_f, r_i, r_c, r_o, r_u, r_d)),
        (columns, COLUMN_PLACES, (c_f, c_i, c_c, c_o, c_u, c_d)),
    ):
        for (a, b), o in zip(places, outs):
            if b - a == 1:
                o[...] = src[a, 0 : o.shape[0]]
            else:
                for k in range(a, b):
                    o[(k - a) * LANES : (k - a + 1) * LANES] = src[k, :]


def finish(packed):
    sds = jax.ShapeDtypeStruct
    f = lambda *s: sds(s, F32)
    block = [f(16), f(128, 128), f(128, 128), f(128, 128), f(32), f(32), f(64, 256), f(16),
             f(128, 256), f(64, 512)]
    states = [f(16), f(128), f(128), f(128), f(128), f(128), f(128), f(32), f(32), f(256), f(64),
              f(16), f(128), f(256), f(512), f(64)]
    outs = tuple(block + block + states + [f(10)])
    vm = pl.BlockSpec(memory_space=pltpu.VMEM)
    return pl.pallas_call(
        finish_kernel,
        out_shape=outs,
        in_specs=[vm] * len(packed),
        out_specs=(vm,) * len(outs),
        name="finish",
    )(*packed)


class FusedRefs:
    def __init__(self, args):
        (
            self.tok_in, self.cot_in, self.fw, self.iw, self.cw, self.ow, self.uw, self.dw,
            self.mg, self.fbv, self.ibv, self.fg,
            self.sec_m, self.row_f, self.col_f, self.row_i, self.col_i, self.row_c, self.col_c,
            self.sec_f, self.sec_i, self.row_o, self.col_o, self.sec_g,
            self.row_u, self.col_u, self.row_d, self.col_d,
            self.block_out, self.tgrad_out,
            self.grad_mix, self.grad_out, self.grad_up, self.grad_down,
            self.new_mix, self.new_out, self.new_up, self.new_down,
            self.vectors, self.rows_out, self.columns_out,
            self.wmix, self.wot, self.wup, self.wdt, self.g1, self.g2, self.fb, self.ib,
            self.vecs, self.vstage, self.fgg, self.mgg, self.fbg, self.ibg,
            self.tok_p, self.fin, self.min_t, self.fin_t, self.cot_p, self.cot_t,
            self.resid, self.dfe,
            self.pre, self.buf, self.dpre, self.slow, self.st,
            self.keep, self.k_f, self.k_i, self.k_c,
            self.loc_s, self.vec_s, self.vec_r, self.gz_s, self.gz_r,
            self.gn_s, self.gn_r, self.gf_s, self.gf_r, self.gp_s, self.gp_r,
            self.vout, self.vin, self.rowst, self.rowin, self.colst, self.colin,
            self.scal, self.scin, self.clip, self.clin,
            self.rp_s, self.rp_r, self.r1_s, self.r1_r, self.r2_s, self.r2_r,
            self.r3_s, self.r3_r, self.vex_s, self.vex_r,
            self.row_s, self.row_r, self.col_s, self.col_r, self.sc_s, self.sc_r,
            self.cl_s, self.cl_r, self.io_s,
        ) = args[:112]
        rest = list(args[112:])
        self.psend, self.precv, self.r1, self.r2, self.r3, self.fin_g = (
            rest[4 * k : 4 * k + 4] for k in range(6)
        )
        self.io = self.dpre.at[:, 0:512]
        self.oacc = self.pre.at[pl.ds(4, 4)]
        self.tok = self.cot = self.block = self.tgrad = self.io
        self.min = self.fin


def halves_of(refs, plane, rows):
    size = rows.size
    low = refs.pre[plane, rows, :]
    high = refs.pre[plane, pl.ds(rows.start + 512, size), :]
    return jnp.concatenate([low, high], axis=1)


def put_halves(refs, plane, value):
    refs.pre[plane, 0:512, :] = value[:, 0:LANES]
    refs.pre[plane, 512:1024, :] = value[:, LANES : 2 * LANES]


def line_rows(z, c):
    return pl.ds(pl.multiple_of((z * 2 + c) * 64, 64), 64)


def put_feed_grads(refs, p, f):
    z, h = f // 2, f % 2
    up = dot(refs.fin_t[...], refs.dpre[:, C : 2 * C])
    put_halves(refs, 1 + h, dot(refs.cot_t[...], refs.dpre[:, 0:C]))

    @pl.when(h == p.c)
    def _():
        put_halves(refs, 0, up)

    @pl.when(h != p.c)
    def _():
        for g in range(4):
            refs.psend[UP][z, g] = up[g * 128 : (g + 1) * 128].astype(BF16)

    half = pl.ds(pl.multiple_of(h * 64, 64), 64)
    for zz in range(4):
        part = halves_of(refs, 1 + h, line_rows(zz, 1 - p.c))
        refs.psend[DOWN][z, zz, half, :] = part.astype(BF16)


def merge_up(refs, p, z):
    rs_pair(refs, p, UP, z).wait()
    for g in range(4):
        rs_merge(refs, p, UP, g, z, halves_of(refs, 0, pl.ds(g * 128, 128)))


def merge_down(refs, p, g):
    rs_pair(refs, p, DOWN, g).wait()
    for z in range(4):
        own = jnp.concatenate(
            [halves_of(refs, 1 + h, line_rows(z, p.c)) for h in range(2)], axis=0
        )
        rs_merge_at(refs, p, DOWN, g, z, own)


def rs_merge_at(refs, p, a, g, z, own):
    e = z % 2
    y, x = g // 2, g % 2
    role = (1 - e) * ((x + p.x) % 2) + e * ((y + p.y) % 2)
    place = spot(a, g, z)
    v = (own + refs.precv[a][place].astype(F32)).astype(BF16)

    @pl.when(role == 1)
    def _():
        refs.psend[a][place] = v

    @pl.when(role == 0)
    def _():
        refs.precv[a][place] = v


def put_out_grads(refs, p):
    def one(g):
        put_halves(refs, g, dot(refs.fin_t[...], refs.slow[g]))
        for z in range(4):
            part = halves_of(refs, g, line_rows(z, 1 - p.c))
            refs.psend[OUT][z, g] = part.astype(BF16)

    loop(4, one)


def merge_out(refs, p):
    rs_pair(refs, p, OUT, 0).wait()

    def one(z):
        for g in range(4):
            rs_merge(refs, p, OUT, g, z, halves_of(refs, g, line_rows(z, p.c)))

    loop(4, one)


def mix_part(refs, g, c):
    cols = []
    for j in range(3):
        q = 3 * c + j
        rows = pl.ds(pl.multiple_of((q % 2) * 512 + g * 128, 128), 128)
        cols.append(refs.pre[q // 2, rows, :])
    return jnp.concatenate(cols, axis=1)


def put_mix_grads(refs, p, z):
    for j in range(3):
        put_halves(refs, j, dot(refs.min_t[...], refs.dpre[:, j * C : (j + 1) * C]))
    for g in range(4):
        refs.psend[MIX][z, g] = mix_part(refs, g, 1 - p.c).astype(BF16)


def merge_mix(refs, p, z):
    rs_pair(refs, p, MIX, z).wait()
    for g in range(4):
        rs_merge(refs, p, MIX, g, z, mix_part(refs, g, p.c))


def all_z(body):
    loop(4, body)


def second(refs, p, a, z):
    rs_second(refs, p, a, z)
    rs_second_copy(refs, p, a, z).start()


def third(refs, p, a, z):
    rs_third(refs, p, a, z)
    rs_third_send(refs, p, a, z)


def feed_order(k):
    return jnp.where(k == 1, 3, jnp.where(k >= 2, k - 1, 0))


def feed_tick(refs, p, f):
    @pl.when((f % 2 == 0) & (f >= 2))
    def _():
        last = feed_order(f // 2 - 1)
        merge_up(refs, p, last)
        merge_down(refs, p, last)
        rs_first_send(refs, p, UP, last)

    @pl.when((f % 2 == 0) & (f >= 4))
    def _():
        second(refs, p, UP, feed_order(f // 2 - 2))

    @pl.when((f % 2 == 0) & (f >= 6))
    def _():
        third(refs, p, UP, feed_order(f // 2 - 3))


def fused_kernel(*args):
    refs = FusedRefs(args)
    refs.fin_grad = refs.fin_g
    T, D = refs.tok_p.shape
    p = Place()
    load = pltpu.make_async_copy(refs.cot_in, refs.io, refs.io_s)
    load.start()
    gather_start(refs, p)
    load.wait()
    cot_in(refs, T)
    load = pltpu.make_async_copy(refs.tok_in, refs.io, refs.io_s)
    load.start()
    gather_vectors(refs, p)
    load.wait()
    norm_in(refs, T)
    gather_hook(refs, p, "Mf0 Mn1 Mn2 Mf1 Mp0 Mn3 Md0")
    mixer_slots(refs, p, T)
    up_own(refs, p, 1)
    mix_out(refs, T)
    gather_hook(refs, p, "Ud0 Ud3 Dd00 Dd01 Dd02 Dd03")
    clear(refs.oacc, T)
    refs.dfe[...] = jnp.zeros_like(refs.dfe)

    def feed_step(f):
        @pl.when(f == 4)
        def _():
            gather_hook(refs, p, "Ud1 Ud2 Dd10 Dd11 Dd12 Dd13")

        feed(refs, feed_order(f // 2) * 2 + f % 2, T)

        @pl.when(f == 0)
        def _():
            gather_hook(refs, p, "Uf1 Uf2 Df10 Df11 Df12 Df13")

        @pl.when(f == 1)
        def _():
            gather_hook(refs, p, "Up1 Up2 Dp10 Dp11 Dp12 Dp13")

        feed_tick(refs, p, f)
        put_feed_grads(refs, p, feed_order(f // 2) * 2 + f % 2)

        @pl.when(f % 2 == 1)
        def _():
            rs_pair(refs, p, UP, feed_order(f // 2)).start()
            rs_pair(refs, p, DOWN, feed_order(f // 2)).start()

    loop(8, feed_step)
    feed_back(refs, T)
    store = pltpu.make_async_copy(refs.io, refs.block_out, refs.io_s)
    store.start()
    gather_drain(refs, p)
    merge_up(refs, p, 2)
    merge_down(refs, p, 2)
    rs_first_send(refs, p, UP, 2)
    all_z(lambda z: rs_first_send(refs, p, DOWN, z))
    second(refs, p, UP, 1)
    third(refs, p, UP, 3)
    put_out_grads(refs, p)
    rs_pair(refs, p, OUT, 0).start()
    clear(refs.oacc, T)
    store.wait()

    def chunk(n):
        return (p.z + 1 + n) % 4

    def mixer_step(n):
        z = chunk(n)
        mixer_back(refs, z, T)

        @pl.when(n == 0)
        def _():
            merge_out(refs, p)
            all_z(lambda z: rs_first_send(refs, p, OUT, z))
            all_z(lambda z: second(refs, p, DOWN, z))
            second(refs, p, UP, 2)
            third(refs, p, UP, 1)

        @pl.when(n >= 1)
        def _():
            merge_mix(refs, p, chunk(n - 1))
            rs_first_send(refs, p, MIX, chunk(n - 1))

        @pl.when(n == 1)
        def _():
            all_z(lambda z: second(refs, p, OUT, z))
            all_z(lambda z: third(refs, p, DOWN, z))
            third(refs, p, UP, 2)

        @pl.when(n >= 2)
        def _():
            second(refs, p, MIX, chunk(n - 2))

        @pl.when(n == 2)
        def _():
            all_z(lambda z: third(refs, p, OUT, z))

        @pl.when(n == 3)
        def _():
            third(refs, p, MIX, chunk(0))

        put_mix_grads(refs, p, z)
        rs_pair(refs, p, MIX, z).start()

    loop(4, mixer_step)
    norm_back(refs, T)
    store = pltpu.make_async_copy(refs.io, refs.tgrad_out, refs.io_s)
    store.start()
    merge_mix(refs, p, chunk(3))
    rs_first_send(refs, p, MIX, chunk(3))
    vector_exchange(refs, p)
    second(refs, p, MIX, chunk(2))
    third(refs, p, MIX, chunk(1))
    for a in (UP, DOWN, OUT):
        rs_last(refs, p, a)
    second(refs, p, MIX, chunk(3))
    third(refs, p, MIX, chunk(2))
    third(refs, p, MIX, chunk(3))
    rs_last(refs, p, MIX)
    rs_drain(refs, p)
    adafactor(refs, p)
    store.wait()


def fused(*args):
    T, D = args[0].shape
    Z, F = 4, 8
    sds = jax.ShapeDtypeStruct
    vm = pl.BlockSpec(memory_space=pltpu.VMEM)
    anyspec = pl.BlockSpec(memory_space=pl.ANY)
    V = pltpu.VMEM
    S = pltpu.SemaphoreType.DMA
    outs = (
        sds((T, D), BF16), sds((T, D), BF16),
        sds((128, 384), F32), sds((64, 256), F32), sds((128, 256), F32), sds((64, 512), F32),
        sds((128, 384), F32), sds((64, 256), F32), sds((128, 256), F32), sds((64, 512), F32),
        sds((8, LANES), F32), sds((16, LANES), F32), sds((8, LANES), F32),
    )
    row = V((1, LANES), F32)
    box = V((32, 1, LANES), F32)
    scratch = [
        V((Z, D, 3 * C), BF16), V((Z, D, C), BF16), V((F, D, C), BF16), V((F, D, C), BF16),
        V((1, D), F32), V((1, D), F32), V((Z, 1, C), F32), V((Z, 1, C), F32),
        box, row, V((1, D), F32), V((1, D), F32), V((Z, 1, C), F32), V((Z, 1, C), F32),
        V((T, D), BF16), V((T, D), BF16), V((D, T), BF16), V((D, T), BF16),
        V((T, D), BF16), V((D, T), BF16),
        V((D // LANES, T, LANES), F32), V((T, D), F32),
        V((8, T, LANES), F32), V((4, T, LANES), F32),
        V((T, 3 * C), BF16), V((Z, T, C), BF16), V((Z, T + SUB, C), F32),
        V((Z, T, C), F32), V((Z, T, C), F32), V((Z, T, C), F32), V((Z, T, C), F32),
        S((7,)), S(()), S(()), S((4, 3)), S((4, 4)),
        S((4, 4)), S((4, 4)), S((4, 4, 2)), S((4, 4, 2)), S((4, 4, 4)), S((4, 4, 4)),
        box, box, V((16, LANES), F32), V((8, 16, LANES), F32),
        V((8, LANES), F32), V((4, 8, LANES), F32), row, box, row, box,
        S((4, 4)), S((4, 4)), S((4, 4, 2)), S((4, 4, 2)), S((4, 4)), S((4, 4)),
        S((4, 4)), S((4, 4)), S(()), S(()),
        S((7,)), S((7,)), S((3,)), S((3,)), S(()), S(()), S(()), S(()), S(()),
    ]
    scratch += (
        [V((4, 4) + s, BF16) for s in SHAPES] * 2
        + [V((4, 2) + s, BF16) for s in SHAPES]
        + [V((4,) + s, BF16) for s in SHAPES] * 2
        + [V(s, F32) for s in SHAPES]
    )
    return pl.pallas_call(
        fused_kernel,
        out_shape=outs,
        in_specs=[anyspec, anyspec] + [vm] * (len(args) - 2),
        out_specs=(anyspec, anyspec) + (vm,) * (len(outs) - 2),
        scratch_shapes=scratch,
        compiler_params=pltpu.CompilerParams(
            vmem_limit_bytes=67043328, collective_id=0, has_side_effects=True
        ),
        name="fused",
    )(*args)


def gathered_layer(tok, cot, mix, ow, uw, dw, mg, fb, ib, fg):
    def whole(w):
        w = lax.all_gather(w, "inner", axis=1, tiled=True)
        return lax.all_gather(w, "grp", axis=0, tiled=True)

    def vec(v):
        return lax.all_gather(v, ("grp", "inner"), axis=0, tiled=True).astype(F32)

    width = tok.shape[1]
    inners = lax.axis_size("inner")
    Z, F = mix[0].shape[1] * inners // C, uw.shape[1] * inners // C
    gates = [whole(w).reshape(width, Z, C // LANES, 1, LANES) for w in mix]
    wmix = jnp.concatenate(gates, axis=3).reshape(width, Z, 3 * C).transpose(1, 0, 2)
    wot = whole(ow).reshape(Z, C, width).transpose(0, 2, 1)
    wup = whole(uw).reshape(width, F, C).transpose(1, 0, 2)
    wdt = whole(dw).reshape(F, C, width).transpose(0, 2, 1)
    return layer(
        tok, cot, wmix, wot, wup, wdt,
        vec(mg).reshape(1, width), vec(fg).reshape(1, width),
        vec(fb).reshape(Z, 1, C), vec(ib).reshape(Z, 1, C),
    )


def body(
    tokens,
    cotangent,
    mixer_gain,
    forget_weight,
    input_gate_weight,
    candidate_weight,
    forget_bias,
    input_bias,
    output_weight,
    feed_norm_gain,
    up_weight,
    down_weight,
    mixer_second,
    forget_rows,
    forget_columns,
    input_rows,
    input_columns,
    candidate_rows,
    candidate_columns,
    forget_second,
    input_second,
    output_rows,
    output_columns,
    feed_second,
    up_rows,
    up_columns,
    down_rows,
    down_columns,
):
    groups = lax.axis_size("grp")
    inners = lax.axis_size("inner")
    seqs, length, width = tokens.shape
    hidden = forget_weight.shape[1] * inners
    ff = up_weight.shape[1] * inners
    paired = (groups, inners) == (4, 8) and (length, width, hidden, ff) == (1024, 512, 1024, 2048)
    Z, F = hidden // C, ff // C
    if paired:
        block_output, tokens_grad, *packed = fused(
            tokens.reshape(length, width), cotangent.reshape(length, width),
            forget_weight, input_gate_weight, candidate_weight,
            output_weight.T, up_weight, down_weight.T,
            mixer_gain, forget_bias, input_bias, feed_norm_gain,
            mixer_second, forget_rows, forget_columns, input_rows, input_columns,
            candidate_rows, candidate_columns, forget_second, input_second,
            output_rows, output_columns, feed_second,
            up_rows, up_columns, down_rows, down_columns,
        )
        done = list(finish(packed))
        for k in (6, 9, 16, 19):
            done[k] = done[k].T
        return (block_output.reshape(tokens.shape), tokens_grad.reshape(tokens.shape), *done)
    results = gathered_layer(
        tokens.reshape(length, width), cotangent.reshape(length, width),
        (forget_weight, input_gate_weight, candidate_weight),
        output_weight, up_weight, down_weight,
        mixer_gain, forget_bias, input_bias, feed_norm_gain,
    )
    block_output, tokens_grad, gmix, got, gup, gdt, fgg, mgg, fbg, ibg = results
    block_output = block_output.reshape(tokens.shape)
    tokens_grad = tokens_grad.reshape(tokens.shape)
    split = gmix.transpose(1, 0, 2).reshape(width, Z, C // LANES, 3, LANES)
    forget_term, input_term, cand_term = [
        split[:, :, :, k].reshape(width, hidden) for k in range(3)
    ]
    output_term = got.transpose(0, 2, 1).reshape(hidden, width)
    up_term = gup.transpose(1, 0, 2).reshape(width, ff)
    down_term = gdt.transpose(0, 2, 1).reshape(ff, width)
    gain_first_term, gain_second_term = mgg.reshape(-1), fgg.reshape(-1)
    fbias_term, ibias_term = fbg.reshape(-1), ibg.reshape(-1)
    part = (
        lax.psum_scatter(
            gain_first_term.reshape(groups, -1), "inner", scatter_dimension=1, tiled=True
        ),
        lax.psum_scatter(forget_term, "inner", scatter_dimension=1, tiled=True),
        lax.psum_scatter(input_term, "inner", scatter_dimension=1, tiled=True),
        lax.psum_scatter(cand_term, "inner", scatter_dimension=1, tiled=True),
        lax.psum_scatter(fbias_term.reshape(groups, -1), "inner", scatter_dimension=1, tiled=True),
        lax.psum_scatter(ibias_term.reshape(groups, -1), "inner", scatter_dimension=1, tiled=True),
        lax.psum_scatter(output_term, "inner", scatter_dimension=1, tiled=True),
        lax.psum_scatter(
            gain_second_term.reshape(groups, -1), "inner", scatter_dimension=1, tiled=True
        ),
        lax.psum_scatter(up_term, "inner", scatter_dimension=1, tiled=True),
        lax.psum_scatter(down_term, "inner", scatter_dimension=1, tiled=True),
    )
    mine = (
        lax.psum_scatter(part[0], "grp", scatter_dimension=0, tiled=True),
        lax.psum_scatter(part[1], "grp", scatter_dimension=0, tiled=True),
        lax.psum_scatter(part[2], "grp", scatter_dimension=0, tiled=True),
        lax.psum_scatter(part[3], "grp", scatter_dimension=0, tiled=True),
        lax.psum_scatter(part[4], "grp", scatter_dimension=0, tiled=True),
        lax.psum_scatter(part[5], "grp", scatter_dimension=0, tiled=True),
        lax.psum_scatter(part[6], "grp", scatter_dimension=0, tiled=True),
        lax.psum_scatter(part[7], "grp", scatter_dimension=0, tiled=True),
        lax.psum_scatter(part[8], "grp", scatter_dimension=0, tiled=True),
        lax.psum_scatter(part[9], "grp", scatter_dimension=0, tiled=True),
    )
    params = [
        mixer_gain,
        forget_weight,
        input_gate_weight,
        candidate_weight,
        forget_bias,
        input_bias,
        output_weight,
        feed_norm_gain,
        up_weight,
        down_weight,
    ]
    locals_f = [p.astype(jnp.float32) for p in params]
    grads = [
        mine[0].reshape(-1),
        mine[1],
        mine[2],
        mine[3],
        mine[4].reshape(-1),
        mine[5].reshape(-1),
        mine[6],
        mine[7].reshape(-1),
        mine[8],
        mine[9],
    ]
    matrix_slots = [1, 2, 3, 6, 8, 9]
    vector_slots = [0, 4, 5, 7]
    rows_old = [forget_rows, input_rows, candidate_rows, output_rows, up_rows, down_rows]
    columns_old = [
        forget_columns,
        input_columns,
        candidate_columns,
        output_columns,
        up_columns,
        down_columns,
    ]
    seconds_old = [mixer_second, forget_second, input_second, feed_second]
    counts = [params[k].size * groups * inners for k in range(10)]
    first_inner = (lax.axis_index("inner") == 0).astype(jnp.float32)
    scales = lax.psum(
        jnp.stack(
            [jnp.sum(w * w) for w in locals_f] + [jnp.sum(r) * first_inner for r in rows_old]
        ),
        ("grp", "inner"),
    )
    mats = [grads[k] for k in matrix_slots]
    row_parts = [jnp.sum(g * g, axis=1) for g in mats]
    column_parts = [jnp.sum(g * g, axis=0) for g in mats]
    row_totals = lax.psum(
        (row_parts[0], row_parts[1], row_parts[2], row_parts[3], row_parts[4], row_parts[5]),
        "inner",
    )
    column_totals = lax.psum(
        (
            column_parts[0],
            column_parts[1],
            column_parts[2],
            column_parts[3],
            column_parts[4],
            column_parts[5],
        ),
        "grp",
    )
    grand = lax.psum(jnp.stack([jnp.sum(v) for v in row_totals]), "grp")
    scaled_all = [None] * 10
    new_states = [None] * 16
    state_places = {1: (1, 2), 2: (3, 4), 3: (5, 6), 6: (9, 10), 8: (12, 13), 9: (14, 15)}
    second_places = {0: 0, 4: 7, 5: 8, 7: 11}
    for k in range(6):
        slot = matrix_slots[k]
        grad = mats[k]
        full_rows = grad.shape[0] * groups
        full_columns = grad.shape[1] * inners
        rows = 0.5 * rows_old[k] + 0.5 * (row_totals[k] / full_columns + TINY)
        columns = 0.5 * columns_old[k] + 0.5 * (column_totals[k] / full_rows + TINY)
        row_mean = 0.5 * scales[10 + k] / full_rows + 0.5 * (
            grand[k] / (full_rows * full_columns) + TINY
        )
        scaled_all[slot] = grad * lax.rsqrt(rows[:, None] * columns[None, :] / row_mean)
        new_states[state_places[slot][0]] = rows
        new_states[state_places[slot][1]] = columns
    for k in range(4):
        slot = vector_slots[k]
        grad = grads[slot]
        second = 0.5 * seconds_old[k] + 0.5 * (grad * grad + TINY)
        scaled_all[slot] = grad * lax.rsqrt(second)
        new_states[second_places[slot]] = second
    clip = lax.psum(jnp.stack([jnp.sum(s * s) for s in scaled_all]), ("grp", "inner"))
    count_array = jnp.array(counts, jnp.float32)
    update_norms = jnp.sqrt(clip / count_array)
    fresh = [
        locals_f[k]
        + -jnp.sqrt(scales[k] / counts[k]) * scaled_all[k] / jnp.maximum(CLIP, update_norms[k])
        for k in range(10)
    ]
    return (
        block_output,
        tokens_grad,
        grads[0],
        grads[1],
        grads[2],
        grads[3],
        grads[4],
        grads[5],
        grads[6],
        grads[7],
        grads[8],
        grads[9],
        fresh[0],
        fresh[1],
        fresh[2],
        fresh[3],
        fresh[4],
        fresh[5],
        fresh[6],
        fresh[7],
        fresh[8],
        fresh[9],
        new_states[0],
        new_states[1],
        new_states[2],
        new_states[3],
        new_states[4],
        new_states[5],
        new_states[6],
        new_states[7],
        new_states[8],
        new_states[9],
        new_states[10],
        new_states[11],
        new_states[12],
        new_states[13],
        new_states[14],
        new_states[15],
        update_norms,
    )


def solution(mesh):
    return jax.shard_map(
        body,
        mesh=mesh,
        in_specs=(
            P(("grp", "inner"), None, None),
            P(("grp", "inner"), None, None),
            P(("grp", "inner")),
            P("grp", "inner"),
            P("grp", "inner"),
            P("grp", "inner"),
            P(("grp", "inner")),
            P(("grp", "inner")),
            P("grp", "inner"),
            P(("grp", "inner")),
            P("grp", "inner"),
            P("grp", "inner"),
            P(("grp", "inner")),
            P("grp"),
            P("inner"),
            P("grp"),
            P("inner"),
            P("grp"),
            P("inner"),
            P(("grp", "inner")),
            P(("grp", "inner")),
            P("grp"),
            P("inner"),
            P(("grp", "inner")),
            P("grp"),
            P("inner"),
            P("grp"),
            P("inner"),
        ),
        out_specs=(
            P(("grp", "inner"), None, None),
            P(("grp", "inner"), None, None),
            P(("grp", "inner")),
            P("grp", "inner"),
            P("grp", "inner"),
            P("grp", "inner"),
            P(("grp", "inner")),
            P(("grp", "inner")),
            P("grp", "inner"),
            P(("grp", "inner")),
            P("grp", "inner"),
            P("grp", "inner"),
            P(("grp", "inner")),
            P("grp", "inner"),
            P("grp", "inner"),
            P("grp", "inner"),
            P(("grp", "inner")),
            P(("grp", "inner")),
            P("grp", "inner"),
            P(("grp", "inner")),
            P("grp", "inner"),
            P("grp", "inner"),
            P(("grp", "inner")),
            P("grp"),
            P("inner"),
            P("grp"),
            P("inner"),
            P("grp"),
            P("inner"),
            P(("grp", "inner")),
            P(("grp", "inner")),
            P("grp"),
            P("inner"),
            P(("grp", "inner")),
            P("grp"),
            P("inner"),
            P("grp"),
            P("inner"),
            P(),
        ),
        check_vma=False,
    )
```

```python
import functools
import math
import jax
import jax.numpy as jnp
from jax import lax
from jax.experimental import pallas as pl
from jax.sharding import PartitionSpec as P
from jax.experimental.pallas import tpu as pltpu

EPS = 1e-06
F32 = jnp.float32
BF16 = jnp.bfloat16
C = 256
LANES = 128
SUB = 8
ERFC = (
    0.2256758669, 0.2256693636, 0.2078460312, 0.1685204197, 0.1415057621,
    -0.005753053848, 0.1692475449, -0.182997133, 0.05028532412,
)


def dot(a, b):
    return jnp.dot(a, b, preferred_element_type=F32)


def dot_t(a, b):
    return lax.dot_general(a, b, (((1,), (1,)), ((), ())), preferred_element_type=F32)


def loop(steps, body):
    def run(i, carry):
        body(i)
        return carry

    lax.fori_loop(0, steps, run, 0)


def at(i, size):
    return pl.ds(pl.multiple_of(i * size, size), size)


def gelu_parts(x):
    e = jnp.exp2((x * x) * (-0.5 / math.log(2.0)))
    t = 1.0 / (1.0 + (0.4 * math.sqrt(0.5)) * jnp.abs(x))
    poly = jnp.full_like(t, 0.5 * ERFC[-1])
    for c in ERFC[-2::-1]:
        poly = poly * t + 0.5 * c
    half = poly * (t * e)
    cdf = jnp.where(x >= 0, 1.0 - half, half)
    return x * cdf, cdf + (x * e) * (1.0 / math.sqrt(2.0 * math.pi))


def gather_rows(tmp, j0, n, D):
    columns = [
        jnp.concatenate([tmp[q, pl.ds(j0 + jj, SUB, stride=n), :] for jj in range(16)], axis=0)
        for q in range(D // LANES)
    ]
    return jnp.concatenate(columns, axis=1)


def scatter_rows(tmp, j0, n, out):
    for q in range(out.shape[1] // LANES):
        for jj in range(16):
            tmp[q, pl.ds(j0 + jj, SUB, stride=n), :] = out[
                jj * SUB : (jj + 1) * SUB, q * LANES : (q + 1) * LANES
            ]


LOG2E = 1.0 / math.log(2.0)


def load_planes(ref, rows, start=0, count=None):
    count = ref.shape[0] if count is None else count
    return jnp.concatenate([ref[q, rows, :] for q in range(start, start + count)], axis=1)


def store_planes(ref, rows, value, start=0):
    for q in range(value.shape[1] // LANES):
        ref[start + q, rows, :] = value[:, q * LANES : (q + 1) * LANES]


def add_planes(ref, rows, value):
    for q in range(value.shape[1] // LANES):
        ref[q, rows, :] += value[:, q * LANES : (q + 1) * LANES]


def clear(ref, T):
    for q in range(4):
        ref[q, 0:T, :] = jnp.zeros((T, LANES), F32)


def norm_in(refs, T):
    n = T // SUB
    tmp, g1 = refs.buf, refs.g1
    D = g1.shape[1]

    def widen(i):
        rows = at(i, LANES)
        wide = refs.tok[rows, :].astype(F32)
        for q in range(D // LANES):
            tmp[q, rows, :] = wide[:, q * LANES : (q + 1) * LANES]

    loop(T // LANES, widen)

    def place(i):
        x = gather_rows(tmp, i * 16, n, D)
        y = x * lax.rsqrt(jnp.mean(x * x, axis=-1, keepdims=True) + EPS) * g1[...]
        rows = at(i, LANES)
        refs.tok_p[rows, :] = x.astype(BF16)
        refs.min[rows, :] = y.astype(BF16)
        refs.min_t[:, rows] = y.T.astype(BF16)

    loop(T // LANES, place)


def cot_in(refs, T):
    n = T // SUB
    tmp = refs.buf
    D = refs.g1.shape[1]

    def widen(i):
        rows = at(i, LANES)
        wide = refs.cot[rows, :].astype(F32)
        for q in range(D // LANES):
            tmp[q, rows, :] = wide[:, q * LANES : (q + 1) * LANES]

    loop(T // LANES, widen)

    def place(i):
        x = gather_rows(tmp, i * 16, n, D)
        rows = at(i, LANES)
        refs.cot_p[rows, :] = x.astype(BF16)
        refs.cot_t[:, rows] = x.T.astype(BF16)

    loop(T // LANES, place)


def mixer_forward(refs, z, T, hook=None):
    pre, ac, st = refs.pre, refs.buf, refs.st
    halves = C // LANES
    width = 3 * LANES

    def project(i):
        rows = at(i, 256)
        out = dot(refs.min[rows, :], refs.wmix[z])
        for q in range(3 * halves):
            pre[q, rows, :] = out[:, q * LANES : (q + 1) * LANES]

    loop(T // 256, project)
    fb = refs.fb[z]
    ib = refs.ib[z]

    def gates(i, carry):
        r0 = pl.multiple_of(i * 64, 64)
        out = []
        for h in range(halves):
            a, b = carry[h]
            lanes = slice(h * LANES, (h + 1) * LANES)
            pf = pre[3 * h, pl.ds(r0, 64), :] + fb[:, lanes]
            pi = pre[3 * h + 1, pl.ds(r0, 64), :] + ib[:, lanes]
            pc = pre[3 * h + 2, pl.ds(r0, 64), :]
            pf, pi = pf * LOG2E, pi * LOG2E
            m = jnp.minimum(jnp.minimum(pf, pi), 0.0)
            e0 = jnp.exp2(m)
            ef = jnp.exp2(m - pf)
            ei = jnp.exp2(m - pi)
            nk = e0 + ei
            na = e0 + ef
            both = nk + na
            floor = jnp.maximum(na, 1e-37)
            rec = 1.0 / (both * floor)
            inv = rec * floor
            keep = nk * inv
            admit = na * inv
            ec = jnp.exp(jnp.minimum(pc, 0.0))
            sg = ec / (1.0 + ec)
            positive = pc >= 0
            value = jnp.where(positive, pc + 0.5, sg)
            slope = jnp.where(positive, 1.0, sg * (1.0 - sg))
            refs.keep[z, pl.ds(r0, 64), lanes] = keep
            refs.k_f[z, pl.ds(r0, 64), lanes] = keep * (ef * (rec * both))
            refs.k_i[z, pl.ds(r0, 64), lanes] = ei * inv
            refs.k_c[z, pl.ds(r0, 64), lanes] = admit * slope
            inflow = admit * value
            alist, blist = [], []
            for j in range(8):
                kj = keep[j * SUB : (j + 1) * SUB]
                b = kj * b + inflow[j * SUB : (j + 1) * SUB]
                a = kj * a
                alist.append(a)
                blist.append(b)
            ac[h, pl.ds(r0, 64), :] = jnp.concatenate(alist, axis=0)
            st[z, pl.ds(r0 + SUB, 64), lanes] = jnp.concatenate(blist, axis=0)
            out.append((a, b))
        return tuple(out)

    one = jnp.ones((SUB, LANES), F32)
    zero = jnp.zeros((SUB, LANES), F32)
    if hook is not None:
        hook(1)
    ends = lax.fori_loop(0, T // 64, gates, tuple((one, zero) for _ in range(halves)))
    if hook is not None:
        hook(2)
    for h in range(halves):
        a, b = ends[h]
        rows = [jnp.zeros((1, LANES), F32)]
        for s in range(SUB - 1):
            rows.append(a[s : s + 1] * rows[-1] + b[s : s + 1])
        st[z, 0:SUB, h * LANES : (h + 1) * LANES] = jnp.concatenate(rows, axis=0)
    first = st[z, 0:SUB, :]

    def finish(i):
        r0 = pl.multiple_of(i * 64, 64)
        a = load_planes(ac, pl.ds(r0, 64), 0, 2).reshape(8, SUB, C)
        b = st[z, pl.ds(r0 + SUB, 64), :].reshape(8, SUB, C)
        s = (b + a * first[None]).reshape(64, C)
        st[z, pl.ds(r0 + SUB, 64), :] = s
        refs.slow[z, pl.ds(r0, 64), :] = s.astype(BF16)

    loop(T // 64, finish)


def mix_out(refs, T):
    Z = refs.wot.shape[0]

    def body(i):
        rows = at(i, 256)
        acc = refs.tok_p[rows, :].astype(F32)
        for z in range(Z):
            acc = acc + dot_t(refs.slow[z, rows, :], refs.wot[z])
        store_planes(refs.resid, rows, acc)
        for k in range(2):
            x = acc[k * LANES : (k + 1) * LANES]
            y = x * lax.rsqrt(jnp.mean(x * x, axis=-1, keepdims=True) + EPS) * refs.g2[...]
            sub = pl.ds(pl.multiple_of(i * 256 + k * LANES, LANES), LANES)
            refs.fin[sub, :] = y.astype(BF16)
            refs.fin_t[:, sub] = y.T.astype(BF16)

    loop(T // 256, body)


def feed(refs, f, T):
    wup, wdt = refs.wup, refs.wdt
    size = 256
    tiles = T // size

    def project(i):
        rows = slice(i * size, (i + 1) * size)
        store_planes(refs.buf, rows, dot(refs.fin[rows, :], wup[f]))
        store_planes(refs.buf, rows, dot(refs.cot_p[rows, :], wdt[f]), 2)

    def activate(i):
        for k in range(size // 32):
            rows = slice(i * size + k * 32, i * size + (k + 1) * 32)
            for q in range(C // LANES):
                act, slope = gelu_parts(refs.buf[q, rows, :])
                lanes = slice(q * LANES, (q + 1) * LANES)
                refs.dpre[rows, lanes] = act.astype(BF16)
                lanes = slice(C + q * LANES, C + (q + 1) * LANES)
                refs.dpre[rows, lanes] = (refs.buf[2 + q, rows, :] * slope).astype(BF16)

    def add(i):
        rows = slice(i * size, (i + 1) * size)
        add_planes(refs.oacc, rows, dot_t(refs.dpre[rows, 0:C], wdt[f]))
        refs.dfe[rows, :] += dot_t(refs.dpre[rows, C : 2 * C], wup[f])

    for i in range(tiles + 2):
        if i < tiles:
            project(i)
        if 1 <= i < tiles + 1:
            activate(i - 1)
        if i >= 2:
            add(i - 2)


def feed_back(refs, T):
    n = T // SUB
    tmp = refs.buf
    D = refs.g1.shape[1]

    def body(i, total):
        rows = at(i, LANES)
        x = load_planes(refs.resid, rows)
        df = refs.dfe[rows, :]
        out = x + load_planes(refs.oacc, rows, 0, D // LANES)
        scatter_rows(tmp, i * 16, n, out)
        r = lax.rsqrt(jnp.mean(x * x, axis=-1, keepdims=True) + EPS)
        nrm = x * r
        dn = df * refs.g2[...]
        mean = jnp.mean(dn * nrm, axis=-1, keepdims=True)
        dres = refs.cot_p[rows, :].astype(F32) + r * (dn - nrm * mean)
        refs.dfe[rows, :] = dres
        refs.fin[rows, :] = dres.astype(BF16)
        refs.fin_t[:, rows] = dres.T.astype(BF16)
        return total + (df * nrm).reshape(16, SUB, D).sum(axis=0)

    total = lax.fori_loop(0, T // LANES, body, jnp.zeros((SUB, D), F32))
    refs.fgg[...] = jnp.sum(total, axis=0, keepdims=True)

    def emit(i):
        rows = at(i, LANES)
        for q in range(D // LANES):
            refs.block[rows, q * LANES : (q + 1) * LANES] = tmp[q, rows, :].astype(BF16)

    loop(T // LANES, emit)


def mixer_back(refs, z, T, hook=None):
    buf, st = refs.buf, refs.st
    halves = C // LANES
    width = 3 * LANES

    def project(i):
        rows = at(i, 256)
        store_planes(buf, rows, dot(refs.fin[rows, :], refs.wot[z]))

    loop(T // 256, project)
    steps = T // 64

    def local(i, carry):
        r0 = pl.multiple_of((steps - 1 - i) * 64, 64)
        d = load_planes(buf, pl.ds(r0, 64), 0, 2)
        k = refs.keep[z, pl.ds(r0, 64), :]
        e, dk = carry
        plist, dlist = [None] * 8, [None] * 8
        for j in range(7, -1, -1):
            kj = k[j * SUB : (j + 1) * SUB]
            p = d[j * SUB : (j + 1) * SUB] + e
            plist[j] = p
            dlist[j] = dk
            e = kj * p
            dk = kj * dk
        store_planes(buf, pl.ds(r0, 64), jnp.concatenate(plist, axis=0))
        store_planes(buf, pl.ds(r0, 64), jnp.concatenate(dlist, axis=0), 2)
        return e, dk

    e, dk = lax.fori_loop(0, steps, local, (jnp.zeros((SUB, C), F32), jnp.ones((SUB, C), F32)))
    rows = [jnp.zeros((1, C), F32)]
    for s in range(SUB - 1, 0, -1):
        rows.insert(0, e[s : s + 1] + dk[s : s + 1] * rows[0])
    tail = jnp.concatenate(rows, axis=0)
    if hook is not None:
        hook()

    def grads(i, sums):
        r0 = pl.multiple_of(i * 64, 64)
        out = []
        for h in range(halves):
            lanes = slice(h * LANES, (h + 1) * LANES)
            sub = pl.ds(r0, 64)
            p0 = buf[h, sub, :].reshape(8, SUB, LANES)
            d0 = buf[2 + h, sub, :].reshape(8, SUB, LANES)
            p = (p0 + d0 * tail[None, :, lanes]).reshape(64, LANES)
            x = p * (st[z, pl.ds(r0 + SUB, 64), lanes] - st[z, sub, lanes])
            df = -(refs.k_f[z, sub, lanes] * x)
            di = refs.k_i[z, sub, lanes] * x
            dcand = refs.k_c[z, sub, lanes] * p
            df16 = df.astype(BF16)
            di16 = di.astype(BF16)
            refs.dpre[sub, h * width : h * width + LANES] = df16
            refs.dpre[sub, h * width + LANES : h * width + 2 * LANES] = di16
            refs.dpre[sub, h * width + 2 * LANES : h * width + 3 * LANES] = dcand.astype(BF16)
            sf, si = sums[h]
            out.append(
                (
                    sf + df16.astype(F32).reshape(8, SUB, LANES).sum(axis=0),
                    si + di16.astype(F32).reshape(8, SUB, LANES).sum(axis=0),
                )
            )
        return tuple(out)

    zero = jnp.zeros((SUB, LANES), F32)
    sums = lax.fori_loop(0, T // 64, grads, tuple((zero, zero) for _ in range(halves)))
    for h in range(halves):
        lanes = slice(h * LANES, (h + 1) * LANES)
        refs.fbg[z, :, lanes] = jnp.sum(sums[h][0], axis=0, keepdims=True)
        refs.ibg[z, :, lanes] = jnp.sum(sums[h][1], axis=0, keepdims=True)


def mixer_input_back(refs, z, T):
    def back(i):
        rows = at(i, 256)
        add_planes(refs.oacc, rows, dot_t(refs.dpre[rows, :], refs.wmix[z]))

    loop(T // 256, back)


def norm_back(refs, T):
    n = T // SUB
    tmp = refs.buf
    D = refs.g1.shape[1]

    def body(i, total):
        rows = at(i, LANES)
        x = refs.tok_p[rows, :].astype(F32)
        d_in = load_planes(refs.oacc, rows, 0, D // LANES)
        r = lax.rsqrt(jnp.mean(x * x, axis=-1, keepdims=True) + EPS)
        nrm = x * r
        dn = d_in * refs.g1[...]
        mean = jnp.mean(dn * nrm, axis=-1, keepdims=True)
        out = refs.dfe[rows, :] + r * (dn - nrm * mean)
        scatter_rows(tmp, i * 16, n, out)
        return total + (d_in * nrm).reshape(16, SUB, D).sum(axis=0)

    total = lax.fori_loop(0, T // LANES, body, jnp.zeros((SUB, D), F32))
    refs.mgg[...] = jnp.sum(total, axis=0, keepdims=True)

    def emit(i):
        rows = at(i, LANES)
        for q in range(D // LANES):
            refs.tgrad[rows, q * LANES : (q + 1) * LANES] = tmp[q, rows, :].astype(BF16)

    loop(T // LANES, emit)


class Refs:
    def __init__(self, args):
        (
            self.tok, self.cot, self.wmix, self.wot, self.wup, self.wdt, self.g1, self.g2, self.fb, self.ib,
            self.block, self.tgrad, self.gmix, self.got, self.gup, self.gdt, self.fgg, self.mgg, self.fbg, self.ibg,
            self.tok_p, self.min, self.min_t, self.fin, self.fin_t, self.cot_p, self.cot_t, self.resid, self.oacc, self.dfe,
            self.pre, self.buf, self.dpre, self.slow, self.st, self.keep, self.k_f,
            self.k_i, self.k_c, self.gst, self.gsem,
        ) = args


def layer_kernel(*args):
    refs = Refs(args)
    T, D = refs.tok.shape
    Z = refs.wmix.shape[0]
    F = refs.wup.shape[0]
    gst, sem = refs.gst, refs.gsem
    cot_in(refs, T)
    norm_in(refs, T)
    loop(Z, lambda z: mixer_forward(refs, z, T))
    mix_out(refs, T)
    clear(refs.oacc, T)
    refs.dfe[...] = jnp.zeros_like(refs.dfe)

    def feed_step(f):
        feed(refs, f, T)
        gst[0, :, 0:C] = dot(refs.cot_t[...], refs.dpre[:, 0:C])
        gst[1, :, 0:C] = dot(refs.fin_t[...], refs.dpre[:, C : 2 * C])
        one = pltpu.make_async_copy(gst.at[0, :, 0:C], refs.gdt.at[f], sem.at[0])
        two = pltpu.make_async_copy(gst.at[1, :, 0:C], refs.gup.at[f], sem.at[1])
        one.start()
        two.start()
        one.wait()
        two.wait()

    loop(F, feed_step)
    feed_back(refs, T)
    clear(refs.oacc, T)

    def mixer_step(z):
        gst[0, :, 0:C] = dot(refs.fin_t[...], refs.slow[z])
        mixer_back(refs, z, T)
        mixer_input_back(refs, z, T)
        gst[1, :, :] = dot(refs.min_t[...], refs.dpre[...])
        one = pltpu.make_async_copy(gst.at[0, :, 0:C], refs.got.at[z], sem.at[0])
        two = pltpu.make_async_copy(gst.at[1], refs.gmix.at[z], sem.at[1])
        one.start()
        two.start()
        one.wait()
        two.wait()

    loop(Z, mixer_step)
    norm_back(refs, T)


def layer(tok, cot, wmix, wot, wup, wdt, g1, g2, fb, ib):
    T, D = tok.shape
    Z, F = wmix.shape[0], wup.shape[0]
    sds = jax.ShapeDtypeStruct
    vm = pl.BlockSpec(memory_space=pltpu.VMEM)
    anyspec = pl.BlockSpec(memory_space=pl.ANY)
    out_shape = (
        sds((T, D), BF16), sds((T, D), BF16),
        sds((Z, D, 3 * C), F32), sds((Z, D, C), F32), sds((F, D, C), F32), sds((F, D, C), F32),
        sds((1, D), F32), sds((1, D), F32), sds((Z, 1, C), F32), sds((Z, 1, C), F32),
    )
    V = pltpu.VMEM
    scratch = [
        V((T, D), BF16), V((T, D), BF16), V((D, T), BF16), V((T, D), BF16), V((D, T), BF16),
        V((T, D), BF16), V((D, T), BF16), V((D // LANES, T, LANES), F32),
        V((D // LANES, T, LANES), F32), V((T, D), F32), V((3 * C // LANES, T, LANES), F32), V((4, T, LANES), F32),
        V((T, 3 * C), BF16), V((Z, T, C), BF16), V((Z, T + SUB, C), F32),
        V((Z, T, C), F32), V((Z, T, C), F32), V((Z, T, C), F32), V((Z, T, C), F32),
        V((2, D, 3 * C), F32), pltpu.SemaphoreType.DMA((2,)),
    ]
    return pl.pallas_call(
        layer_kernel,
        out_shape=out_shape,
        in_specs=[vm] * 10,
        out_specs=(vm, vm, anyspec, anyspec, anyspec, anyspec, vm, vm, vm, vm),
        scratch_shapes=scratch,
        compiler_params=pltpu.CompilerParams(vmem_limit_bytes=67043328),
        name="layer",
    )(tok, cot, wmix, wot, wup, wdt, g1, g2, fb, ib)


MESH = pl.DeviceIdType.MESH


def rcopy(src, dst, send, recv, device):
    return pltpu.make_async_remote_copy(
        src_ref=src, dst_ref=dst, send_sem=send, recv_sem=recv, device_id=device, device_id_type=MESH
    )


class Place:
    def __init__(self):
        self.g = lax.axis_index("grp")
        self.i = lax.axis_index("inner")
        self.y, self.x = self.g // 2, self.g % 2
        self.z, self.c = self.i // 2, self.i % 2
        self.me = self.g * 8 + self.i
        self.partner = (self.g, self.z * 2 + 1 - self.c)

    def flip(self, fx, fy):
        x = (self.x + fx) % 2
        y = (self.y + fy) % 2
        return y * 2 + x

    def turn(self, z):
        return (z + self.c) % 2

    def near(self, z):
        e = self.turn(z)
        return self.flip(1 - e, e)

    def far(self, z):
        e = self.turn(z)
        return self.flip(e, 1 - e)

    def other(self, k):
        t = (self.me + k) % 32
        return (t // 8, t % 8)


def entry_barrier(place):
    barrier = pltpu.get_barrier_semaphore()

    def greet(k):
        pl.semaphore_signal(barrier, inc=1, device_id=place.other(k + 1), device_id_type=MESH)

    loop(31, greet)
    pl.semaphore_wait(barrier, 31)


def spread(values, start, count, total):
    lane = lax.broadcasted_iota(jnp.int32, (LANES, total), 1)
    row = lax.broadcasted_iota(jnp.int32, (LANES, total), 0)
    sel = jnp.where(row == start + lane % count, 1.0, 0.0).astype(BF16)
    picked = dot(values, sel)
    owner = lax.broadcasted_iota(jnp.int32, picked.shape, 0)
    spot = lax.broadcasted_iota(jnp.int32, picked.shape, 1)
    return jnp.sum(jnp.where(spot // count == owner, picked, 0.0), axis=0, keepdims=True)


def pack_vectors(mg, fb, ib, fg):
    parts = [mg, fb, ib, fg]
    used = sum(p.shape[0] for p in parts)
    rows = [p[...].astype(F32).reshape(1, p.shape[0]) for p in parts]
    return jnp.concatenate(rows + [jnp.zeros((1, LANES - used), F32)], axis=1)


FIRST = (3, 0)
LATER = (1, 2)


def block_of(refs, a, g, i):
    if a == 0:
        return refs.wot.at[g, at(i, 64), :]
    if a == 1:
        return refs.wup.at[i, at(g, 128), :]
    if a == 2:
        return refs.wdt.at[pl.ds(2 * g, 2), at(i, 64), :]
    return refs.wmix.at[i // 2, at(g, 128), at(i % 2, 384)]


def blocks_of(refs, a, i):
    if a == 0:
        return refs.wot.at[:, at(i, 64), :]
    if a == 1:
        return refs.wup.at[i]
    if a == 2:
        return refs.wdt.at[:, at(i, 64), :]
    return refs.wmix.at[i // 2, :, at(i % 2, 384)]


def line_send(refs, p, a):
    blk = block_of(refs, a, p.g, p.i)
    for s in range(1, 4):
        peer = (p.g, slot_chunk(p, s) * 2 + p.c)
        rcopy(blk, blk, refs.gz_s.at[a, s - 1], refs.gz_r.at[a, p.z], peer).start()


def near_of(p, a, z):
    return p.near(z + (a in LATER))


def far_of(p, a, z):
    return p.far(z + (a in LATER))


def line_wait(refs, p, a, z):
    @pl.when(z != p.z)
    def _():
        blk = block_of(refs, a, p.g, z * 2 + p.c)
        rcopy(blk, blk, refs.gp_s.at[a, z, 0], refs.gz_r.at[a, z], p.partner).wait_recv()


def near_send(refs, p, a, z):
    blk = block_of(refs, a, p.g, z * 2 + p.c)
    near, far = (near_of(p, a, z), p.i), (far_of(p, a, z), p.i)
    rcopy(blk, blk, refs.gn_s.at[a, z], refs.gn_r.at[a, z], near).start()
    rcopy(blk, blk, refs.gf_s.at[a, z, 0], refs.gf_r.at[a, z, 0], far).start()


def far_send(refs, p, a, z):
    near = block_of(refs, a, near_of(p, a, z), z * 2 + p.c)
    far = (far_of(p, a, z), p.i)
    rcopy(near, near, refs.gn_s.at[a, z], refs.gn_r.at[a, z], p.partner).wait_recv()
    rcopy(near, near, refs.gf_s.at[a, z, 1], refs.gf_r.at[a, z, 1], far).start()


def far_wait(refs, p, a, z, k):
    blk = block_of(refs, a, p.g, z * 2 + p.c)
    rcopy(blk, blk, refs.gf_s.at[a, z, k], refs.gf_r.at[a, z, k], p.partner).wait_recv()


def pair_copy(refs, p, a, z, c):
    full = blocks_of(refs, a, z * 2 + c)
    return rcopy(full, full, refs.gp_s.at[a, z, 0], refs.gp_r.at[a, z, 0], p.partner)


def first_step(refs, p, arrays, kind, s):
    for a in arrays:
        z = slot_chunk(p, s)
        if kind == "n":
            line_wait(refs, p, a, z)
            near_send(refs, p, a, z)
        elif kind == "f":
            far_send(refs, p, a, z)
        elif kind == "p":
            far_wait(refs, p, a, z, 0)
            far_wait(refs, p, a, z, 1)
            pair_copy(refs, p, a, z, p.c).start()
        else:
            pair_copy(refs, p, a, z, 1 - p.c).wait_recv()


def up_step(refs, p, kind, m):
    if kind == "n":

        @pl.when(p.z != m)
        def _():
            line_wait(refs, p, 1, m)
            near_send(refs, p, 1, m)
    elif kind == "f":
        far_send(refs, p, 1, m)
    elif kind == "p":
        far_wait(refs, p, 1, m, 0)
        far_wait(refs, p, 1, m, 1)
        pair_copy(refs, p, 1, m, p.c).start()
    else:
        pair_copy(refs, p, 1, m, 1 - p.c).wait_recv()


def up_own(refs, p, phase):
    inner = (p.z + 1) // 2 % 2

    @pl.when(inner == phase)
    def _():
        near_send(refs, p, 1, p.z)


def down_pair(refs, p, z, phase, k, c):
    g = (1 + k) if phase else 3 * k
    blk = block_of(refs, 2, g, z * 2 + c)
    return rcopy(blk, blk, refs.gp_s.at[2, z, phase * 2 + k], refs.gp_r.at[2, z, phase * 2 + k], p.partner)


def down_step(refs, p, kind, phase, s):
    z = slot_chunk(p, s)
    active = (p.x + p.y) % 2 == phase
    idle = (p.x + p.y) % 2 != phase
    if kind == "n":

        @pl.when(active)
        def _():
            line_wait(refs, p, 2, z)
            near_send(refs, p, 2, z)
    elif kind == "f":

        @pl.when(idle)
        def _():
            far_send(refs, p, 2, z)
    elif kind == "p":

        @pl.when(active)
        def _():
            far_wait(refs, p, 2, z, 1)

        @pl.when(idle)
        def _():
            far_wait(refs, p, 2, z, 0)

        for k in range(2):
            down_pair(refs, p, z, phase, k, p.c).start()
    else:
        for k in range(2):
            down_pair(refs, p, z, phase, k, 1 - p.c).wait_recv()


def gather_drain(refs, p):
    for a in range(4):
        blk = block_of(refs, a, p.g, p.i)
        for k in range(3):
            rcopy(blk, blk, refs.gz_s.at[a, k], refs.gz_r.at[a, p.z], p.partner).wait_send()
        for z in range(4):
            blk = block_of(refs, a, p.g, z * 2 + p.c)
            rcopy(blk, blk, refs.gn_s.at[a, z], refs.gn_r.at[a, z], p.partner).wait_send()
            for k in range(2):
                rcopy(blk, blk, refs.gf_s.at[a, z, k], refs.gf_r.at[a, z, k], p.partner).wait_send()
            if a == 2:
                for k in range(4):
                    down_pair(refs, p, z, k // 2, k % 2, p.c).wait_send()
            else:
                pair_copy(refs, p, a, z, p.c).wait_send()


def gather_hook(refs, p, actions):
    for action in actions.split():
        kind, number = action[1], int(action[-1])
        if action[0] == "M":
            first_step(refs, p, (3,), kind, number)
        elif action[0] == "W":
            first_step(refs, p, (0,), kind, number)
        elif action[0] == "U":
            up_step(refs, p, kind, number)
        else:
            down_step(refs, p, kind, int(action[2]), number)


def gather_start(refs, p):
    local = []
    for k, w in enumerate((refs.fw, refs.iw, refs.cw)):
        spot = pl.ds(pl.multiple_of(p.c * 384 + k * 128, 128), 128)
        local.append(
            pltpu.make_async_copy(w, refs.wmix.at[p.z, at(p.g, 128), spot], refs.loc_s.at[k])
        )
    local.append(pltpu.make_async_copy(refs.ow, block_of(refs, 0, p.g, p.i), refs.loc_s.at[3]))
    local.append(pltpu.make_async_copy(refs.uw, block_of(refs, 1, p.g, p.i), refs.loc_s.at[4]))
    for k in range(2):
        local.append(
            pltpu.make_async_copy(
                refs.dw.at[:, k * 256 : (k + 1) * 256],
                refs.wdt.at[2 * p.g + k, at(p.i, 64), :],
                refs.loc_s.at[5 + k],
            )
        )
    for c in local:
        c.start()
    row = pack_vectors(refs.mg, refs.fbv, refs.ibv, refs.fg)
    refs.vstage[...] = row
    refs.vecs[p.me] = row
    for c in local:
        c.wait()
    entry_barrier(p)

    def vector(k):
        rcopy(refs.vstage, refs.vecs.at[p.me], refs.vec_s, refs.vec_r, p.other(k + 1)).start()

    for a in FIRST:
        near_send(refs, p, a, p.z)
    up_own(refs, p, 0)
    down_step(refs, p, "n", 0, 0)
    loop(31, vector)
    for a in FIRST:
        line_send(refs, p, a)
    inner = (p.z + 1) // 2 % 2

    @pl.when(inner == 0)
    def _():
        line_send(refs, p, 1)

    line_send(refs, p, 2)

    @pl.when(inner == 1)
    def _():
        line_send(refs, p, 1)


def gather_vectors(refs, p):
    rows = refs.vecs.at[pl.ds(0, 31)]
    rcopy(rows, rows, refs.vec_s, refs.vec_r, p.partner).wait()
    v = refs.vecs[...].reshape(32, LANES).astype(BF16)
    refs.g1[...] = spread(v, 0, 16, 512)
    refs.g2[...] = spread(v, 80, 16, 512)
    fb = spread(v, 16, 32, 1024)
    ib = spread(v, 48, 32, 1024)
    for z in range(4):
        refs.fb[z] = fb[:, z * C : (z + 1) * C]
        refs.ib[z] = ib[:, z * C : (z + 1) * C]


def slot_chunk(p, s):
    low = jnp.minimum(p.z, 3 - p.z)
    shift = jnp.where(s == 0, 1, jnp.where(s == 1, -1, 0))
    m = s + low * shift
    return jnp.where(p.z < 2, m, 3 - m)


SLOT_HOOKS = (
    ("", "Mn3", "Mp1 Mf2"),
    ("Md1", "Mf3 Wf0 Wn1 Wn2", "Mp2 Wn3 Wf1 Dn01"),
    ("Md2", "Mp3 Wf2 Wp0 Un0 Un3", "Wf3 Df00 Dn02 Dn03 Df01"),
    ("Md3", "Wp1 Wp2 Wp3 Uf0 Uf3 Df02 Df03", "Dp00 Dp01 Dp02 Dp03 Up0 Up3"),
)


def mixer_slots(refs, p, T):
    def hook(s, j):
        for k in range(4):

            @pl.when(s == k)
            def _():
                gather_hook(refs, p, SLOT_HOOKS[k][j])

    def slot(s):
        hook(s, 0)
        mixer_forward(refs, slot_chunk(p, s), T, lambda j: hook(s, j))

    loop(4, slot)


SHAPES = ((128, 256), (128, 256), (128, 384), (64, 256))
UP, DOWN, MIX, OUT = 0, 1, 2, 3
TINY = 1e-30
CLIP = 0.01
MATRICES = (
    (512, 1024), (512, 1024), (512, 1024), (1024, 512), (512, 2048), (2048, 512)
)
MATRIX_SLOTS = (1, 2, 3, 6, 8, 9)
VECTORS = ((0, 0, 16), (4, 16, 32), (5, 48, 32), (7, 80, 16))
COUNTS = (512, 524288, 524288, 524288, 1024, 1024, 524288, 512, 1048576, 1048576)


def spot(a, g, z):
    return (g, z) if a == DOWN else (z, g)


def rs_store(refs, a, g, z, value):
    refs.psend[a][(*spot(a, g, z),)] = value.astype(BF16)


def rs_role(p, g, z):
    e = p.turn(z)
    y, x = g // 2, g % 2
    return (1 - e) * ((x + p.x) % 2) + e * ((y + p.y) % 2)


def rs_pair(refs, p, a, u):
    if a == OUT:
        src, dst = refs.psend[a], refs.precv[a]
    else:
        src, dst = refs.psend[a].at[u], refs.precv[a].at[u]
    return rcopy(src, dst, refs.rp_s.at[a, u], refs.rp_r.at[a, u], p.partner)


def rs_merge(refs, p, a, g, z, own):
    place = spot(a, g, z)
    v = own + refs.precv[a][place].astype(F32)
    role = rs_role(p, g, z)

    @pl.when(role == 1)
    def _():
        refs.psend[a][place] = v.astype(BF16)

    @pl.when(role == 0)
    def _():
        refs.precv[a][place] = v.astype(BF16)


def rs_group(p, z, k, sent):
    e = p.turn(z)
    x = (1 - e) * ((p.x + sent) % 2) + e * k
    y = (1 - e) * k + e * ((p.y + sent) % 2)
    return y * 2 + x


def rs_first_copy(refs, p, a, z, k):
    g = rs_group(p, z, k, 1)
    return rcopy(
        refs.psend[a].at[spot(a, g, z)], refs.r1[a].at[z, k],
        refs.r1_s.at[a, z, k], refs.r1_r.at[a, z, k], (p.near(z), p.i),
    )


def rs_first_send(refs, p, a, z):
    for k in range(2):
        rs_first_copy(refs, p, a, z, k).start()


def rs_second(refs, p, a, z):
    e = p.turn(z)
    mine = (1 - e) * p.y + e * p.x
    for k in range(2):
        rs_first_copy(refs, p, a, z, k).wait_recv()
    for k in range(2):
        place = spot(a, rs_group(p, z, k, 0), z)
        v = (refs.precv[a][place].astype(F32) + refs.r1[a][z, k].astype(F32)).astype(BF16)

        @pl.when(mine == k)
        def _():
            refs.precv[a][place] = v

        @pl.when(mine != k)
        def _():
            refs.psend[a][place] = v


def rs_second_copy(refs, p, a, z):
    e = p.turn(z)
    other = 1 - ((1 - e) * p.y + e * p.x)
    place = spot(a, rs_group(p, z, other, 0), z)
    return rcopy(
        refs.psend[a].at[place], refs.r2[a].at[z], refs.r2_s.at[a, z], refs.r2_r.at[a, z],
        (p.far(z), p.i),
    )


def rs_third(refs, p, a, z):
    rs_second_copy(refs, p, a, z).wait_recv()
    place = spot(a, p.g, z)
    v = refs.precv[a][place].astype(F32) + refs.r2[a][z].astype(F32)

    @pl.when(z == p.z)
    def _():
        refs.fin_g[a][...] = v

    @pl.when(z != p.z)
    def _():
        refs.psend[a][place] = v.astype(BF16)


def rs_line(refs, p, a, z, owner):
    return rcopy(
        refs.psend[a].at[spot(a, p.g, z)], refs.r3[a].at[owner],
        refs.r3_s.at[a, z], refs.r3_r.at[a, owner], (p.g, z * 2 + p.c),
    )


def rs_third_send(refs, p, a, z):
    @pl.when(z != p.z)
    def _():
        rs_line(refs, p, a, z, p.z).start()


def rs_last(refs, p, a):
    for k in range(1, 4):
        z = (p.z + k) % 4
        rs_line(refs, p, a, z, z).wait_recv()
        refs.fin_g[a][...] += refs.r3[a][z].astype(F32)


def rs_drain(refs, p):
    def one(z):
        for a in range(4):
            for k in range(2):
                rs_first_copy(refs, p, a, z, k).wait_send()
            rs_second_copy(refs, p, a, z).wait_send()

            @pl.when(z != p.z)
            def _():
                rs_line(refs, p, a, z, p.z).wait_send()

    loop(4, one)


def own_row(x):
    return jnp.sum(x, axis=0, keepdims=True)


def lane_sum(x):
    folded = sum(x[:, k : k + LANES] for k in range(0, x.shape[1], LANES))
    return own_row(folded.T)


def wide(row):
    return jnp.concatenate([row, jnp.zeros((1, LANES - row.shape[1]), F32)], axis=1)


def cut(row):
    return [row[:, k : k + LANES] for k in range(0, row.shape[1], LANES)]


def stand(row):
    return jnp.broadcast_to(row, (LANES, LANES)).T


def scalars(values):
    lane = lax.broadcasted_iota(jnp.int32, (1, LANES), 1)
    out = jnp.zeros((1, LANES), F32)
    for k, v in enumerate(values):
        out = out + jnp.where(lane == k, v, 0.0)
    return out


def total(x):
    return jnp.sum(jnp.sum(x, axis=0, keepdims=True), axis=1, keepdims=True)


def segment(row, start, count):
    lane = lax.broadcasted_iota(jnp.int32, row.shape, 1)
    keep = (lane >= start) & (lane < start + count)
    return jnp.sum(jnp.where(keep, row, 0.0), axis=1, keepdims=True)


def gather_row(term, start, count):
    size = term.shape[1]
    owner = lax.broadcasted_iota(jnp.int32, (32, size), 0)
    spot = lax.broadcasted_iota(jnp.int32, (32, size), 1)
    masked = jnp.where(spot // count == owner, term, 0.0)
    lane = lax.broadcasted_iota(jnp.int32, (LANES, size), 0)
    from_spot = lax.broadcasted_iota(jnp.int32, (LANES, size), 1)
    sel = jnp.where(lane == start + from_spot % count, 1.0, 0.0).astype(BF16)
    out = jnp.zeros((32, LANES), F32)
    for _ in range(3):
        part = masked.astype(BF16)
        out = out + dot_t(part, sel)
        masked = masked - part.astype(F32)
    return out


def parameter_blocks(refs):
    return [
        refs.fw[...].astype(F32), refs.iw[...].astype(F32), refs.cw[...].astype(F32),
        refs.ow[...].astype(F32), refs.uw[...].astype(F32), refs.dw[...].astype(F32),
    ]


def old_rows(refs):
    rows = []
    for r in (refs.row_f, refs.row_i, refs.row_c, refs.row_o, refs.row_u, refs.row_d):
        rows += cut(r[...].reshape(1, r.shape[0]))
    return rows


def old_columns(refs):
    rows = []
    for r in (refs.col_f, refs.col_i, refs.col_c, refs.col_o, refs.col_u, refs.col_d):
        row = r[...].reshape(1, r.shape[0])
        rows += [wide(row)] if r.shape[0] < LANES else cut(row)
    return rows


ROW_PLACES = ((0, 1), (1, 2), (2, 3), (3, 5), (5, 6), (6, 10))
COLUMN_PLACES = ((0, 1), (1, 2), (2, 3), (3, 4), (4, 6), (6, 7))


def broadcast_row(src, box, send, recv, p):
    def one(k):
        rcopy(src, box.at[p.me], send, recv, p.other(k + 1)).start()

    loop(31, one)


def settle_row(box, send, recv, p):
    rows = box.at[pl.ds(0, 31)]
    rcopy(rows, rows, send, recv, p.partner).wait()


def vector_exchange(refs, p):
    rows = (
        gather_row(refs.mgg[...], 0, 16)
        + gather_row(jnp.concatenate([refs.fbg[z] for z in range(4)], axis=1), 16, 32)
        + gather_row(jnp.concatenate([refs.ibg[z] for z in range(4)], axis=1), 48, 32)
        + gather_row(refs.fgg[...], 80, 16)
    )
    refs.vout[...] = rows.reshape(32, 1, LANES)
    refs.vin[p.me] = refs.vout[p.me]

    def one(k):
        t = (p.me + k + 1) % 32
        rcopy(refs.vout.at[t], refs.vin.at[p.me], refs.vex_s, refs.vex_r, p.other(k + 1)).start()

    loop(31, one)


def gradient_blocks(refs):
    mix = refs.fin_g[MIX][...]
    down = refs.fin_g[DOWN][...]
    return [
        mix[:, 0:128], mix[:, 128:256], mix[:, 256:384], refs.fin_g[OUT][...], refs.fin_g[UP][...],
        jnp.concatenate([down[0:64], down[64:128]], axis=1),
    ]


def adafactor(refs, p):
    grads = gradient_blocks(refs)
    flipped = (False, False, False, True, False, True)
    row_parts, column_parts, totals = [], [], []
    for grad, flip in zip(grads, flipped):
        sq = grad * grad
        down, across = own_row(sq), lane_sum(sq)
        row_parts += cut(down) if flip else [across]
        column_parts += [wide(across)] if flip else cut(down)
        totals.append(jnp.sum(down, axis=1, keepdims=True))
    refs.rowst[...] = jnp.concatenate(row_parts + [jnp.zeros((6, LANES), F32)], axis=0)
    refs.colst[...] = jnp.concatenate(column_parts + [jnp.zeros((1, LANES), F32)], axis=0)
    weights = parameter_blocks(refs)
    params = pack_vectors(refs.mg, refs.fbv, refs.ibv, refs.fg)
    squares = [None] * 10
    for slot, w in zip(MATRIX_SLOTS, weights):
        squares[slot] = total(w * w)
    for slot, start, count in VECTORS:
        squares[slot] = segment(params * params, start, count)
    rows_old, columns_old = old_rows(refs), old_columns(refs)
    first = jnp.where(p.i == 0, 1.0, 0.0)
    row_sums = [first * total(jnp.concatenate(rows_old[a:b], axis=0)) for a, b in ROW_PLACES]
    refs.scal[...] = scalars(totals + squares + row_sums)
    refs.rowin[p.i] = refs.rowst[...]
    refs.colin[p.g] = refs.colst[...]
    refs.scin[p.me] = refs.scal[...]
    for k in range(1, 8):
        peer = (p.g, (p.i + k) % 8)
        rcopy(
            refs.rowst, refs.rowin.at[p.i], refs.row_s.at[k - 1], refs.row_r.at[k - 1], peer
        ).start()
    for k in range(1, 4):
        peer = ((p.g + k) % 4, p.i)
        rcopy(
            refs.colst, refs.colin.at[p.g], refs.col_s.at[k - 1], refs.col_r.at[k - 1], peer
        ).start()
    broadcast_row(refs.scal, refs.scin, refs.sc_s, refs.sc_r, p)
    vec_rows = refs.vin.at[pl.ds(0, 31)]
    rcopy(vec_rows, vec_rows, refs.vex_s, refs.vex_r, p.partner).wait()
    vector_grad = jnp.sum(refs.vin[...].reshape(32, LANES), axis=0, keepdims=True)
    seconds = pack_vectors(refs.sec_m, refs.sec_f, refs.sec_i, refs.sec_g)
    second = 0.5 * seconds + 0.5 * (vector_grad * vector_grad + TINY)
    vector_scaled = vector_grad * lax.rsqrt(second)
    for k in range(1, 8):
        rcopy(
            refs.rowst, refs.rowin.at[p.i], refs.row_s.at[k - 1], refs.row_r.at[k - 1], p.partner
        ).wait()
    for k in range(1, 4):
        rcopy(
            refs.colst, refs.colin.at[p.g], refs.col_s.at[k - 1], refs.col_r.at[k - 1], p.partner
        ).wait()
    settle_row(refs.scin, refs.sc_s, refs.sc_r, p)
    row_total = sum(refs.rowin[k] for k in range(8))
    column_total = sum(refs.colin[k] for k in range(4))
    sc = jnp.sum(refs.scin[...].reshape(32, LANES), axis=0, keepdims=True)
    rows_new, columns_new, scaled = [], [], []
    for k, (r, c) in enumerate(MATRICES):
        ra, rb = ROW_PLACES[k]
        ca, cb = COLUMN_PLACES[k]
        rows = [
            0.5 * rows_old[j] + 0.5 * (row_total[j : j + 1] / c + TINY) for j in range(ra, rb)
        ]
        columns = [
            0.5 * columns_old[j] + 0.5 * (column_total[j : j + 1] / r + TINY)
            for j in range(ca, cb)
        ]
        mean = 0.5 * sc[:, 16 + k : 17 + k] / r + 0.5 * (sc[:, k : k + 1] / (r * c) + TINY)
        lying, standing = (rows, columns) if flipped[k] else (columns, rows)
        tall = stand(standing[0])[0 : grads[k].shape[0]]
        lying = jnp.concatenate(lying, axis=1)
        tall = jnp.concatenate([tall] * (lying.shape[1] // LANES), axis=1)
        scaled.append(grads[k] * lax.rsqrt(tall * lying / mean))
        rows_new += rows
        columns_new += columns
    refs.rows_out[...] = jnp.concatenate(rows_new + [jnp.zeros((6, LANES), F32)], axis=0)
    refs.columns_out[...] = jnp.concatenate(columns_new + [jnp.zeros((1, LANES), F32)], axis=0)
    clips = [None] * 10
    for slot, s in zip(MATRIX_SLOTS, scaled):
        clips[slot] = total(s * s)
    for slot, start, count in VECTORS:
        clips[slot] = segment(vector_scaled * vector_scaled, start, count)
    refs.clip[...] = scalars(clips)
    refs.clin[p.me] = refs.clip[...]
    broadcast_row(refs.clip, refs.clin, refs.cl_s, refs.cl_r, p)
    settle_row(refs.clin, refs.cl_s, refs.cl_r, p)
    clip = jnp.sum(refs.clin[...].reshape(32, LANES), axis=0, keepdims=True)
    norms = [jnp.sqrt(clip[:, k : k + 1] / COUNTS[k]) for k in range(10)]
    steps = [
        -jnp.sqrt(sc[:, 6 + k : 7 + k] / COUNTS[k]) / jnp.maximum(CLIP, norms[k])
        for k in range(10)
    ]
    fresh = [w + steps[slot] * s for slot, w, s in zip(MATRIX_SLOTS, weights, scaled)]
    refs.grad_mix[...] = refs.fin_g[MIX][...]
    refs.grad_out[...] = grads[3]
    refs.grad_up[...] = grads[4]
    refs.grad_down[...] = grads[5]
    refs.new_mix[...] = jnp.concatenate(fresh[0:3], axis=1)
    refs.new_out[...] = fresh[3]
    refs.new_up[...] = fresh[4]
    refs.new_down[...] = fresh[5]
    lane = lax.broadcasted_iota(jnp.int32, (1, LANES), 1)
    step_row = jnp.zeros((1, LANES), F32)
    for slot, start, count in VECTORS:
        step_row = step_row + jnp.where((lane >= start) & (lane < start + count), steps[slot], 0.0)
    refs.vectors[...] = jnp.concatenate(
        [vector_grad, params + step_row * vector_scaled, second, scalars(norms)]
        + [jnp.zeros((4, LANES), F32)],
        axis=0,
    )


def finish_kernel(
    grad_mix, grad_out, grad_up, grad_down, new_mix, new_out, new_up, new_down,
    vectors, rows, columns, block_in, token_in,
    g_mg, g_f, g_i, g_c, g_fb, g_ib, g_o, g_fg, g_u, g_d,
    n_mg, n_f, n_i, n_c, n_fb, n_ib, n_o, n_fg, n_u, n_d,
    s_m, r_f, c_f, r_i, c_i, r_c, c_c, s_f, s_i, r_o, c_o, s_g, r_u, c_u, r_d, c_d, norms,
    block_out, token_out, stage, sem,
):
    copies = []
    for k, (src, dst) in enumerate(((block_in, block_out), (token_in, token_out))):
        fetch = pltpu.make_async_copy(src, stage.at[k], sem.at[0, k])
        fetch.start()
        copies.append((fetch, pltpu.make_async_copy(stage.at[k], dst, sem.at[1, k])))
    for fetch, put in copies:
        fetch.wait()
        put.start()
    for src, outs in ((grad_mix, (g_f, g_i, g_c)), (new_mix, (n_f, n_i, n_c))):
        for k, o in enumerate(outs):
            o[...] = src[:, k * 128 : (k + 1) * 128]
    for src, o in ((grad_out, g_o), (new_out, n_o), (grad_down, g_d), (new_down, n_d)):
        o[...] = src[...]
    g_u[...] = grad_up[...]
    n_u[...] = new_up[...]
    for row, outs in (
        (0, (g_mg, g_fb, g_ib, g_fg)), (1, (n_mg, n_fb, n_ib, n_fg)), (2, (s_m, s_f, s_i, s_g))
    ):
        for (_, start, count), o in zip(VECTORS, outs):
            o[...] = vectors[row, start : start + count]
    norms[...] = vectors[3, 0:10]
    for src, places, outs in (
        (rows, ROW_PLACES, (r_f, r_i, r_c, r_o, r_u, r_d)),
        (columns, COLUMN_PLACES, (c_f, c_i, c_c, c_o, c_u, c_d)),
    ):
        for (a, b), o in zip(places, outs):
            if b - a == 1:
                o[...] = src[a, 0 : o.shape[0]]
            else:
                for k in range(a, b):
                    o[(k - a) * LANES : (k - a + 1) * LANES] = src[k, :]
    for fetch, put in copies:
        put.wait()


def finish(packed, block, tgrad):
    sds = jax.ShapeDtypeStruct
    f = lambda *s: sds(s, F32)
    small = [f(16), f(128, 128), f(128, 128), f(128, 128), f(32), f(32), f(64, 256), f(16),
             f(128, 256), f(64, 512)]
    states = [f(16), f(128), f(128), f(128), f(128), f(128), f(128), f(32), f(32), f(256), f(64),
              f(16), f(128), f(256), f(512), f(64)]
    big = sds(block.shape, BF16)
    outs = tuple(small + small + states + [f(10), big, big])
    vm = pl.BlockSpec(memory_space=pltpu.VMEM)
    anyspec = pl.BlockSpec(memory_space=pl.ANY)
    return pl.pallas_call(
        finish_kernel,
        out_shape=outs,
        in_specs=[vm] * len(packed) + [anyspec] * 2,
        out_specs=(vm,) * (len(outs) - 2) + (anyspec,) * 2,
        scratch_shapes=[pltpu.VMEM((2,) + block.shape, BF16), pltpu.SemaphoreType.DMA((2, 2))],
        name="finish",
    )(*packed, block, tgrad)


class FusedRefs:
    def __init__(self, args):
        (
            self.tok_in, self.cot_in, self.fw, self.iw, self.cw, self.ow, self.uw, self.dw,
            self.mg, self.fbv, self.ibv, self.fg,
            self.sec_m, self.row_f, self.col_f, self.row_i, self.col_i, self.row_c, self.col_c,
            self.sec_f, self.sec_i, self.row_o, self.col_o, self.sec_g,
            self.row_u, self.col_u, self.row_d, self.col_d,
            self.block_out, self.tgrad_out,
            self.grad_mix, self.grad_out, self.grad_up, self.grad_down,
            self.new_mix, self.new_out, self.new_up, self.new_down,
            self.vectors, self.rows_out, self.columns_out,
            self.wmix, self.wot, self.wup, self.wdt, self.g1, self.g2, self.fb, self.ib,
            self.vecs, self.vstage, self.fgg, self.mgg, self.fbg, self.ibg,
            self.tok_p, self.fin, self.min_t, self.fin_t, self.cot_p, self.cot_t,
            self.resid, self.dfe,
            self.pre, self.buf, self.dpre, self.slow, self.st,
            self.keep, self.k_f, self.k_i, self.k_c,
            self.loc_s, self.vec_s, self.vec_r, self.gz_s, self.gz_r,
            self.gn_s, self.gn_r, self.gf_s, self.gf_r, self.gp_s, self.gp_r,
            self.vout, self.vin, self.rowst, self.rowin, self.colst, self.colin,
            self.scal, self.scin, self.clip, self.clin,
            self.rp_s, self.rp_r, self.r1_s, self.r1_r, self.r2_s, self.r2_r,
            self.r3_s, self.r3_r, self.vex_s, self.vex_r,
            self.row_s, self.row_r, self.col_s, self.col_r, self.sc_s, self.sc_r,
            self.cl_s, self.cl_r, self.io_s,
        ) = args[:112]
        rest = list(args[112:])
        self.psend, self.precv, self.r1, self.r2, self.r3, self.fin_g = (
            rest[4 * k : 4 * k + 4] for k in range(6)
        )
        self.io = self.dpre.at[:, 0:512]
        self.oacc = self.pre.at[pl.ds(4, 4)]
        self.tok = self.cot = self.block = self.tgrad = self.io
        self.min = self.fin


def halves_of(refs, plane, rows):
    size = rows.size
    low = refs.pre[plane, rows, :]
    high = refs.pre[plane, pl.ds(rows.start + 512, size), :]
    return jnp.concatenate([low, high], axis=1)


def put_halves(refs, plane, value):
    refs.pre[plane, 0:512, :] = value[:, 0:LANES]
    refs.pre[plane, 512:1024, :] = value[:, LANES : 2 * LANES]


def line_rows(z, c):
    return pl.ds(pl.multiple_of((z * 2 + c) * 64, 64), 64)


def put_feed_grads(refs, p, f):
    z, h = f // 2, f % 2
    up = dot(refs.fin_t[...], refs.dpre[:, C : 2 * C])
    put_halves(refs, 1 + h, dot(refs.cot_t[...], refs.dpre[:, 0:C]))

    @pl.when(h == p.c)
    def _():
        put_halves(refs, 0, up)

    @pl.when(h != p.c)
    def _():
        for g in range(4):
            refs.psend[UP][z, g] = up[g * 128 : (g + 1) * 128].astype(BF16)

    half = pl.ds(pl.multiple_of(h * 64, 64), 64)
    for zz in range(4):
        part = halves_of(refs, 1 + h, line_rows(zz, 1 - p.c))
        refs.psend[DOWN][z, zz, half, :] = part.astype(BF16)


def merge_up(refs, p, z):
    rs_pair(refs, p, UP, z).wait()
    for g in range(4):
        rs_merge(refs, p, UP, g, z, halves_of(refs, 0, pl.ds(g * 128, 128)))


def merge_down(refs, p, g):
    rs_pair(refs, p, DOWN, g).wait()
    for z in range(4):
        own = jnp.concatenate(
            [halves_of(refs, 1 + h, line_rows(z, p.c)) for h in range(2)], axis=0
        )
        rs_merge_at(refs, p, DOWN, g, z, own)


def rs_merge_at(refs, p, a, g, z, own):
    e = p.turn(z)
    y, x = g // 2, g % 2
    role = (1 - e) * ((x + p.x) % 2) + e * ((y + p.y) % 2)
    place = spot(a, g, z)
    v = (own + refs.precv[a][place].astype(F32)).astype(BF16)

    @pl.when(role == 1)
    def _():
        refs.psend[a][place] = v

    @pl.when(role == 0)
    def _():
        refs.precv[a][place] = v


def put_out_grads(refs, p):
    def one(g):
        put_halves(refs, g, dot(refs.fin_t[...], refs.slow[g]))
        for z in range(4):
            part = halves_of(refs, g, line_rows(z, 1 - p.c))
            refs.psend[OUT][z, g] = part.astype(BF16)

    loop(4, one)


def merge_out(refs, p):
    rs_pair(refs, p, OUT, 0).wait()

    def one(z):
        for g in range(4):
            rs_merge(refs, p, OUT, g, z, halves_of(refs, g, line_rows(z, p.c)))

    loop(4, one)


def mix_part(refs, g, c):
    cols = []
    for j in range(3):
        q = 3 * c + j
        rows = pl.ds(pl.multiple_of((q % 2) * 512 + g * 128, 128), 128)
        cols.append(refs.pre[q // 2, rows, :])
    return jnp.concatenate(cols, axis=1)


def put_mix_grads(refs, p, z):
    for j in range(3):
        put_halves(refs, j, dot(refs.min_t[...], refs.dpre[:, j * C : (j + 1) * C]))
    for g in range(4):
        refs.psend[MIX][z, g] = mix_part(refs, g, 1 - p.c).astype(BF16)


def merge_mix(refs, p, z):
    rs_pair(refs, p, MIX, z).wait()
    for g in range(4):
        rs_merge(refs, p, MIX, g, z, mix_part(refs, g, p.c))


def all_z(body):
    loop(4, body)


def second(refs, p, a, z):
    rs_second(refs, p, a, z)
    rs_second_copy(refs, p, a, z).start()


def third(refs, p, a, z):
    rs_third(refs, p, a, z)
    rs_third_send(refs, p, a, z)


def feed_order(k):
    return jnp.where(k == 1, 3, jnp.where(k >= 2, k - 1, 0))


def feed_tick(refs, p, f):
    @pl.when((f % 2 == 0) & (f >= 2))
    def _():
        last = feed_order(f // 2 - 1)
        merge_up(refs, p, last)
        merge_down(refs, p, last)
        rs_first_send(refs, p, UP, last)

    @pl.when((f % 2 == 0) & (f >= 4))
    def _():
        second(refs, p, UP, feed_order(f // 2 - 2))

    @pl.when((f % 2 == 0) & (f >= 6))
    def _():
        third(refs, p, UP, feed_order(f // 2 - 3))


def fused_kernel(*args):
    refs = FusedRefs(args)
    refs.fin_grad = refs.fin_g
    T, D = refs.tok_p.shape
    p = Place()
    load = pltpu.make_async_copy(refs.cot_in, refs.io, refs.io_s)
    load.start()
    gather_start(refs, p)
    load.wait()
    cot_in(refs, T)
    gather_hook(refs, p, "Mf0 Mn1")
    load = pltpu.make_async_copy(refs.tok_in, refs.io, refs.io_s)
    load.start()
    gather_vectors(refs, p)
    load.wait()
    norm_in(refs, T)
    gather_hook(refs, p, "Mp0 Mf1 Mn2 Md0")
    mixer_slots(refs, p, T)
    up_own(refs, p, 1)
    gather_hook(refs, p, "Wd0 Wd1 Wd2 Wd3 Un1 Un2 Dn10 Dn11 Dn12 Dn13")
    mix_out(refs, T)
    gather_hook(refs, p, "Ud0 Ud3 Dd00 Dd01 Dd02 Dd03")
    clear(refs.oacc, T)
    refs.dfe[...] = jnp.zeros_like(refs.dfe)

    def feed_step(f):
        @pl.when(f == 4)
        def _():
            gather_hook(refs, p, "Ud1 Ud2 Dd10 Dd11 Dd12 Dd13")

        feed(refs, feed_order(f // 2) * 2 + f % 2, T)

        @pl.when(f == 0)
        def _():
            gather_hook(refs, p, "Uf1 Uf2 Df10 Df11 Df12 Df13")

        @pl.when(f == 1)
        def _():
            gather_hook(refs, p, "Up1 Up2 Dp10 Dp11 Dp12 Dp13")

        feed_tick(refs, p, f)
        put_feed_grads(refs, p, feed_order(f // 2) * 2 + f % 2)

        @pl.when(f % 2 == 1)
        def _():
            rs_pair(refs, p, UP, feed_order(f // 2)).start()
            rs_pair(refs, p, DOWN, feed_order(f // 2)).start()

    loop(8, feed_step)
    feed_back(refs, T)
    store = pltpu.make_async_copy(refs.io, refs.block_out, refs.io_s)
    store.start()
    gather_drain(refs, p)
    merge_up(refs, p, 2)
    merge_down(refs, p, 2)
    rs_first_send(refs, p, UP, 2)
    all_z(lambda z: rs_first_send(refs, p, DOWN, z))
    second(refs, p, UP, 1)
    third(refs, p, UP, 3)
    put_out_grads(refs, p)
    rs_pair(refs, p, OUT, 0).start()
    clear(refs.oacc, T)
    store.wait()

    def chunk(n):
        return (p.z + 1 + n) % 4

    def early(n):
        @pl.when(n == 0)
        def _():
            merge_out(refs, p)
            all_z(lambda z: rs_first_send(refs, p, OUT, z))
            all_z(lambda z: second(refs, p, DOWN, z))
            second(refs, p, UP, 2)

        @pl.when(n >= 1)
        def _():
            merge_mix(refs, p, chunk(n - 1))
            rs_first_send(refs, p, MIX, chunk(n - 1))

        @pl.when(n >= 2)
        def _():
            second(refs, p, MIX, chunk(n - 2))

        @pl.when(n == 3)
        def _():
            third(refs, p, MIX, chunk(0))

    def late(n):
        @pl.when(n == 0)
        def _():
            third(refs, p, UP, 1)

        @pl.when(n == 1)
        def _():
            all_z(lambda z: second(refs, p, OUT, z))
            all_z(lambda z: third(refs, p, DOWN, z))
            third(refs, p, UP, 2)

        @pl.when(n == 2)
        def _():
            all_z(lambda z: third(refs, p, OUT, z))

    def mixer_step(n):
        z = chunk(n)
        mixer_back(refs, z, T, lambda: early(n))
        put_mix_grads(refs, p, z)
        rs_pair(refs, p, MIX, z).start()
        mixer_input_back(refs, z, T)
        late(n)

    loop(4, mixer_step)
    merge_mix(refs, p, chunk(3))
    rs_first_send(refs, p, MIX, chunk(3))
    second(refs, p, MIX, chunk(2))
    third(refs, p, MIX, chunk(1))
    norm_back(refs, T)
    store = pltpu.make_async_copy(refs.io, refs.tgrad_out, refs.io_s)
    store.start()
    vector_exchange(refs, p)
    for a in (UP, DOWN, OUT):
        rs_last(refs, p, a)
    third(refs, p, MIX, chunk(2))
    second(refs, p, MIX, chunk(3))
    third(refs, p, MIX, chunk(3))
    rs_last(refs, p, MIX)
    rs_drain(refs, p)
    adafactor(refs, p)
    store.wait()


def fused(*args):
    T, D = args[0].shape
    Z, F = 4, 8
    sds = jax.ShapeDtypeStruct
    vm = pl.BlockSpec(memory_space=pltpu.VMEM)
    anyspec = pl.BlockSpec(memory_space=pl.ANY)
    V = pltpu.VMEM
    S = pltpu.SemaphoreType.DMA
    outs = (
        sds((T, D), BF16), sds((T, D), BF16),
        sds((128, 384), F32), sds((64, 256), F32), sds((128, 256), F32), sds((64, 512), F32),
        sds((128, 384), F32), sds((64, 256), F32), sds((128, 256), F32), sds((64, 512), F32),
        sds((8, LANES), F32), sds((16, LANES), F32), sds((8, LANES), F32),
    )
    row = V((1, LANES), F32)
    box = V((32, 1, LANES), F32)
    scratch = [
        V((Z, D, 3 * C), BF16), V((Z, D, C), BF16), V((F, D, C), BF16), V((F, D, C), BF16),
        V((1, D), F32), V((1, D), F32), V((Z, 1, C), F32), V((Z, 1, C), F32),
        box, row, V((1, D), F32), V((1, D), F32), V((Z, 1, C), F32), V((Z, 1, C), F32),
        V((T, D), BF16), V((T, D), BF16), V((D, T), BF16), V((D, T), BF16),
        V((T, D), BF16), V((D, T), BF16),
        V((D // LANES, T, LANES), F32), V((T, D), F32),
        V((8, T, LANES), F32), V((4, T, LANES), F32),
        V((T, 3 * C), BF16), V((Z, T, C), BF16), V((Z, T + SUB, C), F32),
        V((Z, T, C), F32), V((Z, T, C), F32), V((Z, T, C), F32), V((Z, T, C), F32),
        S((7,)), S(()), S(()), S((4, 3)), S((4, 4)),
        S((4, 4)), S((4, 4)), S((4, 4, 2)), S((4, 4, 2)), S((4, 4, 4)), S((4, 4, 4)),
        box, box, V((16, LANES), F32), V((8, 16, LANES), F32),
        V((8, LANES), F32), V((4, 8, LANES), F32), row, box, row, box,
        S((4, 4)), S((4, 4)), S((4, 4, 2)), S((4, 4, 2)), S((4, 4)), S((4, 4)),
        S((4, 4)), S((4, 4)), S(()), S(()),
        S((7,)), S((7,)), S((3,)), S((3,)), S(()), S(()), S(()), S(()), S(()),
    ]
    scratch += (
        [V((4, 4) + s, BF16) for s in SHAPES] * 2
        + [V((4, 2) + s, BF16) for s in SHAPES]
        + [V((4,) + s, BF16) for s in SHAPES] * 2
        + [V(s, F32) for s in SHAPES]
    )
    return pl.pallas_call(
        fused_kernel,
        out_shape=outs,
        in_specs=[anyspec, anyspec] + [vm] * (len(args) - 2),
        out_specs=(anyspec, anyspec) + (vm,) * (len(outs) - 2),
        scratch_shapes=scratch,
        compiler_params=pltpu.CompilerParams(
            vmem_limit_bytes=67043328, collective_id=0, has_side_effects=True
        ),
        name="fused",
    )(*args)


def gathered_layer(tok, cot, mix, ow, uw, dw, mg, fb, ib, fg):
    def whole(w):
        w = lax.all_gather(w, "inner", axis=1, tiled=True)
        return lax.all_gather(w, "grp", axis=0, tiled=True)

    def vec(v):
        return lax.all_gather(v, ("grp", "inner"), axis=0, tiled=True).astype(F32)

    width = tok.shape[1]
    inners = lax.axis_size("inner")
    Z, F = mix[0].shape[1] * inners // C, uw.shape[1] * inners // C
    gates = [whole(w).reshape(width, Z, C // LANES, 1, LANES) for w in mix]
    wmix = jnp.concatenate(gates, axis=3).reshape(width, Z, 3 * C).transpose(1, 0, 2)
    wot = whole(ow).reshape(Z, C, width).transpose(0, 2, 1)
    wup = whole(uw).reshape(width, F, C).transpose(1, 0, 2)
    wdt = whole(dw).reshape(F, C, width).transpose(0, 2, 1)
    return layer(
        tok, cot, wmix, wot, wup, wdt,
        vec(mg).reshape(1, width), vec(fg).reshape(1, width),
        vec(fb).reshape(Z, 1, C), vec(ib).reshape(Z, 1, C),
    )


def body(
    tokens,
    cotangent,
    mixer_gain,
    forget_weight,
    input_gate_weight,
    candidate_weight,
    forget_bias,
    input_bias,
    output_weight,
    feed_norm_gain,
    up_weight,
    down_weight,
    mixer_second,
    forget_rows,
    forget_columns,
    input_rows,
    input_columns,
    candidate_rows,
    candidate_columns,
    forget_second,
    input_second,
    output_rows,
    output_columns,
    feed_second,
    up_rows,
    up_columns,
    down_rows,
    down_columns,
):
    groups = lax.axis_size("grp")
    inners = lax.axis_size("inner")
    seqs, length, width = tokens.shape
    hidden = forget_weight.shape[1] * inners
    ff = up_weight.shape[1] * inners
    paired = (groups, inners) == (4, 8) and (length, width, hidden, ff) == (1024, 512, 1024, 2048)
    Z, F = hidden // C, ff // C
    if paired:
        block_output, tokens_grad, *packed = fused(
            tokens.reshape(length, width), cotangent.reshape(length, width),
            forget_weight, input_gate_weight, candidate_weight,
            output_weight.T, up_weight, down_weight.T,
            mixer_gain, forget_bias, input_bias, feed_norm_gain,
            mixer_second, forget_rows, forget_columns, input_rows, input_columns,
            candidate_rows, candidate_columns, forget_second, input_second,
            output_rows, output_columns, feed_second,
            up_rows, up_columns, down_rows, down_columns,
        )
        *done, block_output, tokens_grad = finish(packed, block_output, tokens_grad)
        for k in (6, 9, 16, 19):
            done[k] = done[k].T
        return (block_output.reshape(tokens.shape), tokens_grad.reshape(tokens.shape), *done)
    results = gathered_layer(
        tokens.reshape(length, width), cotangent.reshape(length, width),
        (forget_weight, input_gate_weight, candidate_weight),
        output_weight, up_weight, down_weight,
        mixer_gain, forget_bias, input_bias, feed_norm_gain,
    )
    block_output, tokens_grad, gmix, got, gup, gdt, fgg, mgg, fbg, ibg = results
    block_output = block_output.reshape(tokens.shape)
    tokens_grad = tokens_grad.reshape(tokens.shape)
    split = gmix.transpose(1, 0, 2).reshape(width, Z, C // LANES, 3, LANES)
    forget_term, input_term, cand_term = [
        split[:, :, :, k].reshape(width, hidden) for k in range(3)
    ]
    output_term = got.transpose(0, 2, 1).reshape(hidden, width)
    up_term = gup.transpose(1, 0, 2).reshape(width, ff)
    down_term = gdt.transpose(0, 2, 1).reshape(ff, width)
    gain_first_term, gain_second_term = mgg.reshape(-1), fgg.reshape(-1)
    fbias_term, ibias_term = fbg.reshape(-1), ibg.reshape(-1)
    part = (
        lax.psum_scatter(
            gain_first_term.reshape(groups, -1), "inner", scatter_dimension=1, tiled=True
        ),
        lax.psum_scatter(forget_term, "inner", scatter_dimension=1, tiled=True),
        lax.psum_scatter(input_term, "inner", scatter_dimension=1, tiled=True),
        lax.psum_scatter(cand_term, "inner", scatter_dimension=1, tiled=True),
        lax.psum_scatter(fbias_term.reshape(groups, -1), "inner", scatter_dimension=1, tiled=True),
        lax.psum_scatter(ibias_term.reshape(groups, -1), "inner", scatter_dimension=1, tiled=True),
        lax.psum_scatter(output_term, "inner", scatter_dimension=1, tiled=True),
        lax.psum_scatter(
            gain_second_term.reshape(groups, -1), "inner", scatter_dimension=1, tiled=True
        ),
        lax.psum_scatter(up_term, "inner", scatter_dimension=1, tiled=True),
        lax.psum_scatter(down_term, "inner", scatter_dimension=1, tiled=True),
    )
    mine = (
        lax.psum_scatter(part[0], "grp", scatter_dimension=0, tiled=True),
        lax.psum_scatter(part[1], "grp", scatter_dimension=0, tiled=True),
        lax.psum_scatter(part[2], "grp", scatter_dimension=0, tiled=True),
        lax.psum_scatter(part[3], "grp", scatter_dimension=0, tiled=True),
        lax.psum_scatter(part[4], "grp", scatter_dimension=0, tiled=True),
        lax.psum_scatter(part[5], "grp", scatter_dimension=0, tiled=True),
        lax.psum_scatter(part[6], "grp", scatter_dimension=0, tiled=True),
        lax.psum_scatter(part[7], "grp", scatter_dimension=0, tiled=True),
        lax.psum_scatter(part[8], "grp", scatter_dimension=0, tiled=True),
        lax.psum_scatter(part[9], "grp", scatter_dimension=0, tiled=True),
    )
    params = [
        mixer_gain,
        forget_weight,
        input_gate_weight,
        candidate_weight,
        forget_bias,
        input_bias,
        output_weight,
        feed_norm_gain,
        up_weight,
        down_weight,
    ]
    locals_f = [p.astype(jnp.float32) for p in params]
    grads = [
        mine[0].reshape(-1),
        mine[1],
        mine[2],
        mine[3],
        mine[4].reshape(-1),
        mine[5].reshape(-1),
        mine[6],
        mine[7].reshape(-1),
        mine[8],
        mine[9],
    ]
    matrix_slots = [1, 2, 3, 6, 8, 9]
    vector_slots = [0, 4, 5, 7]
    rows_old = [forget_rows, input_rows, candidate_rows, output_rows, up_rows, down_rows]
    columns_old = [
        forget_columns,
        input_columns,
        candidate_columns,
        output_columns,
        up_columns,
        down_columns,
    ]
    seconds_old = [mixer_second, forget_second, input_second, feed_second]
    counts = [params[k].size * groups * inners for k in range(10)]
    first_inner = (lax.axis_index("inner") == 0).astype(jnp.float32)
    scales = lax.psum(
        jnp.stack(
            [jnp.sum(w * w) for w in locals_f] + [jnp.sum(r) * first_inner for r in rows_old]
        ),
        ("grp", "inner"),
    )
    mats = [grads[k] for k in matrix_slots]
    row_parts = [jnp.sum(g * g, axis=1) for g in mats]
    column_parts = [jnp.sum(g * g, axis=0) for g in mats]
    row_totals = lax.psum(
        (row_parts[0], row_parts[1], row_parts[2], row_parts[3], row_parts[4], row_parts[5]),
        "inner",
    )
    column_totals = lax.psum(
        (
            column_parts[0],
            column_parts[1],
            column_parts[2],
            column_parts[3],
            column_parts[4],
            column_parts[5],
        ),
        "grp",
    )
    grand = lax.psum(jnp.stack([jnp.sum(v) for v in row_totals]), "grp")
    scaled_all = [None] * 10
    new_states = [None] * 16
    state_places = {1: (1, 2), 2: (3, 4), 3: (5, 6), 6: (9, 10), 8: (12, 13), 9: (14, 15)}
    second_places = {0: 0, 4: 7, 5: 8, 7: 11}
    for k in range(6):
        slot = matrix_slots[k]
        grad = mats[k]
        full_rows = grad.shape[0] * groups
        full_columns = grad.shape[1] * inners
        rows = 0.5 * rows_old[k] + 0.5 * (row_totals[k] / full_columns + TINY)
        columns = 0.5 * columns_old[k] + 0.5 * (column_totals[k] / full_rows + TINY)
        row_mean = 0.5 * scales[10 + k] / full_rows + 0.5 * (
            grand[k] / (full_rows * full_columns) + TINY
        )
        scaled_all[slot] = grad * lax.rsqrt(rows[:, None] * columns[None, :] / row_mean)
        new_states[state_places[slot][0]] = rows
        new_states[state_places[slot][1]] = columns
    for k in range(4):
        slot = vector_slots[k]
        grad = grads[slot]
        second = 0.5 * seconds_old[k] + 0.5 * (grad * grad + TINY)
        scaled_all[slot] = grad * lax.rsqrt(second)
        new_states[second_places[slot]] = second
    clip = lax.psum(jnp.stack([jnp.sum(s * s) for s in scaled_all]), ("grp", "inner"))
    count_array = jnp.array(counts, jnp.float32)
    update_norms = jnp.sqrt(clip / count_array)
    fresh = [
        locals_f[k]
        + -jnp.sqrt(scales[k] / counts[k]) * scaled_all[k] / jnp.maximum(CLIP, update_norms[k])
        for k in range(10)
    ]
    return (
        block_output,
        tokens_grad,
        grads[0],
        grads[1],
        grads[2],
        grads[3],
        grads[4],
        grads[5],
        grads[6],
        grads[7],
        grads[8],
        grads[9],
        fresh[0],
        fresh[1],
        fresh[2],
        fresh[3],
        fresh[4],
        fresh[5],
        fresh[6],
        fresh[7],
        fresh[8],
        fresh[9],
        new_states[0],
        new_states[1],
        new_states[2],
        new_states[3],
        new_states[4],
        new_states[5],
        new_states[6],
        new_states[7],
        new_states[8],
        new_states[9],
        new_states[10],
        new_states[11],
        new_states[12],
        new_states[13],
        new_states[14],
        new_states[15],
        update_norms,
    )


def solution(mesh):
    return jax.shard_map(
        body,
        mesh=mesh,
        in_specs=(
            P(("grp", "inner"), None, None),
            P(("grp", "inner"), None, None),
            P(("grp", "inner")),
            P("grp", "inner"),
            P("grp", "inner"),
            P("grp", "inner"),
            P(("grp", "inner")),
            P(("grp", "inner")),
            P("grp", "inner"),
            P(("grp", "inner")),
            P("grp", "inner"),
            P("grp", "inner"),
            P(("grp", "inner")),
            P("grp"),
            P("inner"),
            P("grp"),
            P("inner"),
            P("grp"),
            P("inner"),
            P(("grp", "inner")),
            P(("grp", "inner")),
            P("grp"),
            P("inner"),
            P(("grp", "inner")),
            P("grp"),
            P("inner"),
            P("grp"),
            P("inner"),
        ),
        out_specs=(
            P(("grp", "inner"), None, None),
            P(("grp", "inner"), None, None),
            P(("grp", "inner")),
            P("grp", "inner"),
            P("grp", "inner"),
            P("grp", "inner"),
            P(("grp", "inner")),
            P(("grp", "inner")),
            P("grp", "inner"),
            P(("grp", "inner")),
            P("grp", "inner"),
            P("grp", "inner"),
            P(("grp", "inner")),
            P("grp", "inner"),
            P("grp", "inner"),
            P("grp", "inner"),
            P(("grp", "inner")),
            P(("grp", "inner")),
            P("grp", "inner"),
            P(("grp", "inner")),
            P("grp", "inner"),
            P("grp", "inner"),
            P(("grp", "inner")),
            P("grp"),
            P("inner"),
            P("grp"),
            P("inner"),
            P("grp"),
            P("inner"),
            P(("grp", "inner")),
            P(("grp", "inner")),
            P("grp"),
            P("inner"),
            P(("grp", "inner")),
            P("grp"),
            P("inner"),
            P("grp"),
            P("inner"),
            P(),
        ),
        check_vma=False,
    )
```

```python
import functools
import math
import jax
import jax.numpy as jnp
from jax import lax
from jax.experimental import pallas as pl
from jax.sharding import PartitionSpec as P
from jax.experimental.pallas import tpu as pltpu

EPS = 1e-06
F32 = jnp.float32
BF16 = jnp.bfloat16
C = 256
LANES = 128
SUB = 8
ERFC = (
    0.2256758669, 0.2256693636, 0.2078460312, 0.1685204197, 0.1415057621,
    -0.005753053848, 0.1692475449, -0.182997133, 0.05028532412,
)


def dot(a, b):
    return jnp.dot(a, b, preferred_element_type=F32)


def dot_t(a, b):
    return lax.dot_general(a, b, (((1,), (1,)), ((), ())), preferred_element_type=F32)


def loop(steps, body):
    def run(i, carry):
        body(i)
        return carry

    lax.fori_loop(0, steps, run, 0)


def at(i, size):
    return pl.ds(pl.multiple_of(i * size, size), size)


def gelu_parts(x):
    e = jnp.exp2((x * x) * (-0.5 / math.log(2.0)))
    t = 1.0 / (1.0 + (0.4 * math.sqrt(0.5)) * jnp.abs(x))
    poly = jnp.full_like(t, 0.5 * ERFC[-1])
    for c in ERFC[-2::-1]:
        poly = poly * t + 0.5 * c
    half = poly * (t * e)
    cdf = jnp.where(x >= 0, 1.0 - half, half)
    return x * cdf, cdf + (x * e) * (1.0 / math.sqrt(2.0 * math.pi))


def reorder(inverse):
    row = lax.broadcasted_iota(jnp.int32, (LANES, LANES), 0)
    col = lax.broadcasted_iota(jnp.int32, (LANES, LANES), 1)
    step = LANES // SUB
    source = (row % step) * SUB + row // step if inverse else (row % SUB) * step + row // SUB
    return jnp.where(col == source, 1.0, 0.0).astype(BF16)


def tile_rows(i, s, T):
    step = LANES // SUB
    return pl.ds(pl.multiple_of(i * step + s * (T // SUB), step), step)


def gather_rows(ref, i, order, T):
    return dot(order, jnp.concatenate([ref[tile_rows(i, s, T), :] for s in range(SUB)], axis=0))


def scatter_rows(ref, i, order, out, T):
    step = LANES // SUB
    flat = dot(order, out.astype(BF16)).astype(BF16)
    for s in range(SUB):
        ref[tile_rows(i, s, T), :] = flat[s * step : (s + 1) * step]


LOG2E = 1.0 / math.log(2.0)


def load_planes(ref, rows, start=0, count=None):
    count = ref.shape[0] if count is None else count
    return jnp.concatenate([ref[q, rows, :] for q in range(start, start + count)], axis=1)


def store_planes(ref, rows, value, start=0):
    for q in range(value.shape[1] // LANES):
        ref[start + q, rows, :] = value[:, q * LANES : (q + 1) * LANES]


def add_planes(ref, rows, value):
    for q in range(value.shape[1] // LANES):
        ref[q, rows, :] += value[:, q * LANES : (q + 1) * LANES]


def clear(ref, T):
    for q in range(4):
        ref[q, 0:T, :] = jnp.zeros((T, LANES), F32)


def norm_in(refs, T):
    order = reorder(False)

    def place(i):
        x = gather_rows(refs.tok, i, order, T)
        y = x * lax.rsqrt(jnp.mean(x * x, axis=-1, keepdims=True) + EPS) * refs.g1[...]
        rows = at(i, LANES)
        refs.tok_p[rows, :] = x.astype(BF16)
        refs.min[rows, :] = y.astype(BF16)
        refs.min_t[:, rows] = y.T.astype(BF16)

    loop(T // LANES, place)


def cot_in(refs, T):
    order = reorder(False)

    def place(i):
        x = gather_rows(refs.cot, i, order, T)
        rows = at(i, LANES)
        refs.cot_p[rows, :] = x.astype(BF16)
        refs.cot_t[:, rows] = x.T.astype(BF16)

    loop(T // LANES, place)


def mixer_forward(refs, z, T, hook=None):
    pre, ac, st = refs.pre, refs.buf, refs.st
    halves = C // LANES
    width = 3 * LANES

    def project(i):
        rows = at(i, 256)
        out = dot(refs.min[rows, :], refs.wmix[z])
        for q in range(3 * halves):
            pre[q, rows, :] = out[:, q * LANES : (q + 1) * LANES]

    loop(T // 256, project)
    fb = refs.fb[z]
    ib = refs.ib[z]

    def gates(i, carry):
        r0 = pl.multiple_of(i * 64, 64)
        out = []
        for h in range(halves):
            a, b = carry[h]
            lanes = slice(h * LANES, (h + 1) * LANES)
            pf = pre[3 * h, pl.ds(r0, 64), :] + fb[:, lanes]
            pi = pre[3 * h + 1, pl.ds(r0, 64), :] + ib[:, lanes]
            pc = pre[3 * h + 2, pl.ds(r0, 64), :]
            pf, pi = pf * LOG2E, pi * LOG2E
            m = jnp.minimum(jnp.minimum(pf, pi), 0.0)
            e0 = jnp.exp2(m)
            ef = jnp.exp2(m - pf)
            ei = jnp.exp2(m - pi)
            nk = e0 + ei
            na = e0 + ef
            both = nk + na
            floor = jnp.maximum(na, 1e-37)
            rec = 1.0 / (both * floor)
            inv = rec * floor
            keep = nk * inv
            admit = na * inv
            ec = jnp.exp(jnp.minimum(pc, 0.0))
            sg = ec / (1.0 + ec)
            positive = pc >= 0
            value = jnp.where(positive, pc + 0.5, sg)
            slope = jnp.where(positive, 1.0, sg * (1.0 - sg))
            refs.keep[z, pl.ds(r0, 64), lanes] = keep
            refs.k_f[z, pl.ds(r0, 64), lanes] = keep * (ef * (rec * both))
            refs.k_i[z, pl.ds(r0, 64), lanes] = ei * inv
            refs.k_c[z, pl.ds(r0, 64), lanes] = admit * slope
            inflow = admit * value
            alist, blist = [], []
            for j in range(8):
                kj = keep[j * SUB : (j + 1) * SUB]
                b = kj * b + inflow[j * SUB : (j + 1) * SUB]
                a = kj * a
                alist.append(a)
                blist.append(b)
            ac[h, pl.ds(r0, 64), :] = jnp.concatenate(alist, axis=0)
            st[z, pl.ds(r0 + SUB, 64), lanes] = jnp.concatenate(blist, axis=0)
            out.append((a, b))
        return tuple(out)

    one = jnp.ones((SUB, LANES), F32)
    zero = jnp.zeros((SUB, LANES), F32)
    if hook is not None:
        hook(1)
    ends = lax.fori_loop(0, T // 64, gates, tuple((one, zero) for _ in range(halves)))
    if hook is not None:
        hook(2)
    for h in range(halves):
        a, b = ends[h]
        rows = [jnp.zeros((1, LANES), F32)]
        for s in range(SUB - 1):
            rows.append(a[s : s + 1] * rows[-1] + b[s : s + 1])
        st[z, 0:SUB, h * LANES : (h + 1) * LANES] = jnp.concatenate(rows, axis=0)
    first = st[z, 0:SUB, :]

    def finish(i):
        r0 = pl.multiple_of(i * 64, 64)
        a = load_planes(ac, pl.ds(r0, 64), 0, 2).reshape(8, SUB, C)
        b = st[z, pl.ds(r0 + SUB, 64), :].reshape(8, SUB, C)
        s = (b + a * first[None]).reshape(64, C)
        st[z, pl.ds(r0 + SUB, 64), :] = s
        refs.slow[z, pl.ds(r0, 64), :] = s.astype(BF16)

    loop(T // 64, finish)


def mix_out(refs, T):
    Z = refs.wot.shape[0]

    def body(i):
        rows = at(i, 256)
        acc = refs.tok_p[rows, :].astype(F32)
        for z in range(Z):
            acc = acc + dot_t(refs.slow[z, rows, :], refs.wot[z])
        store_planes(refs.resid, rows, acc)
        for k in range(2):
            x = acc[k * LANES : (k + 1) * LANES]
            y = x * lax.rsqrt(jnp.mean(x * x, axis=-1, keepdims=True) + EPS) * refs.g2[...]
            sub = pl.ds(pl.multiple_of(i * 256 + k * LANES, LANES), LANES)
            refs.fin[sub, :] = y.astype(BF16)
            refs.fin_t[:, sub] = y.T.astype(BF16)

    loop(T // 256, body)


def feed(refs, f, T):
    wup, wdt = refs.wup, refs.wdt
    size = 256
    tiles = T // size

    def project(i):
        rows = slice(i * size, (i + 1) * size)
        store_planes(refs.buf, rows, dot(refs.fin[rows, :], wup[f]))
        store_planes(refs.buf, rows, dot(refs.cot_p[rows, :], wdt[f]), 2)

    def activate(i):
        for k in range(size // 32):
            rows = slice(i * size + k * 32, i * size + (k + 1) * 32)
            for q in range(C // LANES):
                act, slope = gelu_parts(refs.buf[q, rows, :])
                lanes = slice(q * LANES, (q + 1) * LANES)
                refs.dpre[rows, lanes] = act.astype(BF16)
                lanes = slice(C + q * LANES, C + (q + 1) * LANES)
                refs.dpre[rows, lanes] = (refs.buf[2 + q, rows, :] * slope).astype(BF16)

    def add(i):
        rows = slice(i * size, (i + 1) * size)
        add_planes(refs.oacc, rows, dot_t(refs.dpre[rows, 0:C], wdt[f]))
        refs.dfe[rows, :] += dot_t(refs.dpre[rows, C : 2 * C], wup[f])

    for i in range(tiles + 2):
        if i < tiles:
            project(i)
        if 1 <= i < tiles + 1:
            activate(i - 1)
        if i >= 2:
            add(i - 2)


def feed_back(refs, T):
    order = reorder(True)
    D = refs.g1.shape[1]

    def body(i, total):
        rows = at(i, LANES)
        x = load_planes(refs.resid, rows)
        df = refs.dfe[rows, :]
        out = x + load_planes(refs.oacc, rows, 0, D // LANES)
        scatter_rows(refs.block, i, order, out, T)
        r = lax.rsqrt(jnp.mean(x * x, axis=-1, keepdims=True) + EPS)
        nrm = x * r
        dn = df * refs.g2[...]
        mean = jnp.mean(dn * nrm, axis=-1, keepdims=True)
        dres = refs.cot_p[rows, :].astype(F32) + r * (dn - nrm * mean)
        refs.dfe[rows, :] = dres
        refs.fin[rows, :] = dres.astype(BF16)
        refs.fin_t[:, rows] = dres.T.astype(BF16)
        return total + (df * nrm).reshape(16, SUB, D).sum(axis=0)

    total = lax.fori_loop(0, T // LANES, body, jnp.zeros((SUB, D), F32))
    refs.fgg[...] = jnp.sum(total, axis=0, keepdims=True)


def mixer_back(refs, z, T, hook=None):
    buf, st = refs.buf, refs.st
    halves = C // LANES
    width = 3 * LANES

    def project(i):
        rows = at(i, 256)
        store_planes(buf, rows, dot(refs.fin[rows, :], refs.wot[z]))

    loop(T // 256, project)
    steps = T // 64

    def local(i, carry):
        r0 = pl.multiple_of((steps - 1 - i) * 64, 64)
        d = load_planes(buf, pl.ds(r0, 64), 0, 2)
        k = refs.keep[z, pl.ds(r0, 64), :]
        e, dk = carry
        plist, dlist = [None] * 8, [None] * 8
        for j in range(7, -1, -1):
            kj = k[j * SUB : (j + 1) * SUB]
            p = d[j * SUB : (j + 1) * SUB] + e
            plist[j] = p
            dlist[j] = dk
            e = kj * p
            dk = kj * dk
        store_planes(buf, pl.ds(r0, 64), jnp.concatenate(plist, axis=0))
        store_planes(buf, pl.ds(r0, 64), jnp.concatenate(dlist, axis=0), 2)
        return e, dk

    e, dk = lax.fori_loop(0, steps, local, (jnp.zeros((SUB, C), F32), jnp.ones((SUB, C), F32)))
    rows = [jnp.zeros((1, C), F32)]
    for s in range(SUB - 1, 0, -1):
        rows.insert(0, e[s : s + 1] + dk[s : s + 1] * rows[0])
    tail = jnp.concatenate(rows, axis=0)
    if hook is not None:
        hook()

    def grads(i, sums):
        r0 = pl.multiple_of(i * 64, 64)
        out = []
        for h in range(halves):
            lanes = slice(h * LANES, (h + 1) * LANES)
            sub = pl.ds(r0, 64)
            p0 = buf[h, sub, :].reshape(8, SUB, LANES)
            d0 = buf[2 + h, sub, :].reshape(8, SUB, LANES)
            p = (p0 + d0 * tail[None, :, lanes]).reshape(64, LANES)
            x = p * (st[z, pl.ds(r0 + SUB, 64), lanes] - st[z, sub, lanes])
            df = -(refs.k_f[z, sub, lanes] * x)
            di = refs.k_i[z, sub, lanes] * x
            dcand = refs.k_c[z, sub, lanes] * p
            df16 = df.astype(BF16)
            di16 = di.astype(BF16)
            refs.dpre[sub, h * width : h * width + LANES] = df16
            refs.dpre[sub, h * width + LANES : h * width + 2 * LANES] = di16
            refs.dpre[sub, h * width + 2 * LANES : h * width + 3 * LANES] = dcand.astype(BF16)
            sf, si = sums[h]
            out.append(
                (
                    sf + df16.astype(F32).reshape(8, SUB, LANES).sum(axis=0),
                    si + di16.astype(F32).reshape(8, SUB, LANES).sum(axis=0),
                )
            )
        return tuple(out)

    zero = jnp.zeros((SUB, LANES), F32)
    sums = lax.fori_loop(0, T // 64, grads, tuple((zero, zero) for _ in range(halves)))
    for h in range(halves):
        lanes = slice(h * LANES, (h + 1) * LANES)
        refs.fbg[z, :, lanes] = jnp.sum(sums[h][0], axis=0, keepdims=True)
        refs.ibg[z, :, lanes] = jnp.sum(sums[h][1], axis=0, keepdims=True)


def mixer_input_back(refs, z, T):
    def back(i):
        rows = at(i, 256)
        add_planes(refs.oacc, rows, dot_t(refs.dpre[rows, :], refs.wmix[z]))

    loop(T // 256, back)


def norm_back(refs, T):
    order = reorder(True)
    D = refs.g1.shape[1]

    def body(i, total):
        rows = at(i, LANES)
        x = refs.tok_p[rows, :].astype(F32)
        d_in = load_planes(refs.oacc, rows, 0, D // LANES)
        r = lax.rsqrt(jnp.mean(x * x, axis=-1, keepdims=True) + EPS)
        nrm = x * r
        dn = d_in * refs.g1[...]
        mean = jnp.mean(dn * nrm, axis=-1, keepdims=True)
        out = refs.dfe[rows, :] + r * (dn - nrm * mean)
        scatter_rows(refs.tgrad, i, order, out, T)
        return total + (d_in * nrm).reshape(16, SUB, D).sum(axis=0)

    total = lax.fori_loop(0, T // LANES, body, jnp.zeros((SUB, D), F32))
    refs.mgg[...] = jnp.sum(total, axis=0, keepdims=True)


class Refs:
    def __init__(self, args):
        (
            self.tok, self.cot, self.wmix, self.wot, self.wup, self.wdt, self.g1, self.g2, self.fb, self.ib,
            self.block, self.tgrad, self.gmix, self.got, self.gup, self.gdt, self.fgg, self.mgg, self.fbg, self.ibg,
            self.tok_p, self.min, self.min_t, self.fin, self.fin_t, self.cot_p, self.cot_t, self.resid, self.oacc, self.dfe,
            self.pre, self.buf, self.dpre, self.slow, self.st, self.keep, self.k_f,
            self.k_i, self.k_c, self.gst, self.gsem,
        ) = args


def layer_kernel(*args):
    refs = Refs(args)
    T, D = refs.tok.shape
    Z = refs.wmix.shape[0]
    F = refs.wup.shape[0]
    gst, sem = refs.gst, refs.gsem
    cot_in(refs, T)
    norm_in(refs, T)
    loop(Z, lambda z: mixer_forward(refs, z, T))
    mix_out(refs, T)
    clear(refs.oacc, T)
    refs.dfe[...] = jnp.zeros_like(refs.dfe)

    def feed_step(f):
        feed(refs, f, T)
        gst[0, :, 0:C] = dot(refs.cot_t[...], refs.dpre[:, 0:C])
        gst[1, :, 0:C] = dot(refs.fin_t[...], refs.dpre[:, C : 2 * C])
        one = pltpu.make_async_copy(gst.at[0, :, 0:C], refs.gdt.at[f], sem.at[0])
        two = pltpu.make_async_copy(gst.at[1, :, 0:C], refs.gup.at[f], sem.at[1])
        one.start()
        two.start()
        one.wait()
        two.wait()

    loop(F, feed_step)
    feed_back(refs, T)
    clear(refs.oacc, T)

    def mixer_step(z):
        gst[0, :, 0:C] = dot(refs.fin_t[...], refs.slow[z])
        mixer_back(refs, z, T)
        mixer_input_back(refs, z, T)
        gst[1, :, :] = dot(refs.min_t[...], refs.dpre[...])
        one = pltpu.make_async_copy(gst.at[0, :, 0:C], refs.got.at[z], sem.at[0])
        two = pltpu.make_async_copy(gst.at[1], refs.gmix.at[z], sem.at[1])
        one.start()
        two.start()
        one.wait()
        two.wait()

    loop(Z, mixer_step)
    norm_back(refs, T)


def layer(tok, cot, wmix, wot, wup, wdt, g1, g2, fb, ib):
    T, D = tok.shape
    Z, F = wmix.shape[0], wup.shape[0]
    sds = jax.ShapeDtypeStruct
    vm = pl.BlockSpec(memory_space=pltpu.VMEM)
    anyspec = pl.BlockSpec(memory_space=pl.ANY)
    out_shape = (
        sds((T, D), BF16), sds((T, D), BF16),
        sds((Z, D, 3 * C), F32), sds((Z, D, C), F32), sds((F, D, C), F32), sds((F, D, C), F32),
        sds((1, D), F32), sds((1, D), F32), sds((Z, 1, C), F32), sds((Z, 1, C), F32),
    )
    V = pltpu.VMEM
    scratch = [
        V((T, D), BF16), V((T, D), BF16), V((D, T), BF16), V((T, D), BF16), V((D, T), BF16),
        V((T, D), BF16), V((D, T), BF16), V((D // LANES, T, LANES), F32),
        V((D // LANES, T, LANES), F32), V((T, D), F32), V((3 * C // LANES, T, LANES), F32), V((4, T, LANES), F32),
        V((T, 3 * C), BF16), V((Z, T, C), BF16), V((Z, T + SUB, C), F32),
        V((Z, T, C), F32), V((Z, T, C), F32), V((Z, T, C), F32), V((Z, T, C), F32),
        V((2, D, 3 * C), F32), pltpu.SemaphoreType.DMA((2,)),
    ]
    return pl.pallas_call(
        layer_kernel,
        out_shape=out_shape,
        in_specs=[vm] * 10,
        out_specs=(vm, vm, anyspec, anyspec, anyspec, anyspec, vm, vm, vm, vm),
        scratch_shapes=scratch,
        compiler_params=pltpu.CompilerParams(vmem_limit_bytes=67043328),
        name="layer",
    )(tok, cot, wmix, wot, wup, wdt, g1, g2, fb, ib)


MESH = pl.DeviceIdType.MESH


def rcopy(src, dst, send, recv, device):
    return pltpu.make_async_remote_copy(
        src_ref=src, dst_ref=dst, send_sem=send, recv_sem=recv, device_id=device, device_id_type=MESH
    )


class Place:
    def __init__(self):
        self.g = lax.axis_index("grp")
        self.i = lax.axis_index("inner")
        self.y, self.x = self.g // 2, self.g % 2
        self.z, self.c = self.i // 2, self.i % 2
        self.me = self.g * 8 + self.i
        self.partner = (self.g, self.z * 2 + 1 - self.c)

    def flip(self, fx, fy):
        x = (self.x + fx) % 2
        y = (self.y + fy) % 2
        return y * 2 + x

    def turn(self, z):
        return (z + self.c) % 2

    def near(self, z):
        e = self.turn(z)
        return self.flip(1 - e, e)

    def far(self, z):
        e = self.turn(z)
        return self.flip(e, 1 - e)

    def other(self, k):
        t = (self.me + k) % 32
        return (t // 8, t % 8)


def entry_barrier(place):
    barrier = pltpu.get_barrier_semaphore()

    def greet(k):
        pl.semaphore_signal(barrier, inc=1, device_id=place.other(k + 1), device_id_type=MESH)

    loop(31, greet)
    pl.semaphore_wait(barrier, 31)


def spread(values, start, count, total):
    lane = lax.broadcasted_iota(jnp.int32, (LANES, total), 1)
    row = lax.broadcasted_iota(jnp.int32, (LANES, total), 0)
    sel = jnp.where(row == start + lane % count, 1.0, 0.0).astype(BF16)
    picked = dot(values, sel)
    owner = lax.broadcasted_iota(jnp.int32, picked.shape, 0)
    spot = lax.broadcasted_iota(jnp.int32, picked.shape, 1)
    return jnp.sum(jnp.where(spot // count == owner, picked, 0.0), axis=0, keepdims=True)


def pack_vectors(mg, fb, ib, fg):
    parts = [mg, fb, ib, fg]
    used = sum(p.shape[0] for p in parts)
    rows = [p[...].astype(F32).reshape(1, p.shape[0]) for p in parts]
    return jnp.concatenate(rows + [jnp.zeros((1, LANES - used), F32)], axis=1)


FIRST = (3, 0)
LATER = (1, 2)


def block_of(refs, a, g, i):
    if a == 0:
        return refs.wot.at[g, at(i, 64), :]
    if a == 1:
        return refs.wup.at[i, at(g, 128), :]
    if a == 2:
        return refs.wdt.at[pl.ds(2 * g, 2), at(i, 64), :]
    return refs.wmix.at[i // 2, at(g, 128), at(i % 2, 384)]


def blocks_of(refs, a, i):
    if a == 0:
        return refs.wot.at[:, at(i, 64), :]
    if a == 1:
        return refs.wup.at[i]
    if a == 2:
        return refs.wdt.at[:, at(i, 64), :]
    return refs.wmix.at[i // 2, :, at(i % 2, 384)]


def line_send(refs, p, a):
    blk = block_of(refs, a, p.g, p.i)
    for s in range(1, 4):
        peer = (p.g, slot_chunk(p, s) * 2 + p.c)
        rcopy(blk, blk, refs.gz_s.at[a, s - 1], refs.gz_r.at[a, p.z], peer).start()


def near_of(p, a, z):
    return p.near(z + (a in LATER))


def far_of(p, a, z):
    return p.far(z + (a in LATER))


def line_wait(refs, p, a, z):
    @pl.when(z != p.z)
    def _():
        blk = block_of(refs, a, p.g, z * 2 + p.c)
        rcopy(blk, blk, refs.gp_s.at[a, z, 0], refs.gz_r.at[a, z], p.partner).wait_recv()


def near_send(refs, p, a, z):
    blk = block_of(refs, a, p.g, z * 2 + p.c)
    near, far = (near_of(p, a, z), p.i), (far_of(p, a, z), p.i)
    rcopy(blk, blk, refs.gn_s.at[a, z], refs.gn_r.at[a, z], near).start()
    rcopy(blk, blk, refs.gf_s.at[a, z, 0], refs.gf_r.at[a, z, 0], far).start()


def far_send(refs, p, a, z):
    near = block_of(refs, a, near_of(p, a, z), z * 2 + p.c)
    far = (far_of(p, a, z), p.i)
    rcopy(near, near, refs.gn_s.at[a, z], refs.gn_r.at[a, z], p.partner).wait_recv()
    rcopy(near, near, refs.gf_s.at[a, z, 1], refs.gf_r.at[a, z, 1], far).start()


def far_wait(refs, p, a, z, k):
    blk = block_of(refs, a, p.g, z * 2 + p.c)
    rcopy(blk, blk, refs.gf_s.at[a, z, k], refs.gf_r.at[a, z, k], p.partner).wait_recv()


def pair_copy(refs, p, a, z, c):
    full = blocks_of(refs, a, z * 2 + c)
    return rcopy(full, full, refs.gp_s.at[a, z, 0], refs.gp_r.at[a, z, 0], p.partner)


def first_step(refs, p, arrays, kind, s):
    for a in arrays:
        z = slot_chunk(p, s)
        if kind == "n":
            line_wait(refs, p, a, z)
            near_send(refs, p, a, z)
        elif kind == "f":
            far_send(refs, p, a, z)
        elif kind == "p":
            far_wait(refs, p, a, z, 0)
            far_wait(refs, p, a, z, 1)
            pair_copy(refs, p, a, z, p.c).start()
        else:
            pair_copy(refs, p, a, z, 1 - p.c).wait_recv()


def up_step(refs, p, kind, m):
    if kind == "n":

        @pl.when(p.z != m)
        def _():
            line_wait(refs, p, 1, m)
            near_send(refs, p, 1, m)
    elif kind == "f":
        far_send(refs, p, 1, m)
    elif kind == "p":
        far_wait(refs, p, 1, m, 0)
        far_wait(refs, p, 1, m, 1)
        pair_copy(refs, p, 1, m, p.c).start()
    else:
        pair_copy(refs, p, 1, m, 1 - p.c).wait_recv()


def up_own(refs, p, phase):
    inner = (p.z + 1) // 2 % 2

    @pl.when(inner == phase)
    def _():
        near_send(refs, p, 1, p.z)


def down_pair(refs, p, z, phase, k, c):
    g = (1 + k) if phase else 3 * k
    blk = block_of(refs, 2, g, z * 2 + c)
    return rcopy(blk, blk, refs.gp_s.at[2, z, phase * 2 + k], refs.gp_r.at[2, z, phase * 2 + k], p.partner)


def down_step(refs, p, kind, phase, s):
    z = slot_chunk(p, s)
    active = (p.x + p.y) % 2 == phase
    idle = (p.x + p.y) % 2 != phase
    if kind == "n":

        @pl.when(active)
        def _():
            line_wait(refs, p, 2, z)
            near_send(refs, p, 2, z)
    elif kind == "f":

        @pl.when(idle)
        def _():
            far_send(refs, p, 2, z)
    elif kind == "p":

        @pl.when(active)
        def _():
            far_wait(refs, p, 2, z, 1)

        @pl.when(idle)
        def _():
            far_wait(refs, p, 2, z, 0)

        for k in range(2):
            down_pair(refs, p, z, phase, k, p.c).start()
    else:
        for k in range(2):
            down_pair(refs, p, z, phase, k, 1 - p.c).wait_recv()


def gather_drain(refs, p):
    for a in range(4):
        blk = block_of(refs, a, p.g, p.i)
        for k in range(3):
            rcopy(blk, blk, refs.gz_s.at[a, k], refs.gz_r.at[a, p.z], p.partner).wait_send()
        for z in range(4):
            blk = block_of(refs, a, p.g, z * 2 + p.c)
            rcopy(blk, blk, refs.gn_s.at[a, z], refs.gn_r.at[a, z], p.partner).wait_send()
            for k in range(2):
                rcopy(blk, blk, refs.gf_s.at[a, z, k], refs.gf_r.at[a, z, k], p.partner).wait_send()
            if a == 2:
                for k in range(4):
                    down_pair(refs, p, z, k // 2, k % 2, p.c).wait_send()
            else:
                pair_copy(refs, p, a, z, p.c).wait_send()


def gather_hook(refs, p, actions):
    for action in actions.split():
        kind, number = action[1], int(action[-1])
        if action[0] == "M":
            first_step(refs, p, (3,), kind, number)
        elif action[0] == "W":
            first_step(refs, p, (0,), kind, number)
        elif action[0] == "U":
            up_step(refs, p, kind, number)
        else:
            down_step(refs, p, kind, int(action[2]), number)


def gather_start(refs, p):
    local = []
    for k, w in enumerate((refs.fw, refs.iw, refs.cw)):
        spot = pl.ds(pl.multiple_of(p.c * 384 + k * 128, 128), 128)
        local.append(
            pltpu.make_async_copy(w, refs.wmix.at[p.z, at(p.g, 128), spot], refs.loc_s.at[k])
        )
    local.append(pltpu.make_async_copy(refs.ow, block_of(refs, 0, p.g, p.i), refs.loc_s.at[3]))
    local.append(pltpu.make_async_copy(refs.uw, block_of(refs, 1, p.g, p.i), refs.loc_s.at[4]))
    for k in range(2):
        local.append(
            pltpu.make_async_copy(
                refs.dw.at[:, k * 256 : (k + 1) * 256],
                refs.wdt.at[2 * p.g + k, at(p.i, 64), :],
                refs.loc_s.at[5 + k],
            )
        )
    for c in local:
        c.start()
    row = pack_vectors(refs.mg, refs.fbv, refs.ibv, refs.fg)
    refs.vstage[...] = row
    refs.vecs[p.me] = row
    for c in local:
        c.wait()
    entry_barrier(p)

    def vector(k):
        rcopy(refs.vstage, refs.vecs.at[p.me], refs.vec_s, refs.vec_r, p.other(k + 1)).start()

    for a in FIRST:
        near_send(refs, p, a, p.z)
    up_own(refs, p, 0)
    down_step(refs, p, "n", 0, 0)
    loop(31, vector)
    for a in FIRST:
        line_send(refs, p, a)
    inner = (p.z + 1) // 2 % 2

    @pl.when(inner == 0)
    def _():
        line_send(refs, p, 1)

    line_send(refs, p, 2)

    @pl.when(inner == 1)
    def _():
        line_send(refs, p, 1)


def gather_vectors(refs, p):
    rows = refs.vecs.at[pl.ds(0, 31)]
    rcopy(rows, rows, refs.vec_s, refs.vec_r, p.partner).wait()
    v = refs.vecs[...].reshape(32, LANES).astype(BF16)
    refs.g1[...] = spread(v, 0, 16, 512)
    refs.g2[...] = spread(v, 80, 16, 512)
    fb = spread(v, 16, 32, 1024)
    ib = spread(v, 48, 32, 1024)
    for z in range(4):
        refs.fb[z] = fb[:, z * C : (z + 1) * C]
        refs.ib[z] = ib[:, z * C : (z + 1) * C]


def slot_chunk(p, s):
    low = jnp.minimum(p.z, 3 - p.z)
    shift = jnp.where(s == 0, 1, jnp.where(s == 1, -1, 0))
    m = s + low * shift
    return jnp.where(p.z < 2, m, 3 - m)


SLOT_HOOKS = (
    ("", "Mn3", "Mp1 Mf2"),
    ("Md1", "Mf3 Wf0 Wn1 Wn2", "Mp2 Wn3 Wf1 Dn01"),
    ("Md2", "Mp3 Wf2 Wp0 Un0 Un3", "Wf3 Df00 Dn02 Dn03 Df01"),
    ("Md3", "Wp1 Wp2 Wp3 Uf0 Uf3 Df02 Df03", "Dp00 Dp01 Dp02 Dp03 Up0 Up3"),
)


def mixer_slots(refs, p, T):
    def hook(s, j):
        for k in range(4):

            @pl.when(s == k)
            def _():
                gather_hook(refs, p, SLOT_HOOKS[k][j])

    def slot(s):
        hook(s, 0)
        mixer_forward(refs, slot_chunk(p, s), T, lambda j: hook(s, j))

    loop(4, slot)


SHAPES = ((128, 256), (128, 256), (128, 384), (64, 256))
UP, DOWN, MIX, OUT = 0, 1, 2, 3
TINY = 1e-30
CLIP = 0.01
MATRICES = (
    (512, 1024), (512, 1024), (512, 1024), (1024, 512), (512, 2048), (2048, 512)
)
MATRIX_SLOTS = (1, 2, 3, 6, 8, 9)
VECTORS = ((0, 0, 16), (4, 16, 32), (5, 48, 32), (7, 80, 16))
COUNTS = (512, 524288, 524288, 524288, 1024, 1024, 524288, 512, 1048576, 1048576)


def spot(a, g, z):
    return (g, z) if a == DOWN else (z, g)


def rs_store(refs, a, g, z, value):
    refs.psend[a][(*spot(a, g, z),)] = value.astype(BF16)


def rs_role(p, g, z):
    e = p.turn(z)
    y, x = g // 2, g % 2
    return (1 - e) * ((x + p.x) % 2) + e * ((y + p.y) % 2)


def rs_pair(refs, p, a, u):
    if a == OUT:
        src, dst = refs.psend[a], refs.precv[a]
    else:
        src, dst = refs.psend[a].at[u], refs.precv[a].at[u]
    return rcopy(src, dst, refs.rp_s.at[a, u], refs.rp_r.at[a, u], p.partner)


def rs_merge(refs, p, a, g, z, own):
    place = spot(a, g, z)
    v = own + refs.precv[a][place].astype(F32)
    role = rs_role(p, g, z)

    @pl.when(role == 1)
    def _():
        refs.psend[a][place] = v.astype(BF16)

    @pl.when(role == 0)
    def _():
        refs.precv[a][place] = v.astype(BF16)


def rs_group(p, z, k, sent):
    e = p.turn(z)
    x = (1 - e) * ((p.x + sent) % 2) + e * k
    y = (1 - e) * k + e * ((p.y + sent) % 2)
    return y * 2 + x


def rs_first_copy(refs, p, a, z, k):
    g = rs_group(p, z, k, 1)
    return rcopy(
        refs.psend[a].at[spot(a, g, z)], refs.r1[a].at[z, k],
        refs.r1_s.at[a, z, k], refs.r1_r.at[a, z, k], (p.near(z), p.i),
    )


def rs_first_send(refs, p, a, z):
    for k in range(2):
        rs_first_copy(refs, p, a, z, k).start()


def rs_second(refs, p, a, z):
    e = p.turn(z)
    mine = (1 - e) * p.y + e * p.x
    for k in range(2):
        rs_first_copy(refs, p, a, z, k).wait_recv()
    for k in range(2):
        place = spot(a, rs_group(p, z, k, 0), z)
        v = (refs.precv[a][place].astype(F32) + refs.r1[a][z, k].astype(F32)).astype(BF16)

        @pl.when(mine == k)
        def _():
            refs.precv[a][place] = v

        @pl.when(mine != k)
        def _():
            refs.psend[a][place] = v


def rs_second_copy(refs, p, a, z):
    e = p.turn(z)
    other = 1 - ((1 - e) * p.y + e * p.x)
    place = spot(a, rs_group(p, z, other, 0), z)
    return rcopy(
        refs.psend[a].at[place], refs.r2[a].at[z], refs.r2_s.at[a, z], refs.r2_r.at[a, z],
        (p.far(z), p.i),
    )


def rs_third(refs, p, a, z):
    rs_second_copy(refs, p, a, z).wait_recv()
    place = spot(a, p.g, z)
    v = refs.precv[a][place].astype(F32) + refs.r2[a][z].astype(F32)

    @pl.when(z == p.z)
    def _():
        refs.fin_g[a][...] = v

    @pl.when(z != p.z)
    def _():
        refs.psend[a][place] = v.astype(BF16)


def rs_line(refs, p, a, z, owner):
    return rcopy(
        refs.psend[a].at[spot(a, p.g, z)], refs.r3[a].at[owner],
        refs.r3_s.at[a, z], refs.r3_r.at[a, owner], (p.g, z * 2 + p.c),
    )


def rs_third_send(refs, p, a, z):
    @pl.when(z != p.z)
    def _():
        rs_line(refs, p, a, z, p.z).start()


def rs_last(refs, p, a):
    for k in range(1, 4):
        z = (p.z + k) % 4
        rs_line(refs, p, a, z, z).wait_recv()
        refs.fin_g[a][...] += refs.r3[a][z].astype(F32)


def rs_drain(refs, p):
    def one(z):
        for a in range(4):
            for k in range(2):
                rs_first_copy(refs, p, a, z, k).wait_send()
            rs_second_copy(refs, p, a, z).wait_send()

            @pl.when(z != p.z)
            def _():
                rs_line(refs, p, a, z, p.z).wait_send()

    loop(4, one)


def own_row(x):
    return jnp.sum(x, axis=0, keepdims=True)


def lane_sum(x):
    folded = sum(x[:, k : k + LANES] for k in range(0, x.shape[1], LANES))
    return own_row(folded.T)


def wide(row):
    return jnp.concatenate([row, jnp.zeros((1, LANES - row.shape[1]), F32)], axis=1)


def cut(row):
    return [row[:, k : k + LANES] for k in range(0, row.shape[1], LANES)]


def stand(row):
    return jnp.broadcast_to(row, (LANES, LANES)).T


def scalars(values):
    lane = lax.broadcasted_iota(jnp.int32, (1, LANES), 1)
    out = jnp.zeros((1, LANES), F32)
    for k, v in enumerate(values):
        out = out + jnp.where(lane == k, v, 0.0)
    return out


def total(x):
    return jnp.sum(jnp.sum(x, axis=0, keepdims=True), axis=1, keepdims=True)


def segment(row, start, count):
    lane = lax.broadcasted_iota(jnp.int32, row.shape, 1)
    keep = (lane >= start) & (lane < start + count)
    return jnp.sum(jnp.where(keep, row, 0.0), axis=1, keepdims=True)


def gather_row(term, start, count):
    size = term.shape[1]
    owner = lax.broadcasted_iota(jnp.int32, (32, size), 0)
    spot = lax.broadcasted_iota(jnp.int32, (32, size), 1)
    masked = jnp.where(spot // count == owner, term, 0.0)
    lane = lax.broadcasted_iota(jnp.int32, (LANES, size), 0)
    from_spot = lax.broadcasted_iota(jnp.int32, (LANES, size), 1)
    sel = jnp.where(lane == start + from_spot % count, 1.0, 0.0).astype(BF16)
    out = jnp.zeros((32, LANES), F32)
    for _ in range(3):
        part = masked.astype(BF16)
        out = out + dot_t(part, sel)
        masked = masked - part.astype(F32)
    return out


def parameter_blocks(refs):
    return [
        refs.fw[...].astype(F32), refs.iw[...].astype(F32), refs.cw[...].astype(F32),
        refs.ow[...].astype(F32), refs.uw[...].astype(F32), refs.dw[...].astype(F32),
    ]


def old_rows(refs):
    rows = []
    for r in (refs.row_f, refs.row_i, refs.row_c, refs.row_o, refs.row_u, refs.row_d):
        rows += cut(r[...].reshape(1, r.shape[0]))
    return rows


def old_columns(refs):
    rows = []
    for r in (refs.col_f, refs.col_i, refs.col_c, refs.col_o, refs.col_u, refs.col_d):
        row = r[...].reshape(1, r.shape[0])
        rows += [wide(row)] if r.shape[0] < LANES else cut(row)
    return rows


ROW_PLACES = ((0, 1), (1, 2), (2, 3), (3, 5), (5, 6), (6, 10))
COLUMN_PLACES = ((0, 1), (1, 2), (2, 3), (3, 4), (4, 6), (6, 7))


def broadcast_row(src, box, send, recv, p):
    def one(k):
        rcopy(src, box.at[p.me], send, recv, p.other(k + 1)).start()

    loop(31, one)


def settle_row(box, send, recv, p):
    rows = box.at[pl.ds(0, 31)]
    rcopy(rows, rows, send, recv, p.partner).wait()


def vector_exchange(refs, p):
    rows = (
        gather_row(refs.mgg[...], 0, 16)
        + gather_row(jnp.concatenate([refs.fbg[z] for z in range(4)], axis=1), 16, 32)
        + gather_row(jnp.concatenate([refs.ibg[z] for z in range(4)], axis=1), 48, 32)
        + gather_row(refs.fgg[...], 80, 16)
    )
    refs.vout[...] = rows.reshape(32, 1, LANES)
    refs.vin[p.me] = refs.vout[p.me]

    def one(k):
        t = (p.me + k + 1) % 32
        rcopy(refs.vout.at[t], refs.vin.at[p.me], refs.vex_s, refs.vex_r, p.other(k + 1)).start()

    loop(31, one)


def gradient_blocks(refs, start):
    down = refs.fin_g[DOWN][...]
    rest = [
        refs.fin_g[OUT][...], refs.fin_g[UP][...],
        jnp.concatenate([down[0:64], down[64:128]], axis=1),
    ]
    if start:
        return rest
    mix = refs.fin_g[MIX][...]
    return [mix[:, 0:128], mix[:, 128:256], mix[:, 256:384]] + rest


FLIPPED = (False, False, False, True, False, True)


def part_stats(grads, flips):
    row_parts, column_parts, totals = [], [], []
    for grad, flip in zip(grads, flips):
        sq = grad * grad
        down, across = own_row(sq), lane_sum(sq)
        row_parts += cut(down) if flip else [across]
        column_parts += [wide(across)] if flip else cut(down)
        totals.append(jnp.sum(down, axis=1, keepdims=True))
    return row_parts, column_parts, totals


def adafactor_early(refs, p):
    rows, columns, totals = part_stats(gradient_blocks(refs, 3), FLIPPED[3:])
    refs.rowst[...] = jnp.concatenate([jnp.zeros((3, LANES), F32)] + rows + [jnp.zeros((6, LANES), F32)], axis=0)
    refs.colst[...] = jnp.concatenate(
        [jnp.zeros((3, LANES), F32)] + columns + [jnp.zeros((1, LANES), F32)], axis=0
    )
    params = pack_vectors(refs.mg, refs.fbv, refs.ibv, refs.fg)
    squares = [None] * 10
    for slot, w in zip(MATRIX_SLOTS, parameter_blocks(refs)):
        squares[slot] = total(w * w)
    for slot, start, count in VECTORS:
        squares[slot] = segment(params * params, start, count)
    rows_old = old_rows(refs)
    first = jnp.where(p.i == 0, 1.0, 0.0)
    row_sums = [first * total(jnp.concatenate(rows_old[a:b], axis=0)) for a, b in ROW_PLACES]
    refs.scal[...] = scalars([0.0] * 3 + totals + squares + row_sums)


def adafactor(refs, p):
    grads = gradient_blocks(refs, 0)
    flipped = FLIPPED
    rows, columns, totals = part_stats(grads[0:3], FLIPPED[0:3])
    refs.rowst[0:3, :] = jnp.concatenate(rows, axis=0)
    refs.colst[0:3, :] = jnp.concatenate(columns, axis=0)
    refs.scal[...] += scalars(totals)
    refs.rowin[p.i] = refs.rowst[...]
    refs.colin[p.g] = refs.colst[...]
    refs.scin[p.me] = refs.scal[...]
    for k in range(1, 8):
        peer = (p.g, (p.i + k) % 8)
        rcopy(
            refs.rowst, refs.rowin.at[p.i], refs.row_s.at[k - 1], refs.row_r.at[k - 1], peer
        ).start()
    for k in range(1, 4):
        peer = ((p.g + k) % 4, p.i)
        rcopy(
            refs.colst, refs.colin.at[p.g], refs.col_s.at[k - 1], refs.col_r.at[k - 1], peer
        ).start()
    broadcast_row(refs.scal, refs.scin, refs.sc_s, refs.sc_r, p)
    weights = parameter_blocks(refs)
    params = pack_vectors(refs.mg, refs.fbv, refs.ibv, refs.fg)
    rows_old, columns_old = old_rows(refs), old_columns(refs)
    vec_rows = refs.vin.at[pl.ds(0, 31)]
    rcopy(vec_rows, vec_rows, refs.vex_s, refs.vex_r, p.partner).wait()
    vector_grad = jnp.sum(refs.vin[...].reshape(32, LANES), axis=0, keepdims=True)
    seconds = pack_vectors(refs.sec_m, refs.sec_f, refs.sec_i, refs.sec_g)
    second = 0.5 * seconds + 0.5 * (vector_grad * vector_grad + TINY)
    vector_scaled = vector_grad * lax.rsqrt(second)
    for k in range(1, 8):
        rcopy(
            refs.rowst, refs.rowin.at[p.i], refs.row_s.at[k - 1], refs.row_r.at[k - 1], p.partner
        ).wait()
    for k in range(1, 4):
        rcopy(
            refs.colst, refs.colin.at[p.g], refs.col_s.at[k - 1], refs.col_r.at[k - 1], p.partner
        ).wait()
    settle_row(refs.scin, refs.sc_s, refs.sc_r, p)
    row_total = sum(refs.rowin[k] for k in range(8))
    column_total = sum(refs.colin[k] for k in range(4))
    sc = jnp.sum(refs.scin[...].reshape(32, LANES), axis=0, keepdims=True)
    rows_new, columns_new, scaled = [], [], []
    for k, (r, c) in enumerate(MATRICES):
        ra, rb = ROW_PLACES[k]
        ca, cb = COLUMN_PLACES[k]
        rows = [
            0.5 * rows_old[j] + 0.5 * (row_total[j : j + 1] / c + TINY) for j in range(ra, rb)
        ]
        columns = [
            0.5 * columns_old[j] + 0.5 * (column_total[j : j + 1] / r + TINY)
            for j in range(ca, cb)
        ]
        mean = 0.5 * sc[:, 16 + k : 17 + k] / r + 0.5 * (sc[:, k : k + 1] / (r * c) + TINY)
        lying, standing = (rows, columns) if flipped[k] else (columns, rows)
        tall = stand(standing[0])[0 : grads[k].shape[0]]
        lying = jnp.concatenate(lying, axis=1)
        tall = jnp.concatenate([tall] * (lying.shape[1] // LANES), axis=1)
        scaled.append(grads[k] * lax.rsqrt(tall * lying / mean))
        rows_new += rows
        columns_new += columns
    refs.rows_out[...] = jnp.concatenate(rows_new + [jnp.zeros((6, LANES), F32)], axis=0)
    refs.columns_out[...] = jnp.concatenate(columns_new + [jnp.zeros((1, LANES), F32)], axis=0)
    clips = [None] * 10
    for slot, s in zip(MATRIX_SLOTS, scaled):
        clips[slot] = total(s * s)
    for slot, start, count in VECTORS:
        clips[slot] = segment(vector_scaled * vector_scaled, start, count)
    refs.clip[...] = scalars(clips)
    refs.clin[p.me] = refs.clip[...]
    broadcast_row(refs.clip, refs.clin, refs.cl_s, refs.cl_r, p)
    settle_row(refs.clin, refs.cl_s, refs.cl_r, p)
    clip = jnp.sum(refs.clin[...].reshape(32, LANES), axis=0, keepdims=True)
    norms = [jnp.sqrt(clip[:, k : k + 1] / COUNTS[k]) for k in range(10)]
    steps = [
        -jnp.sqrt(sc[:, 6 + k : 7 + k] / COUNTS[k]) / jnp.maximum(CLIP, norms[k])
        for k in range(10)
    ]
    fresh = [w + steps[slot] * s for slot, w, s in zip(MATRIX_SLOTS, weights, scaled)]
    refs.grad_mix[...] = refs.fin_g[MIX][...]
    refs.grad_out[...] = grads[3]
    refs.grad_up[...] = grads[4]
    refs.grad_down[...] = grads[5]
    refs.new_mix[...] = jnp.concatenate(fresh[0:3], axis=1)
    refs.new_out[...] = fresh[3]
    refs.new_up[...] = fresh[4]
    refs.new_down[...] = fresh[5]
    lane = lax.broadcasted_iota(jnp.int32, (1, LANES), 1)
    step_row = jnp.zeros((1, LANES), F32)
    for slot, start, count in VECTORS:
        step_row = step_row + jnp.where((lane >= start) & (lane < start + count), steps[slot], 0.0)
    refs.vectors[...] = jnp.concatenate(
        [vector_grad, params + step_row * vector_scaled, second, scalars(norms)]
        + [jnp.zeros((4, LANES), F32)],
        axis=0,
    )


def finish_kernel(
    grad_mix, grad_out, grad_up, grad_down, new_mix, new_out, new_up, new_down,
    vectors, rows, columns, block_in, token_in,
    g_mg, g_f, g_i, g_c, g_fb, g_ib, g_o, g_fg, g_u, g_d,
    n_mg, n_f, n_i, n_c, n_fb, n_ib, n_o, n_fg, n_u, n_d,
    s_m, r_f, c_f, r_i, c_i, r_c, c_c, s_f, s_i, r_o, c_o, s_g, r_u, c_u, r_d, c_d, norms,
    block_out, token_out, stage, sem,
):
    copies = []
    for k, (src, dst) in enumerate(((block_in, block_out), (token_in, token_out))):
        fetch = pltpu.make_async_copy(src, stage.at[k], sem.at[0, k])
        fetch.start()
        copies.append((fetch, pltpu.make_async_copy(stage.at[k], dst, sem.at[1, k])))
    for fetch, put in copies:
        fetch.wait()
        put.start()
    for src, outs in ((grad_mix, (g_f, g_i, g_c)), (new_mix, (n_f, n_i, n_c))):
        for k, o in enumerate(outs):
            o[...] = src[:, k * 128 : (k + 1) * 128]
    for src, o in ((grad_out, g_o), (new_out, n_o), (grad_down, g_d), (new_down, n_d)):
        o[...] = src[...]
    g_u[...] = grad_up[...]
    n_u[...] = new_up[...]
    for row, outs in (
        (0, (g_mg, g_fb, g_ib, g_fg)), (1, (n_mg, n_fb, n_ib, n_fg)), (2, (s_m, s_f, s_i, s_g))
    ):
        for (_, start, count), o in zip(VECTORS, outs):
            o[...] = vectors[row, start : start + count]
    norms[...] = vectors[3, 0:10]
    for src, places, outs in (
        (rows, ROW_PLACES, (r_f, r_i, r_c, r_o, r_u, r_d)),
        (columns, COLUMN_PLACES, (c_f, c_i, c_c, c_o, c_u, c_d)),
    ):
        for (a, b), o in zip(places, outs):
            if b - a == 1:
                o[...] = src[a, 0 : o.shape[0]]
            else:
                for k in range(a, b):
                    o[(k - a) * LANES : (k - a + 1) * LANES] = src[k, :]
    for fetch, put in copies:
        put.wait()


def finish(packed, block, tgrad):
    sds = jax.ShapeDtypeStruct
    f = lambda *s: sds(s, F32)
    small = [f(16), f(128, 128), f(128, 128), f(128, 128), f(32), f(32), f(64, 256), f(16),
             f(128, 256), f(64, 512)]
    states = [f(16), f(128), f(128), f(128), f(128), f(128), f(128), f(32), f(32), f(256), f(64),
              f(16), f(128), f(256), f(512), f(64)]
    big = sds(block.shape, BF16)
    outs = tuple(small + small + states + [f(10), big, big])
    vm = pl.BlockSpec(memory_space=pltpu.VMEM)
    anyspec = pl.BlockSpec(memory_space=pl.ANY)
    return pl.pallas_call(
        finish_kernel,
        out_shape=outs,
        in_specs=[vm] * len(packed) + [anyspec] * 2,
        out_specs=(vm,) * (len(outs) - 2) + (anyspec,) * 2,
        scratch_shapes=[pltpu.VMEM((2,) + block.shape, BF16), pltpu.SemaphoreType.DMA((2, 2))],
        name="finish",
    )(*packed, block, tgrad)


class FusedRefs:
    def __init__(self, args):
        (
            self.tok_in, self.cot_in, self.fw, self.iw, self.cw, self.ow, self.uw, self.dw,
            self.mg, self.fbv, self.ibv, self.fg,
            self.sec_m, self.row_f, self.col_f, self.row_i, self.col_i, self.row_c, self.col_c,
            self.sec_f, self.sec_i, self.row_o, self.col_o, self.sec_g,
            self.row_u, self.col_u, self.row_d, self.col_d,
            self.block_out, self.tgrad_out,
            self.grad_mix, self.grad_out, self.grad_up, self.grad_down,
            self.new_mix, self.new_out, self.new_up, self.new_down,
            self.vectors, self.rows_out, self.columns_out,
            self.wmix, self.wot, self.wup, self.wdt, self.g1, self.g2, self.fb, self.ib,
            self.vecs, self.vstage, self.fgg, self.mgg, self.fbg, self.ibg,
            self.tok_p, self.fin, self.min_t, self.fin_t, self.cot_p, self.cot_t,
            self.resid, self.dfe,
            self.pre, self.buf, self.dpre, self.slow, self.st,
            self.keep, self.k_f, self.k_i, self.k_c,
            self.loc_s, self.vec_s, self.vec_r, self.gz_s, self.gz_r,
            self.gn_s, self.gn_r, self.gf_s, self.gf_r, self.gp_s, self.gp_r,
            self.vout, self.vin, self.rowst, self.rowin, self.colst, self.colin,
            self.scal, self.scin, self.clip, self.clin,
            self.rp_s, self.rp_r, self.r1_s, self.r1_r, self.r2_s, self.r2_r,
            self.r3_s, self.r3_r, self.vex_s, self.vex_r,
            self.row_s, self.row_r, self.col_s, self.col_r, self.sc_s, self.sc_r,
            self.cl_s, self.cl_r, self.io_s,
        ) = args[:112]
        rest = list(args[112:])
        self.psend, self.precv, self.r1, self.r2, self.r3, self.fin_g = (
            rest[4 * k : 4 * k + 4] for k in range(6)
        )
        self.io = self.dpre.at[:, 0:512]
        self.oacc = self.pre.at[pl.ds(4, 4)]
        self.tok = self.cot = self.block = self.tgrad = self.io
        self.min = self.fin


def halves_of(refs, plane, rows):
    size = rows.size
    low = refs.pre[plane, rows, :]
    high = refs.pre[plane, pl.ds(rows.start + 512, size), :]
    return jnp.concatenate([low, high], axis=1)


def put_halves(refs, plane, value):
    refs.pre[plane, 0:512, :] = value[:, 0:LANES]
    refs.pre[plane, 512:1024, :] = value[:, LANES : 2 * LANES]


def line_rows(z, c):
    return pl.ds(pl.multiple_of((z * 2 + c) * 64, 64), 64)


def put_feed_grads(refs, p, f):
    z, h = f // 2, f % 2
    up = dot(refs.fin_t[...], refs.dpre[:, C : 2 * C])
    put_halves(refs, 1 + h, dot(refs.cot_t[...], refs.dpre[:, 0:C]))

    @pl.when(h == p.c)
    def _():
        put_halves(refs, 0, up)

    @pl.when(h != p.c)
    def _():
        for g in range(4):
            refs.psend[UP][z, g] = up[g * 128 : (g + 1) * 128].astype(BF16)

    half = pl.ds(pl.multiple_of(h * 64, 64), 64)
    for zz in range(4):
        part = halves_of(refs, 1 + h, line_rows(zz, 1 - p.c))
        refs.psend[DOWN][z, zz, half, :] = part.astype(BF16)


def merge_up(refs, p, z):
    rs_pair(refs, p, UP, z).wait()
    for g in range(4):
        rs_merge(refs, p, UP, g, z, halves_of(refs, 0, pl.ds(g * 128, 128)))


def merge_down(refs, p, g):
    rs_pair(refs, p, DOWN, g).wait()
    for z in range(4):
        own = jnp.concatenate(
            [halves_of(refs, 1 + h, line_rows(z, p.c)) for h in range(2)], axis=0
        )
        rs_merge_at(refs, p, DOWN, g, z, own)


def rs_merge_at(refs, p, a, g, z, own):
    e = p.turn(z)
    y, x = g // 2, g % 2
    role = (1 - e) * ((x + p.x) % 2) + e * ((y + p.y) % 2)
    place = spot(a, g, z)
    v = (own + refs.precv[a][place].astype(F32)).astype(BF16)

    @pl.when(role == 1)
    def _():
        refs.psend[a][place] = v

    @pl.when(role == 0)
    def _():
        refs.precv[a][place] = v


def down_first_send(refs, p, g):
    def one(z):
        e = p.turn(z)
        y, x = g // 2, g % 2

        @pl.when(rs_role(p, g, z) == 1)
        def _():
            rs_first_copy(refs, p, DOWN, z, (1 - e) * y + e * x).start()

    loop(4, one)


def put_out_grads(refs, p):
    def one(g):
        put_halves(refs, g, dot(refs.fin_t[...], refs.slow[g]))
        for z in range(4):
            part = halves_of(refs, g, line_rows(z, 1 - p.c))
            refs.psend[OUT][z, g] = part.astype(BF16)

    loop(4, one)


def merge_out(refs, p):
    rs_pair(refs, p, OUT, 0).wait()

    def one(z):
        for g in range(4):
            rs_merge(refs, p, OUT, g, z, halves_of(refs, g, line_rows(z, p.c)))

    loop(4, one)


def mix_part(refs, g, c):
    cols = []
    for j in range(3):
        q = 3 * c + j
        rows = pl.ds(pl.multiple_of((q % 2) * 512 + g * 128, 128), 128)
        cols.append(refs.pre[q // 2, rows, :])
    return jnp.concatenate(cols, axis=1)


def put_mix_grads(refs, p, z):
    for j in range(3):
        put_halves(refs, j, dot(refs.min_t[...], refs.dpre[:, j * C : (j + 1) * C]))
    for g in range(4):
        refs.psend[MIX][z, g] = mix_part(refs, g, 1 - p.c).astype(BF16)


def merge_mix(refs, p, z):
    rs_pair(refs, p, MIX, z).wait()
    for g in range(4):
        rs_merge(refs, p, MIX, g, z, mix_part(refs, g, p.c))


def all_z(body):
    loop(4, body)


def second(refs, p, a, z):
    rs_second(refs, p, a, z)
    rs_second_copy(refs, p, a, z).start()


def third(refs, p, a, z):
    rs_third(refs, p, a, z)
    rs_third_send(refs, p, a, z)


def feed_order(k):
    return jnp.where(k == 1, 3, jnp.where(k >= 2, k - 1, 0))


def feed_tick(refs, p, f):
    @pl.when((f % 2 == 0) & (f >= 2))
    def _():
        last = feed_order(f // 2 - 1)
        merge_up(refs, p, last)
        merge_down(refs, p, last)
        rs_first_send(refs, p, UP, last)
        down_first_send(refs, p, last)

    @pl.when((f % 2 == 0) & (f >= 4))
    def _():
        second(refs, p, UP, feed_order(f // 2 - 2))

    @pl.when((f % 2 == 0) & (f >= 6))
    def _():
        third(refs, p, UP, feed_order(f // 2 - 3))


def fused_kernel(*args):
    refs = FusedRefs(args)
    refs.fin_grad = refs.fin_g
    T, D = refs.tok_p.shape
    p = Place()
    load = pltpu.make_async_copy(refs.cot_in, refs.io, refs.io_s)
    load.start()
    gather_start(refs, p)
    load.wait()
    cot_in(refs, T)
    gather_hook(refs, p, "Mf0 Mn1")
    load = pltpu.make_async_copy(refs.tok_in, refs.io, refs.io_s)
    load.start()
    gather_vectors(refs, p)
    load.wait()
    norm_in(refs, T)
    gather_hook(refs, p, "Mp0 Mf1 Mn2 Md0")
    mixer_slots(refs, p, T)
    up_own(refs, p, 1)
    gather_hook(refs, p, "Wd0 Wd1 Wd2 Wd3 Un1 Un2 Dn10 Dn11 Dn12 Dn13")
    mix_out(refs, T)
    gather_hook(refs, p, "Ud0 Ud3 Dd00 Dd01 Dd02 Dd03")
    clear(refs.oacc, T)
    refs.dfe[...] = jnp.zeros_like(refs.dfe)

    def feed_step(f):
        @pl.when(f == 4)
        def _():
            gather_hook(refs, p, "Ud1 Ud2 Dd10 Dd11 Dd12 Dd13")

        feed(refs, feed_order(f // 2) * 2 + f % 2, T)

        @pl.when(f == 0)
        def _():
            gather_hook(refs, p, "Uf1 Uf2 Df10 Df11 Df12 Df13")

        @pl.when(f == 1)
        def _():
            gather_hook(refs, p, "Up1 Up2 Dp10 Dp11 Dp12 Dp13")

        feed_tick(refs, p, f)
        put_feed_grads(refs, p, feed_order(f // 2) * 2 + f % 2)

        @pl.when(f % 2 == 1)
        def _():
            rs_pair(refs, p, UP, feed_order(f // 2)).start()
            rs_pair(refs, p, DOWN, feed_order(f // 2)).start()

    loop(8, feed_step)
    feed_back(refs, T)
    store = pltpu.make_async_copy(refs.io, refs.block_out, refs.io_s)
    store.start()
    gather_drain(refs, p)
    merge_up(refs, p, 2)
    merge_down(refs, p, 2)
    rs_first_send(refs, p, UP, 2)
    down_first_send(refs, p, 2)
    second(refs, p, UP, 1)
    third(refs, p, UP, 3)
    put_out_grads(refs, p)
    rs_pair(refs, p, OUT, 0).start()
    clear(refs.oacc, T)
    store.wait()

    def chunk(n):
        return (p.z + 1 + n) % 4

    def early(n):
        @pl.when(n == 0)
        def _():
            merge_out(refs, p)
            all_z(lambda z: rs_first_send(refs, p, OUT, z))

        @pl.when(n >= 1)
        def _():
            merge_mix(refs, p, chunk(n - 1))
            rs_first_send(refs, p, MIX, chunk(n - 1))

        @pl.when(n >= 2)
        def _():
            second(refs, p, MIX, chunk(n - 2))

        @pl.when(n == 2)
        def _():
            all_z(lambda z: third(refs, p, DOWN, z))

        @pl.when(n == 3)
        def _():
            third(refs, p, MIX, chunk(0))

    def late(n):
        @pl.when(n == 0)
        def _():
            second(refs, p, UP, 2)
            all_z(lambda z: second(refs, p, DOWN, z))
            third(refs, p, UP, 1)

        @pl.when(n == 1)
        def _():
            all_z(lambda z: second(refs, p, OUT, z))
            third(refs, p, UP, 2)

        @pl.when(n == 2)
        def _():
            all_z(lambda z: third(refs, p, OUT, z))

    def mixer_step(n):
        z = chunk(n)
        mixer_back(refs, z, T, lambda: early(n))
        put_mix_grads(refs, p, z)
        rs_pair(refs, p, MIX, z).start()
        mixer_input_back(refs, z, T)
        late(n)

    loop(4, mixer_step)
    merge_mix(refs, p, chunk(3))
    rs_first_send(refs, p, MIX, chunk(3))
    second(refs, p, MIX, chunk(2))
    third(refs, p, MIX, chunk(1))
    norm_back(refs, T)
    store = pltpu.make_async_copy(refs.io, refs.tgrad_out, refs.io_s)
    store.start()
    vector_exchange(refs, p)
    for a in (UP, DOWN, OUT):
        rs_last(refs, p, a)
    adafactor_early(refs, p)
    third(refs, p, MIX, chunk(2))
    second(refs, p, MIX, chunk(3))
    third(refs, p, MIX, chunk(3))
    rs_last(refs, p, MIX)
    rs_drain(refs, p)
    adafactor(refs, p)
    store.wait()


def fused(*args):
    T, D = args[0].shape
    Z, F = 4, 8
    sds = jax.ShapeDtypeStruct
    vm = pl.BlockSpec(memory_space=pltpu.VMEM)
    anyspec = pl.BlockSpec(memory_space=pl.ANY)
    V = pltpu.VMEM
    S = pltpu.SemaphoreType.DMA
    outs = (
        sds((T, D), BF16), sds((T, D), BF16),
        sds((128, 384), F32), sds((64, 256), F32), sds((128, 256), F32), sds((64, 512), F32),
        sds((128, 384), F32), sds((64, 256), F32), sds((128, 256), F32), sds((64, 512), F32),
        sds((8, LANES), F32), sds((16, LANES), F32), sds((8, LANES), F32),
    )
    row = V((1, LANES), F32)
    box = V((32, 1, LANES), F32)
    scratch = [
        V((Z, D, 3 * C), BF16), V((Z, D, C), BF16), V((F, D, C), BF16), V((F, D, C), BF16),
        V((1, D), F32), V((1, D), F32), V((Z, 1, C), F32), V((Z, 1, C), F32),
        box, row, V((1, D), F32), V((1, D), F32), V((Z, 1, C), F32), V((Z, 1, C), F32),
        V((T, D), BF16), V((T, D), BF16), V((D, T), BF16), V((D, T), BF16),
        V((T, D), BF16), V((D, T), BF16),
        V((D // LANES, T, LANES), F32), V((T, D), F32),
        V((8, T, LANES), F32), V((4, T, LANES), F32),
        V((T, 3 * C), BF16), V((Z, T, C), BF16), V((Z, T + SUB, C), F32),
        V((Z, T, C), F32), V((Z, T, C), F32), V((Z, T, C), F32), V((Z, T, C), F32),
        S((7,)), S(()), S(()), S((4, 3)), S((4, 4)),
        S((4, 4)), S((4, 4)), S((4, 4, 2)), S((4, 4, 2)), S((4, 4, 4)), S((4, 4, 4)),
        box, box, V((16, LANES), F32), V((8, 16, LANES), F32),
        V((8, LANES), F32), V((4, 8, LANES), F32), row, box, row, box,
        S((4, 4)), S((4, 4)), S((4, 4, 2)), S((4, 4, 2)), S((4, 4)), S((4, 4)),
        S((4, 4)), S((4, 4)), S(()), S(()),
        S((7,)), S((7,)), S((3,)), S((3,)), S(()), S(()), S(()), S(()), S(()),
    ]
    scratch += (
        [V((4, 4) + s, BF16) for s in SHAPES] * 2
        + [V((4, 2) + s, BF16) for s in SHAPES]
        + [V((4,) + s, BF16) for s in SHAPES] * 2
        + [V(s, F32) for s in SHAPES]
    )
    return pl.pallas_call(
        fused_kernel,
        out_shape=outs,
        in_specs=[anyspec, anyspec] + [vm] * (len(args) - 2),
        out_specs=(anyspec, anyspec) + (vm,) * (len(outs) - 2),
        scratch_shapes=scratch,
        compiler_params=pltpu.CompilerParams(
            vmem_limit_bytes=67043328, collective_id=0, has_side_effects=True
        ),
        name="fused",
    )(*args)


def gathered_layer(tok, cot, mix, ow, uw, dw, mg, fb, ib, fg):
    def whole(w):
        w = lax.all_gather(w, "inner", axis=1, tiled=True)
        return lax.all_gather(w, "grp", axis=0, tiled=True)

    def vec(v):
        return lax.all_gather(v, ("grp", "inner"), axis=0, tiled=True).astype(F32)

    width = tok.shape[1]
    inners = lax.axis_size("inner")
    Z, F = mix[0].shape[1] * inners // C, uw.shape[1] * inners // C
    gates = [whole(w).reshape(width, Z, C // LANES, 1, LANES) for w in mix]
    wmix = jnp.concatenate(gates, axis=3).reshape(width, Z, 3 * C).transpose(1, 0, 2)
    wot = whole(ow).reshape(Z, C, width).transpose(0, 2, 1)
    wup = whole(uw).reshape(width, F, C).transpose(1, 0, 2)
    wdt = whole(dw).reshape(F, C, width).transpose(0, 2, 1)
    return layer(
        tok, cot, wmix, wot, wup, wdt,
        vec(mg).reshape(1, width), vec(fg).reshape(1, width),
        vec(fb).reshape(Z, 1, C), vec(ib).reshape(Z, 1, C),
    )


def body(
    tokens,
    cotangent,
    mixer_gain,
    forget_weight,
    input_gate_weight,
    candidate_weight,
    forget_bias,
    input_bias,
    output_weight,
    feed_norm_gain,
    up_weight,
    down_weight,
    mixer_second,
    forget_rows,
    forget_columns,
    input_rows,
    input_columns,
    candidate_rows,
    candidate_columns,
    forget_second,
    input_second,
    output_rows,
    output_columns,
    feed_second,
    up_rows,
    up_columns,
    down_rows,
    down_columns,
):
    groups = lax.axis_size("grp")
    inners = lax.axis_size("inner")
    seqs, length, width = tokens.shape
    hidden = forget_weight.shape[1] * inners
    ff = up_weight.shape[1] * inners
    paired = (groups, inners) == (4, 8) and (length, width, hidden, ff) == (1024, 512, 1024, 2048)
    Z, F = hidden // C, ff // C
    if paired:
        block_output, tokens_grad, *packed = fused(
            tokens.reshape(length, width), cotangent.reshape(length, width),
            forget_weight, input_gate_weight, candidate_weight,
            output_weight.T, up_weight, down_weight.T,
            mixer_gain, forget_bias, input_bias, feed_norm_gain,
            mixer_second, forget_rows, forget_columns, input_rows, input_columns,
            candidate_rows, candidate_columns, forget_second, input_second,
            output_rows, output_columns, feed_second,
            up_rows, up_columns, down_rows, down_columns,
        )
        *done, block_output, tokens_grad = finish(packed, block_output, tokens_grad)
        for k in (6, 9, 16, 19):
            done[k] = done[k].T
        return (block_output.reshape(tokens.shape), tokens_grad.reshape(tokens.shape), *done)
    results = gathered_layer(
        tokens.reshape(length, width), cotangent.reshape(length, width),
        (forget_weight, input_gate_weight, candidate_weight),
        output_weight, up_weight, down_weight,
        mixer_gain, forget_bias, input_bias, feed_norm_gain,
    )
    block_output, tokens_grad, gmix, got, gup, gdt, fgg, mgg, fbg, ibg = results
    block_output = block_output.reshape(tokens.shape)
    tokens_grad = tokens_grad.reshape(tokens.shape)
    split = gmix.transpose(1, 0, 2).reshape(width, Z, C // LANES, 3, LANES)
    forget_term, input_term, cand_term = [
        split[:, :, :, k].reshape(width, hidden) for k in range(3)
    ]
    output_term = got.transpose(0, 2, 1).reshape(hidden, width)
    up_term = gup.transpose(1, 0, 2).reshape(width, ff)
    down_term = gdt.transpose(0, 2, 1).reshape(ff, width)
    gain_first_term, gain_second_term = mgg.reshape(-1), fgg.reshape(-1)
    fbias_term, ibias_term = fbg.reshape(-1), ibg.reshape(-1)
    part = (
        lax.psum_scatter(
            gain_first_term.reshape(groups, -1), "inner", scatter_dimension=1, tiled=True
        ),
        lax.psum_scatter(forget_term, "inner", scatter_dimension=1, tiled=True),
        lax.psum_scatter(input_term, "inner", scatter_dimension=1, tiled=True),
        lax.psum_scatter(cand_term, "inner", scatter_dimension=1, tiled=True),
        lax.psum_scatter(fbias_term.reshape(groups, -1), "inner", scatter_dimension=1, tiled=True),
        lax.psum_scatter(ibias_term.reshape(groups, -1), "inner", scatter_dimension=1, tiled=True),
        lax.psum_scatter(output_term, "inner", scatter_dimension=1, tiled=True),
        lax.psum_scatter(
            gain_second_term.reshape(groups, -1), "inner", scatter_dimension=1, tiled=True
        ),
        lax.psum_scatter(up_term, "inner", scatter_dimension=1, tiled=True),
        lax.psum_scatter(down_term, "inner", scatter_dimension=1, tiled=True),
    )
    mine = (
        lax.psum_scatter(part[0], "grp", scatter_dimension=0, tiled=True),
        lax.psum_scatter(part[1], "grp", scatter_dimension=0, tiled=True),
        lax.psum_scatter(part[2], "grp", scatter_dimension=0, tiled=True),
        lax.psum_scatter(part[3], "grp", scatter_dimension=0, tiled=True),
        lax.psum_scatter(part[4], "grp", scatter_dimension=0, tiled=True),
        lax.psum_scatter(part[5], "grp", scatter_dimension=0, tiled=True),
        lax.psum_scatter(part[6], "grp", scatter_dimension=0, tiled=True),
        lax.psum_scatter(part[7], "grp", scatter_dimension=0, tiled=True),
        lax.psum_scatter(part[8], "grp", scatter_dimension=0, tiled=True),
        lax.psum_scatter(part[9], "grp", scatter_dimension=0, tiled=True),
    )
    params = [
        mixer_gain,
        forget_weight,
        input_gate_weight,
        candidate_weight,
        forget_bias,
        input_bias,
        output_weight,
        feed_norm_gain,
        up_weight,
        down_weight,
    ]
    locals_f = [p.astype(jnp.float32) for p in params]
    grads = [
        mine[0].reshape(-1),
        mine[1],
        mine[2],
        mine[3],
        mine[4].reshape(-1),
        mine[5].reshape(-1),
        mine[6],
        mine[7].reshape(-1),
        mine[8],
        mine[9],
    ]
    matrix_slots = [1, 2, 3, 6, 8, 9]
    vector_slots = [0, 4, 5, 7]
    rows_old = [forget_rows, input_rows, candidate_rows, output_rows, up_rows, down_rows]
    columns_old = [
        forget_columns,
        input_columns,
        candidate_columns,
        output_columns,
        up_columns,
        down_columns,
    ]
    seconds_old = [mixer_second, forget_second, input_second, feed_second]
    counts = [params[k].size * groups * inners for k in range(10)]
    first_inner = (lax.axis_index("inner") == 0).astype(jnp.float32)
    scales = lax.psum(
        jnp.stack(
            [jnp.sum(w * w) for w in locals_f] + [jnp.sum(r) * first_inner for r in rows_old]
        ),
        ("grp", "inner"),
    )
    mats = [grads[k] for k in matrix_slots]
    row_parts = [jnp.sum(g * g, axis=1) for g in mats]
    column_parts = [jnp.sum(g * g, axis=0) for g in mats]
    row_totals = lax.psum(
        (row_parts[0], row_parts[1], row_parts[2], row_parts[3], row_parts[4], row_parts[5]),
        "inner",
    )
    column_totals = lax.psum(
        (
            column_parts[0],
            column_parts[1],
            column_parts[2],
            column_parts[3],
            column_parts[4],
            column_parts[5],
        ),
        "grp",
    )
    grand = lax.psum(jnp.stack([jnp.sum(v) for v in row_totals]), "grp")
    scaled_all = [None] * 10
    new_states = [None] * 16
    state_places = {1: (1, 2), 2: (3, 4), 3: (5, 6), 6: (9, 10), 8: (12, 13), 9: (14, 15)}
    second_places = {0: 0, 4: 7, 5: 8, 7: 11}
    for k in range(6):
        slot = matrix_slots[k]
        grad = mats[k]
        full_rows = grad.shape[0] * groups
        full_columns = grad.shape[1] * inners
        rows = 0.5 * rows_old[k] + 0.5 * (row_totals[k] / full_columns + TINY)
        columns = 0.5 * columns_old[k] + 0.5 * (column_totals[k] / full_rows + TINY)
        row_mean = 0.5 * scales[10 + k] / full_rows + 0.5 * (
            grand[k] / (full_rows * full_columns) + TINY
        )
        scaled_all[slot] = grad * lax.rsqrt(rows[:, None] * columns[None, :] / row_mean)
        new_states[state_places[slot][0]] = rows
        new_states[state_places[slot][1]] = columns
    for k in range(4):
        slot = vector_slots[k]
        grad = grads[slot]
        second = 0.5 * seconds_old[k] + 0.5 * (grad * grad + TINY)
        scaled_all[slot] = grad * lax.rsqrt(second)
        new_states[second_places[slot]] = second
    clip = lax.psum(jnp.stack([jnp.sum(s * s) for s in scaled_all]), ("grp", "inner"))
    count_array = jnp.array(counts, jnp.float32)
    update_norms = jnp.sqrt(clip / count_array)
    fresh = [
        locals_f[k]
        + -jnp.sqrt(scales[k] / counts[k]) * scaled_all[k] / jnp.maximum(CLIP, update_norms[k])
        for k in range(10)
    ]
    return (
        block_output,
        tokens_grad,
        grads[0],
        grads[1],
        grads[2],
        grads[3],
        grads[4],
        grads[5],
        grads[6],
        grads[7],
        grads[8],
        grads[9],
        fresh[0],
        fresh[1],
        fresh[2],
        fresh[3],
        fresh[4],
        fresh[5],
        fresh[6],
        fresh[7],
        fresh[8],
        fresh[9],
        new_states[0],
        new_states[1],
        new_states[2],
        new_states[3],
        new_states[4],
        new_states[5],
        new_states[6],
        new_states[7],
        new_states[8],
        new_states[9],
        new_states[10],
        new_states[11],
        new_states[12],
        new_states[13],
        new_states[14],
        new_states[15],
        update_norms,
    )


def solution(mesh):
    return jax.shard_map(
        body,
        mesh=mesh,
        in_specs=(
            P(("grp", "inner"), None, None),
            P(("grp", "inner"), None, None),
            P(("grp", "inner")),
            P("grp", "inner"),
            P("grp", "inner"),
            P("grp", "inner"),
            P(("grp", "inner")),
            P(("grp", "inner")),
            P("grp", "inner"),
            P(("grp", "inner")),
            P("grp", "inner"),
            P("grp", "inner"),
            P(("grp", "inner")),
            P("grp"),
            P("inner"),
            P("grp"),
            P("inner"),
            P("grp"),
            P("inner"),
            P(("grp", "inner")),
            P(("grp", "inner")),
            P("grp"),
            P("inner"),
            P(("grp", "inner")),
            P("grp"),
            P("inner"),
            P("grp"),
            P("inner"),
        ),
        out_specs=(
            P(("grp", "inner"), None, None),
            P(("grp", "inner"), None, None),
            P(("grp", "inner")),
            P("grp", "inner"),
            P("grp", "inner"),
            P("grp", "inner"),
            P(("grp", "inner")),
            P(("grp", "inner")),
            P("grp", "inner"),
            P(("grp", "inner")),
            P("grp", "inner"),
            P("grp", "inner"),
            P(("grp", "inner")),
            P("grp", "inner"),
            P("grp", "inner"),
            P("grp", "inner"),
            P(("grp", "inner")),
            P(("grp", "inner")),
            P("grp", "inner"),
            P(("grp", "inner")),
            P("grp", "inner"),
            P("grp", "inner"),
            P(("grp", "inner")),
            P("grp"),
            P("inner"),
            P("grp"),
            P("inner"),
            P("grp"),
            P("inner"),
            P(("grp", "inner")),
            P(("grp", "inner")),
            P("grp"),
            P("inner"),
            P(("grp", "inner")),
            P("grp"),
            P("inner"),
            P("grp"),
            P("inner"),
            P(),
        ),
        check_vma=False,
    )
```

```python
import functools
import math
import jax
import jax.numpy as jnp
from jax import lax
from jax.experimental import pallas as pl
from jax.sharding import PartitionSpec as P
from jax.experimental.pallas import tpu as pltpu

EPS = 1e-06
F32 = jnp.float32
BF16 = jnp.bfloat16
C = 256
LANES = 128
SUB = 8
ERFC = (
    0.2256758669, 0.2256693636, 0.2078460312, 0.1685204197, 0.1415057621,
    -0.005753053848, 0.1692475449, -0.182997133, 0.05028532412,
)


def dot(a, b):
    return jnp.dot(a, b, preferred_element_type=F32)


def dot_t(a, b):
    return lax.dot_general(a, b, (((1,), (1,)), ((), ())), preferred_element_type=F32)


def loop(steps, body):
    def run(i, carry):
        body(i)
        return carry

    lax.fori_loop(0, steps, run, 0)


def at(i, size):
    return pl.ds(pl.multiple_of(i * size, size), size)


def gelu_parts(x):
    e = jnp.exp2((x * x) * (-0.5 / math.log(2.0)))
    t = 1.0 / (1.0 + (0.4 * math.sqrt(0.5)) * jnp.abs(x))
    poly = jnp.full_like(t, 0.5 * ERFC[-1])
    for c in ERFC[-2::-1]:
        poly = poly * t + 0.5 * c
    half = poly * (t * e)
    cdf = jnp.where(x >= 0, 1.0 - half, half)
    return x * cdf, cdf + (x * e) * (1.0 / math.sqrt(2.0 * math.pi))


def reorder(inverse):
    row = lax.broadcasted_iota(jnp.int32, (LANES, LANES), 0)
    col = lax.broadcasted_iota(jnp.int32, (LANES, LANES), 1)
    step = LANES // SUB
    source = (row % step) * SUB + row // step if inverse else (row % SUB) * step + row // SUB
    return jnp.where(col == source, 1.0, 0.0).astype(BF16)


def tile_rows(i, s, T):
    step = LANES // SUB
    return pl.ds(pl.multiple_of(i * step + s * (T // SUB), step), step)


def gather_rows(ref, i, order, T):
    return dot(order, jnp.concatenate([ref[tile_rows(i, s, T), :] for s in range(SUB)], axis=0))


def scatter_rows(ref, i, order, out, T):
    step = LANES // SUB
    flat = dot(order, out.astype(BF16)).astype(BF16)
    for s in range(SUB):
        ref[tile_rows(i, s, T), :] = flat[s * step : (s + 1) * step]


LOG2E = 1.0 / math.log(2.0)


def load_planes(ref, rows, start=0, count=None):
    count = ref.shape[0] if count is None else count
    return jnp.concatenate([ref[q, rows, :] for q in range(start, start + count)], axis=1)


def store_planes(ref, rows, value, start=0):
    for q in range(value.shape[1] // LANES):
        ref[start + q, rows, :] = value[:, q * LANES : (q + 1) * LANES]


def add_planes(ref, rows, value):
    for q in range(value.shape[1] // LANES):
        ref[q, rows, :] += value[:, q * LANES : (q + 1) * LANES]


def clear(ref, T):
    for q in range(4):
        ref[q, 0:T, :] = jnp.zeros((T, LANES), F32)


def norm_in(refs, T):
    order = reorder(False)

    def place(i):
        x = gather_rows(refs.tok, i, order, T)
        y = x * lax.rsqrt(jnp.mean(x * x, axis=-1, keepdims=True) + EPS) * refs.g1[...]
        rows = at(i, LANES)
        refs.tok_p[rows, :] = x.astype(BF16)
        refs.min[rows, :] = y.astype(BF16)
        refs.min_t[:, rows] = y.T.astype(BF16)

    loop(T // LANES, place)


def cot_in(refs, T):
    order = reorder(False)

    def place(i):
        x = gather_rows(refs.cot, i, order, T)
        rows = at(i, LANES)
        refs.cot_p[rows, :] = x.astype(BF16)
        refs.cot_t[:, rows] = x.T.astype(BF16)

    loop(T // LANES, place)


def mixer_forward(refs, z, T, hook=None):
    pre, ac, st = refs.pre, refs.buf, refs.st
    halves = C // LANES
    width = 3 * LANES

    def project(i):
        rows = at(i, 256)
        out = dot(refs.min[rows, :], refs.wmix[z])
        for q in range(3 * halves):
            pre[q, rows, :] = out[:, q * LANES : (q + 1) * LANES]

    loop(T // 256, project)
    fb = refs.fb[z]
    ib = refs.ib[z]

    def gates(i, carry):
        r0 = pl.multiple_of(i * 64, 64)
        out = []
        for h in range(halves):
            a, b = carry[h]
            lanes = slice(h * LANES, (h + 1) * LANES)
            pf = pre[3 * h, pl.ds(r0, 64), :] + fb[:, lanes]
            pi = pre[3 * h + 1, pl.ds(r0, 64), :] + ib[:, lanes]
            pc = pre[3 * h + 2, pl.ds(r0, 64), :]
            pf, pi = pf * LOG2E, pi * LOG2E
            m = jnp.minimum(jnp.minimum(pf, pi), 0.0)
            e0 = jnp.exp2(m)
            ef = jnp.exp2(m - pf)
            ei = jnp.exp2(m - pi)
            nk = e0 + ei
            na = e0 + ef
            both = nk + na
            floor = jnp.maximum(na, 1e-37)
            rec = 1.0 / (both * floor)
            inv = rec * floor
            keep = nk * inv
            admit = na * inv
            ec = jnp.exp(jnp.minimum(pc, 0.0))
            sg = ec / (1.0 + ec)
            positive = pc >= 0
            value = jnp.where(positive, pc + 0.5, sg)
            slope = jnp.where(positive, 1.0, sg * (1.0 - sg))
            refs.keep[z, pl.ds(r0, 64), lanes] = keep
            refs.k_f[z, pl.ds(r0, 64), lanes] = keep * (ef * (rec * both))
            refs.k_i[z, pl.ds(r0, 64), lanes] = ei * inv
            refs.k_c[z, pl.ds(r0, 64), lanes] = admit * slope
            inflow = admit * value
            alist, blist = [], []
            for j in range(8):
                kj = keep[j * SUB : (j + 1) * SUB]
                b = kj * b + inflow[j * SUB : (j + 1) * SUB]
                a = kj * a
                alist.append(a)
                blist.append(b)
            ac[h, pl.ds(r0, 64), :] = jnp.concatenate(alist, axis=0)
            st[z, pl.ds(r0 + SUB, 64), lanes] = jnp.concatenate(blist, axis=0)
            out.append((a, b))
        return tuple(out)

    one = jnp.ones((SUB, LANES), F32)
    zero = jnp.zeros((SUB, LANES), F32)
    if hook is not None:
        hook(1)
    ends = lax.fori_loop(0, T // 64, gates, tuple((one, zero) for _ in range(halves)))
    if hook is not None:
        hook(2)
    for h in range(halves):
        a, b = ends[h]
        rows = [jnp.zeros((1, LANES), F32)]
        for s in range(SUB - 1):
            rows.append(a[s : s + 1] * rows[-1] + b[s : s + 1])
        st[z, 0:SUB, h * LANES : (h + 1) * LANES] = jnp.concatenate(rows, axis=0)
    first = st[z, 0:SUB, :]

    def finish(i):
        r0 = pl.multiple_of(i * 64, 64)
        a = load_planes(ac, pl.ds(r0, 64), 0, 2).reshape(8, SUB, C)
        b = st[z, pl.ds(r0 + SUB, 64), :].reshape(8, SUB, C)
        s = (b + a * first[None]).reshape(64, C)
        st[z, pl.ds(r0 + SUB, 64), :] = s
        refs.slow[z, pl.ds(r0, 64), :] = s.astype(BF16)

    loop(T // 64, finish)


def mix_out(refs, T):
    Z = refs.wot.shape[0]

    def body(i):
        rows = at(i, 256)
        acc = refs.tok_p[rows, :].astype(F32)
        for z in range(Z):
            acc = acc + dot_t(refs.slow[z, rows, :], refs.wot[z])
        store_planes(refs.resid, rows, acc)
        for k in range(2):
            x = acc[k * LANES : (k + 1) * LANES]
            y = x * lax.rsqrt(jnp.mean(x * x, axis=-1, keepdims=True) + EPS) * refs.g2[...]
            sub = pl.ds(pl.multiple_of(i * 256 + k * LANES, LANES), LANES)
            refs.fin[sub, :] = y.astype(BF16)
            refs.fin_t[:, sub] = y.T.astype(BF16)

    loop(T // 256, body)


def feed(refs, f, T):
    wup, wdt = refs.wup, refs.wdt
    size = 256
    tiles = T // size

    up, back = {}, {}

    def project(i):
        rows = slice(i * size, (i + 1) * size)
        up[i] = dot(refs.fin[rows, :], wup[f])
        back[i] = dot(refs.cot_p[rows, :], wdt[f])

    def activate(i):
        for k in range(size // 32):
            part = slice(k * 32, (k + 1) * 32)
            rows = slice(i * size + k * 32, i * size + (k + 1) * 32)
            act, slope = gelu_parts(up[i][part])
            refs.dpre[rows, 0:C] = act.astype(BF16)
            refs.dpre[rows, C : 2 * C] = (back[i][part] * slope).astype(BF16)

    def add(i):
        rows = slice(i * size, (i + 1) * size)
        add_planes(refs.oacc, rows, dot_t(refs.dpre[rows, 0:C], wdt[f]))
        refs.dfe[rows, :] += dot_t(refs.dpre[rows, C : 2 * C], wup[f])

    for i in range(tiles + 2):
        if i < tiles:
            project(i)
        if 1 <= i < tiles + 1:
            activate(i - 1)
        if i >= 2:
            add(i - 2)


def feed_back(refs, T):
    order = reorder(True)
    D = refs.g1.shape[1]

    def body(i, total):
        rows = at(i, LANES)
        x = load_planes(refs.resid, rows)
        df = refs.dfe[rows, :]
        out = x + load_planes(refs.oacc, rows, 0, D // LANES)
        scatter_rows(refs.block, i, order, out, T)
        r = lax.rsqrt(jnp.mean(x * x, axis=-1, keepdims=True) + EPS)
        nrm = x * r
        dn = df * refs.g2[...]
        mean = jnp.mean(dn * nrm, axis=-1, keepdims=True)
        dres = refs.cot_p[rows, :].astype(F32) + r * (dn - nrm * mean)
        refs.dfe[rows, :] = dres
        refs.fin[rows, :] = dres.astype(BF16)
        refs.fin_t[:, rows] = dres.T.astype(BF16)
        return total + (df * nrm).reshape(16, SUB, D).sum(axis=0)

    total = lax.fori_loop(0, T // LANES, body, jnp.zeros((SUB, D), F32))
    refs.fgg[...] = jnp.sum(total, axis=0, keepdims=True)


def mixer_back(refs, z, T, hook=None):
    buf, st = refs.buf, refs.st
    halves = C // LANES
    width = 3 * LANES

    def project(i):
        rows = at(i, 256)
        store_planes(buf, rows, dot(refs.fin[rows, :], refs.wot[z]))

    loop(T // 256, project)
    steps = T // 64

    def local(i, carry):
        r0 = pl.multiple_of((steps - 1 - i) * 64, 64)
        d = load_planes(buf, pl.ds(r0, 64), 0, 2)
        k = refs.keep[z, pl.ds(r0, 64), :]
        e, dk = carry
        plist, dlist = [None] * 8, [None] * 8
        for j in range(7, -1, -1):
            kj = k[j * SUB : (j + 1) * SUB]
            p = d[j * SUB : (j + 1) * SUB] + e
            plist[j] = p
            dlist[j] = dk
            e = kj * p
            dk = kj * dk
        store_planes(buf, pl.ds(r0, 64), jnp.concatenate(plist, axis=0))
        store_planes(buf, pl.ds(r0, 64), jnp.concatenate(dlist, axis=0), 2)
        return e, dk

    e, dk = lax.fori_loop(0, steps, local, (jnp.zeros((SUB, C), F32), jnp.ones((SUB, C), F32)))
    rows = [jnp.zeros((1, C), F32)]
    for s in range(SUB - 1, 0, -1):
        rows.insert(0, e[s : s + 1] + dk[s : s + 1] * rows[0])
    tail = jnp.concatenate(rows, axis=0)
    if hook is not None:
        hook()

    def grads(i, sums):
        r0 = pl.multiple_of(i * 64, 64)
        out = []
        for h in range(halves):
            lanes = slice(h * LANES, (h + 1) * LANES)
            sub = pl.ds(r0, 64)
            p0 = buf[h, sub, :].reshape(8, SUB, LANES)
            d0 = buf[2 + h, sub, :].reshape(8, SUB, LANES)
            p = (p0 + d0 * tail[None, :, lanes]).reshape(64, LANES)
            x = p * (st[z, pl.ds(r0 + SUB, 64), lanes] - st[z, sub, lanes])
            df = -(refs.k_f[z, sub, lanes] * x)
            di = refs.k_i[z, sub, lanes] * x
            dcand = refs.k_c[z, sub, lanes] * p
            df16 = df.astype(BF16)
            di16 = di.astype(BF16)
            refs.dpre[sub, h * width : h * width + LANES] = df16
            refs.dpre[sub, h * width + LANES : h * width + 2 * LANES] = di16
            refs.dpre[sub, h * width + 2 * LANES : h * width + 3 * LANES] = dcand.astype(BF16)
            sf, si = sums[h]
            out.append(
                (
                    sf + df16.astype(F32).reshape(8, SUB, LANES).sum(axis=0),
                    si + di16.astype(F32).reshape(8, SUB, LANES).sum(axis=0),
                )
            )
        return tuple(out)

    zero = jnp.zeros((SUB, LANES), F32)
    sums = lax.fori_loop(0, T // 64, grads, tuple((zero, zero) for _ in range(halves)))
    for h in range(halves):
        lanes = slice(h * LANES, (h + 1) * LANES)
        refs.fbg[z, :, lanes] = jnp.sum(sums[h][0], axis=0, keepdims=True)
        refs.ibg[z, :, lanes] = jnp.sum(sums[h][1], axis=0, keepdims=True)


def mixer_input_back(refs, z, T):
    def back(i):
        rows = at(i, 256)
        add_planes(refs.oacc, rows, dot_t(refs.dpre[rows, :], refs.wmix[z]))

    loop(T // 256, back)


def norm_back(refs, T):
    order = reorder(True)
    D = refs.g1.shape[1]

    def body(i, total):
        rows = at(i, LANES)
        x = refs.tok_p[rows, :].astype(F32)
        d_in = load_planes(refs.oacc, rows, 0, D // LANES)
        r = lax.rsqrt(jnp.mean(x * x, axis=-1, keepdims=True) + EPS)
        nrm = x * r
        dn = d_in * refs.g1[...]
        mean = jnp.mean(dn * nrm, axis=-1, keepdims=True)
        out = refs.dfe[rows, :] + r * (dn - nrm * mean)
        scatter_rows(refs.tgrad, i, order, out, T)
        return total + (d_in * nrm).reshape(16, SUB, D).sum(axis=0)

    total = lax.fori_loop(0, T // LANES, body, jnp.zeros((SUB, D), F32))
    refs.mgg[...] = jnp.sum(total, axis=0, keepdims=True)


class Refs:
    def __init__(self, args):
        (
            self.tok, self.cot, self.wmix, self.wot, self.wup, self.wdt, self.g1, self.g2, self.fb, self.ib,
            self.block, self.tgrad, self.gmix, self.got, self.gup, self.gdt, self.fgg, self.mgg, self.fbg, self.ibg,
            self.tok_p, self.min, self.min_t, self.fin, self.fin_t, self.cot_p, self.cot_t, self.resid, self.oacc, self.dfe,
            self.pre, self.buf, self.dpre, self.slow, self.st, self.keep, self.k_f,
            self.k_i, self.k_c, self.gst, self.gsem,
        ) = args


def layer_kernel(*args):
    refs = Refs(args)
    T, D = refs.tok.shape
    Z = refs.wmix.shape[0]
    F = refs.wup.shape[0]
    gst, sem = refs.gst, refs.gsem
    cot_in(refs, T)
    norm_in(refs, T)
    loop(Z, lambda z: mixer_forward(refs, z, T))
    mix_out(refs, T)
    clear(refs.oacc, T)
    refs.dfe[...] = jnp.zeros_like(refs.dfe)

    def feed_step(f):
        feed(refs, f, T)
        gst[0, :, 0:C] = dot(refs.cot_t[...], refs.dpre[:, 0:C])
        gst[1, :, 0:C] = dot(refs.fin_t[...], refs.dpre[:, C : 2 * C])
        one = pltpu.make_async_copy(gst.at[0, :, 0:C], refs.gdt.at[f], sem.at[0])
        two = pltpu.make_async_copy(gst.at[1, :, 0:C], refs.gup.at[f], sem.at[1])
        one.start()
        two.start()
        one.wait()
        two.wait()

    loop(F, feed_step)
    feed_back(refs, T)
    clear(refs.oacc, T)

    def mixer_step(z):
        gst[0, :, 0:C] = dot(refs.fin_t[...], refs.slow[z])
        mixer_back(refs, z, T)
        mixer_input_back(refs, z, T)
        gst[1, :, :] = dot(refs.min_t[...], refs.dpre[...])
        one = pltpu.make_async_copy(gst.at[0, :, 0:C], refs.got.at[z], sem.at[0])
        two = pltpu.make_async_copy(gst.at[1], refs.gmix.at[z], sem.at[1])
        one.start()
        two.start()
        one.wait()
        two.wait()

    loop(Z, mixer_step)
    norm_back(refs, T)


def layer(tok, cot, wmix, wot, wup, wdt, g1, g2, fb, ib):
    T, D = tok.shape
    Z, F = wmix.shape[0], wup.shape[0]
    sds = jax.ShapeDtypeStruct
    vm = pl.BlockSpec(memory_space=pltpu.VMEM)
    anyspec = pl.BlockSpec(memory_space=pl.ANY)
    out_shape = (
        sds((T, D), BF16), sds((T, D), BF16),
        sds((Z, D, 3 * C), F32), sds((Z, D, C), F32), sds((F, D, C), F32), sds((F, D, C), F32),
        sds((1, D), F32), sds((1, D), F32), sds((Z, 1, C), F32), sds((Z, 1, C), F32),
    )
    V = pltpu.VMEM
    scratch = [
        V((T, D), BF16), V((T, D), BF16), V((D, T), BF16), V((T, D), BF16), V((D, T), BF16),
        V((T, D), BF16), V((D, T), BF16), V((D // LANES, T, LANES), F32),
        V((D // LANES, T, LANES), F32), V((T, D), F32), V((3 * C // LANES, T, LANES), F32), V((4, T, LANES), F32),
        V((T, 3 * C), BF16), V((Z, T, C), BF16), V((Z, T + SUB, C), F32),
        V((Z, T, C), F32), V((Z, T, C), F32), V((Z, T, C), F32), V((Z, T, C), F32),
        V((2, D, 3 * C), F32), pltpu.SemaphoreType.DMA((2,)),
    ]
    return pl.pallas_call(
        layer_kernel,
        out_shape=out_shape,
        in_specs=[vm] * 10,
        out_specs=(vm, vm, anyspec, anyspec, anyspec, anyspec, vm, vm, vm, vm),
        scratch_shapes=scratch,
        compiler_params=pltpu.CompilerParams(vmem_limit_bytes=67043328),
        name="layer",
    )(tok, cot, wmix, wot, wup, wdt, g1, g2, fb, ib)


MESH = pl.DeviceIdType.MESH


def rcopy(src, dst, send, recv, device):
    return pltpu.make_async_remote_copy(
        src_ref=src, dst_ref=dst, send_sem=send, recv_sem=recv, device_id=device, device_id_type=MESH
    )


class Place:
    def __init__(self):
        self.g = lax.axis_index("grp")
        self.i = lax.axis_index("inner")
        self.y, self.x = self.g // 2, self.g % 2
        self.z, self.c = self.i // 2, self.i % 2
        self.me = self.g * 8 + self.i
        self.partner = (self.g, self.z * 2 + 1 - self.c)

    def flip(self, fx, fy):
        x = (self.x + fx) % 2
        y = (self.y + fy) % 2
        return y * 2 + x

    def turn(self, z):
        return (z + self.c) % 2

    def near(self, z):
        e = self.turn(z)
        return self.flip(1 - e, e)

    def far(self, z):
        e = self.turn(z)
        return self.flip(e, 1 - e)

    def other(self, k):
        t = (self.me + k) % 32
        return (t // 8, t % 8)


def entry_signal(place):
    barrier = pltpu.get_barrier_semaphore()

    def greet(k):
        pl.semaphore_signal(barrier, inc=1, device_id=place.other(k + 1), device_id_type=MESH)

    loop(31, greet)


def entry_wait():
    pl.semaphore_wait(pltpu.get_barrier_semaphore(), 31)


def spread(values, start, count, total):
    lane = lax.broadcasted_iota(jnp.int32, (LANES, total), 1)
    row = lax.broadcasted_iota(jnp.int32, (LANES, total), 0)
    sel = jnp.where(row == start + lane % count, 1.0, 0.0).astype(BF16)
    picked = dot(values, sel)
    owner = lax.broadcasted_iota(jnp.int32, picked.shape, 0)
    spot = lax.broadcasted_iota(jnp.int32, picked.shape, 1)
    return jnp.sum(jnp.where(spot // count == owner, picked, 0.0), axis=0, keepdims=True)


def pack_vectors(mg, fb, ib, fg):
    parts = [mg, fb, ib, fg]
    used = sum(p.shape[0] for p in parts)
    rows = [p[...].astype(F32).reshape(1, p.shape[0]) for p in parts]
    return jnp.concatenate(rows + [jnp.zeros((1, LANES - used), F32)], axis=1)


FIRST = (3, 0)
LATER = (1, 2)


def block_of(refs, a, g, i):
    if a == 0:
        return refs.wot.at[g, at(i, 64), :]
    if a == 1:
        return refs.wup.at[i, at(g, 128), :]
    if a == 2:
        return refs.wdt.at[pl.ds(2 * g, 2), at(i, 64), :]
    return refs.wmix.at[i // 2, at(g, 128), at(i % 2, 384)]


def blocks_of(refs, a, i):
    if a == 0:
        return refs.wot.at[:, at(i, 64), :]
    if a == 1:
        return refs.wup.at[i]
    if a == 2:
        return refs.wdt.at[:, at(i, 64), :]
    return refs.wmix.at[i // 2, :, at(i % 2, 384)]


def line_send(refs, p, a):
    blk = block_of(refs, a, p.g, p.i)
    for s in range(1, 4):
        peer = (p.g, slot_chunk(p, s) * 2 + p.c)
        rcopy(blk, blk, refs.gz_s.at[a, s - 1], refs.gz_r.at[a, p.z], peer).start()


def near_of(p, a, z):
    return p.near(z + (a in LATER))


def far_of(p, a, z):
    return p.far(z + (a in LATER))


def line_wait(refs, p, a, z):
    @pl.when(z != p.z)
    def _():
        blk = block_of(refs, a, p.g, z * 2 + p.c)
        rcopy(blk, blk, refs.gp_s.at[a, z, 0], refs.gz_r.at[a, z], p.partner).wait_recv()


def near_send(refs, p, a, z):
    blk = block_of(refs, a, p.g, z * 2 + p.c)
    near, far = (near_of(p, a, z), p.i), (far_of(p, a, z), p.i)
    rcopy(blk, blk, refs.gn_s.at[a, z], refs.gn_r.at[a, z], near).start()
    rcopy(blk, blk, refs.gf_s.at[a, z, 0], refs.gf_r.at[a, z, 0], far).start()


def far_send(refs, p, a, z):
    near = block_of(refs, a, near_of(p, a, z), z * 2 + p.c)
    far = (far_of(p, a, z), p.i)
    rcopy(near, near, refs.gn_s.at[a, z], refs.gn_r.at[a, z], p.partner).wait_recv()
    rcopy(near, near, refs.gf_s.at[a, z, 1], refs.gf_r.at[a, z, 1], far).start()


def far_wait(refs, p, a, z, k):
    blk = block_of(refs, a, p.g, z * 2 + p.c)
    rcopy(blk, blk, refs.gf_s.at[a, z, k], refs.gf_r.at[a, z, k], p.partner).wait_recv()


def pair_copy(refs, p, a, z, c):
    full = blocks_of(refs, a, z * 2 + c)
    return rcopy(full, full, refs.gp_s.at[a, z, 0], refs.gp_r.at[a, z, 0], p.partner)


def first_step(refs, p, arrays, kind, s):
    for a in arrays:
        z = slot_chunk(p, s)
        if kind == "n":
            line_wait(refs, p, a, z)
            near_send(refs, p, a, z)
        elif kind == "f":
            far_send(refs, p, a, z)
        elif kind == "p":
            far_wait(refs, p, a, z, 0)
            far_wait(refs, p, a, z, 1)
            pair_copy(refs, p, a, z, p.c).start()
        else:
            pair_copy(refs, p, a, z, 1 - p.c).wait_recv()


def up_step(refs, p, kind, m):
    if kind == "n":

        @pl.when(p.z != m)
        def _():
            line_wait(refs, p, 1, m)
            near_send(refs, p, 1, m)
    elif kind == "f":
        far_send(refs, p, 1, m)
    elif kind == "p":
        far_wait(refs, p, 1, m, 0)
        far_wait(refs, p, 1, m, 1)
        pair_copy(refs, p, 1, m, p.c).start()
    else:
        pair_copy(refs, p, 1, m, 1 - p.c).wait_recv()


def up_own(refs, p, phase):
    inner = (p.z + 1) // 2 % 2

    @pl.when(inner == phase)
    def _():
        near_send(refs, p, 1, p.z)


def down_pair(refs, p, z, phase, k, c):
    g = (1 + k) if phase else 3 * k
    blk = block_of(refs, 2, g, z * 2 + c)
    return rcopy(blk, blk, refs.gp_s.at[2, z, phase * 2 + k], refs.gp_r.at[2, z, phase * 2 + k], p.partner)


def down_step(refs, p, kind, phase, s):
    z = slot_chunk(p, s)
    active = (p.x + p.y) % 2 == phase
    idle = (p.x + p.y) % 2 != phase
    if kind == "n":

        @pl.when(active)
        def _():
            line_wait(refs, p, 2, z)
            near_send(refs, p, 2, z)
    elif kind == "f":

        @pl.when(idle)
        def _():
            far_send(refs, p, 2, z)
    elif kind == "p":

        @pl.when(active)
        def _():
            far_wait(refs, p, 2, z, 1)

        @pl.when(idle)
        def _():
            far_wait(refs, p, 2, z, 0)

        for k in range(2):
            down_pair(refs, p, z, phase, k, p.c).start()
    else:
        down_pair(refs, p, z, phase, 0 if kind == "d" else 1, 1 - p.c).wait_recv()


def gather_drain(refs, p):
    for a in range(4):
        blk = block_of(refs, a, p.g, p.i)
        for k in range(3):
            rcopy(blk, blk, refs.gz_s.at[a, k], refs.gz_r.at[a, p.z], p.partner).wait_send()
        for z in range(4):
            blk = block_of(refs, a, p.g, z * 2 + p.c)
            rcopy(blk, blk, refs.gn_s.at[a, z], refs.gn_r.at[a, z], p.partner).wait_send()
            for k in range(2):
                rcopy(blk, blk, refs.gf_s.at[a, z, k], refs.gf_r.at[a, z, k], p.partner).wait_send()
            if a == 2:
                for k in range(4):
                    down_pair(refs, p, z, k // 2, k % 2, p.c).wait_send()
            else:
                pair_copy(refs, p, a, z, p.c).wait_send()


def gather_hook(refs, p, actions):
    for action in actions.split():
        kind, number = action[1], int(action[-1])
        if action[0] == "M":
            first_step(refs, p, (3,), kind, number)
        elif action[0] == "W":
            first_step(refs, p, (0,), kind, number)
        elif action[0] == "U":
            up_step(refs, p, kind, number)
        else:
            down_step(refs, p, kind, int(action[2]), number)


def gather_start(refs, p):
    local = []
    for k, w in enumerate((refs.fw, refs.iw, refs.cw)):
        spot = pl.ds(pl.multiple_of(p.c * 384 + k * 128, 128), 128)
        local.append(
            pltpu.make_async_copy(w, refs.wmix.at[p.z, at(p.g, 128), spot], refs.loc_s.at[k])
        )
    local.append(pltpu.make_async_copy(refs.ow, block_of(refs, 0, p.g, p.i), refs.loc_s.at[3]))
    local.append(pltpu.make_async_copy(refs.uw, block_of(refs, 1, p.g, p.i), refs.loc_s.at[4]))
    for k in range(2):
        local.append(
            pltpu.make_async_copy(
                refs.dw.at[:, k * 256 : (k + 1) * 256],
                refs.wdt.at[2 * p.g + k, at(p.i, 64), :],
                refs.loc_s.at[5 + k],
            )
        )
    for c in local:
        c.start()
    row = pack_vectors(refs.mg, refs.fbv, refs.ibv, refs.fg)
    refs.vstage[...] = row
    refs.vecs[p.me] = row
    for c in local:
        c.wait()
    entry_wait()

    def vector(k):
        rcopy(refs.vstage, refs.vecs.at[p.me], refs.vec_s, refs.vec_r, p.other(k + 1)).start()

    for a in FIRST:
        near_send(refs, p, a, p.z)
    up_own(refs, p, 0)
    down_step(refs, p, "n", 0, 0)
    for k in range(31):
        vector(k)
    for a in FIRST:
        line_send(refs, p, a)
    inner = (p.z + 1) // 2 % 2

    @pl.when(inner == 0)
    def _():
        line_send(refs, p, 1)

    line_send(refs, p, 2)

    @pl.when(inner == 1)
    def _():
        line_send(refs, p, 1)


def gather_vectors(refs, p):
    rows = refs.vecs.at[pl.ds(0, 31)]
    rcopy(rows, rows, refs.vec_s, refs.vec_r, p.partner).wait()
    v = refs.vecs[...].reshape(32, LANES).astype(BF16)
    refs.g1[...] = spread(v, 0, 16, 512)
    refs.g2[...] = spread(v, 80, 16, 512)
    fb = spread(v, 16, 32, 1024)
    ib = spread(v, 48, 32, 1024)
    for z in range(4):
        refs.fb[z] = fb[:, z * C : (z + 1) * C]
        refs.ib[z] = ib[:, z * C : (z + 1) * C]


def slot_chunk(p, s):
    low = jnp.minimum(p.z, 3 - p.z)
    shift = jnp.where(s == 0, 1, jnp.where(s == 1, -1, 0))
    m = s + low * shift
    return jnp.where(p.z < 2, m, 3 - m)


SLOT_HOOKS = (
    ("", "Mn3", "Mp1 Mf2"),
    ("Md1", "Mf3 Wf0 Wn1 Wn2", "Mp2 Wn3 Wf1 Dn01"),
    ("Md2", "Mp3 Wf2 Wp0 Un0 Un3", "Wf3 Df00 Dn02 Dn03 Df01"),
    ("Md3", "Wp1 Wp2 Wp3 Uf0 Uf3 Df02 Df03", "Dp00 Dp01 Dp02 Dp03 Up0 Up3"),
)


def mixer_slots(refs, p, T):
    def hook(s, j):
        for k in range(4):

            @pl.when(s == k)
            def _():
                gather_hook(refs, p, SLOT_HOOKS[k][j])

    def slot(s):
        hook(s, 0)
        mixer_forward(refs, slot_chunk(p, s), T, lambda j: hook(s, j))

    loop(4, slot)


SHAPES = ((128, 256), (128, 256), (128, 384), (64, 256))
UP, DOWN, MIX, OUT = 0, 1, 2, 3
TINY = 1e-30
CLIP = 0.01
MATRICES = (
    (512, 1024), (512, 1024), (512, 1024), (1024, 512), (512, 2048), (2048, 512)
)
MATRIX_SLOTS = (1, 2, 3, 6, 8, 9)
VECTORS = ((0, 0, 16), (4, 16, 32), (5, 48, 32), (7, 80, 16))
COUNTS = (512, 524288, 524288, 524288, 1024, 1024, 524288, 512, 1048576, 1048576)


def spot(a, g, z):
    return (g, z) if a == DOWN else (z, g)


def rs_store(refs, a, g, z, value):
    refs.psend[a][(*spot(a, g, z),)] = value.astype(BF16)


def rs_role(p, g, z):
    e = p.turn(z)
    y, x = g // 2, g % 2
    return (1 - e) * ((x + p.x) % 2) + e * ((y + p.y) % 2)


def rs_pair(refs, p, a, u):
    if a == OUT:
        src, dst = refs.psend[a], refs.precv[a]
    else:
        src, dst = refs.psend[a].at[u], refs.precv[a].at[u]
    return rcopy(src, dst, refs.rp_s.at[a, u], refs.rp_r.at[a, u], p.partner)


def rs_merge(refs, p, a, g, z, own):
    place = spot(a, g, z)
    v = own + refs.precv[a][place].astype(F32)
    role = rs_role(p, g, z)

    @pl.when(role == 1)
    def _():
        refs.psend[a][place] = v.astype(BF16)

    @pl.when(role == 0)
    def _():
        refs.precv[a][place] = v.astype(BF16)


def rs_group(p, z, k, sent):
    e = p.turn(z)
    x = (1 - e) * ((p.x + sent) % 2) + e * k
    y = (1 - e) * k + e * ((p.y + sent) % 2)
    return y * 2 + x


def rs_first_copy(refs, p, a, z, k):
    g = rs_group(p, z, k, 1)
    return rcopy(
        refs.psend[a].at[spot(a, g, z)], refs.r1[a].at[z, k],
        refs.r1_s.at[a, z, k], refs.r1_r.at[a, z, k], (p.near(z), p.i),
    )


def rs_first_send(refs, p, a, z):
    for k in range(2):
        rs_first_copy(refs, p, a, z, k).start()


def rs_second(refs, p, a, z):
    e = p.turn(z)
    mine = (1 - e) * p.y + e * p.x
    for k in range(2):
        rs_first_copy(refs, p, a, z, k).wait_recv()
    for k in range(2):
        place = spot(a, rs_group(p, z, k, 0), z)
        v = (refs.precv[a][place].astype(F32) + refs.r1[a][z, k].astype(F32)).astype(BF16)

        @pl.when(mine == k)
        def _():
            refs.precv[a][place] = v

        @pl.when(mine != k)
        def _():
            refs.psend[a][place] = v


def rs_second_copy(refs, p, a, z):
    e = p.turn(z)
    other = 1 - ((1 - e) * p.y + e * p.x)
    place = spot(a, rs_group(p, z, other, 0), z)
    return rcopy(
        refs.psend[a].at[place], refs.r2[a].at[z], refs.r2_s.at[a, z], refs.r2_r.at[a, z],
        (p.far(z), p.i),
    )


def rs_third(refs, p, a, z):
    rs_second_copy(refs, p, a, z).wait_recv()
    place = spot(a, p.g, z)
    v = refs.precv[a][place].astype(F32) + refs.r2[a][z].astype(F32)

    @pl.when(z == p.z)
    def _():
        refs.fin_g[a][...] = v

    @pl.when(z != p.z)
    def _():
        refs.psend[a][place] = v.astype(BF16)


def rs_line(refs, p, a, z, owner):
    return rcopy(
        refs.psend[a].at[spot(a, p.g, z)], refs.r3[a].at[owner],
        refs.r3_s.at[a, z], refs.r3_r.at[a, owner], (p.g, z * 2 + p.c),
    )


def rs_third_send(refs, p, a, z):
    @pl.when(z != p.z)
    def _():
        rs_line(refs, p, a, z, p.z).start()


def rs_last(refs, p, a):
    for k in range(1, 4):
        z = (p.z + k) % 4
        rs_line(refs, p, a, z, z).wait_recv()
        refs.fin_g[a][...] += refs.r3[a][z].astype(F32)


def rs_drain(refs, p):
    def one(z):
        for a in range(4):
            for k in range(2):
                rs_first_copy(refs, p, a, z, k).wait_send()
            rs_second_copy(refs, p, a, z).wait_send()

            @pl.when(z != p.z)
            def _():
                rs_line(refs, p, a, z, p.z).wait_send()

    loop(4, one)


def own_row(x):
    return jnp.sum(x, axis=0, keepdims=True)


def lane_sum(x):
    folded = sum(x[:, k : k + LANES] for k in range(0, x.shape[1], LANES))
    return own_row(folded.T)


def wide(row):
    return jnp.concatenate([row, jnp.zeros((1, LANES - row.shape[1]), F32)], axis=1)


def cut(row):
    return [row[:, k : k + LANES] for k in range(0, row.shape[1], LANES)]


def stand(row):
    return jnp.broadcast_to(row, (LANES, LANES)).T


def scalars(values):
    lane = lax.broadcasted_iota(jnp.int32, (1, LANES), 1)
    out = jnp.zeros((1, LANES), F32)
    for k, v in enumerate(values):
        out = out + jnp.where(lane == k, v, 0.0)
    return out


def total(x):
    return jnp.sum(jnp.sum(x, axis=0, keepdims=True), axis=1, keepdims=True)


def segment(row, start, count):
    lane = lax.broadcasted_iota(jnp.int32, row.shape, 1)
    keep = (lane >= start) & (lane < start + count)
    return jnp.sum(jnp.where(keep, row, 0.0), axis=1, keepdims=True)


def gather_row(term, start, count):
    size = term.shape[1]
    owner = lax.broadcasted_iota(jnp.int32, (32, size), 0)
    spot = lax.broadcasted_iota(jnp.int32, (32, size), 1)
    masked = jnp.where(spot // count == owner, term, 0.0)
    lane = lax.broadcasted_iota(jnp.int32, (LANES, size), 0)
    from_spot = lax.broadcasted_iota(jnp.int32, (LANES, size), 1)
    sel = jnp.where(lane == start + from_spot % count, 1.0, 0.0).astype(BF16)
    out = jnp.zeros((32, LANES), F32)
    for _ in range(3):
        part = masked.astype(BF16)
        out = out + dot_t(part, sel)
        masked = masked - part.astype(F32)
    return out


def parameter_blocks(refs):
    return [
        refs.fw[...].astype(F32), refs.iw[...].astype(F32), refs.cw[...].astype(F32),
        refs.ow[...].astype(F32), refs.uw[...].astype(F32), refs.dw[...].astype(F32),
    ]


def old_rows(refs):
    rows = []
    for r in (refs.row_f, refs.row_i, refs.row_c, refs.row_o, refs.row_u, refs.row_d):
        rows += cut(r[...].reshape(1, r.shape[0]))
    return rows


def old_columns(refs):
    rows = []
    for r in (refs.col_f, refs.col_i, refs.col_c, refs.col_o, refs.col_u, refs.col_d):
        row = r[...].reshape(1, r.shape[0])
        rows += [wide(row)] if r.shape[0] < LANES else cut(row)
    return rows


ROW_PLACES = ((0, 1), (1, 2), (2, 3), (3, 5), (5, 6), (6, 10))
COLUMN_PLACES = ((0, 1), (1, 2), (2, 3), (3, 4), (4, 6), (6, 7))


def broadcast_row(src, box, send, recv, p):
    def one(k):
        rcopy(src, box.at[p.me], send, recv, p.other(k + 1)).start()

    for k in range(31):
        one(k)


def settle_row(box, send, recv, p):
    rows = box.at[pl.ds(0, 31)]
    rcopy(rows, rows, send, recv, p.partner).wait()


def vector_exchange(refs, p):
    rows = (
        gather_row(refs.mgg[...], 0, 16)
        + gather_row(jnp.concatenate([refs.fbg[z] for z in range(4)], axis=1), 16, 32)
        + gather_row(jnp.concatenate([refs.ibg[z] for z in range(4)], axis=1), 48, 32)
        + gather_row(refs.fgg[...], 80, 16)
    )
    refs.vout[...] = rows.reshape(32, 1, LANES)
    refs.vin[p.me] = refs.vout[p.me]

    def one(k):
        t = (p.me + k + 1) % 32
        rcopy(refs.vout.at[t], refs.vin.at[p.me], refs.vex_s, refs.vex_r, p.other(k + 1)).start()

    for k in range(31):
        one(k)


def gradient_blocks(refs, start):
    down = refs.fin_g[DOWN][...]
    rest = [
        refs.fin_g[OUT][...], refs.fin_g[UP][...],
        jnp.concatenate([down[0:64], down[64:128]], axis=1),
    ]
    if start:
        return rest
    mix = refs.fin_g[MIX][...]
    return [mix[:, 0:128], mix[:, 128:256], mix[:, 256:384]] + rest


FLIPPED = (False, False, False, True, False, True)


def part_stats(grads, flips):
    row_parts, column_parts, totals = [], [], []
    for grad, flip in zip(grads, flips):
        sq = grad * grad
        down, across = own_row(sq), lane_sum(sq)
        row_parts += cut(down) if flip else [across]
        column_parts += [wide(across)] if flip else cut(down)
        totals.append(jnp.sum(down, axis=1, keepdims=True))
    return row_parts, column_parts, totals


def adafactor_early(refs, p):
    rows, columns, totals = part_stats(gradient_blocks(refs, 3), FLIPPED[3:])
    refs.rowst[...] = jnp.concatenate([jnp.zeros((3, LANES), F32)] + rows + [jnp.zeros((6, LANES), F32)], axis=0)
    refs.colst[...] = jnp.concatenate(
        [jnp.zeros((3, LANES), F32)] + columns + [jnp.zeros((1, LANES), F32)], axis=0
    )
    params = pack_vectors(refs.mg, refs.fbv, refs.ibv, refs.fg)
    squares = [None] * 10
    for slot, w in zip(MATRIX_SLOTS, parameter_blocks(refs)):
        squares[slot] = total(w * w)
    for slot, start, count in VECTORS:
        squares[slot] = segment(params * params, start, count)
    rows_old = old_rows(refs)
    first = jnp.where(p.i == 0, 1.0, 0.0)
    row_sums = [first * total(jnp.concatenate(rows_old[a:b], axis=0)) for a, b in ROW_PLACES]
    refs.scal[...] = scalars([0.0] * 3 + totals + squares + row_sums)


def adafactor(refs, p):
    grads = gradient_blocks(refs, 0)
    flipped = FLIPPED
    rows, columns, totals = part_stats(grads[0:3], FLIPPED[0:3])
    refs.rowst[0:3, :] = jnp.concatenate(rows, axis=0)
    refs.colst[0:3, :] = jnp.concatenate(columns, axis=0)
    refs.scal[...] += scalars(totals)
    refs.rowin[p.i] = refs.rowst[...]
    refs.colin[p.g] = refs.colst[...]
    refs.scin[p.me] = refs.scal[...]
    for k in range(1, 8):
        peer = (p.g, (p.i + k) % 8)
        rcopy(
            refs.rowst, refs.rowin.at[p.i], refs.row_s.at[k - 1], refs.row_r.at[k - 1], peer
        ).start()
    for k in range(1, 4):
        peer = ((p.g + k) % 4, p.i)
        rcopy(
            refs.colst, refs.colin.at[p.g], refs.col_s.at[k - 1], refs.col_r.at[k - 1], peer
        ).start()
    broadcast_row(refs.scal, refs.scin, refs.sc_s, refs.sc_r, p)
    weights = parameter_blocks(refs)
    params = pack_vectors(refs.mg, refs.fbv, refs.ibv, refs.fg)
    rows_old, columns_old = old_rows(refs), old_columns(refs)
    vec_rows = refs.vin.at[pl.ds(0, 31)]
    rcopy(vec_rows, vec_rows, refs.vex_s, refs.vex_r, p.partner).wait()
    vector_grad = jnp.sum(refs.vin[...].reshape(32, LANES), axis=0, keepdims=True)
    seconds = pack_vectors(refs.sec_m, refs.sec_f, refs.sec_i, refs.sec_g)
    second = 0.5 * seconds + 0.5 * (vector_grad * vector_grad + TINY)
    vector_scaled = vector_grad * lax.rsqrt(second)
    for k in range(1, 8):
        rcopy(
            refs.rowst, refs.rowin.at[p.i], refs.row_s.at[k - 1], refs.row_r.at[k - 1], p.partner
        ).wait()
    for k in range(1, 4):
        rcopy(
            refs.colst, refs.colin.at[p.g], refs.col_s.at[k - 1], refs.col_r.at[k - 1], p.partner
        ).wait()
    settle_row(refs.scin, refs.sc_s, refs.sc_r, p)
    row_total = sum(refs.rowin[k] for k in range(8))
    column_total = sum(refs.colin[k] for k in range(4))
    sc = jnp.sum(refs.scin[...].reshape(32, LANES), axis=0, keepdims=True)
    rows_new, columns_new, scaled = [], [], []
    for k, (r, c) in enumerate(MATRICES):
        ra, rb = ROW_PLACES[k]
        ca, cb = COLUMN_PLACES[k]
        rows = [
            0.5 * rows_old[j] + 0.5 * (row_total[j : j + 1] / c + TINY) for j in range(ra, rb)
        ]
        columns = [
            0.5 * columns_old[j] + 0.5 * (column_total[j : j + 1] / r + TINY)
            for j in range(ca, cb)
        ]
        mean = 0.5 * sc[:, 16 + k : 17 + k] / r + 0.5 * (sc[:, k : k + 1] / (r * c) + TINY)
        lying, standing = (rows, columns) if flipped[k] else (columns, rows)
        tall = stand(standing[0])[0 : grads[k].shape[0]]
        lying = jnp.concatenate(lying, axis=1)
        tall = jnp.concatenate([tall] * (lying.shape[1] // LANES), axis=1)
        scaled.append(grads[k] * lax.rsqrt(tall * lying / mean))
        rows_new += rows
        columns_new += columns
    refs.rows_out[...] = jnp.concatenate(rows_new + [jnp.zeros((6, LANES), F32)], axis=0)
    refs.columns_out[...] = jnp.concatenate(columns_new + [jnp.zeros((1, LANES), F32)], axis=0)
    clips = [None] * 10
    for slot, s in zip(MATRIX_SLOTS, scaled):
        clips[slot] = total(s * s)
    for slot, start, count in VECTORS:
        clips[slot] = segment(vector_scaled * vector_scaled, start, count)
    refs.clip[...] = scalars(clips)
    refs.clin[p.me] = refs.clip[...]
    broadcast_row(refs.clip, refs.clin, refs.cl_s, refs.cl_r, p)
    settle_row(refs.clin, refs.cl_s, refs.cl_r, p)
    clip = jnp.sum(refs.clin[...].reshape(32, LANES), axis=0, keepdims=True)
    norms = [jnp.sqrt(clip[:, k : k + 1] / COUNTS[k]) for k in range(10)]
    steps = [
        -jnp.sqrt(sc[:, 6 + k : 7 + k] / COUNTS[k]) / jnp.maximum(CLIP, norms[k])
        for k in range(10)
    ]
    fresh = [w + steps[slot] * s for slot, w, s in zip(MATRIX_SLOTS, weights, scaled)]
    refs.grad_mix[...] = refs.fin_g[MIX][...]
    refs.grad_out[...] = grads[3]
    refs.grad_up[...] = grads[4]
    refs.grad_down[...] = grads[5]
    refs.new_mix[...] = jnp.concatenate(fresh[0:3], axis=1)
    refs.new_out[...] = fresh[3]
    refs.new_up[...] = fresh[4]
    refs.new_down[...] = fresh[5]
    lane = lax.broadcasted_iota(jnp.int32, (1, LANES), 1)
    step_row = jnp.zeros((1, LANES), F32)
    for slot, start, count in VECTORS:
        step_row = step_row + jnp.where((lane >= start) & (lane < start + count), steps[slot], 0.0)
    refs.vectors[...] = jnp.concatenate(
        [vector_grad, params + step_row * vector_scaled, second, scalars(norms)]
        + [jnp.zeros((4, LANES), F32)],
        axis=0,
    )


def finish_kernel(
    grad_mix, grad_out, grad_up, grad_down, new_mix, new_out, new_up, new_down,
    vectors, rows, columns, block_in, token_in,
    g_mg, g_f, g_i, g_c, g_fb, g_ib, g_o, g_fg, g_u, g_d,
    n_mg, n_f, n_i, n_c, n_fb, n_ib, n_o, n_fg, n_u, n_d,
    s_m, r_f, c_f, r_i, c_i, r_c, c_c, s_f, s_i, r_o, c_o, s_g, r_u, c_u, r_d, c_d, norms,
    block_out, token_out, stage, sem,
):
    copies = []
    for k, (src, dst) in enumerate(((block_in, block_out), (token_in, token_out))):
        fetch = pltpu.make_async_copy(src, stage.at[k], sem.at[0, k])
        fetch.start()
        copies.append((fetch, pltpu.make_async_copy(stage.at[k], dst, sem.at[1, k])))
    for fetch, put in copies:
        fetch.wait()
        put.start()
    for src, outs in ((grad_mix, (g_f, g_i, g_c)), (new_mix, (n_f, n_i, n_c))):
        for k, o in enumerate(outs):
            o[...] = src[:, k * 128 : (k + 1) * 128]
    for src, o in ((grad_out, g_o), (new_out, n_o), (grad_down, g_d), (new_down, n_d)):
        o[...] = src[...]
    g_u[...] = grad_up[...]
    n_u[...] = new_up[...]
    for row, outs in (
        (0, (g_mg, g_fb, g_ib, g_fg)), (1, (n_mg, n_fb, n_ib, n_fg)), (2, (s_m, s_f, s_i, s_g))
    ):
        for (_, start, count), o in zip(VECTORS, outs):
            o[...] = vectors[row, start : start + count]
    norms[...] = vectors[3, 0:10]
    for src, places, outs in (
        (rows, ROW_PLACES, (r_f, r_i, r_c, r_o, r_u, r_d)),
        (columns, COLUMN_PLACES, (c_f, c_i, c_c, c_o, c_u, c_d)),
    ):
        for (a, b), o in zip(places, outs):
            if b - a == 1:
                o[...] = src[a, 0 : o.shape[0]]
            else:
                for k in range(a, b):
                    o[(k - a) * LANES : (k - a + 1) * LANES] = src[k, :]
    for fetch, put in copies:
        put.wait()


def finish(packed, block, tgrad):
    sds = jax.ShapeDtypeStruct
    f = lambda *s: sds(s, F32)
    small = [f(16), f(128, 128), f(128, 128), f(128, 128), f(32), f(32), f(64, 256), f(16),
             f(128, 256), f(64, 512)]
    states = [f(16), f(128), f(128), f(128), f(128), f(128), f(128), f(32), f(32), f(256), f(64),
              f(16), f(128), f(256), f(512), f(64)]
    big = sds(block.shape, BF16)
    outs = tuple(small + small + states + [f(10), big, big])
    vm = pl.BlockSpec(memory_space=pltpu.VMEM)
    anyspec = pl.BlockSpec(memory_space=pl.ANY)
    return pl.pallas_call(
        finish_kernel,
        out_shape=outs,
        in_specs=[vm] * len(packed) + [anyspec] * 2,
        out_specs=(vm,) * (len(outs) - 2) + (anyspec,) * 2,
        scratch_shapes=[pltpu.VMEM((2,) + block.shape, BF16), pltpu.SemaphoreType.DMA((2, 2))],
        name="finish",
    )(*packed, block, tgrad)


class FusedRefs:
    def __init__(self, args):
        (
            self.tok_in, self.cot_in, self.fw, self.iw, self.cw, self.ow, self.uw, self.dw,
            self.mg, self.fbv, self.ibv, self.fg,
            self.sec_m, self.row_f, self.col_f, self.row_i, self.col_i, self.row_c, self.col_c,
            self.sec_f, self.sec_i, self.row_o, self.col_o, self.sec_g,
            self.row_u, self.col_u, self.row_d, self.col_d,
            self.block_out, self.tgrad_out,
            self.grad_mix, self.grad_out, self.grad_up, self.grad_down,
            self.new_mix, self.new_out, self.new_up, self.new_down,
            self.vectors, self.rows_out, self.columns_out,
            self.wmix, self.wot, self.wup, self.wdt, self.g1, self.g2, self.fb, self.ib,
            self.vecs, self.vstage, self.fgg, self.mgg, self.fbg, self.ibg,
            self.tok_p, self.fin, self.min_t, self.fin_t, self.cot_p, self.cot_t,
            self.resid, self.dfe,
            self.pre, self.buf, self.dpre, self.slow, self.st,
            self.keep, self.k_f, self.k_i, self.k_c,
            self.loc_s, self.vec_s, self.vec_r, self.gz_s, self.gz_r,
            self.gn_s, self.gn_r, self.gf_s, self.gf_r, self.gp_s, self.gp_r,
            self.vout, self.vin, self.rowst, self.rowin, self.colst, self.colin,
            self.scal, self.scin, self.clip, self.clin,
            self.rp_s, self.rp_r, self.r1_s, self.r1_r, self.r2_s, self.r2_r,
            self.r3_s, self.r3_r, self.vex_s, self.vex_r,
            self.row_s, self.row_r, self.col_s, self.col_r, self.sc_s, self.sc_r,
            self.cl_s, self.cl_r, self.io_s,
        ) = args[:112]
        rest = list(args[112:])
        self.psend, self.precv, self.r1, self.r2, self.r3, self.fin_g = (
            rest[4 * k : 4 * k + 4] for k in range(6)
        )
        self.io = self.dpre.at[:, 0:512]
        self.oacc = self.pre.at[pl.ds(4, 4)]
        self.tok = self.cot = self.block = self.tgrad = self.io
        self.min = self.fin


def halves_of(refs, plane, rows):
    size = rows.size
    low = refs.pre[plane, rows, :]
    high = refs.pre[plane, pl.ds(rows.start + 512, size), :]
    return jnp.concatenate([low, high], axis=1)


def put_halves(refs, plane, value):
    refs.pre[plane, 0:512, :] = value[:, 0:LANES]
    refs.pre[plane, 512:1024, :] = value[:, LANES : 2 * LANES]


def line_rows(z, c):
    return pl.ds(pl.multiple_of((z * 2 + c) * 64, 64), 64)


def put_feed_grads(refs, p, f):
    z, h = f // 2, f % 2
    up = dot(refs.fin_t[...], refs.dpre[:, C : 2 * C])
    put_halves(refs, 1 + h, dot(refs.cot_t[...], refs.dpre[:, 0:C]))

    @pl.when(h == p.c)
    def _():
        put_halves(refs, 0, up)

    @pl.when(h != p.c)
    def _():
        for g in range(4):
            refs.psend[UP][z, g] = up[g * 128 : (g + 1) * 128].astype(BF16)

    half = pl.ds(pl.multiple_of(h * 64, 64), 64)
    for zz in range(4):
        part = halves_of(refs, 1 + h, line_rows(zz, 1 - p.c))
        refs.psend[DOWN][z, zz, half, :] = part.astype(BF16)


def merge_up(refs, p, z):
    rs_pair(refs, p, UP, z).wait()
    for g in range(4):
        rs_merge(refs, p, UP, g, z, halves_of(refs, 0, pl.ds(g * 128, 128)))


def merge_down(refs, p, g):
    rs_pair(refs, p, DOWN, g).wait()
    for z in range(4):
        own = jnp.concatenate(
            [halves_of(refs, 1 + h, line_rows(z, p.c)) for h in range(2)], axis=0
        )
        rs_merge_at(refs, p, DOWN, g, z, own)


def rs_merge_at(refs, p, a, g, z, own):
    e = p.turn(z)
    y, x = g // 2, g % 2
    role = (1 - e) * ((x + p.x) % 2) + e * ((y + p.y) % 2)
    place = spot(a, g, z)
    v = (own + refs.precv[a][place].astype(F32)).astype(BF16)

    @pl.when(role == 1)
    def _():
        refs.psend[a][place] = v

    @pl.when(role == 0)
    def _():
        refs.precv[a][place] = v


def down_first_send(refs, p, g):
    def one(z):
        e = p.turn(z)
        y, x = g // 2, g % 2

        @pl.when(rs_role(p, g, z) == 1)
        def _():
            rs_first_copy(refs, p, DOWN, z, (1 - e) * y + e * x).start()

    loop(4, one)


def put_out_grads(refs, p):
    def one(g):
        put_halves(refs, g, dot(refs.fin_t[...], refs.slow[g]))
        for z in range(4):
            part = halves_of(refs, g, line_rows(z, 1 - p.c))
            refs.psend[OUT][z, g] = part.astype(BF16)

    loop(4, one)


def merge_out(refs, p):
    rs_pair(refs, p, OUT, 0).wait()

    def one(z):
        for g in range(4):
            rs_merge(refs, p, OUT, g, z, halves_of(refs, g, line_rows(z, p.c)))

    loop(4, one)


def mix_part(refs, g, c):
    cols = []
    for j in range(3):
        q = 3 * c + j
        rows = pl.ds(pl.multiple_of((q % 2) * 512 + g * 128, 128), 128)
        cols.append(refs.pre[q // 2, rows, :])
    return jnp.concatenate(cols, axis=1)


def put_mix_grads(refs, p, z):
    for j in range(3):
        put_halves(refs, j, dot(refs.min_t[...], refs.dpre[:, j * C : (j + 1) * C]))
    for g in range(4):
        refs.psend[MIX][z, g] = mix_part(refs, g, 1 - p.c).astype(BF16)


def merge_mix(refs, p, z):
    rs_pair(refs, p, MIX, z).wait()
    for g in range(4):
        rs_merge(refs, p, MIX, g, z, mix_part(refs, g, p.c))


def all_z(body):
    loop(4, body)


def second(refs, p, a, z):
    rs_second(refs, p, a, z)
    rs_second_copy(refs, p, a, z).start()


def third(refs, p, a, z):
    rs_third(refs, p, a, z)
    rs_third_send(refs, p, a, z)


def feed_order(k):
    return jnp.where(k == 1, 3, jnp.where(k >= 2, k - 1, 0))


def feed_tick(refs, p, f):
    @pl.when((f % 2 == 0) & (f >= 2))
    def _():
        last = feed_order(f // 2 - 1)
        merge_up(refs, p, last)
        merge_down(refs, p, last)
        rs_first_send(refs, p, UP, last)
        down_first_send(refs, p, last)

    @pl.when((f % 2 == 0) & (f >= 4))
    def _():
        second(refs, p, UP, feed_order(f // 2 - 2))

    @pl.when((f % 2 == 0) & (f >= 6))
    def _():
        third(refs, p, UP, feed_order(f // 2 - 3))


def fused_kernel(*args):
    refs = FusedRefs(args)
    refs.fin_grad = refs.fin_g
    T, D = refs.tok_p.shape
    p = Place()
    entry_signal(p)
    load = pltpu.make_async_copy(refs.cot_in, refs.io, refs.io_s)
    load.start()
    gather_start(refs, p)
    load.wait()
    cot_in(refs, T)
    gather_hook(refs, p, "Mf0 Mn1")
    load = pltpu.make_async_copy(refs.tok_in, refs.io, refs.io_s)
    load.start()
    gather_vectors(refs, p)
    load.wait()
    norm_in(refs, T)
    gather_hook(refs, p, "Mp0 Mf1 Mn2 Md0")
    mixer_slots(refs, p, T)
    up_own(refs, p, 1)
    gather_hook(refs, p, "Wd0 Wd1 Wd2 Wd3 Un1 Un2 Dn10 Dn11 Dn12 Dn13")
    mix_out(refs, T)
    gather_hook(refs, p, "Ud0 Dd00 Dd01 Dd02 Dd03")
    clear(refs.oacc, T)
    refs.dfe[...] = jnp.zeros_like(refs.dfe)

    def feed_step(f):
        @pl.when(f == 2)
        def _():
            gather_hook(refs, p, "Ud3 De00 De01 De02 De03")

        @pl.when(f == 4)
        def _():
            gather_hook(refs, p, "Ud1 Dd10 Dd11 Dd12 Dd13")

        @pl.when(f == 6)
        def _():
            gather_hook(refs, p, "Ud2 De10 De11 De12 De13")

        feed(refs, feed_order(f // 2) * 2 + f % 2, T)

        @pl.when(f == 0)
        def _():
            gather_hook(refs, p, "Uf1 Uf2 Df10 Df11 Df12 Df13")

        @pl.when(f == 1)
        def _():
            gather_hook(refs, p, "Up1 Up2 Dp10 Dp11 Dp12 Dp13")

        feed_tick(refs, p, f)
        put_feed_grads(refs, p, feed_order(f // 2) * 2 + f % 2)

        @pl.when(f % 2 == 1)
        def _():
            rs_pair(refs, p, UP, feed_order(f // 2)).start()
            rs_pair(refs, p, DOWN, feed_order(f // 2)).start()

    loop(8, feed_step)
    feed_back(refs, T)
    store = pltpu.make_async_copy(refs.io, refs.block_out, refs.io_s)
    store.start()
    gather_drain(refs, p)
    merge_up(refs, p, 2)
    merge_down(refs, p, 2)
    rs_first_send(refs, p, UP, 2)
    down_first_send(refs, p, 2)
    second(refs, p, UP, 1)
    third(refs, p, UP, 3)
    put_out_grads(refs, p)
    rs_pair(refs, p, OUT, 0).start()
    clear(refs.oacc, T)
    store.wait()

    def chunk(n):
        return (p.z + 1 + n) % 4

    def early(n):
        @pl.when(n == 0)
        def _():
            merge_out(refs, p)
            all_z(lambda z: rs_first_send(refs, p, OUT, z))

        @pl.when(n >= 1)
        def _():
            merge_mix(refs, p, chunk(n - 1))
            rs_first_send(refs, p, MIX, chunk(n - 1))

        @pl.when(n >= 2)
        def _():
            second(refs, p, MIX, chunk(n - 2))

        @pl.when(n == 2)
        def _():
            all_z(lambda z: third(refs, p, DOWN, z))

        @pl.when(n == 3)
        def _():
            third(refs, p, MIX, chunk(0))

    def late(n):
        @pl.when(n == 0)
        def _():
            second(refs, p, UP, 2)
            all_z(lambda z: second(refs, p, DOWN, z))
            third(refs, p, UP, 1)

        @pl.when(n == 1)
        def _():
            all_z(lambda z: second(refs, p, OUT, z))
            third(refs, p, UP, 2)

        @pl.when(n == 2)
        def _():
            all_z(lambda z: third(refs, p, OUT, z))

    def mixer_step(n):
        z = chunk(n)
        mixer_back(refs, z, T, lambda: early(n))
        put_mix_grads(refs, p, z)
        rs_pair(refs, p, MIX, z).start()
        mixer_input_back(refs, z, T)
        late(n)

    loop(4, mixer_step)
    merge_mix(refs, p, chunk(3))
    rs_first_send(refs, p, MIX, chunk(3))
    second(refs, p, MIX, chunk(2))
    third(refs, p, MIX, chunk(1))
    norm_back(refs, T)
    store = pltpu.make_async_copy(refs.io, refs.tgrad_out, refs.io_s)
    store.start()
    vector_exchange(refs, p)
    for a in (UP, DOWN, OUT):
        rs_last(refs, p, a)
    adafactor_early(refs, p)
    third(refs, p, MIX, chunk(2))
    second(refs, p, MIX, chunk(3))
    third(refs, p, MIX, chunk(3))
    rs_last(refs, p, MIX)
    rs_drain(refs, p)
    adafactor(refs, p)
    store.wait()


def fused(*args):
    T, D = args[0].shape
    Z, F = 4, 8
    sds = jax.ShapeDtypeStruct
    vm = pl.BlockSpec(memory_space=pltpu.VMEM)
    anyspec = pl.BlockSpec(memory_space=pl.ANY)
    V = pltpu.VMEM
    S = pltpu.SemaphoreType.DMA
    outs = (
        sds((T, D), BF16), sds((T, D), BF16),
        sds((128, 384), F32), sds((64, 256), F32), sds((128, 256), F32), sds((64, 512), F32),
        sds((128, 384), F32), sds((64, 256), F32), sds((128, 256), F32), sds((64, 512), F32),
        sds((8, LANES), F32), sds((16, LANES), F32), sds((8, LANES), F32),
    )
    row = V((1, LANES), F32)
    box = V((32, 1, LANES), F32)
    scratch = [
        V((Z, D, 3 * C), BF16), V((Z, D, C), BF16), V((F, D, C), BF16), V((F, D, C), BF16),
        V((1, D), F32), V((1, D), F32), V((Z, 1, C), F32), V((Z, 1, C), F32),
        box, row, V((1, D), F32), V((1, D), F32), V((Z, 1, C), F32), V((Z, 1, C), F32),
        V((T, D), BF16), V((T, D), BF16), V((D, T), BF16), V((D, T), BF16),
        V((T, D), BF16), V((D, T), BF16),
        V((D // LANES, T, LANES), F32), V((T, D), F32),
        V((8, T, LANES), F32), V((4, T, LANES), F32),
        V((T, 3 * C), BF16), V((Z, T, C), BF16), V((Z, T + SUB, C), F32),
        V((Z, T, C), F32), V((Z, T, C), F32), V((Z, T, C), F32), V((Z, T, C), F32),
        S((7,)), S(()), S(()), S((4, 3)), S((4, 4)),
        S((4, 4)), S((4, 4)), S((4, 4, 2)), S((4, 4, 2)), S((4, 4, 4)), S((4, 4, 4)),
        box, box, V((16, LANES), F32), V((8, 16, LANES), F32),
        V((8, LANES), F32), V((4, 8, LANES), F32), row, box, row, box,
        S((4, 4)), S((4, 4)), S((4, 4, 2)), S((4, 4, 2)), S((4, 4)), S((4, 4)),
        S((4, 4)), S((4, 4)), S(()), S(()),
        S((7,)), S((7,)), S((3,)), S((3,)), S(()), S(()), S(()), S(()), S(()),
    ]
    scratch += (
        [V((4, 4) + s, BF16) for s in SHAPES] * 2
        + [V((4, 2) + s, BF16) for s in SHAPES]
        + [V((4,) + s, BF16) for s in SHAPES] * 2
        + [V(s, F32) for s in SHAPES]
    )
    return pl.pallas_call(
        fused_kernel,
        out_shape=outs,
        in_specs=[anyspec, anyspec] + [vm] * (len(args) - 2),
        out_specs=(anyspec, anyspec) + (vm,) * (len(outs) - 2),
        scratch_shapes=scratch,
        compiler_params=pltpu.CompilerParams(
            vmem_limit_bytes=67043328, collective_id=0, has_side_effects=True
        ),
        name="fused",
    )(*args)


def gathered_layer(tok, cot, mix, ow, uw, dw, mg, fb, ib, fg):
    def whole(w):
        w = lax.all_gather(w, "inner", axis=1, tiled=True)
        return lax.all_gather(w, "grp", axis=0, tiled=True)

    def vec(v):
        return lax.all_gather(v, ("grp", "inner"), axis=0, tiled=True).astype(F32)

    width = tok.shape[1]
    inners = lax.axis_size("inner")
    Z, F = mix[0].shape[1] * inners // C, uw.shape[1] * inners // C
    gates = [whole(w).reshape(width, Z, C // LANES, 1, LANES) for w in mix]
    wmix = jnp.concatenate(gates, axis=3).reshape(width, Z, 3 * C).transpose(1, 0, 2)
    wot = whole(ow).reshape(Z, C, width).transpose(0, 2, 1)
    wup = whole(uw).reshape(width, F, C).transpose(1, 0, 2)
    wdt = whole(dw).reshape(F, C, width).transpose(0, 2, 1)
    return layer(
        tok, cot, wmix, wot, wup, wdt,
        vec(mg).reshape(1, width), vec(fg).reshape(1, width),
        vec(fb).reshape(Z, 1, C), vec(ib).reshape(Z, 1, C),
    )


def body(
    tokens,
    cotangent,
    mixer_gain,
    forget_weight,
    input_gate_weight,
    candidate_weight,
    forget_bias,
    input_bias,
    output_weight,
    feed_norm_gain,
    up_weight,
    down_weight,
    mixer_second,
    forget_rows,
    forget_columns,
    input_rows,
    input_columns,
    candidate_rows,
    candidate_columns,
    forget_second,
    input_second,
    output_rows,
    output_columns,
    feed_second,
    up_rows,
    up_columns,
    down_rows,
    down_columns,
):
    groups = lax.axis_size("grp")
    inners = lax.axis_size("inner")
    seqs, length, width = tokens.shape
    hidden = forget_weight.shape[1] * inners
    ff = up_weight.shape[1] * inners
    paired = (groups, inners) == (4, 8) and (length, width, hidden, ff) == (1024, 512, 1024, 2048)
    Z, F = hidden // C, ff // C
    if paired:
        block_output, tokens_grad, *packed = fused(
            tokens.reshape(length, width), cotangent.reshape(length, width),
            forget_weight, input_gate_weight, candidate_weight,
            output_weight.T, up_weight, down_weight.T,
            mixer_gain, forget_bias, input_bias, feed_norm_gain,
            mixer_second, forget_rows, forget_columns, input_rows, input_columns,
            candidate_rows, candidate_columns, forget_second, input_second,
            output_rows, output_columns, feed_second,
            up_rows, up_columns, down_rows, down_columns,
        )
        *done, block_output, tokens_grad = finish(packed, block_output, tokens_grad)
        for k in (6, 9, 16, 19):
            done[k] = done[k].T
        return (block_output.reshape(tokens.shape), tokens_grad.reshape(tokens.shape), *done)
    results = gathered_layer(
        tokens.reshape(length, width), cotangent.reshape(length, width),
        (forget_weight, input_gate_weight, candidate_weight),
        output_weight, up_weight, down_weight,
        mixer_gain, forget_bias, input_bias, feed_norm_gain,
    )
    block_output, tokens_grad, gmix, got, gup, gdt, fgg, mgg, fbg, ibg = results
    block_output = block_output.reshape(tokens.shape)
    tokens_grad = tokens_grad.reshape(tokens.shape)
    split = gmix.transpose(1, 0, 2).reshape(width, Z, C // LANES, 3, LANES)
    forget_term, input_term, cand_term = [
        split[:, :, :, k].reshape(width, hidden) for k in range(3)
    ]
    output_term = got.transpose(0, 2, 1).reshape(hidden, width)
    up_term = gup.transpose(1, 0, 2).reshape(width, ff)
    down_term = gdt.transpose(0, 2, 1).reshape(ff, width)
    gain_first_term, gain_second_term = mgg.reshape(-1), fgg.reshape(-1)
    fbias_term, ibias_term = fbg.reshape(-1), ibg.reshape(-1)
    part = (
        lax.psum_scatter(
            gain_first_term.reshape(groups, -1), "inner", scatter_dimension=1, tiled=True
        ),
        lax.psum_scatter(forget_term, "inner", scatter_dimension=1, tiled=True),
        lax.psum_scatter(input_term, "inner", scatter_dimension=1, tiled=True),
        lax.psum_scatter(cand_term, "inner", scatter_dimension=1, tiled=True),
        lax.psum_scatter(fbias_term.reshape(groups, -1), "inner", scatter_dimension=1, tiled=True),
        lax.psum_scatter(ibias_term.reshape(groups, -1), "inner", scatter_dimension=1, tiled=True),
        lax.psum_scatter(output_term, "inner", scatter_dimension=1, tiled=True),
        lax.psum_scatter(
            gain_second_term.reshape(groups, -1), "inner", scatter_dimension=1, tiled=True
        ),
        lax.psum_scatter(up_term, "inner", scatter_dimension=1, tiled=True),
        lax.psum_scatter(down_term, "inner", scatter_dimension=1, tiled=True),
    )
    mine = (
        lax.psum_scatter(part[0], "grp", scatter_dimension=0, tiled=True),
        lax.psum_scatter(part[1], "grp", scatter_dimension=0, tiled=True),
        lax.psum_scatter(part[2], "grp", scatter_dimension=0, tiled=True),
        lax.psum_scatter(part[3], "grp", scatter_dimension=0, tiled=True),
        lax.psum_scatter(part[4], "grp", scatter_dimension=0, tiled=True),
        lax.psum_scatter(part[5], "grp", scatter_dimension=0, tiled=True),
        lax.psum_scatter(part[6], "grp", scatter_dimension=0, tiled=True),
        lax.psum_scatter(part[7], "grp", scatter_dimension=0, tiled=True),
        lax.psum_scatter(part[8], "grp", scatter_dimension=0, tiled=True),
        lax.psum_scatter(part[9], "grp", scatter_dimension=0, tiled=True),
    )
    params = [
        mixer_gain,
        forget_weight,
        input_gate_weight,
        candidate_weight,
        forget_bias,
        input_bias,
        output_weight,
        feed_norm_gain,
        up_weight,
        down_weight,
    ]
    locals_f = [p.astype(jnp.float32) for p in params]
    grads = [
        mine[0].reshape(-1),
        mine[1],
        mine[2],
        mine[3],
        mine[4].reshape(-1),
        mine[5].reshape(-1),
        mine[6],
        mine[7].reshape(-1),
        mine[8],
        mine[9],
    ]
    matrix_slots = [1, 2, 3, 6, 8, 9]
    vector_slots = [0, 4, 5, 7]
    rows_old = [forget_rows, input_rows, candidate_rows, output_rows, up_rows, down_rows]
    columns_old = [
        forget_columns,
        input_columns,
        candidate_columns,
        output_columns,
        up_columns,
        down_columns,
    ]
    seconds_old = [mixer_second, forget_second, input_second, feed_second]
    counts = [params[k].size * groups * inners for k in range(10)]
    first_inner = (lax.axis_index("inner") == 0).astype(jnp.float32)
    scales = lax.psum(
        jnp.stack(
            [jnp.sum(w * w) for w in locals_f] + [jnp.sum(r) * first_inner for r in rows_old]
        ),
        ("grp", "inner"),
    )
    mats = [grads[k] for k in matrix_slots]
    row_parts = [jnp.sum(g * g, axis=1) for g in mats]
    column_parts = [jnp.sum(g * g, axis=0) for g in mats]
    row_totals = lax.psum(
        (row_parts[0], row_parts[1], row_parts[2], row_parts[3], row_parts[4], row_parts[5]),
        "inner",
    )
    column_totals = lax.psum(
        (
            column_parts[0],
            column_parts[1],
            column_parts[2],
            column_parts[3],
            column_parts[4],
            column_parts[5],
        ),
        "grp",
    )
    grand = lax.psum(jnp.stack([jnp.sum(v) for v in row_totals]), "grp")
    scaled_all = [None] * 10
    new_states = [None] * 16
    state_places = {1: (1, 2), 2: (3, 4), 3: (5, 6), 6: (9, 10), 8: (12, 13), 9: (14, 15)}
    second_places = {0: 0, 4: 7, 5: 8, 7: 11}
    for k in range(6):
        slot = matrix_slots[k]
        grad = mats[k]
        full_rows = grad.shape[0] * groups
        full_columns = grad.shape[1] * inners
        rows = 0.5 * rows_old[k] + 0.5 * (row_totals[k] / full_columns + TINY)
        columns = 0.5 * columns_old[k] + 0.5 * (column_totals[k] / full_rows + TINY)
        row_mean = 0.5 * scales[10 + k] / full_rows + 0.5 * (
            grand[k] / (full_rows * full_columns) + TINY
        )
        scaled_all[slot] = grad * lax.rsqrt(rows[:, None] * columns[None, :] / row_mean)
        new_states[state_places[slot][0]] = rows
        new_states[state_places[slot][1]] = columns
    for k in range(4):
        slot = vector_slots[k]
        grad = grads[slot]
        second = 0.5 * seconds_old[k] + 0.5 * (grad * grad + TINY)
        scaled_all[slot] = grad * lax.rsqrt(second)
        new_states[second_places[slot]] = second
    clip = lax.psum(jnp.stack([jnp.sum(s * s) for s in scaled_all]), ("grp", "inner"))
    count_array = jnp.array(counts, jnp.float32)
    update_norms = jnp.sqrt(clip / count_array)
    fresh = [
        locals_f[k]
        + -jnp.sqrt(scales[k] / counts[k]) * scaled_all[k] / jnp.maximum(CLIP, update_norms[k])
        for k in range(10)
    ]
    return (
        block_output,
        tokens_grad,
        grads[0],
        grads[1],
        grads[2],
        grads[3],
        grads[4],
        grads[5],
        grads[6],
        grads[7],
        grads[8],
        grads[9],
        fresh[0],
        fresh[1],
        fresh[2],
        fresh[3],
        fresh[4],
        fresh[5],
        fresh[6],
        fresh[7],
        fresh[8],
        fresh[9],
        new_states[0],
        new_states[1],
        new_states[2],
        new_states[3],
        new_states[4],
        new_states[5],
        new_states[6],
        new_states[7],
        new_states[8],
        new_states[9],
        new_states[10],
        new_states[11],
        new_states[12],
        new_states[13],
        new_states[14],
        new_states[15],
        update_norms,
    )


def solution(mesh):
    return jax.shard_map(
        body,
        mesh=mesh,
        in_specs=(
            P(("grp", "inner"), None, None),
            P(("grp", "inner"), None, None),
            P(("grp", "inner")),
            P("grp", "inner"),
            P("grp", "inner"),
            P("grp", "inner"),
            P(("grp", "inner")),
            P(("grp", "inner")),
            P("grp", "inner"),
            P(("grp", "inner")),
            P("grp", "inner"),
            P("grp", "inner"),
            P(("grp", "inner")),
            P("grp"),
            P("inner"),
            P("grp"),
            P("inner"),
            P("grp"),
            P("inner"),
            P(("grp", "inner")),
            P(("grp", "inner")),
            P("grp"),
            P("inner"),
            P(("grp", "inner")),
            P("grp"),
            P("inner"),
            P("grp"),
            P("inner"),
        ),
        out_specs=(
            P(("grp", "inner"), None, None),
            P(("grp", "inner"), None, None),
            P(("grp", "inner")),
            P("grp", "inner"),
            P("grp", "inner"),
            P("grp", "inner"),
            P(("grp", "inner")),
            P(("grp", "inner")),
            P("grp", "inner"),
            P(("grp", "inner")),
            P("grp", "inner"),
            P("grp", "inner"),
            P(("grp", "inner")),
            P("grp", "inner"),
            P("grp", "inner"),
            P("grp", "inner"),
            P(("grp", "inner")),
            P(("grp", "inner")),
            P("grp", "inner"),
            P(("grp", "inner")),
            P("grp", "inner"),
            P("grp", "inner"),
            P(("grp", "inner")),
            P("grp"),
            P("inner"),
            P("grp"),
            P("inner"),
            P("grp"),
            P("inner"),
            P(("grp", "inner")),
            P(("grp", "inner")),
            P("grp"),
            P("inner"),
            P(("grp", "inner")),
            P("grp"),
            P("inner"),
            P("grp"),
            P("inner"),
            P(),
        ),
        check_vma=False,
    )
```

```python
import functools
import math
import jax
import jax.numpy as jnp
from jax import lax
from jax.experimental import pallas as pl
from jax.sharding import PartitionSpec as P
from jax.experimental.pallas import tpu as pltpu

EPS = 1e-06
F32 = jnp.float32
BF16 = jnp.bfloat16
C = 256
LANES = 128
SUB = 8
ERFC = (
    0.2256758669, 0.2256693636, 0.2078460312, 0.1685204197, 0.1415057621,
    -0.005753053848, 0.1692475449, -0.182997133, 0.05028532412,
)


def dot(a, b):
    return jnp.dot(a, b, preferred_element_type=F32)


def dot_t(a, b):
    return lax.dot_general(a, b, (((1,), (1,)), ((), ())), preferred_element_type=F32)


def loop(steps, body):
    def run(i, carry):
        body(i)
        return carry

    lax.fori_loop(0, steps, run, 0)


def at(i, size):
    return pl.ds(pl.multiple_of(i * size, size), size)


def gelu_parts(x):
    e = jnp.exp2((x * x) * (-0.5 / math.log(2.0)))
    t = 1.0 / (1.0 + (0.4 * math.sqrt(0.5)) * jnp.abs(x))
    poly = jnp.full_like(t, 0.5 * ERFC[-1])
    for c in ERFC[-2::-1]:
        poly = poly * t + 0.5 * c
    half = poly * (t * e)
    cdf = jnp.where(x >= 0, 1.0 - half, half)
    return x * cdf, cdf + (x * e) * (1.0 / math.sqrt(2.0 * math.pi))


def reorder(inverse):
    row = lax.broadcasted_iota(jnp.int32, (LANES, LANES), 0)
    col = lax.broadcasted_iota(jnp.int32, (LANES, LANES), 1)
    step = LANES // SUB
    source = (row % step) * SUB + row // step if inverse else (row % SUB) * step + row // SUB
    return jnp.where(col == source, 1.0, 0.0).astype(BF16)


def tile_rows(i, s, T):
    step = LANES // SUB
    return pl.ds(pl.multiple_of(i * step + s * (T // SUB), step), step)


def gather_rows(ref, i, order, T):
    return dot(order, jnp.concatenate([ref[tile_rows(i, s, T), :] for s in range(SUB)], axis=0))


def scatter_rows(ref, i, order, out, T):
    step = LANES // SUB
    flat = dot(order, out.astype(BF16)).astype(BF16)
    for s in range(SUB):
        ref[tile_rows(i, s, T), :] = flat[s * step : (s + 1) * step]


LOG2E = 1.0 / math.log(2.0)


def load_planes(ref, rows, start=0, count=None):
    count = ref.shape[0] if count is None else count
    return jnp.concatenate([ref[q, rows, :] for q in range(start, start + count)], axis=1)


def store_planes(ref, rows, value, start=0):
    for q in range(value.shape[1] // LANES):
        ref[start + q, rows, :] = value[:, q * LANES : (q + 1) * LANES]


def add_planes(ref, rows, value):
    for q in range(value.shape[1] // LANES):
        ref[q, rows, :] += value[:, q * LANES : (q + 1) * LANES]


def clear(ref, T):
    for q in range(4):
        ref[q, 0:T, :] = jnp.zeros((T, LANES), F32)


def norm_in(refs, T):
    order = reorder(False)

    def place(i):
        x = gather_rows(refs.tok, i, order, T)
        y = x * lax.rsqrt(jnp.mean(x * x, axis=-1, keepdims=True) + EPS) * refs.g1[...]
        rows = at(i, LANES)
        refs.tok_p[rows, :] = x.astype(BF16)
        refs.min[rows, :] = y.astype(BF16)
        refs.min_t[:, rows] = y.T.astype(BF16)

    loop(T // LANES, place)


def cot_in(refs, T):
    order = reorder(False)

    def place(i):
        x = gather_rows(refs.cot, i, order, T)
        rows = at(i, LANES)
        refs.cot_p[rows, :] = x.astype(BF16)
        refs.cot_t[:, rows] = x.T.astype(BF16)

    loop(T // LANES, place)


def mixer_forward(refs, z, T, hook=None):
    pre, ac, st = refs.pre, refs.buf, refs.st
    halves = C // LANES
    width = 3 * LANES

    def project(i):
        rows = at(i, 256)
        out = dot(refs.min[rows, :], refs.wmix[z])
        for q in range(3 * halves):
            pre[q, rows, :] = out[:, q * LANES : (q + 1) * LANES]

    loop(T // 256, project)
    fb = refs.fb[z]
    ib = refs.ib[z]

    def gates(i, carry):
        r0 = pl.multiple_of(i * 64, 64)
        out = []
        for h in range(halves):
            a, b = carry[h]
            lanes = slice(h * LANES, (h + 1) * LANES)
            pf = pre[3 * h, pl.ds(r0, 64), :] + fb[:, lanes]
            pi = pre[3 * h + 1, pl.ds(r0, 64), :] + ib[:, lanes]
            pc = pre[3 * h + 2, pl.ds(r0, 64), :]
            pf, pi = pf * LOG2E, pi * LOG2E
            m = jnp.minimum(jnp.minimum(pf, pi), 0.0)
            e0 = jnp.exp2(m)
            ef = jnp.exp2(m - pf)
            ei = jnp.exp2(m - pi)
            nk = e0 + ei
            na = e0 + ef
            both = nk + na
            floor = jnp.maximum(na, 1e-37)
            rec = 1.0 / (both * floor)
            inv = rec * floor
            keep = nk * inv
            admit = na * inv
            ec = jnp.exp(jnp.minimum(pc, 0.0))
            sg = ec / (1.0 + ec)
            positive = pc >= 0
            value = jnp.where(positive, pc + 0.5, sg)
            slope = jnp.where(positive, 1.0, sg * (1.0 - sg))
            refs.keep[z, pl.ds(r0, 64), lanes] = keep
            refs.k_f[z, pl.ds(r0, 64), lanes] = keep * (ef * (rec * both))
            refs.k_i[z, pl.ds(r0, 64), lanes] = ei * inv
            refs.k_c[z, pl.ds(r0, 64), lanes] = admit * slope
            inflow = admit * value
            alist, blist = [], []
            for j in range(8):
                kj = keep[j * SUB : (j + 1) * SUB]
                b = kj * b + inflow[j * SUB : (j + 1) * SUB]
                a = kj * a
                alist.append(a)
                blist.append(b)
            ac[h, pl.ds(r0, 64), :] = jnp.concatenate(alist, axis=0)
            st[z, pl.ds(r0 + SUB, 64), lanes] = jnp.concatenate(blist, axis=0)
            out.append((a, b))
        return tuple(out)

    one = jnp.ones((SUB, LANES), F32)
    zero = jnp.zeros((SUB, LANES), F32)
    if hook is not None:
        hook(1)
    ends = lax.fori_loop(0, T // 64, gates, tuple((one, zero) for _ in range(halves)))
    if hook is not None:
        hook(2)
    for h in range(halves):
        a, b = ends[h]
        rows = [jnp.zeros((1, LANES), F32)]
        for s in range(SUB - 1):
            rows.append(a[s : s + 1] * rows[-1] + b[s : s + 1])
        st[z, 0:SUB, h * LANES : (h + 1) * LANES] = jnp.concatenate(rows, axis=0)
    first = st[z, 0:SUB, :]

    def finish(i):
        r0 = pl.multiple_of(i * 64, 64)
        a = load_planes(ac, pl.ds(r0, 64), 0, 2).reshape(8, SUB, C)
        b = st[z, pl.ds(r0 + SUB, 64), :].reshape(8, SUB, C)
        s = (b + a * first[None]).reshape(64, C)
        st[z, pl.ds(r0 + SUB, 64), :] = s
        refs.slow[z, pl.ds(r0, 64), :] = s.astype(BF16)

    loop(T // 64, finish)


def mix_out(refs, T):
    Z = refs.wot.shape[0]

    def body(i):
        rows = at(i, 256)
        acc = refs.tok_p[rows, :].astype(F32)
        for z in range(Z):
            acc = acc + dot_t(refs.slow[z, rows, :], refs.wot[z])
        store_planes(refs.resid, rows, acc)
        for k in range(2):
            x = acc[k * LANES : (k + 1) * LANES]
            y = x * lax.rsqrt(jnp.mean(x * x, axis=-1, keepdims=True) + EPS) * refs.g2[...]
            sub = pl.ds(pl.multiple_of(i * 256 + k * LANES, LANES), LANES)
            refs.fin[sub, :] = y.astype(BF16)
            refs.fin_t[:, sub] = y.T.astype(BF16)

    loop(T // 256, body)


def feed(refs, f, T):
    wup, wdt = refs.wup, refs.wdt
    size = 256
    tiles = T // size

    up, back = {}, {}

    def project(i):
        rows = slice(i * size, (i + 1) * size)
        up[i] = dot(refs.fin[rows, :], wup[f])
        back[i] = dot(refs.cot_p[rows, :], wdt[f])

    def activate(i):
        for k in range(size // 32):
            part = slice(k * 32, (k + 1) * 32)
            rows = slice(i * size + k * 32, i * size + (k + 1) * 32)
            act, slope = gelu_parts(up[i][part])
            refs.dpre[rows, 0:C] = act.astype(BF16)
            refs.dpre[rows, C : 2 * C] = (back[i][part] * slope).astype(BF16)

    def add(i):
        rows = slice(i * size, (i + 1) * size)
        add_planes(refs.oacc, rows, dot_t(refs.dpre[rows, 0:C], wdt[f]))
        refs.dfe[rows, :] += dot_t(refs.dpre[rows, C : 2 * C], wup[f])

    for i in range(tiles + 2):
        if i < tiles:
            project(i)
        if 1 <= i < tiles + 1:
            activate(i - 1)
        if i >= 2:
            add(i - 2)


def feed_back(refs, T):
    order = reorder(True)
    D = refs.g1.shape[1]

    def body(i, total):
        rows = at(i, LANES)
        x = load_planes(refs.resid, rows)
        df = refs.dfe[rows, :]
        out = x + load_planes(refs.oacc, rows, 0, D // LANES)
        scatter_rows(refs.block, i, order, out, T)
        r = lax.rsqrt(jnp.mean(x * x, axis=-1, keepdims=True) + EPS)
        nrm = x * r
        dn = df * refs.g2[...]
        mean = jnp.mean(dn * nrm, axis=-1, keepdims=True)
        dres = refs.cot_p[rows, :].astype(F32) + r * (dn - nrm * mean)
        refs.dfe[rows, :] = dres
        refs.fin[rows, :] = dres.astype(BF16)
        refs.fin_t[:, rows] = dres.T.astype(BF16)
        return total + (df * nrm).reshape(16, SUB, D).sum(axis=0)

    total = lax.fori_loop(0, T // LANES, body, jnp.zeros((SUB, D), F32))
    refs.fgg[...] = jnp.sum(total, axis=0, keepdims=True)


def mixer_back(refs, z, T, hook=None):
    buf, st = refs.buf, refs.st
    halves = C // LANES
    width = 3 * LANES

    def project(i):
        rows = at(i, 256)
        store_planes(buf, rows, dot(refs.fin[rows, :], refs.wot[z]))

    loop(T // 256, project)
    steps = T // 64

    def local(i, carry):
        r0 = pl.multiple_of((steps - 1 - i) * 64, 64)
        d = load_planes(buf, pl.ds(r0, 64), 0, 2)
        k = refs.keep[z, pl.ds(r0, 64), :]
        e, dk = carry
        plist, dlist = [None] * 8, [None] * 8
        for j in range(7, -1, -1):
            kj = k[j * SUB : (j + 1) * SUB]
            p = d[j * SUB : (j + 1) * SUB] + e
            plist[j] = p
            dlist[j] = dk
            e = kj * p
            dk = kj * dk
        store_planes(buf, pl.ds(r0, 64), jnp.concatenate(plist, axis=0))
        store_planes(buf, pl.ds(r0, 64), jnp.concatenate(dlist, axis=0), 2)
        return e, dk

    e, dk = lax.fori_loop(0, steps, local, (jnp.zeros((SUB, C), F32), jnp.ones((SUB, C), F32)))
    rows = [jnp.zeros((1, C), F32)]
    for s in range(SUB - 1, 0, -1):
        rows.insert(0, e[s : s + 1] + dk[s : s + 1] * rows[0])
    tail = jnp.concatenate(rows, axis=0)
    if hook is not None:
        hook()

    def grads(i, sums):
        r0 = pl.multiple_of(i * 64, 64)
        out = []
        for h in range(halves):
            lanes = slice(h * LANES, (h + 1) * LANES)
            sub = pl.ds(r0, 64)
            p0 = buf[h, sub, :].reshape(8, SUB, LANES)
            d0 = buf[2 + h, sub, :].reshape(8, SUB, LANES)
            p = (p0 + d0 * tail[None, :, lanes]).reshape(64, LANES)
            x = p * (st[z, pl.ds(r0 + SUB, 64), lanes] - st[z, sub, lanes])
            df = -(refs.k_f[z, sub, lanes] * x)
            di = refs.k_i[z, sub, lanes] * x
            dcand = refs.k_c[z, sub, lanes] * p
            df16 = df.astype(BF16)
            di16 = di.astype(BF16)
            refs.dpre[sub, h * width : h * width + LANES] = df16
            refs.dpre[sub, h * width + LANES : h * width + 2 * LANES] = di16
            refs.dpre[sub, h * width + 2 * LANES : h * width + 3 * LANES] = dcand.astype(BF16)
            sf, si = sums[h]
            out.append(
                (
                    sf + df16.astype(F32).reshape(8, SUB, LANES).sum(axis=0),
                    si + di16.astype(F32).reshape(8, SUB, LANES).sum(axis=0),
                )
            )
        return tuple(out)

    zero = jnp.zeros((SUB, LANES), F32)
    sums = lax.fori_loop(0, T // 64, grads, tuple((zero, zero) for _ in range(halves)))
    for h in range(halves):
        lanes = slice(h * LANES, (h + 1) * LANES)
        refs.fbg[z, :, lanes] = jnp.sum(sums[h][0], axis=0, keepdims=True)
        refs.ibg[z, :, lanes] = jnp.sum(sums[h][1], axis=0, keepdims=True)


def mixer_input_back(refs, z, T):
    def back(i):
        rows = at(i, 256)
        add_planes(refs.oacc, rows, dot_t(refs.dpre[rows, :], refs.wmix[z]))

    loop(T // 256, back)


def norm_back(refs, T):
    order = reorder(True)
    D = refs.g1.shape[1]

    def body(i, total):
        rows = at(i, LANES)
        x = refs.tok_p[rows, :].astype(F32)
        d_in = load_planes(refs.oacc, rows, 0, D // LANES)
        r = lax.rsqrt(jnp.mean(x * x, axis=-1, keepdims=True) + EPS)
        nrm = x * r
        dn = d_in * refs.g1[...]
        mean = jnp.mean(dn * nrm, axis=-1, keepdims=True)
        out = refs.dfe[rows, :] + r * (dn - nrm * mean)
        scatter_rows(refs.tgrad, i, order, out, T)
        return total + (d_in * nrm).reshape(16, SUB, D).sum(axis=0)

    total = lax.fori_loop(0, T // LANES, body, jnp.zeros((SUB, D), F32))
    refs.mgg[...] = jnp.sum(total, axis=0, keepdims=True)


class Refs:
    def __init__(self, args):
        (
            self.tok, self.cot, self.wmix, self.wot, self.wup, self.wdt, self.g1, self.g2, self.fb, self.ib,
            self.block, self.tgrad, self.gmix, self.got, self.gup, self.gdt, self.fgg, self.mgg, self.fbg, self.ibg,
            self.tok_p, self.min, self.min_t, self.fin, self.fin_t, self.cot_p, self.cot_t, self.resid, self.oacc, self.dfe,
            self.pre, self.buf, self.dpre, self.slow, self.st, self.keep, self.k_f,
            self.k_i, self.k_c, self.gst, self.gsem,
        ) = args


def layer_kernel(*args):
    refs = Refs(args)
    T, D = refs.tok.shape
    Z = refs.wmix.shape[0]
    F = refs.wup.shape[0]
    gst, sem = refs.gst, refs.gsem
    cot_in(refs, T)
    norm_in(refs, T)
    loop(Z, lambda z: mixer_forward(refs, z, T))
    mix_out(refs, T)
    clear(refs.oacc, T)
    refs.dfe[...] = jnp.zeros_like(refs.dfe)

    def feed_step(f):
        feed(refs, f, T)
        gst[0, :, 0:C] = dot(refs.cot_t[...], refs.dpre[:, 0:C])
        gst[1, :, 0:C] = dot(refs.fin_t[...], refs.dpre[:, C : 2 * C])
        one = pltpu.make_async_copy(gst.at[0, :, 0:C], refs.gdt.at[f], sem.at[0])
        two = pltpu.make_async_copy(gst.at[1, :, 0:C], refs.gup.at[f], sem.at[1])
        one.start()
        two.start()
        one.wait()
        two.wait()

    loop(F, feed_step)
    feed_back(refs, T)
    clear(refs.oacc, T)

    def mixer_step(z):
        gst[0, :, 0:C] = dot(refs.fin_t[...], refs.slow[z])
        mixer_back(refs, z, T)
        mixer_input_back(refs, z, T)
        gst[1, :, :] = dot(refs.min_t[...], refs.dpre[...])
        one = pltpu.make_async_copy(gst.at[0, :, 0:C], refs.got.at[z], sem.at[0])
        two = pltpu.make_async_copy(gst.at[1], refs.gmix.at[z], sem.at[1])
        one.start()
        two.start()
        one.wait()
        two.wait()

    loop(Z, mixer_step)
    norm_back(refs, T)


def layer(tok, cot, wmix, wot, wup, wdt, g1, g2, fb, ib):
    T, D = tok.shape
    Z, F = wmix.shape[0], wup.shape[0]
    sds = jax.ShapeDtypeStruct
    vm = pl.BlockSpec(memory_space=pltpu.VMEM)
    anyspec = pl.BlockSpec(memory_space=pl.ANY)
    out_shape = (
        sds((T, D), BF16), sds((T, D), BF16),
        sds((Z, D, 3 * C), F32), sds((Z, D, C), F32), sds((F, D, C), F32), sds((F, D, C), F32),
        sds((1, D), F32), sds((1, D), F32), sds((Z, 1, C), F32), sds((Z, 1, C), F32),
    )
    V = pltpu.VMEM
    scratch = [
        V((T, D), BF16), V((T, D), BF16), V((D, T), BF16), V((T, D), BF16), V((D, T), BF16),
        V((T, D), BF16), V((D, T), BF16), V((D // LANES, T, LANES), F32),
        V((D // LANES, T, LANES), F32), V((T, D), F32), V((3 * C // LANES, T, LANES), F32), V((4, T, LANES), F32),
        V((T, 3 * C), BF16), V((Z, T, C), BF16), V((Z, T + SUB, C), F32),
        V((Z, T, C), F32), V((Z, T, C), F32), V((Z, T, C), F32), V((Z, T, C), F32),
        V((2, D, 3 * C), F32), pltpu.SemaphoreType.DMA((2,)),
    ]
    return pl.pallas_call(
        layer_kernel,
        out_shape=out_shape,
        in_specs=[vm] * 10,
        out_specs=(vm, vm, anyspec, anyspec, anyspec, anyspec, vm, vm, vm, vm),
        scratch_shapes=scratch,
        compiler_params=pltpu.CompilerParams(vmem_limit_bytes=67043328),
        name="layer",
    )(tok, cot, wmix, wot, wup, wdt, g1, g2, fb, ib)


MESH = pl.DeviceIdType.MESH


def rcopy(src, dst, send, recv, device):
    return pltpu.make_async_remote_copy(
        src_ref=src, dst_ref=dst, send_sem=send, recv_sem=recv, device_id=device, device_id_type=MESH
    )


class Place:
    def __init__(self):
        self.g = lax.axis_index("grp")
        self.i = lax.axis_index("inner")
        self.y, self.x = self.g // 2, self.g % 2
        self.z, self.c = self.i // 2, self.i % 2
        self.me = self.g * 8 + self.i
        self.partner = (self.g, self.z * 2 + 1 - self.c)

    def flip(self, fx, fy):
        x = (self.x + fx) % 2
        y = (self.y + fy) % 2
        return y * 2 + x

    def turn(self, z):
        return (z + self.c) % 2

    def near(self, z):
        e = self.turn(z)
        return self.flip(1 - e, e)

    def far(self, z):
        e = self.turn(z)
        return self.flip(e, 1 - e)

    def other(self, k):
        t = (self.me + k) % 32
        return (t // 8, t % 8)


def entry_signal(place):
    barrier = pltpu.get_barrier_semaphore()

    def greet(k):
        pl.semaphore_signal(barrier, inc=1, device_id=place.other(k + 1), device_id_type=MESH)

    for k in range(31):
        greet(k)


def entry_wait():
    pl.semaphore_wait(pltpu.get_barrier_semaphore(), 31)


def spread(values, start, count, total):
    lane = lax.broadcasted_iota(jnp.int32, (LANES, total), 1)
    row = lax.broadcasted_iota(jnp.int32, (LANES, total), 0)
    sel = jnp.where(row == start + lane % count, 1.0, 0.0).astype(BF16)
    picked = dot(values, sel)
    owner = lax.broadcasted_iota(jnp.int32, picked.shape, 0)
    spot = lax.broadcasted_iota(jnp.int32, picked.shape, 1)
    return jnp.sum(jnp.where(spot // count == owner, picked, 0.0), axis=0, keepdims=True)


def pack_vectors(mg, fb, ib, fg):
    parts = [mg, fb, ib, fg]
    used = sum(p.shape[0] for p in parts)
    rows = [p[...].astype(F32).reshape(1, p.shape[0]) for p in parts]
    return jnp.concatenate(rows + [jnp.zeros((1, LANES - used), F32)], axis=1)


FIRST = (3, 0)
LATER = (1, 2)


def block_of(refs, a, g, i):
    if a == 0:
        return refs.wot.at[g, at(i, 64), :]
    if a == 1:
        return refs.wup.at[i, at(g, 128), :]
    if a == 2:
        return refs.wdt.at[pl.ds(2 * g, 2), at(i, 64), :]
    return refs.wmix.at[i // 2, at(g, 128), at(i % 2, 384)]


def blocks_of(refs, a, i):
    if a == 0:
        return refs.wot.at[:, at(i, 64), :]
    if a == 1:
        return refs.wup.at[i]
    if a == 2:
        return refs.wdt.at[:, at(i, 64), :]
    return refs.wmix.at[i // 2, :, at(i % 2, 384)]


def line_send(refs, p, a):
    blk = block_of(refs, a, p.g, p.i)
    for s in range(1, 4):
        peer = (p.g, slot_chunk(p, s) * 2 + p.c)
        rcopy(blk, blk, refs.gz_s.at[a, s - 1], refs.gz_r.at[a, p.z], peer).start()


def near_of(p, a, z):
    return p.near(z + (a in LATER))


def far_of(p, a, z):
    return p.far(z + (a in LATER))


def line_wait(refs, p, a, z):
    @pl.when(z != p.z)
    def _():
        blk = block_of(refs, a, p.g, z * 2 + p.c)
        rcopy(blk, blk, refs.gp_s.at[a, z, 0], refs.gz_r.at[a, z], p.partner).wait_recv()


def near_send(refs, p, a, z):
    blk = block_of(refs, a, p.g, z * 2 + p.c)
    near, far = (near_of(p, a, z), p.i), (far_of(p, a, z), p.i)
    rcopy(blk, blk, refs.gn_s.at[a, z], refs.gn_r.at[a, z], near).start()
    rcopy(blk, blk, refs.gf_s.at[a, z, 0], refs.gf_r.at[a, z, 0], far).start()


def far_send(refs, p, a, z):
    near = block_of(refs, a, near_of(p, a, z), z * 2 + p.c)
    far = (far_of(p, a, z), p.i)
    rcopy(near, near, refs.gn_s.at[a, z], refs.gn_r.at[a, z], p.partner).wait_recv()
    rcopy(near, near, refs.gf_s.at[a, z, 1], refs.gf_r.at[a, z, 1], far).start()


def far_wait(refs, p, a, z, k):
    blk = block_of(refs, a, p.g, z * 2 + p.c)
    rcopy(blk, blk, refs.gf_s.at[a, z, k], refs.gf_r.at[a, z, k], p.partner).wait_recv()


def pair_copy(refs, p, a, z, c):
    full = blocks_of(refs, a, z * 2 + c)
    return rcopy(full, full, refs.gp_s.at[a, z, 0], refs.gp_r.at[a, z, 0], p.partner)


def first_step(refs, p, arrays, kind, s):
    for a in arrays:
        z = slot_chunk(p, s)
        if kind == "n":
            line_wait(refs, p, a, z)
            near_send(refs, p, a, z)
        elif kind == "f":
            far_send(refs, p, a, z)
        elif kind == "p":
            far_wait(refs, p, a, z, 0)
            far_wait(refs, p, a, z, 1)
            pair_copy(refs, p, a, z, p.c).start()
        else:
            pair_copy(refs, p, a, z, 1 - p.c).wait_recv()


def up_step(refs, p, kind, m):
    if kind == "n":

        @pl.when(p.z != m)
        def _():
            line_wait(refs, p, 1, m)
            near_send(refs, p, 1, m)
    elif kind == "f":
        far_send(refs, p, 1, m)
    elif kind == "p":
        far_wait(refs, p, 1, m, 0)
        far_wait(refs, p, 1, m, 1)
        pair_copy(refs, p, 1, m, p.c).start()
    else:
        pair_copy(refs, p, 1, m, 1 - p.c).wait_recv()


def up_own(refs, p, phase):
    inner = (p.z + 1) // 2 % 2

    @pl.when(inner == phase)
    def _():
        near_send(refs, p, 1, p.z)


def down_pair(refs, p, z, phase, k, c):
    g = (1 + k) if phase else 3 * k
    blk = block_of(refs, 2, g, z * 2 + c)
    return rcopy(blk, blk, refs.gp_s.at[2, z, phase * 2 + k], refs.gp_r.at[2, z, phase * 2 + k], p.partner)


def down_step(refs, p, kind, phase, s):
    z = slot_chunk(p, s)
    active = (p.x + p.y) % 2 == phase
    idle = (p.x + p.y) % 2 != phase
    if kind == "n":

        @pl.when(active)
        def _():
            line_wait(refs, p, 2, z)
            near_send(refs, p, 2, z)
    elif kind == "f":

        @pl.when(idle)
        def _():
            far_send(refs, p, 2, z)
    elif kind == "p":

        @pl.when(active)
        def _():
            far_wait(refs, p, 2, z, 1)

        @pl.when(idle)
        def _():
            far_wait(refs, p, 2, z, 0)

        for k in range(2):
            down_pair(refs, p, z, phase, k, p.c).start()
    else:
        down_pair(refs, p, z, phase, 0 if kind == "d" else 1, 1 - p.c).wait_recv()


def gather_drain(refs, p):
    for a in range(4):
        blk = block_of(refs, a, p.g, p.i)
        for k in range(3):
            rcopy(blk, blk, refs.gz_s.at[a, k], refs.gz_r.at[a, p.z], p.partner).wait_send()
        for z in range(4):
            blk = block_of(refs, a, p.g, z * 2 + p.c)
            rcopy(blk, blk, refs.gn_s.at[a, z], refs.gn_r.at[a, z], p.partner).wait_send()
            for k in range(2):
                rcopy(blk, blk, refs.gf_s.at[a, z, k], refs.gf_r.at[a, z, k], p.partner).wait_send()
            if a == 2:
                for k in range(4):
                    down_pair(refs, p, z, k // 2, k % 2, p.c).wait_send()
            else:
                pair_copy(refs, p, a, z, p.c).wait_send()


def gather_hook(refs, p, actions):
    for action in actions.split():
        kind, number = action[1], int(action[-1])
        if action[0] == "M":
            first_step(refs, p, (3,), kind, number)
        elif action[0] == "W":
            first_step(refs, p, (0,), kind, number)
        elif action[0] == "U":
            up_step(refs, p, kind, number)
        else:
            down_step(refs, p, kind, int(action[2]), number)


def gather_start(refs, p):
    local = []
    for k, w in enumerate((refs.fw, refs.iw, refs.cw)):
        spot = pl.ds(pl.multiple_of(p.c * 384 + k * 128, 128), 128)
        local.append(
            pltpu.make_async_copy(w, refs.wmix.at[p.z, at(p.g, 128), spot], refs.loc_s.at[k])
        )
    local.append(pltpu.make_async_copy(refs.ow, block_of(refs, 0, p.g, p.i), refs.loc_s.at[3]))
    local.append(pltpu.make_async_copy(refs.uw, block_of(refs, 1, p.g, p.i), refs.loc_s.at[4]))
    for k in range(2):
        local.append(
            pltpu.make_async_copy(
                refs.dw.at[:, k * 256 : (k + 1) * 256],
                refs.wdt.at[2 * p.g + k, at(p.i, 64), :],
                refs.loc_s.at[5 + k],
            )
        )
    for c in local:
        c.start()
    row = pack_vectors(refs.mg, refs.fbv, refs.ibv, refs.fg)
    refs.vstage[...] = row
    refs.vecs[p.me] = row
    for c in local:
        c.wait()
    entry_wait()

    def vector(k):
        rcopy(refs.vstage, refs.vecs.at[p.me], refs.vec_s, refs.vec_r, p.other(k + 1)).start()

    for a in FIRST:
        near_send(refs, p, a, p.z)
    up_own(refs, p, 0)
    down_step(refs, p, "n", 0, 0)
    for k in range(31):
        vector(k)
    for a in FIRST:
        line_send(refs, p, a)
    inner = (p.z + 1) // 2 % 2

    @pl.when(inner == 0)
    def _():
        line_send(refs, p, 1)

    line_send(refs, p, 2)

    @pl.when(inner == 1)
    def _():
        line_send(refs, p, 1)


def gather_vectors(refs, p):
    rows = refs.vecs.at[pl.ds(0, 31)]
    rcopy(rows, rows, refs.vec_s, refs.vec_r, p.partner).wait()
    v = refs.vecs[...].reshape(32, LANES).astype(BF16)
    refs.g1[...] = spread(v, 0, 16, 512)
    refs.g2[...] = spread(v, 80, 16, 512)
    fb = spread(v, 16, 32, 1024)
    ib = spread(v, 48, 32, 1024)
    for z in range(4):
        refs.fb[z] = fb[:, z * C : (z + 1) * C]
        refs.ib[z] = ib[:, z * C : (z + 1) * C]


def slot_chunk(p, s):
    low = jnp.minimum(p.z, 3 - p.z)
    shift = jnp.where(s == 0, 1, jnp.where(s == 1, -1, 0))
    m = s + low * shift
    return jnp.where(p.z < 2, m, 3 - m)


SLOT_HOOKS = (
    ("", "Mn3", "Mp1 Mf2"),
    ("Md1", "Mf3 Wf0 Wn1 Wn2", "Mp2 Wn3 Wf1 Dn01"),
    ("Md2", "Mp3 Wf2 Wp0 Un0 Un3", "Wf3 Df00 Dn02 Dn03 Df01"),
    ("Md3", "Wp1 Wp2 Wp3 Uf0 Uf3 Df02 Df03", "Dp00 Dp01 Dp02 Dp03 Up0 Up3"),
)


def mixer_slots(refs, p, T):
    def hook(s, j):
        for k in range(4):

            @pl.when(s == k)
            def _():
                gather_hook(refs, p, SLOT_HOOKS[k][j])

    def slot(s):
        hook(s, 0)
        mixer_forward(refs, slot_chunk(p, s), T, lambda j: hook(s, j))

    loop(4, slot)


SHAPES = ((128, 256), (128, 256), (128, 384), (64, 256))
UP, DOWN, MIX, OUT = 0, 1, 2, 3
TINY = 1e-30
CLIP = 0.01
MATRICES = (
    (512, 1024), (512, 1024), (512, 1024), (1024, 512), (512, 2048), (2048, 512)
)
MATRIX_SLOTS = (1, 2, 3, 6, 8, 9)
VECTORS = ((0, 0, 16), (4, 16, 32), (5, 48, 32), (7, 80, 16))
COUNTS = (512, 524288, 524288, 524288, 1024, 1024, 524288, 512, 1048576, 1048576)


def spot(a, g, z):
    return (g, z) if a == DOWN else (z, g)


def rs_store(refs, a, g, z, value):
    refs.psend[a][(*spot(a, g, z),)] = value.astype(BF16)


def rs_role(p, g, z):
    e = p.turn(z)
    y, x = g // 2, g % 2
    return (1 - e) * ((x + p.x) % 2) + e * ((y + p.y) % 2)


def rs_pair(refs, p, a, u):
    if a == OUT:
        src, dst = refs.psend[a], refs.precv[a]
    else:
        src, dst = refs.psend[a].at[u], refs.precv[a].at[u]
    return rcopy(src, dst, refs.rp_s.at[a, u], refs.rp_r.at[a, u], p.partner)


def rs_merge(refs, p, a, g, z, own):
    place = spot(a, g, z)
    v = own + refs.precv[a][place].astype(F32)
    role = rs_role(p, g, z)

    @pl.when(role == 1)
    def _():
        refs.psend[a][place] = v.astype(BF16)

    @pl.when(role == 0)
    def _():
        refs.precv[a][place] = v.astype(BF16)


def rs_group(p, z, k, sent):
    e = p.turn(z)
    x = (1 - e) * ((p.x + sent) % 2) + e * k
    y = (1 - e) * k + e * ((p.y + sent) % 2)
    return y * 2 + x


def rs_first_copy(refs, p, a, z, k):
    g = rs_group(p, z, k, 1)
    return rcopy(
        refs.psend[a].at[spot(a, g, z)], refs.r1[a].at[z, k],
        refs.r1_s.at[a, z, k], refs.r1_r.at[a, z, k], (p.near(z), p.i),
    )


def rs_first_send(refs, p, a, z):
    for k in range(2):
        rs_first_copy(refs, p, a, z, k).start()


def rs_second(refs, p, a, z):
    e = p.turn(z)
    mine = (1 - e) * p.y + e * p.x
    for k in range(2):
        rs_first_copy(refs, p, a, z, k).wait_recv()
    for k in range(2):
        place = spot(a, rs_group(p, z, k, 0), z)
        v = (refs.precv[a][place].astype(F32) + refs.r1[a][z, k].astype(F32)).astype(BF16)

        @pl.when(mine == k)
        def _():
            refs.precv[a][place] = v

        @pl.when(mine != k)
        def _():
            refs.psend[a][place] = v


def rs_second_copy(refs, p, a, z):
    e = p.turn(z)
    other = 1 - ((1 - e) * p.y + e * p.x)
    place = spot(a, rs_group(p, z, other, 0), z)
    return rcopy(
        refs.psend[a].at[place], refs.r2[a].at[z], refs.r2_s.at[a, z], refs.r2_r.at[a, z],
        (p.far(z), p.i),
    )


def rs_third(refs, p, a, z):
    rs_second_copy(refs, p, a, z).wait_recv()
    place = spot(a, p.g, z)
    v = refs.precv[a][place].astype(F32) + refs.r2[a][z].astype(F32)

    @pl.when(z == p.z)
    def _():
        refs.fin_g[a][...] = v

    @pl.when(z != p.z)
    def _():
        refs.psend[a][place] = v.astype(BF16)


def rs_line(refs, p, a, z, owner):
    return rcopy(
        refs.psend[a].at[spot(a, p.g, z)], refs.r3[a].at[owner],
        refs.r3_s.at[a, z], refs.r3_r.at[a, owner], (p.g, z * 2 + p.c),
    )


def rs_third_send(refs, p, a, z):
    @pl.when(z != p.z)
    def _():
        rs_line(refs, p, a, z, p.z).start()


def rs_last(refs, p, a):
    for k in range(1, 4):
        z = (p.z + k) % 4
        rs_line(refs, p, a, z, z).wait_recv()
        refs.fin_g[a][...] += refs.r3[a][z].astype(F32)


def rs_drain(refs, p):
    def one(z):
        for a in range(4):
            for k in range(2):
                rs_first_copy(refs, p, a, z, k).wait_send()
            rs_second_copy(refs, p, a, z).wait_send()

            @pl.when(z != p.z)
            def _():
                rs_line(refs, p, a, z, p.z).wait_send()

    loop(4, one)


def own_row(x):
    return jnp.sum(x, axis=0, keepdims=True)


def lane_sum(x):
    folded = sum(x[:, k : k + LANES] for k in range(0, x.shape[1], LANES))
    return own_row(folded.T)


def wide(row):
    return jnp.concatenate([row, jnp.zeros((1, LANES - row.shape[1]), F32)], axis=1)


def cut(row):
    return [row[:, k : k + LANES] for k in range(0, row.shape[1], LANES)]


def stand(row):
    return jnp.broadcast_to(row, (LANES, LANES)).T


def scalars(values):
    lane = lax.broadcasted_iota(jnp.int32, (1, LANES), 1)
    out = jnp.zeros((1, LANES), F32)
    for k, v in enumerate(values):
        out = out + jnp.where(lane == k, v, 0.0)
    return out


def total(x):
    return jnp.sum(jnp.sum(x, axis=0, keepdims=True), axis=1, keepdims=True)


def segment(row, start, count):
    lane = lax.broadcasted_iota(jnp.int32, row.shape, 1)
    keep = (lane >= start) & (lane < start + count)
    return jnp.sum(jnp.where(keep, row, 0.0), axis=1, keepdims=True)


def gather_row(term, start, count):
    size = term.shape[1]
    owner = lax.broadcasted_iota(jnp.int32, (32, size), 0)
    spot = lax.broadcasted_iota(jnp.int32, (32, size), 1)
    masked = jnp.where(spot // count == owner, term, 0.0)
    lane = lax.broadcasted_iota(jnp.int32, (LANES, size), 0)
    from_spot = lax.broadcasted_iota(jnp.int32, (LANES, size), 1)
    sel = jnp.where(lane == start + from_spot % count, 1.0, 0.0).astype(BF16)
    out = jnp.zeros((32, LANES), F32)
    for _ in range(3):
        part = masked.astype(BF16)
        out = out + dot_t(part, sel)
        masked = masked - part.astype(F32)
    return out


def parameter_blocks(refs):
    return [
        refs.fw[...].astype(F32), refs.iw[...].astype(F32), refs.cw[...].astype(F32),
        refs.ow[...].astype(F32), refs.uw[...].astype(F32), refs.dw[...].astype(F32),
    ]


def old_rows(refs):
    rows = []
    for r in (refs.row_f, refs.row_i, refs.row_c, refs.row_o, refs.row_u, refs.row_d):
        rows += cut(r[...].reshape(1, r.shape[0]))
    return rows


def old_columns(refs):
    rows = []
    for r in (refs.col_f, refs.col_i, refs.col_c, refs.col_o, refs.col_u, refs.col_d):
        row = r[...].reshape(1, r.shape[0])
        rows += [wide(row)] if r.shape[0] < LANES else cut(row)
    return rows


ROW_PLACES = ((0, 1), (1, 2), (2, 3), (3, 5), (5, 6), (6, 10))
COLUMN_PLACES = ((0, 1), (1, 2), (2, 3), (3, 4), (4, 6), (6, 7))


def broadcast_row(src, box, send, recv, p):
    def one(k):
        rcopy(src, box.at[p.me], send, recv, p.other(k + 1)).start()

    for k in range(31):
        one(k)


def settle_row(box, send, recv, p):
    rows = box.at[pl.ds(0, 31)]
    rcopy(rows, rows, send, recv, p.partner).wait()


def vector_exchange(refs, p):
    rows = (
        gather_row(refs.mgg[...], 0, 16)
        + gather_row(jnp.concatenate([refs.fbg[z] for z in range(4)], axis=1), 16, 32)
        + gather_row(jnp.concatenate([refs.ibg[z] for z in range(4)], axis=1), 48, 32)
        + gather_row(refs.fgg[...], 80, 16)
    )
    refs.vout[...] = rows.reshape(32, 1, LANES)
    refs.vin[p.me] = refs.vout[p.me]

    def one(k):
        t = (p.me + k + 1) % 32
        rcopy(refs.vout.at[t], refs.vin.at[p.me], refs.vex_s, refs.vex_r, p.other(k + 1)).start()

    for k in range(31):
        one(k)


def gradient_blocks(refs, start):
    down = refs.fin_g[DOWN][...]
    rest = [
        refs.fin_g[OUT][...], refs.fin_g[UP][...],
        jnp.concatenate([down[0:64], down[64:128]], axis=1),
    ]
    if start:
        return rest
    mix = refs.fin_g[MIX][...]
    return [mix[:, 0:128], mix[:, 128:256], mix[:, 256:384]] + rest


FLIPPED = (False, False, False, True, False, True)


def part_stats(grads, flips):
    row_parts, column_parts, totals = [], [], []
    for grad, flip in zip(grads, flips):
        sq = grad * grad
        down, across = own_row(sq), lane_sum(sq)
        row_parts += cut(down) if flip else [across]
        column_parts += [wide(across)] if flip else cut(down)
        totals.append(jnp.sum(down, axis=1, keepdims=True))
    return row_parts, column_parts, totals


def adafactor_early(refs, p):
    rows, columns, totals = part_stats(gradient_blocks(refs, 3), FLIPPED[3:])
    refs.rowst[...] = jnp.concatenate([jnp.zeros((3, LANES), F32)] + rows + [jnp.zeros((6, LANES), F32)], axis=0)
    refs.colst[...] = jnp.concatenate(
        [jnp.zeros((3, LANES), F32)] + columns + [jnp.zeros((1, LANES), F32)], axis=0
    )
    params = pack_vectors(refs.mg, refs.fbv, refs.ibv, refs.fg)
    squares = [None] * 10
    for slot, w in zip(MATRIX_SLOTS, parameter_blocks(refs)):
        squares[slot] = total(w * w)
    for slot, start, count in VECTORS:
        squares[slot] = segment(params * params, start, count)
    rows_old = old_rows(refs)
    first = jnp.where(p.i == 0, 1.0, 0.0)
    row_sums = [first * total(jnp.concatenate(rows_old[a:b], axis=0)) for a, b in ROW_PLACES]
    refs.scal[...] = scalars([0.0] * 3 + totals + squares + row_sums)


def adafactor(refs, p):
    grads = gradient_blocks(refs, 0)
    flipped = FLIPPED
    rows, columns, totals = part_stats(grads[0:3], FLIPPED[0:3])
    refs.rowst[0:3, :] = jnp.concatenate(rows, axis=0)
    refs.colst[0:3, :] = jnp.concatenate(columns, axis=0)
    refs.scal[...] += scalars(totals)
    refs.rowin[p.i] = refs.rowst[...]
    refs.colin[p.g] = refs.colst[...]
    refs.scin[p.me] = refs.scal[...]
    for k in range(1, 8):
        peer = (p.g, (p.i + k) % 8)
        rcopy(
            refs.rowst, refs.rowin.at[p.i], refs.row_s.at[k - 1], refs.row_r.at[k - 1], peer
        ).start()
    for k in range(1, 4):
        peer = ((p.g + k) % 4, p.i)
        rcopy(
            refs.colst, refs.colin.at[p.g], refs.col_s.at[k - 1], refs.col_r.at[k - 1], peer
        ).start()
    broadcast_row(refs.scal, refs.scin, refs.sc_s, refs.sc_r, p)
    weights = parameter_blocks(refs)
    params = pack_vectors(refs.mg, refs.fbv, refs.ibv, refs.fg)
    rows_old, columns_old = old_rows(refs), old_columns(refs)
    vec_rows = refs.vin.at[pl.ds(0, 31)]
    rcopy(vec_rows, vec_rows, refs.vex_s, refs.vex_r, p.partner).wait()
    vector_grad = jnp.sum(refs.vin[...].reshape(32, LANES), axis=0, keepdims=True)
    seconds = pack_vectors(refs.sec_m, refs.sec_f, refs.sec_i, refs.sec_g)
    second = 0.5 * seconds + 0.5 * (vector_grad * vector_grad + TINY)
    vector_scaled = vector_grad * lax.rsqrt(second)
    for k in range(1, 8):
        rcopy(
            refs.rowst, refs.rowin.at[p.i], refs.row_s.at[k - 1], refs.row_r.at[k - 1], p.partner
        ).wait()
    for k in range(1, 4):
        rcopy(
            refs.colst, refs.colin.at[p.g], refs.col_s.at[k - 1], refs.col_r.at[k - 1], p.partner
        ).wait()
    settle_row(refs.scin, refs.sc_s, refs.sc_r, p)
    row_total = sum(refs.rowin[k] for k in range(8))
    column_total = sum(refs.colin[k] for k in range(4))
    sc = jnp.sum(refs.scin[...].reshape(32, LANES), axis=0, keepdims=True)
    rows_new, columns_new, scaled = [], [], []
    for k, (r, c) in enumerate(MATRICES):
        ra, rb = ROW_PLACES[k]
        ca, cb = COLUMN_PLACES[k]
        rows = [
            0.5 * rows_old[j] + 0.5 * (row_total[j : j + 1] / c + TINY) for j in range(ra, rb)
        ]
        columns = [
            0.5 * columns_old[j] + 0.5 * (column_total[j : j + 1] / r + TINY)
            for j in range(ca, cb)
        ]
        mean = 0.5 * sc[:, 16 + k : 17 + k] / r + 0.5 * (sc[:, k : k + 1] / (r * c) + TINY)
        lying, standing = (rows, columns) if flipped[k] else (columns, rows)
        tall = stand(standing[0])[0 : grads[k].shape[0]]
        lying = jnp.concatenate(lying, axis=1)
        tall = jnp.concatenate([tall] * (lying.shape[1] // LANES), axis=1)
        scaled.append(grads[k] * lax.rsqrt(tall * lying / mean))
        rows_new += rows
        columns_new += columns
    refs.rows_out[...] = jnp.concatenate(rows_new + [jnp.zeros((6, LANES), F32)], axis=0)
    refs.columns_out[...] = jnp.concatenate(columns_new + [jnp.zeros((1, LANES), F32)], axis=0)
    clips = [None] * 10
    for slot, s in zip(MATRIX_SLOTS, scaled):
        clips[slot] = total(s * s)
    for slot, start, count in VECTORS:
        clips[slot] = segment(vector_scaled * vector_scaled, start, count)
    refs.clip[...] = scalars(clips)
    refs.clin[p.me] = refs.clip[...]
    broadcast_row(refs.clip, refs.clin, refs.cl_s, refs.cl_r, p)
    settle_row(refs.clin, refs.cl_s, refs.cl_r, p)
    clip = jnp.sum(refs.clin[...].reshape(32, LANES), axis=0, keepdims=True)
    norms = [jnp.sqrt(clip[:, k : k + 1] / COUNTS[k]) for k in range(10)]
    steps = [
        -jnp.sqrt(sc[:, 6 + k : 7 + k] / COUNTS[k]) / jnp.maximum(CLIP, norms[k])
        for k in range(10)
    ]
    fresh = [w + steps[slot] * s for slot, w, s in zip(MATRIX_SLOTS, weights, scaled)]
    refs.grad_mix[...] = refs.fin_g[MIX][...]
    refs.grad_out[...] = grads[3]
    refs.grad_up[...] = grads[4]
    refs.grad_down[...] = grads[5]
    refs.new_mix[...] = jnp.concatenate(fresh[0:3], axis=1)
    refs.new_out[...] = fresh[3]
    refs.new_up[...] = fresh[4]
    refs.new_down[...] = fresh[5]
    lane = lax.broadcasted_iota(jnp.int32, (1, LANES), 1)
    step_row = jnp.zeros((1, LANES), F32)
    for slot, start, count in VECTORS:
        step_row = step_row + jnp.where((lane >= start) & (lane < start + count), steps[slot], 0.0)
    refs.vectors[...] = jnp.concatenate(
        [vector_grad, params + step_row * vector_scaled, second, scalars(norms)]
        + [jnp.zeros((4, LANES), F32)],
        axis=0,
    )


def finish_kernel(
    grad_mix, grad_out, grad_up, grad_down, new_mix, new_out, new_up, new_down,
    vectors, rows, columns, block_in, token_in,
    g_mg, g_f, g_i, g_c, g_fb, g_ib, g_o, g_fg, g_u, g_d,
    n_mg, n_f, n_i, n_c, n_fb, n_ib, n_o, n_fg, n_u, n_d,
    s_m, r_f, c_f, r_i, c_i, r_c, c_c, s_f, s_i, r_o, c_o, s_g, r_u, c_u, r_d, c_d, norms,
    block_out, token_out, stage, sem,
):
    copies = []
    for k, (src, dst) in enumerate(((block_in, block_out), (token_in, token_out))):
        fetch = pltpu.make_async_copy(src, stage.at[k], sem.at[0, k])
        fetch.start()
        copies.append((fetch, pltpu.make_async_copy(stage.at[k], dst, sem.at[1, k])))
    for fetch, put in copies:
        fetch.wait()
        put.start()
    for src, outs in ((grad_mix, (g_f, g_i, g_c)), (new_mix, (n_f, n_i, n_c))):
        for k, o in enumerate(outs):
            o[...] = src[:, k * 128 : (k + 1) * 128]
    for src, o in ((grad_out, g_o), (new_out, n_o), (grad_down, g_d), (new_down, n_d)):
        o[...] = src[...]
    g_u[...] = grad_up[...]
    n_u[...] = new_up[...]
    for row, outs in (
        (0, (g_mg, g_fb, g_ib, g_fg)), (1, (n_mg, n_fb, n_ib, n_fg)), (2, (s_m, s_f, s_i, s_g))
    ):
        for (_, start, count), o in zip(VECTORS, outs):
            o[...] = vectors[row, start : start + count]
    norms[...] = vectors[3, 0:10]
    for src, places, outs in (
        (rows, ROW_PLACES, (r_f, r_i, r_c, r_o, r_u, r_d)),
        (columns, COLUMN_PLACES, (c_f, c_i, c_c, c_o, c_u, c_d)),
    ):
        for (a, b), o in zip(places, outs):
            if b - a == 1:
                o[...] = src[a, 0 : o.shape[0]]
            else:
                for k in range(a, b):
                    o[(k - a) * LANES : (k - a + 1) * LANES] = src[k, :]
    for fetch, put in copies:
        put.wait()


def finish(packed, block, tgrad):
    sds = jax.ShapeDtypeStruct
    f = lambda *s: sds(s, F32)
    small = [f(16), f(128, 128), f(128, 128), f(128, 128), f(32), f(32), f(64, 256), f(16),
             f(128, 256), f(64, 512)]
    states = [f(16), f(128), f(128), f(128), f(128), f(128), f(128), f(32), f(32), f(256), f(64),
              f(16), f(128), f(256), f(512), f(64)]
    big = sds(block.shape, BF16)
    outs = tuple(small + small + states + [f(10), big, big])
    vm = pl.BlockSpec(memory_space=pltpu.VMEM)
    anyspec = pl.BlockSpec(memory_space=pl.ANY)
    return pl.pallas_call(
        finish_kernel,
        out_shape=outs,
        in_specs=[vm] * len(packed) + [anyspec] * 2,
        out_specs=(vm,) * (len(outs) - 2) + (anyspec,) * 2,
        scratch_shapes=[pltpu.VMEM((2,) + block.shape, BF16), pltpu.SemaphoreType.DMA((2, 2))],
        name="finish",
    )(*packed, block, tgrad)


class FusedRefs:
    def __init__(self, args):
        (
            self.tok_in, self.cot_in, self.fw, self.iw, self.cw, self.ow, self.uw, self.dw,
            self.mg, self.fbv, self.ibv, self.fg,
            self.sec_m, self.row_f, self.col_f, self.row_i, self.col_i, self.row_c, self.col_c,
            self.sec_f, self.sec_i, self.row_o, self.col_o, self.sec_g,
            self.row_u, self.col_u, self.row_d, self.col_d,
            self.block_out, self.tgrad_out,
            self.grad_mix, self.grad_out, self.grad_up, self.grad_down,
            self.new_mix, self.new_out, self.new_up, self.new_down,
            self.vectors, self.rows_out, self.columns_out,
            self.wmix, self.wot, self.wup, self.wdt, self.g1, self.g2, self.fb, self.ib,
            self.vecs, self.vstage, self.fgg, self.mgg, self.fbg, self.ibg,
            self.tok_p, self.fin, self.min_t, self.fin_t, self.cot_p, self.cot_t,
            self.resid, self.dfe,
            self.pre, self.buf, self.dpre, self.slow, self.st,
            self.keep, self.k_f, self.k_i, self.k_c,
            self.loc_s, self.vec_s, self.vec_r, self.gz_s, self.gz_r,
            self.gn_s, self.gn_r, self.gf_s, self.gf_r, self.gp_s, self.gp_r,
            self.vout, self.vin, self.rowst, self.rowin, self.colst, self.colin,
            self.scal, self.scin, self.clip, self.clin,
            self.rp_s, self.rp_r, self.r1_s, self.r1_r, self.r2_s, self.r2_r,
            self.r3_s, self.r3_r, self.vex_s, self.vex_r,
            self.row_s, self.row_r, self.col_s, self.col_r, self.sc_s, self.sc_r,
            self.cl_s, self.cl_r, self.io_s,
        ) = args[:112]
        rest = list(args[112:])
        self.psend, self.precv, self.r1, self.r2, self.r3, self.fin_g = (
            rest[4 * k : 4 * k + 4] for k in range(6)
        )
        self.io = self.dpre.at[:, 0:512]
        self.oacc = self.pre.at[pl.ds(4, 4)]
        self.tok = self.cot = self.block = self.tgrad = self.io
        self.min = self.fin


def halves_of(refs, plane, rows):
    size = rows.size
    low = refs.pre[plane, rows, :]
    high = refs.pre[plane, pl.ds(rows.start + 512, size), :]
    return jnp.concatenate([low, high], axis=1)


def put_halves(refs, plane, value):
    refs.pre[plane, 0:512, :] = value[:, 0:LANES]
    refs.pre[plane, 512:1024, :] = value[:, LANES : 2 * LANES]


def line_rows(z, c):
    return pl.ds(pl.multiple_of((z * 2 + c) * 64, 64), 64)


def put_feed_grads(refs, p, f):
    z, h = f // 2, f % 2
    up = dot(refs.fin_t[...], refs.dpre[:, C : 2 * C])
    put_halves(refs, 1 + h, dot(refs.cot_t[...], refs.dpre[:, 0:C]))

    @pl.when(h == p.c)
    def _():
        put_halves(refs, 0, up)

    @pl.when(h != p.c)
    def _():
        for g in range(4):
            refs.psend[UP][z, g] = up[g * 128 : (g + 1) * 128].astype(BF16)

    half = pl.ds(pl.multiple_of(h * 64, 64), 64)
    for zz in range(4):
        part = halves_of(refs, 1 + h, line_rows(zz, 1 - p.c))
        refs.psend[DOWN][z, zz, half, :] = part.astype(BF16)


def merge_up(refs, p, z):
    rs_pair(refs, p, UP, z).wait()
    for g in range(4):
        rs_merge(refs, p, UP, g, z, halves_of(refs, 0, pl.ds(g * 128, 128)))


def merge_down(refs, p, g):
    rs_pair(refs, p, DOWN, g).wait()
    for z in range(4):
        own = jnp.concatenate(
            [halves_of(refs, 1 + h, line_rows(z, p.c)) for h in range(2)], axis=0
        )
        rs_merge_at(refs, p, DOWN, g, z, own)


def rs_merge_at(refs, p, a, g, z, own):
    e = p.turn(z)
    y, x = g // 2, g % 2
    role = (1 - e) * ((x + p.x) % 2) + e * ((y + p.y) % 2)
    place = spot(a, g, z)
    v = (own + refs.precv[a][place].astype(F32)).astype(BF16)

    @pl.when(role == 1)
    def _():
        refs.psend[a][place] = v

    @pl.when(role == 0)
    def _():
        refs.precv[a][place] = v


def down_first_send(refs, p, g):
    def one(z):
        e = p.turn(z)
        y, x = g // 2, g % 2

        @pl.when(rs_role(p, g, z) == 1)
        def _():
            rs_first_copy(refs, p, DOWN, z, (1 - e) * y + e * x).start()

    loop(4, one)


def put_out_grads(refs, p):
    def one(g):
        put_halves(refs, g, dot(refs.fin_t[...], refs.slow[g]))
        for z in range(4):
            part = halves_of(refs, g, line_rows(z, 1 - p.c))
            refs.psend[OUT][z, g] = part.astype(BF16)

    loop(4, one)


def merge_out(refs, p):
    rs_pair(refs, p, OUT, 0).wait()

    def one(z):
        for g in range(4):
            rs_merge(refs, p, OUT, g, z, halves_of(refs, g, line_rows(z, p.c)))

    loop(4, one)


def mix_part(refs, g, c):
    cols = []
    for j in range(3):
        q = 3 * c + j
        rows = pl.ds(pl.multiple_of((q % 2) * 512 + g * 128, 128), 128)
        cols.append(refs.pre[q // 2, rows, :])
    return jnp.concatenate(cols, axis=1)


def put_mix_grads(refs, p, z):
    for j in range(3):
        put_halves(refs, j, dot(refs.min_t[...], refs.dpre[:, j * C : (j + 1) * C]))
    for g in range(4):
        refs.psend[MIX][z, g] = mix_part(refs, g, 1 - p.c).astype(BF16)


def merge_mix(refs, p, z):
    rs_pair(refs, p, MIX, z).wait()
    for g in range(4):
        rs_merge(refs, p, MIX, g, z, mix_part(refs, g, p.c))


def all_z(body):
    loop(4, body)


def second(refs, p, a, z):
    rs_second(refs, p, a, z)
    rs_second_copy(refs, p, a, z).start()


def third(refs, p, a, z):
    rs_third(refs, p, a, z)
    rs_third_send(refs, p, a, z)


def feed_order(k):
    return jnp.where(k == 1, 3, jnp.where(k >= 2, k - 1, 0))


def feed_tick(refs, p, f):
    @pl.when((f % 2 == 0) & (f >= 2))
    def _():
        last = feed_order(f // 2 - 1)
        merge_up(refs, p, last)
        merge_down(refs, p, last)
        rs_first_send(refs, p, UP, last)
        down_first_send(refs, p, last)

    @pl.when((f % 2 == 0) & (f >= 4))
    def _():
        second(refs, p, UP, feed_order(f // 2 - 2))

    @pl.when((f % 2 == 0) & (f >= 6))
    def _():
        third(refs, p, UP, feed_order(f // 2 - 3))


def fused_kernel(*args):
    refs = FusedRefs(args)
    refs.fin_grad = refs.fin_g
    T, D = refs.tok_p.shape
    p = Place()
    entry_signal(p)
    load = pltpu.make_async_copy(refs.cot_in, refs.io, refs.io_s)
    load.start()
    gather_start(refs, p)
    load.wait()
    cot_in(refs, T)
    gather_hook(refs, p, "Mf0 Mn1")
    load = pltpu.make_async_copy(refs.tok_in, refs.io, refs.io_s)
    load.start()
    gather_vectors(refs, p)
    load.wait()
    norm_in(refs, T)
    gather_hook(refs, p, "Mp0 Mf1 Mn2 Md0")
    mixer_slots(refs, p, T)
    up_own(refs, p, 1)
    gather_hook(refs, p, "Wd0 Wd1 Wd2 Wd3 Un1 Un2 Dn10 Dn11 Dn12 Dn13")
    mix_out(refs, T)
    gather_hook(refs, p, "Ud0 Dd00 Dd01 Dd02 Dd03")
    clear(refs.oacc, T)
    refs.dfe[...] = jnp.zeros_like(refs.dfe)

    def feed_step(f):
        @pl.when(f == 2)
        def _():
            gather_hook(refs, p, "Ud3 De00 De01 De02 De03")

        @pl.when(f == 4)
        def _():
            gather_hook(refs, p, "Ud1 Dd10 Dd11 Dd12 Dd13")

        @pl.when(f == 6)
        def _():
            gather_hook(refs, p, "Ud2 De10 De11 De12 De13")

        feed(refs, feed_order(f // 2) * 2 + f % 2, T)

        @pl.when(f == 0)
        def _():
            gather_hook(refs, p, "Uf1 Uf2 Df10 Df11 Df12 Df13")

        @pl.when(f == 1)
        def _():
            gather_hook(refs, p, "Up1 Up2 Dp10 Dp11 Dp12 Dp13")

        feed_tick(refs, p, f)
        put_feed_grads(refs, p, feed_order(f // 2) * 2 + f % 2)

        @pl.when(f % 2 == 1)
        def _():
            rs_pair(refs, p, UP, feed_order(f // 2)).start()
            rs_pair(refs, p, DOWN, feed_order(f // 2)).start()

    loop(8, feed_step)
    feed_back(refs, T)
    store = pltpu.make_async_copy(refs.io, refs.block_out, refs.io_s)
    store.start()
    gather_drain(refs, p)
    merge_up(refs, p, 2)
    merge_down(refs, p, 2)
    rs_first_send(refs, p, UP, 2)
    down_first_send(refs, p, 2)
    second(refs, p, UP, 1)
    third(refs, p, UP, 3)
    put_out_grads(refs, p)
    rs_pair(refs, p, OUT, 0).start()
    clear(refs.oacc, T)
    store.wait()

    def chunk(n):
        return (p.z + 1 + n) % 4

    def early(n):
        @pl.when(n == 0)
        def _():
            merge_out(refs, p)
            all_z(lambda z: rs_first_send(refs, p, OUT, z))

        @pl.when(n >= 1)
        def _():
            merge_mix(refs, p, chunk(n - 1))
            rs_first_send(refs, p, MIX, chunk(n - 1))

        @pl.when(n >= 2)
        def _():
            second(refs, p, MIX, chunk(n - 2))

        @pl.when(n == 2)
        def _():
            all_z(lambda z: third(refs, p, DOWN, z))

        @pl.when(n == 3)
        def _():
            third(refs, p, MIX, chunk(0))

    def late(n):
        @pl.when(n == 0)
        def _():
            second(refs, p, UP, 2)
            all_z(lambda z: second(refs, p, DOWN, z))
            third(refs, p, UP, 1)

        @pl.when(n == 1)
        def _():
            all_z(lambda z: second(refs, p, OUT, z))
            third(refs, p, UP, 2)

        @pl.when(n == 2)
        def _():
            all_z(lambda z: third(refs, p, OUT, z))

    def mixer_step(n):
        z = chunk(n)
        mixer_back(refs, z, T, lambda: early(n))
        put_mix_grads(refs, p, z)
        rs_pair(refs, p, MIX, z).start()
        mixer_input_back(refs, z, T)
        late(n)

    loop(4, mixer_step)
    merge_mix(refs, p, chunk(3))
    rs_first_send(refs, p, MIX, chunk(3))
    second(refs, p, MIX, chunk(2))
    third(refs, p, MIX, chunk(1))
    norm_back(refs, T)
    store = pltpu.make_async_copy(refs.io, refs.tgrad_out, refs.io_s)
    store.start()
    second(refs, p, MIX, chunk(3))
    third(refs, p, MIX, chunk(2))
    vector_exchange(refs, p)
    for a in (UP, DOWN, OUT):
        rs_last(refs, p, a)
    adafactor_early(refs, p)
    third(refs, p, MIX, chunk(3))
    rs_last(refs, p, MIX)
    rs_drain(refs, p)
    adafactor(refs, p)
    store.wait()


def fused(*args):
    T, D = args[0].shape
    Z, F = 4, 8
    sds = jax.ShapeDtypeStruct
    vm = pl.BlockSpec(memory_space=pltpu.VMEM)
    anyspec = pl.BlockSpec(memory_space=pl.ANY)
    V = pltpu.VMEM
    S = pltpu.SemaphoreType.DMA
    outs = (
        sds((T, D), BF16), sds((T, D), BF16),
        sds((128, 384), F32), sds((64, 256), F32), sds((128, 256), F32), sds((64, 512), F32),
        sds((128, 384), F32), sds((64, 256), F32), sds((128, 256), F32), sds((64, 512), F32),
        sds((8, LANES), F32), sds((16, LANES), F32), sds((8, LANES), F32),
    )
    row = V((1, LANES), F32)
    box = V((32, 1, LANES), F32)
    scratch = [
        V((Z, D, 3 * C), BF16), V((Z, D, C), BF16), V((F, D, C), BF16), V((F, D, C), BF16),
        V((1, D), F32), V((1, D), F32), V((Z, 1, C), F32), V((Z, 1, C), F32),
        box, row, V((1, D), F32), V((1, D), F32), V((Z, 1, C), F32), V((Z, 1, C), F32),
        V((T, D), BF16), V((T, D), BF16), V((D, T), BF16), V((D, T), BF16),
        V((T, D), BF16), V((D, T), BF16),
        V((D // LANES, T, LANES), F32), V((T, D), F32),
        V((8, T, LANES), F32), V((4, T, LANES), F32),
        V((T, 3 * C), BF16), V((Z, T, C), BF16), V((Z, T + SUB, C), F32),
        V((Z, T, C), F32), V((Z, T, C), F32), V((Z, T, C), F32), V((Z, T, C), F32),
        S((7,)), S(()), S(()), S((4, 3)), S((4, 4)),
        S((4, 4)), S((4, 4)), S((4, 4, 2)), S((4, 4, 2)), S((4, 4, 4)), S((4, 4, 4)),
        box, box, V((16, LANES), F32), V((8, 16, LANES), F32),
        V((8, LANES), F32), V((4, 8, LANES), F32), row, box, row, box,
        S((4, 4)), S((4, 4)), S((4, 4, 2)), S((4, 4, 2)), S((4, 4)), S((4, 4)),
        S((4, 4)), S((4, 4)), S(()), S(()),
        S((7,)), S((7,)), S((3,)), S((3,)), S(()), S(()), S(()), S(()), S(()),
    ]
    scratch += (
        [V((4, 4) + s, BF16) for s in SHAPES] * 2
        + [V((4, 2) + s, BF16) for s in SHAPES]
        + [V((4,) + s, BF16) for s in SHAPES] * 2
        + [V(s, F32) for s in SHAPES]
    )
    return pl.pallas_call(
        fused_kernel,
        out_shape=outs,
        in_specs=[anyspec, anyspec] + [vm] * (len(args) - 2),
        out_specs=(anyspec, anyspec) + (vm,) * (len(outs) - 2),
        scratch_shapes=scratch,
        compiler_params=pltpu.CompilerParams(
            vmem_limit_bytes=67043328, collective_id=0, has_side_effects=True
        ),
        name="fused",
    )(*args)


def gathered_layer(tok, cot, mix, ow, uw, dw, mg, fb, ib, fg):
    def whole(w):
        w = lax.all_gather(w, "inner", axis=1, tiled=True)
        return lax.all_gather(w, "grp", axis=0, tiled=True)

    def vec(v):
        return lax.all_gather(v, ("grp", "inner"), axis=0, tiled=True).astype(F32)

    width = tok.shape[1]
    inners = lax.axis_size("inner")
    Z, F = mix[0].shape[1] * inners // C, uw.shape[1] * inners // C
    gates = [whole(w).reshape(width, Z, C // LANES, 1, LANES) for w in mix]
    wmix = jnp.concatenate(gates, axis=3).reshape(width, Z, 3 * C).transpose(1, 0, 2)
    wot = whole(ow).reshape(Z, C, width).transpose(0, 2, 1)
    wup = whole(uw).reshape(width, F, C).transpose(1, 0, 2)
    wdt = whole(dw).reshape(F, C, width).transpose(0, 2, 1)
    return layer(
        tok, cot, wmix, wot, wup, wdt,
        vec(mg).reshape(1, width), vec(fg).reshape(1, width),
        vec(fb).reshape(Z, 1, C), vec(ib).reshape(Z, 1, C),
    )


def body(
    tokens,
    cotangent,
    mixer_gain,
    forget_weight,
    input_gate_weight,
    candidate_weight,
    forget_bias,
    input_bias,
    output_weight,
    feed_norm_gain,
    up_weight,
    down_weight,
    mixer_second,
    forget_rows,
    forget_columns,
    input_rows,
    input_columns,
    candidate_rows,
    candidate_columns,
    forget_second,
    input_second,
    output_rows,
    output_columns,
    feed_second,
    up_rows,
    up_columns,
    down_rows,
    down_columns,
):
    groups = lax.axis_size("grp")
    inners = lax.axis_size("inner")
    seqs, length, width = tokens.shape
    hidden = forget_weight.shape[1] * inners
    ff = up_weight.shape[1] * inners
    paired = (groups, inners) == (4, 8) and (length, width, hidden, ff) == (1024, 512, 1024, 2048)
    Z, F = hidden // C, ff // C
    if paired:
        block_output, tokens_grad, *packed = fused(
            tokens.reshape(length, width), cotangent.reshape(length, width),
            forget_weight, input_gate_weight, candidate_weight,
            output_weight.T, up_weight, down_weight.T,
            mixer_gain, forget_bias, input_bias, feed_norm_gain,
            mixer_second, forget_rows, forget_columns, input_rows, input_columns,
            candidate_rows, candidate_columns, forget_second, input_second,
            output_rows, output_columns, feed_second,
            up_rows, up_columns, down_rows, down_columns,
        )
        *done, block_output, tokens_grad = finish(packed, block_output, tokens_grad)
        for k in (6, 9, 16, 19):
            done[k] = done[k].T
        return (block_output.reshape(tokens.shape), tokens_grad.reshape(tokens.shape), *done)
    results = gathered_layer(
        tokens.reshape(length, width), cotangent.reshape(length, width),
        (forget_weight, input_gate_weight, candidate_weight),
        output_weight, up_weight, down_weight,
        mixer_gain, forget_bias, input_bias, feed_norm_gain,
    )
    block_output, tokens_grad, gmix, got, gup, gdt, fgg, mgg, fbg, ibg = results
    block_output = block_output.reshape(tokens.shape)
    tokens_grad = tokens_grad.reshape(tokens.shape)
    split = gmix.transpose(1, 0, 2).reshape(width, Z, C // LANES, 3, LANES)
    forget_term, input_term, cand_term = [
        split[:, :, :, k].reshape(width, hidden) for k in range(3)
    ]
    output_term = got.transpose(0, 2, 1).reshape(hidden, width)
    up_term = gup.transpose(1, 0, 2).reshape(width, ff)
    down_term = gdt.transpose(0, 2, 1).reshape(ff, width)
    gain_first_term, gain_second_term = mgg.reshape(-1), fgg.reshape(-1)
    fbias_term, ibias_term = fbg.reshape(-1), ibg.reshape(-1)
    part = (
        lax.psum_scatter(
            gain_first_term.reshape(groups, -1), "inner", scatter_dimension=1, tiled=True
        ),
        lax.psum_scatter(forget_term, "inner", scatter_dimension=1, tiled=True),
        lax.psum_scatter(input_term, "inner", scatter_dimension=1, tiled=True),
        lax.psum_scatter(cand_term, "inner", scatter_dimension=1, tiled=True),
        lax.psum_scatter(fbias_term.reshape(groups, -1), "inner", scatter_dimension=1, tiled=True),
        lax.psum_scatter(ibias_term.reshape(groups, -1), "inner", scatter_dimension=1, tiled=True),
        lax.psum_scatter(output_term, "inner", scatter_dimension=1, tiled=True),
        lax.psum_scatter(
            gain_second_term.reshape(groups, -1), "inner", scatter_dimension=1, tiled=True
        ),
        lax.psum_scatter(up_term, "inner", scatter_dimension=1, tiled=True),
        lax.psum_scatter(down_term, "inner", scatter_dimension=1, tiled=True),
    )
    mine = (
        lax.psum_scatter(part[0], "grp", scatter_dimension=0, tiled=True),
        lax.psum_scatter(part[1], "grp", scatter_dimension=0, tiled=True),
        lax.psum_scatter(part[2], "grp", scatter_dimension=0, tiled=True),
        lax.psum_scatter(part[3], "grp", scatter_dimension=0, tiled=True),
        lax.psum_scatter(part[4], "grp", scatter_dimension=0, tiled=True),
        lax.psum_scatter(part[5], "grp", scatter_dimension=0, tiled=True),
        lax.psum_scatter(part[6], "grp", scatter_dimension=0, tiled=True),
        lax.psum_scatter(part[7], "grp", scatter_dimension=0, tiled=True),
        lax.psum_scatter(part[8], "grp", scatter_dimension=0, tiled=True),
        lax.psum_scatter(part[9], "grp", scatter_dimension=0, tiled=True),
    )
    params = [
        mixer_gain,
        forget_weight,
        input_gate_weight,
        candidate_weight,
        forget_bias,
        input_bias,
        output_weight,
        feed_norm_gain,
        up_weight,
        down_weight,
    ]
    locals_f = [p.astype(jnp.float32) for p in params]
    grads = [
        mine[0].reshape(-1),
        mine[1],
        mine[2],
        mine[3],
        mine[4].reshape(-1),
        mine[5].reshape(-1),
        mine[6],
        mine[7].reshape(-1),
        mine[8],
        mine[9],
    ]
    matrix_slots = [1, 2, 3, 6, 8, 9]
    vector_slots = [0, 4, 5, 7]
    rows_old = [forget_rows, input_rows, candidate_rows, output_rows, up_rows, down_rows]
    columns_old = [
        forget_columns,
        input_columns,
        candidate_columns,
        output_columns,
        up_columns,
        down_columns,
    ]
    seconds_old = [mixer_second, forget_second, input_second, feed_second]
    counts = [params[k].size * groups * inners for k in range(10)]
    first_inner = (lax.axis_index("inner") == 0).astype(jnp.float32)
    scales = lax.psum(
        jnp.stack(
            [jnp.sum(w * w) for w in locals_f] + [jnp.sum(r) * first_inner for r in rows_old]
        ),
        ("grp", "inner"),
    )
    mats = [grads[k] for k in matrix_slots]
    row_parts = [jnp.sum(g * g, axis=1) for g in mats]
    column_parts = [jnp.sum(g * g, axis=0) for g in mats]
    row_totals = lax.psum(
        (row_parts[0], row_parts[1], row_parts[2], row_parts[3], row_parts[4], row_parts[5]),
        "inner",
    )
    column_totals = lax.psum(
        (
            column_parts[0],
            column_parts[1],
            column_parts[2],
            column_parts[3],
            column_parts[4],
            column_parts[5],
        ),
        "grp",
    )
    grand = lax.psum(jnp.stack([jnp.sum(v) for v in row_totals]), "grp")
    scaled_all = [None] * 10
    new_states = [None] * 16
    state_places = {1: (1, 2), 2: (3, 4), 3: (5, 6), 6: (9, 10), 8: (12, 13), 9: (14, 15)}
    second_places = {0: 0, 4: 7, 5: 8, 7: 11}
    for k in range(6):
        slot = matrix_slots[k]
        grad = mats[k]
        full_rows = grad.shape[0] * groups
        full_columns = grad.shape[1] * inners
        rows = 0.5 * rows_old[k] + 0.5 * (row_totals[k] / full_columns + TINY)
        columns = 0.5 * columns_old[k] + 0.5 * (column_totals[k] / full_rows + TINY)
        row_mean = 0.5 * scales[10 + k] / full_rows + 0.5 * (
            grand[k] / (full_rows * full_columns) + TINY
        )
        scaled_all[slot] = grad * lax.rsqrt(rows[:, None] * columns[None, :] / row_mean)
        new_states[state_places[slot][0]] = rows
        new_states[state_places[slot][1]] = columns
    for k in range(4):
        slot = vector_slots[k]
        grad = grads[slot]
        second = 0.5 * seconds_old[k] + 0.5 * (grad * grad + TINY)
        scaled_all[slot] = grad * lax.rsqrt(second)
        new_states[second_places[slot]] = second
    clip = lax.psum(jnp.stack([jnp.sum(s * s) for s in scaled_all]), ("grp", "inner"))
    count_array = jnp.array(counts, jnp.float32)
    update_norms = jnp.sqrt(clip / count_array)
    fresh = [
        locals_f[k]
        + -jnp.sqrt(scales[k] / counts[k]) * scaled_all[k] / jnp.maximum(CLIP, update_norms[k])
        for k in range(10)
    ]
    return (
        block_output,
        tokens_grad,
        grads[0],
        grads[1],
        grads[2],
        grads[3],
        grads[4],
        grads[5],
        grads[6],
        grads[7],
        grads[8],
        grads[9],
        fresh[0],
        fresh[1],
        fresh[2],
        fresh[3],
        fresh[4],
        fresh[5],
        fresh[6],
        fresh[7],
        fresh[8],
        fresh[9],
        new_states[0],
        new_states[1],
        new_states[2],
        new_states[3],
        new_states[4],
        new_states[5],
        new_states[6],
        new_states[7],
        new_states[8],
        new_states[9],
        new_states[10],
        new_states[11],
        new_states[12],
        new_states[13],
        new_states[14],
        new_states[15],
        update_norms,
    )


def solution(mesh):
    return jax.shard_map(
        body,
        mesh=mesh,
        in_specs=(
            P(("grp", "inner"), None, None),
            P(("grp", "inner"), None, None),
            P(("grp", "inner")),
            P("grp", "inner"),
            P("grp", "inner"),
            P("grp", "inner"),
            P(("grp", "inner")),
            P(("grp", "inner")),
            P("grp", "inner"),
            P(("grp", "inner")),
            P("grp", "inner"),
            P("grp", "inner"),
            P(("grp", "inner")),
            P("grp"),
            P("inner"),
            P("grp"),
            P("inner"),
            P("grp"),
            P("inner"),
            P(("grp", "inner")),
            P(("grp", "inner")),
            P("grp"),
            P("inner"),
            P(("grp", "inner")),
            P("grp"),
            P("inner"),
            P("grp"),
            P("inner"),
        ),
        out_specs=(
            P(("grp", "inner"), None, None),
            P(("grp", "inner"), None, None),
            P(("grp", "inner")),
            P("grp", "inner"),
            P("grp", "inner"),
            P("grp", "inner"),
            P(("grp", "inner")),
            P(("grp", "inner")),
            P("grp", "inner"),
            P(("grp", "inner")),
            P("grp", "inner"),
            P("grp", "inner"),
            P(("grp", "inner")),
            P("grp", "inner"),
            P("grp", "inner"),
            P("grp", "inner"),
            P(("grp", "inner")),
            P(("grp", "inner")),
            P("grp", "inner"),
            P(("grp", "inner")),
            P("grp", "inner"),
            P("grp", "inner"),
            P(("grp", "inner")),
            P("grp"),
            P("inner"),
            P("grp"),
            P("inner"),
            P("grp"),
            P("inner"),
            P(("grp", "inner")),
            P(("grp", "inner")),
            P("grp"),
            P("inner"),
            P(("grp", "inner")),
            P("grp"),
            P("inner"),
            P("grp"),
            P("inner"),
            P(),
        ),
        check_vma=False,
    )
```
